32 devices in a mesh: shard: 4 (over z), ctx: 2 (over x), tp: 4 (over y, core).
Axes of the slice: x: 2, y: 2, z: 4, core: 2. Of those that a mesh axis runs over, the one named last changes fastest.
Arguments:
- tokens: bfloat16 [8, 1024, 1280], P('shard', ('ctx', 'tp')), may hold values from -6 to 6
- norm1_gain: float32 [1280], replicated, may hold values from 0.1 to 1.9
- norm1_bias: float32 [1280], replicated, may hold values from -3 to 3
- qkv_weight: bfloat16 [3, 1280, 1280], P(None, ('shard', 'ctx'), 'tp'), may hold values from -0.15625 to 0.15625
- qv_bias: float32 [2, 1280], replicated, may hold values from -3 to 3
- rel_rows: bfloat16 [31, 80], replicated, may hold values from -0.8984375 to 0.8984375
- rel_cols: bfloat16 [127, 80], replicated, may hold values from -0.8984375 to 0.8984375
- proj_weight: bfloat16 [1280, 1280], P('tp', ('shard', 'ctx')), may hold values from -1.25 to 1.25
- proj_bias: float32 [1280], replicated, may hold values from -3 to 3
- norm2_gain: float32 [1280], replicated, may hold values from 0.1 to 1.9
- norm2_bias: float32 [1280], replicated, may hold values from -3 to 3
- fc1_weight: bfloat16 [1280, 5120], P(('shard', 'ctx'), 'tp'), may hold values from -0.15625 to 0.15625
- fc1_bias: float32 [5120], replicated, may hold values from -3 to 3
- fc2_weight: bfloat16 [5120, 1280], P('tp', ('shard', 'ctx')), may hold values from -0.078125 to 0.078125
- fc2_bias: float32 [1280], replicated, may hold values from -3 to 3
- cotangent: bfloat16 [8, 1024, 1280], P('shard', ('ctx', 'tp')), may hold values from -6 to 6
Outputs:
- output: bfloat16 [8, 1024, 1280], P('shard', ('ctx', 'tp'))
- tokens_grad: bfloat16 [8, 1024, 1280], P('shard', ('ctx', 'tp'))
- norm1_gain_grad: float32 [1280], replicated
- norm1_bias_grad: float32 [1280], replicated
- qkv_weight_grad: float32 [3, 1280, 1280], P(None, ('shard', 'ctx'), 'tp')
- qv_bias_grad: float32 [2, 1280], replicated
- rel_rows_grad: float32 [31, 80], replicated
- rel_cols_grad: float32 [127, 80], replicated
- proj_weight_grad: float32 [1280, 1280], P('tp', ('shard', 'ctx'))
- proj_bias_grad: float32 [1280], replicated
- norm2_gain_grad: float32 [1280], replicated
- norm2_bias_grad: float32 [1280], replicated
- fc1_weight_grad: float32 [1280, 5120], P(('shard', 'ctx'), 'tp')
- fc1_bias_grad: float32 [5120], replicated
- fc2_weight_grad: float32 [5120, 1280], P('tp', ('shard', 'ctx'))
- fc2_bias_grad: float32 [1280], replicated
The draws below stay inside these ranges and needn't reach their ends.
All inputs are finite; a program needn't handle non-finite values.
Results may differ from the reference program's by a relative error of at most 0.02.
Values may be sent and summed in bfloat16 or wider, within the bound.
A program may use at most 128 MiB of HBM per device.

```python
import jax
import jax.numpy as jnp
from jax import lax

D = 1280
H = 16
HD = 80
FF = 5120
COLS = 64
TOK_IMG = 1024
IMAGES = 8
REL_ROWS = 31
REL_COLS = 127


def levels(rng, dims, cuts, low, high):
    loudness = 1.0
    for position, shards_of in cuts:
        draws = jax.random.uniform(jax.random.fold_in(jax.random.fold_in(rng, 6), position), (shards_of,), jnp.float32, low / len(cuts), high / len(cuts))
        loudness = loudness * jnp.repeat(jnp.exp(draws), dims[position] // shards_of).reshape((-1,) + (1,) * (len(dims) - 1 - position))
    return loudness


def scatter_about(stream_key, dims, deviation, most, cuts=(), held_as=jnp.bfloat16):
    values = jax.random.normal(stream_key, dims, jnp.float32) * deviation
    if len(cuts) > 0:
        values = levels(stream_key, dims, cuts, -0.22, 0.18) * values
    return jnp.clip(values, min=-most, max=most).astype(held_as)


def setup_inputs(seed: int = 0) -> dict:
    streams_of = jax.random.split(jax.random.key(seed), 17)
    return {
        "tokens": scatter_about(streams_of[0], (IMAGES, TOK_IMG, D), 1.0, 6.0, ((0, 4), (1, 8))),
        "norm1_gain": jnp.clip(1.0 + 0.18 * jax.random.normal(streams_of[1], (D,), jnp.float32), 0.1, 1.9),
        "norm1_bias": scatter_about(streams_of[2], (D,), 0.5, 3.0, (), jnp.float32),
        "qkv_weight": scatter_about(streams_of[3], (3, D, D), D ** -0.5, 0.15625, ((1, 8), (2, 4))),
        "qv_bias": scatter_about(streams_of[4], (2, D), 0.5, 3.0, (), jnp.float32),
        "rel_rows": scatter_about(streams_of[5], (REL_ROWS, HD), 0.15, 0.8984375),
        "rel_cols": scatter_about(streams_of[6], (REL_COLS, HD), 0.15, 0.8984375),
        "proj_weight": scatter_about(streams_of[7], (D, D), (D // 64) ** -0.5, 1.25, ((0, 4), (1, 8))),
        "proj_bias": scatter_about(streams_of[8], (D,), 0.5, 3.0, (), jnp.float32),
        "norm2_gain": jnp.clip(1.0 + 0.18 * jax.random.normal(streams_of[9], (D,), jnp.float32), 0.1, 1.9),
        "norm2_bias": scatter_about(streams_of[10], (D,), 0.5, 3.0, (), jnp.float32),
        "fc1_weight": scatter_about(streams_of[11], (D, FF), D ** -0.5, 0.15625, ((0, 8), (1, 4))),
        "fc1_bias": scatter_about(streams_of[12], (FF,), 0.5, 3.0, (), jnp.float32),
        "fc2_weight": scatter_about(streams_of[13], (FF, D), FF ** -0.5, 0.078125, ((0, 4), (1, 8))),
        "fc2_bias": scatter_about(streams_of[14], (D,), 0.5, 3.0, (), jnp.float32),
        "cotangent": scatter_about(streams_of[15], (IMAGES, TOK_IMG, D), 1.0, 6.0, ((0, 4), (1, 8))),
    }


PRECISE = lax.Precision.HIGHEST
EPSILON = 1e-06

@jax.custom_vjp
def low(v):
    return lax.optimization_barrier(v.astype(jnp.bfloat16)).astype(jnp.float32)

@jax.custom_vjp
def low_back(v):
    return v

def low_keep(v):
    return (low(v), None)

def low_pass(kept, grad):
    return (grad,)

def back_keep(v):
    return (v, None)

def back_low(kept, grad):
    return (low(grad),)
low.defvjp(low_keep, low_pass)
low_back.defvjp(back_keep, back_low)

def layer_norm(values_in, gain_vec, shift_vec):
    average = lax.optimization_barrier(jnp.mean(values_in, -1, keepdims=True))
    centred = values_in - average
    variance = lax.optimization_barrier(jnp.mean(centred * centred, -1, keepdims=True))
    return centred * lax.rsqrt(variance + EPSILON) * gain_vec + shift_vec

def image_block(params, one_image):
    norm1_gain, norm1_bias, qkv_weight, qv_bias, rel_rows, rel_cols, proj_weight, proj_bias, norm2_gain, norm2_bias, fc1_weight, fc1_bias, fc2_weight, fc2_bias = params
    tokens_here = one_image.shape[0]
    grid_rows = tokens_here // COLS
    normed1 = low(layer_norm(one_image, norm1_gain, norm1_bias))
    queries = low(low_back(jnp.dot(normed1, qkv_weight[0], precision=PRECISE) + qv_bias[0]))
    keys_all = low(low_back(jnp.dot(normed1, qkv_weight[1], precision=PRECISE)))
    values_all = low(low_back(jnp.dot(normed1, qkv_weight[2], precision=PRECISE) + qv_bias[1]))
    row_ids = jnp.arange(grid_rows, dtype=jnp.int32)
    table_rows = rel_rows[row_ids[:, None] - row_ids[None, :] + grid_rows - 1]
    col_ids = jnp.arange(COLS, dtype=jnp.int32)
    table_cols = rel_cols[col_ids[:, None] - col_ids[None, :] + COLS - 1]
    grid_form = queries.reshape(grid_rows, COLS, H, HD)
    along_rows = jnp.einsum('rwhc,rkc->hrwk', grid_form, table_rows, precision=PRECISE).reshape(H, tokens_here, grid_rows)
    along_cols = jnp.einsum('rwhc,wkc->hrwk', grid_form, table_cols, precision=PRECISE).reshape(H, tokens_here, COLS)
    query_heads = queries.reshape(tokens_here, H, HD).transpose(1, 0, 2)
    key_heads = keys_all.reshape(tokens_here, H, HD).transpose(1, 0, 2)
    value_heads = values_all.reshape(tokens_here, H, HD).transpose(1, 0, 2)
    block_len = 512 if tokens_here % 512 == 0 else tokens_here
    blocks = tokens_here // block_len

    def attend(inputs):
        query_blk, rows_blk, cols_blk = inputs
        scores = HD ** (-0.5) * jnp.einsum('hqc,hkc->hqk', query_blk, key_heads, precision=PRECISE)
        scores = scores + (rows_blk[:, :, :, None] + cols_blk[:, :, None, :]).reshape(H, block_len, tokens_here)
        soft_probs = jax.nn.softmax(low_back(scores), axis=-1)
        return jnp.einsum('hqk,hkc->hqc', low(soft_probs), value_heads, precision=PRECISE)
    split_query = query_heads.reshape(H, blocks, block_len, HD).transpose(1, 0, 2, 3)
    split_rows = along_rows.reshape(H, blocks, block_len, grid_rows).transpose(1, 0, 2, 3)
    split_cols = along_cols.reshape(H, blocks, block_len, COLS).transpose(1, 0, 2, 3)
    attended = lax.map(jax.checkpoint(attend), (split_query, split_rows, split_cols))
    attended = attended.transpose(0, 2, 1, 3).reshape(tokens_here, H * HD)
    attended = low(low_back(attended))
    branch = low_back(jnp.dot(attended, proj_weight, precision=PRECISE) + proj_bias)
    middle = one_image + branch
    normed2 = low(layer_norm(middle, norm2_gain, norm2_bias))
    hidden_pre = low_back(jnp.dot(normed2, fc1_weight, precision=PRECISE) + fc1_bias)
    activated = low(jax.nn.gelu(hidden_pre, approximate=False))
    return middle + jnp.dot(activated, fc2_weight, precision=PRECISE) + fc2_bias

def reference(tokens, norm1_gain, norm1_bias, qkv_weight, qv_bias, rel_rows, rel_cols, proj_weight, proj_bias, norm2_gain, norm2_bias, fc1_weight, fc1_bias, fc2_weight, fc2_bias, cotangent):
    params = tuple((member.astype(jnp.float32) for member in (norm1_gain, norm1_bias, qkv_weight, qv_bias, rel_rows, rel_cols, proj_weight, proj_bias, norm2_gain, norm2_bias, fc1_weight, fc1_bias, fc2_weight, fc2_bias)))

    def one_step(summed, paired):
        one_image, one_cot = paired
        result, pullback = jax.vjp(image_block, params, one_image.astype(jnp.float32))
        param_grads, input_grad = pullback(one_cot.astype(jnp.float32))
        summed = jax.tree.map(lambda before, addend: before + addend, summed, param_grads)
        return (summed, (result.astype(jnp.bfloat16), input_grad.astype(jnp.bfloat16)))
    start_sums = tuple((jnp.zeros(member.shape, jnp.float32) for member in params))
    all_grads, (output, tokens_grad) = lax.scan(one_step, start_sums, (tokens, cotangent))
    return (output, tokens_grad, all_grads[0], all_grads[1], all_grads[2], all_grads[3], all_grads[4], all_grads[5], all_grads[6], all_grads[7], all_grads[8], all_grads[9], all_grads[10], all_grads[11], all_grads[12], all_grads[13])
```

```python
from functools import partial
import math

import jax
import jax.numpy as jnp
from jax import lax
from jax.experimental import pallas as pl
from jax.experimental.pallas import tpu as pltpu
from jax.sharding import PartitionSpec as P

D = 1280
H = 16
HD = 80
FF = 5120
COLS = 64
ROWS_DEV = 8


PRECISE = lax.Precision.HIGHEST
EPSILON = 1e-06
NEGATIVE = -1e30


def layer_norm(values_in, gain_vec, shift_vec):
    average = jnp.mean(values_in, -1, keepdims=True)
    centred = values_in - average
    variance = jnp.mean(centred * centred, -1, keepdims=True)
    return centred * lax.rsqrt(variance + EPSILON) * gain_vec + shift_vec


def block_size():
    return 512


def to_heads(flat_rows, heads_local):
    images, length, feat_width = flat_rows.shape
    return flat_rows.reshape(images, length, heads_local, feat_width // heads_local).transpose(
        0, 2, 1, 3
    )


def from_heads(per_head):
    images, heads_local, length, head_dim = per_head.shape
    return per_head.transpose(0, 2, 1, 3).reshape(images, length, heads_local * head_dim)


def block_scores(query_heads, key_flat, rows_bias, cols_bias, first_key, scale_factor):
    key_heads = to_heads(key_flat, query_heads.shape[1])
    key_len = key_flat.shape[1]
    key_rows = key_len // COLS
    scores = scale_factor * jnp.einsum(
        "ihqc,ihkc->ihqk", query_heads, key_heads, preferred_element_type=jnp.float32
    )
    images, heads_local, query_len, unused_len = scores.shape
    row_part = lax.dynamic_slice_in_dim(rows_bias, first_key // COLS, key_rows, 3)
    scores = scores.reshape(images, heads_local, query_len, key_rows, COLS)
    scores = scores + row_part[..., :, None] + cols_bias[..., None, :]
    return scores.reshape(images, heads_local, query_len, key_len)


def relative_terms(query_flat, rows_param, cols_param, first_row, heads_local):
    images, length, feat_width = query_flat.shape
    rows_dev = length // COLS
    grid_rows = (rows_param.shape[0] + 1) // 2
    own_rows = first_row + jnp.arange(rows_dev, dtype=jnp.int32)
    key_rows = jnp.arange(grid_rows, dtype=jnp.int32)
    row_slots = jnp.arange(rows_param.shape[0], dtype=jnp.int32)
    pick_rows = (
        row_slots[None, None, :]
        == own_rows[:, None, None] - key_rows[None, :, None] + grid_rows - 1
    ).astype(jnp.float32)
    table_rows = jnp.einsum("rkj,jc->rkc", pick_rows, rows_param, precision=PRECISE)
    col_ids = jnp.arange(COLS, dtype=jnp.int32)
    col_slots = jnp.arange(cols_param.shape[0], dtype=jnp.int32)
    pick_cols = (
        col_slots[None, None, :] == col_ids[:, None, None] - col_ids[None, :, None] + COLS - 1
    ).astype(jnp.float32)
    table_cols = jnp.einsum("wkj,jc->wkc", pick_cols, cols_param, precision=PRECISE)
    grid_form = query_flat.reshape(images, rows_dev, COLS, heads_local, feat_width // heads_local)
    along_rows = jnp.einsum("irwhc,rkc->ihrwk", grid_form, table_rows, precision=PRECISE).reshape(
        images, heads_local, length, grid_rows
    )
    along_cols = jnp.einsum("irwhc,wkc->ihrwk", grid_form, table_cols, precision=PRECISE).reshape(
        images, heads_local, length, COLS
    )
    return (along_rows, along_cols)


def on_device_rows(
    tokens,
    norm1_gain,
    norm1_bias,
    qkv_weight,
    qv_bias,
    rel_rows,
    rel_cols,
    proj_weight,
    proj_bias,
    norm2_gain,
    norm2_bias,
    fc1_weight,
    fc1_bias,
    fc2_weight,
    fc2_bias,
    cotangent,
):
    scale_factor = HD ** (-0.5)
    tp_count = lax.axis_size("tp")
    ctx_count = lax.axis_size("ctx")
    tp_rank = lax.axis_index("tp")
    ctx_rank = lax.axis_index("ctx")
    grid_rows = ROWS_DEV * ctx_count
    tok_image = grid_rows * COLS
    tok_ctx = ROWS_DEV * COLS
    heads_local = H // tp_count
    width_local = heads_local * HD
    ff_local = FF // tp_count
    images = tokens.shape[0]
    rows_table = rel_rows.astype(jnp.float32)
    cols_table = rel_cols.astype(jnp.float32)
    qkv_full, proj_full, fc1_full, fc2_full = (
        lax.all_gather(qkv_weight, ("shard", "ctx"), axis=1, tiled=True),
        lax.all_gather(proj_weight, ("shard", "ctx"), axis=1, tiled=True),
        lax.all_gather(fc1_weight, ("shard", "ctx"), axis=0, tiled=True),
        lax.all_gather(fc2_weight, ("shard", "ctx"), axis=1, tiled=True),
    )
    qv_local = lax.dynamic_slice_in_dim(qv_bias, tp_rank * width_local, width_local, 1)
    fc1_local = lax.dynamic_slice_in_dim(fc1_bias, tp_rank * ff_local, ff_local, 0)
    resid_in = tokens.astype(jnp.float32)
    normed1 = layer_norm(resid_in, norm1_gain, norm1_bias).astype(jnp.bfloat16)
    normed1_full = lax.all_gather(normed1, "tp", axis=1, tiled=True)
    projected = jnp.einsum(
        "itd,sde->itse", normed1_full, qkv_full, preferred_element_type=jnp.float32
    )
    queries = (projected[:, :, 0] + qv_local[0]).astype(jnp.bfloat16)
    keys_own = projected[:, :, 1].astype(jnp.bfloat16)
    values_own = (projected[:, :, 2] + qv_local[1]).astype(jnp.bfloat16)
    first_row = ctx_rank * ROWS_DEV
    rel_fn = partial(relative_terms, first_row=first_row, heads_local=heads_local)
    (along_rows, along_cols), rel_pull = jax.vjp(
        rel_fn, queries.astype(jnp.float32), rows_table, cols_table
    )
    query_heads = to_heads(queries, heads_local)
    start_state = (
        jnp.full((images, heads_local, tok_ctx), NEGATIVE, jnp.float32),
        jnp.zeros((images, heads_local, tok_ctx), jnp.float32),
        jnp.zeros((images, heads_local, tok_ctx, HD), jnp.float32),
        jnp.zeros((images, tok_image, width_local), jnp.bfloat16),
        jnp.zeros((images, tok_image, width_local), jnp.bfloat16),
    )
    shard_piece = (
        lax.all_gather(keys_own, "ctx", axis=1, tiled=True),
        lax.all_gather(values_own, "ctx", axis=1, tiled=True),
    )
    piece_len = shard_piece[0].shape[1]
    step_len = block_size()

    def one_step(inner, offset):
        run_max, run_sum, run_acc, keys_all, values_all = inner
        key_blk = lax.dynamic_slice_in_dim(shard_piece[0], offset, step_len, 1)
        value_blk = lax.dynamic_slice_in_dim(shard_piece[1], offset, step_len, 1)
        scores = block_scores(query_heads, key_blk, along_rows, along_cols, offset, scale_factor)
        new_max = jnp.maximum(run_max, jnp.max(scores, -1))
        factor = jnp.exp(run_max - new_max)
        weights_blk = jnp.exp(scores - new_max[..., None])
        run_sum = run_sum * factor + jnp.sum(weights_blk, -1)
        value_heads = to_heads(value_blk, heads_local)
        run_acc = run_acc * factor[..., None] + jnp.einsum(
            "ihqk,ihkc->ihqc",
            weights_blk.astype(jnp.bfloat16),
            value_heads,
            preferred_element_type=jnp.float32,
        )
        keys_all = lax.dynamic_update_slice_in_dim(keys_all, key_blk, offset, 1)
        values_all = lax.dynamic_update_slice_in_dim(values_all, value_blk, offset, 1)
        return ((new_max, run_sum, run_acc, keys_all, values_all), None)

    offsets = jnp.arange(piece_len // step_len, dtype=jnp.int32) * step_len
    result, unused = lax.scan(one_step, start_state, offsets)
    run_max, run_sum, run_acc, keys_all, values_all = result
    attn_heads = run_acc / run_sum[..., None]
    log_total = run_max + jnp.log(run_sum)
    attn_low = from_heads(attn_heads).astype(jnp.bfloat16)
    proj_part = jnp.einsum("itd,de->ite", attn_low, proj_full, preferred_element_type=jnp.float32)
    branch = lax.psum_scatter(
        proj_part.astype(jnp.bfloat16), "tp", scatter_dimension=1, tiled=True
    ).astype(jnp.float32)
    middle = resid_in + branch + proj_bias
    normed2 = layer_norm(middle, norm2_gain, norm2_bias).astype(jnp.bfloat16)
    normed2_full = lax.all_gather(normed2, "tp", axis=1, tiled=True)
    hidden_pre = (
        jnp.einsum("itd,df->itf", normed2_full, fc1_full, preferred_element_type=jnp.float32)
        + fc1_local
    )
    gelu_exact = partial(jax.nn.gelu, approximate=False)
    activated_f, gelu_pull = jax.vjp(gelu_exact, hidden_pre)
    activated = activated_f.astype(jnp.bfloat16)
    mlp_part = jnp.einsum("itf,fe->ite", activated, fc2_full, preferred_element_type=jnp.float32)
    mlp_out = lax.psum_scatter(
        mlp_part.astype(jnp.bfloat16), "tp", scatter_dimension=1, tiled=True
    ).astype(jnp.float32)
    output = (middle + mlp_out + fc2_bias).astype(jnp.bfloat16)
    cot_full = lax.all_gather(cotangent, "tp", axis=1, tiled=True)
    d_act = jnp.einsum("ite,fe->itf", cot_full, fc2_full, preferred_element_type=jnp.float32)
    d_hidden = gelu_pull(d_act)[0].astype(jnp.bfloat16)
    fc2_grad = jnp.einsum("itf,ite->fe", activated, cot_full, preferred_element_type=jnp.float32)
    fc1_grad = jnp.einsum("itd,itf->df", normed2_full, d_hidden, preferred_element_type=jnp.float32)
    fc1_bias_part = jnp.sum(d_hidden.astype(jnp.float32), (0, 1))
    fc2_bias_part = jnp.sum(cotangent.astype(jnp.float32), (0, 1))
    d_norm2_part = jnp.einsum("itf,df->itd", d_hidden, fc1_full, preferred_element_type=jnp.float32)
    d_norm2 = lax.psum_scatter(
        d_norm2_part.astype(jnp.bfloat16), "tp", scatter_dimension=1, tiled=True
    ).astype(jnp.float32)
    unused_out, norm2_pull = jax.vjp(layer_norm, middle, norm2_gain, norm2_bias)
    d_mid_part, gain2_part, bias2_part = norm2_pull(d_norm2)
    d_middle = cotangent.astype(jnp.float32) + d_mid_part
    d_branch = d_middle.astype(jnp.bfloat16)
    proj_bias_part = jnp.sum(d_branch.astype(jnp.float32), (0, 1))
    d_branch_full = lax.all_gather(d_branch, "tp", axis=1, tiled=True)
    proj_grad = jnp.einsum(
        "itd,ite->de", attn_low, d_branch_full, preferred_element_type=jnp.float32
    )
    d_attn = jnp.einsum(
        "ite,de->itd", d_branch_full, proj_full, preferred_element_type=jnp.float32
    ).astype(jnp.bfloat16)
    d_attn_heads = to_heads(d_attn, heads_local)
    delta_rows = jnp.sum(d_attn_heads.astype(jnp.float32) * attn_heads, -1)
    key_step = block_size()
    key_rows = key_step // COLS
    key_offsets = jnp.arange(tok_image // key_step, dtype=jnp.int32) * key_step

    def back_step(carried, offset):
        grad_query, grad_rows, grad_cols = carried
        key_blk = lax.dynamic_slice_in_dim(keys_all, offset, key_step, 1)
        value_blk = lax.dynamic_slice_in_dim(values_all, offset, key_step, 1)
        scores = block_scores(query_heads, key_blk, along_rows, along_cols, offset, scale_factor)
        soft_probs = jnp.exp(scores - log_total[..., None])
        value_heads = to_heads(value_blk, heads_local)
        key_heads = to_heads(key_blk, heads_local)
        d_probs = jnp.einsum(
            "ihqc,ihkc->ihqk", d_attn_heads, value_heads, preferred_element_type=jnp.float32
        )
        d_scores = (soft_probs * (d_probs - delta_rows[..., None])).astype(jnp.bfloat16)
        grad_query = grad_query + jnp.einsum(
            "ihqk,ihkc->ihqc", d_scores, key_heads, preferred_element_type=jnp.float32
        )
        grid_scores = d_scores.astype(jnp.float32).reshape(
            images, heads_local, tok_ctx, key_rows, COLS
        )
        row_sums = jnp.sum(grid_scores, 4)
        row_now = lax.dynamic_slice_in_dim(grad_rows, offset // COLS, key_rows, 3)
        grad_rows = lax.dynamic_update_slice_in_dim(
            grad_rows, row_now + row_sums, offset // COLS, 3
        )
        grad_cols = grad_cols + jnp.sum(grid_scores, 3)
        key_part = scale_factor * jnp.einsum(
            "ihqk,ihqc->ikhc", d_scores, query_heads, preferred_element_type=jnp.float32
        )
        value_part = jnp.einsum(
            "ihqk,ihqc->ikhc",
            soft_probs.astype(jnp.bfloat16),
            d_attn_heads,
            preferred_element_type=jnp.float32,
        )
        emitted = (
            key_part.reshape(images, key_step, width_local),
            value_part.reshape(images, key_step, width_local),
        )
        return ((grad_query, grad_rows, grad_cols), emitted)

    back_start = (
        jnp.zeros((images, heads_local, tok_ctx, HD), jnp.float32),
        jnp.zeros((images, heads_local, tok_ctx, grid_rows), jnp.float32),
        jnp.zeros((images, heads_local, tok_ctx, COLS), jnp.float32),
    )
    (grad_query, grad_rows, grad_cols), emitted = lax.scan(back_step, back_start, key_offsets)
    key_terms = emitted[0].transpose(1, 0, 2, 3).reshape(images, tok_image, width_local)
    value_terms = emitted[1].transpose(1, 0, 2, 3).reshape(images, tok_image, width_local)
    grad_keys, grad_values = (
        lax.psum_scatter(
            key_terms.astype(jnp.bfloat16), "ctx", scatter_dimension=1, tiled=True
        ).astype(jnp.float32),
        lax.psum_scatter(
            value_terms.astype(jnp.bfloat16), "ctx", scatter_dimension=1, tiled=True
        ).astype(jnp.float32),
    )
    d_query_rel, rows_grad_part, cols_grad_part = rel_pull((grad_rows, grad_cols))
    d_query = (scale_factor * from_heads(grad_query) + d_query_rel).astype(jnp.bfloat16)
    d_keys = grad_keys.astype(jnp.bfloat16)
    d_values = grad_values.astype(jnp.bfloat16)
    d_projected = jnp.stack((d_query, d_keys, d_values), axis=2)
    qkv_grad = jnp.einsum(
        "itd,itse->sde", normed1_full, d_projected, preferred_element_type=jnp.float32
    )
    qv_bias_part = jnp.stack(
        (
            jnp.sum(d_query.astype(jnp.float32), (0, 1)),
            jnp.sum(d_values.astype(jnp.float32), (0, 1)),
        )
    )
    d_norm1_part = jnp.einsum(
        "itse,sde->itd", d_projected, qkv_full, preferred_element_type=jnp.float32
    )
    d_norm1 = lax.psum_scatter(
        d_norm1_part.astype(jnp.bfloat16), "tp", scatter_dimension=1, tiled=True
    ).astype(jnp.float32)
    unused_in, norm1_pull = jax.vjp(layer_norm, resid_in, norm1_gain, norm1_bias)
    d_in_part, gain1_part, bias1_part = norm1_pull(d_norm1)
    tokens_grad = (d_middle + d_in_part).astype(jnp.bfloat16)
    qkv_out, proj_out, fc1_out, fc2_out = (
        lax.psum_scatter(
            qkv_grad.astype(jnp.bfloat16), ("shard", "ctx"), scatter_dimension=1, tiled=True
        ).astype(jnp.float32),
        lax.psum_scatter(
            proj_grad.astype(jnp.bfloat16), ("shard", "ctx"), scatter_dimension=1, tiled=True
        ).astype(jnp.float32),
        lax.psum_scatter(
            fc1_grad.astype(jnp.bfloat16), ("shard", "ctx"), scatter_dimension=0, tiled=True
        ).astype(jnp.float32),
        lax.psum_scatter(
            fc2_grad.astype(jnp.bfloat16), ("shard", "ctx"), scatter_dimension=1, tiled=True
        ).astype(jnp.float32),
    )
    qv_placed = lax.dynamic_update_slice_in_dim(
        jnp.zeros((2, D), jnp.float32), qv_bias_part, tp_rank * width_local, 1
    )
    fc1_placed = lax.dynamic_update_slice_in_dim(
        jnp.zeros((FF,), jnp.float32), fc1_bias_part, tp_rank * ff_local, 0
    )
    (
        gain1_sum,
        bias1_sum,
        qv_sum,
        rows_sum,
        cols_sum,
        projb_sum,
        gain2_sum,
        bias2_sum,
        fc1b_sum,
        fc2b_sum,
    ) = lax.psum(
        (
            gain1_part,
            bias1_part,
            qv_placed,
            rows_grad_part,
            cols_grad_part,
            proj_bias_part,
            gain2_part,
            bias2_part,
            fc1_placed,
            fc2_bias_part,
        ),
        ("shard", "ctx", "tp"),
    )
    return (
        output,
        tokens_grad,
        gain1_sum,
        bias1_sum,
        qkv_out,
        qv_sum,
        rows_sum,
        cols_sum,
        proj_out,
        projb_sum,
        gain2_sum,
        bias2_sum,
        fc1_out,
        fc1b_sum,
        fc2_out,
        fc2b_sum,
    )


F32 = jnp.float32
BF16 = jnp.bfloat16
NT = (((1,), (1,)), ((), ()))
NN = (((1,), (0,)), ((), ()))
TN = (((0,), (0,)), ((), ()))
VMEM_GRANT = 60 * 2**20


def mm(left, right, dims=NN):
    return lax.dot_general(left, right, dims, preferred_element_type=F32)


def lane_ids(shape):
    return lax.broadcasted_iota(jnp.int32, shape, 1)


def fwd_kernel(
    heads, hd, cols, rows, qb, q_ref, k_ref, v_ref, tab_ref, hot_ref, o_ref, ob_ref, lse_ref, qa_ref, ka_ref
):
    tok = q_ref.shape[0]
    c = hd**-0.5 * math.log2(math.e)
    up = hd**0.5
    for h in range(heads):
        sl = slice(h * hd, (h + 1) * hd)
        pad = jnp.zeros((tok, 128 - hd), BF16)
        qp = jnp.concatenate([q_ref[:, sl], pad], 1)
        kp = jnp.concatenate([k_ref[:, sl], pad], 1)
        vt = jnp.concatenate([v_ref[:, sl], pad], 1).T
        ka_ref[h, :, 0:128] = jnp.where(lane_ids((tok, 128)) < hd, kp, hot_ref[:, 0:128])
        ka_ref[h, :, 128:256] = hot_ref[:, 128:256]
        terms = mm(qp, tab_ref[...]) * up
        ln = lane_ids((cols, 128))
        for r in range(rows):
            rs = slice(r * cols, (r + 1) * cols)
            tr = pltpu.roll(terms[rs, 0:128], (65 + r) % 128, 1)
            tc = pltpu.roll(terms[rs, 128:256], 65, 1, stride=1, stride_axis=0)
            rh = tr.astype(BF16).astype(F32)
            rl = pltpu.roll(tr - rh, rows, 1)
            ch = tc.astype(BF16).astype(F32)
            cl = pltpu.roll(tc - ch, 64, 1)
            low = jnp.where(ln < hd + 2 * rows, rl, jnp.zeros_like(tr))
            left = jnp.where(ln < hd, qp[rs].astype(F32), jnp.where(ln < hd + rows, rh, low))
            qa_ref[h, rs, 0:128] = left.astype(BF16)
            qa_ref[h, rs, 128:256] = jnp.where(ln < 64, ch, cl).astype(BF16)

        def blk(i, _):
            at = pl.ds(pl.multiple_of(i * qb, qb), qb)
            s = mm(ka_ref[h], qa_ref[h, at, :], NT)
            m = jnp.max(s, 0, keepdims=True)
            p = jnp.exp2((s - m) * c)
            l = jnp.sum(p, 0, keepdims=True)
            o = (mm(vt, p.astype(BF16)) / l).T[:, 0:hd]
            lse_ref[h : h + 1, at] = m * c + jnp.log2(l)
            o_ref[at, sl] = o
            ob_ref[at, sl] = o.astype(BF16)
            return 0

        lax.fori_loop(0, tok // qb, blk, 0)


def attn_fwd(q, k, v, tab, hot, heads, hd, cols, rows, qb=256):
    tok = q.shape[0]
    S = jax.ShapeDtypeStruct
    return pl.pallas_call(
        partial(fwd_kernel, heads, hd, cols, rows, qb),
        out_shape=(
            S((tok, heads * hd), F32),
            S((tok, heads * hd), BF16),
            S((heads, tok), F32),
            S((heads, tok, 256), BF16),
            S((heads, tok, 256), BF16),
        ),
        compiler_params=pltpu.CompilerParams(vmem_limit_bytes=VMEM_GRANT),
        name="attn_fwd",
    )(q, k, v, tab, hot)


def bwd_kernel(
    heads, hd, cols, rows, qb,
    qa_ref, ka_ref, v_ref, do_ref, o_ref, lse_ref, tab_ref, hot_ref,
    dq_ref, dk_ref, dv_ref, rg_ref, kt_ref, acc_k, acc_v, del_ref,
):
    tok = v_ref.shape[0]
    scale = hd**-0.5
    c = scale * math.log2(math.e)
    rg_ref[...] = jnp.zeros_like(rg_ref)
    for h in range(heads):
        sl = slice(h * hd, (h + 1) * hd)
        pad = jnp.zeros((tok, 128 - hd), BF16)
        vp = jnp.concatenate([v_ref[:, sl], pad], 1)
        kt_ref[0:128, :] = jnp.where(lane_ids((tok, 128)) < hd, ka_ref[h, :, 0:128], hot_ref[:, 0:128]).T
        kt_ref[128:256, :] = hot_ref[:, 128:256].T
        prod = jnp.concatenate([do_ref[:, sl].astype(F32) * o_ref[:, sl], pad.astype(F32)], 1)
        del_ref[...] = lax.dot_general(
            jnp.ones((8, 128), F32), prod, NT, preferred_element_type=F32, precision=PRECISE
        )
        acc_k[...] = jnp.zeros_like(acc_k)
        acc_v[...] = jnp.zeros_like(acc_v)

        def blk(i, _):
            at = pl.ds(pl.multiple_of(i * qb, qb), qb)
            qblk = qa_ref[h, at, :]
            dob = jnp.concatenate([do_ref[at, sl], jnp.zeros((qb, 128 - hd), BF16)], 1)
            s = mm(ka_ref[h], qblk, NT)
            p = jnp.exp2(s * c - lse_ref[h : h + 1, at])
            dp = mm(vp, dob, NT)
            ds = (p * (dp - del_ref[0:1, at])).astype(BF16)
            acc_v[...] += mm(p.astype(BF16), dob)
            acc_k[...] += mm(ds, qblk[:, 0:128])
            dqa = mm(kt_ref[...], ds).T
            ln = lane_ids((cols, 128))
            parts = []
            for j in range(qb // cols):
                r = i * (qb // cols) + j
                js = slice(j * cols, (j + 1) * cols)
                dr = dqa[js, 0:128]
                dr = jnp.where((ln >= hd) & (ln < hd + rows), dr, 0.0)
                dr = pltpu.roll(dr, (48 + r) % 128, 1)
                dc = pltpu.roll(dqa[js, 128:256], 0, 1, stride=1, stride_axis=0)
                parts.append(jnp.concatenate([dr, dc], 1))
            d = jnp.concatenate(parts, 0).astype(BF16)
            rel = mm(d, tab_ref[...])
            rg_ref[...] += mm(d, qblk[:, 0:128], TN)
            dq_ref[at, sl] = (scale * dqa[:, 0:128] + rel)[:, 0:hd].astype(BF16)
            return 0

        lax.fori_loop(0, tok // qb, blk, 0)
        dk_ref[:, sl] = (scale * acc_k[...])[:, 0:hd].astype(BF16)
        dv_ref[:, sl] = acc_v[...][:, 0:hd].astype(BF16)


def attn_bwd(qa, ka, v, do, o, lse, tab, hot, heads, hd, cols, rows, qb=256):
    tok = v.shape[0]
    S = jax.ShapeDtypeStruct
    return pl.pallas_call(
        partial(bwd_kernel, heads, hd, cols, rows, qb),
        out_shape=(S((tok, heads * hd), BF16),) * 3 + (S((256, 128), F32),),
        scratch_shapes=[
            pltpu.VMEM((256, tok), BF16),
            pltpu.VMEM((tok, 128), F32),
            pltpu.VMEM((tok, 128), F32),
            pltpu.VMEM((8, tok), F32),
        ],
        compiler_params=pltpu.CompilerParams(vmem_limit_bytes=VMEM_GRANT),
        name="attn_bwd",
    )(qa, ka, v, do, o, lse, tab, hot)


def position_tables(rel_rows, rel_cols, hd):
    gap = 128 - hd
    rr = jnp.pad(rel_rows, ((0, 128 - rel_rows.shape[0]), (0, gap)))
    rc = jnp.pad(rel_cols, ((0, 128 - rel_cols.shape[0]), (0, gap)))
    fr = jnp.pad(rel_rows[::-1], ((0, 128 - rel_rows.shape[0]), (0, gap)))
    fc = jnp.pad(rel_cols[::-1], ((0, 128 - rel_cols.shape[0]), (0, gap)))
    return jnp.concatenate([fr, fc], 0).T, jnp.concatenate([rr, rc], 0)


def position_hots(tok, hd, cols, rows):
    t = lax.broadcasted_iota(jnp.int32, (tok, 256), 0)
    l = lax.broadcasted_iota(jnp.int32, (tok, 256), 1)
    kr = t // cols
    kw = t % cols
    first = (l == hd + kr) | (l == hd + rows + kr) | (l == 128 + kw) | (l == 192 + kw)
    second = (l == hd + rows - 1 - kr) | (l == 128 + cols - 1 - kw)
    return first.astype(BF16), second.astype(BF16)


def swap_halves(block):
    mine = lax.axis_index("ctx")
    keep = lax.dynamic_index_in_dim(block, mine, 0, keepdims=False)
    give = lax.dynamic_index_in_dim(block, 1 - mine, 0, keepdims=False)
    got = lax.ppermute(give, "ctx", [(0, 1), (1, 0)])
    first = mine == 0
    return jnp.stack([jnp.where(first, keep, got), jnp.where(first, got, keep)])


def ln_stats(values):
    average = jnp.mean(values, -1, keepdims=True)
    centred = values - average
    inverse = lax.rsqrt(jnp.mean(centred * centred, -1, keepdims=True) + EPSILON)
    return centred * inverse, inverse


def ln_back(unit, inverse, gain, grad):
    scaled = grad * gain
    first = jnp.mean(scaled, -1, keepdims=True)
    second = jnp.mean(scaled * unit, -1, keepdims=True)
    return inverse * (scaled - first - unit * second)


def on_device_images(
    tokens, norm1_gain, norm1_bias, qkv_weight, qv_bias, rel_rows, rel_cols, proj_weight, proj_bias,
    norm2_gain, norm2_bias, fc1_weight, fc1_bias, fc2_weight, fc2_bias, cotangent,
):
    tp_count = lax.axis_size("tp")
    tp_rank = lax.axis_index("tp")
    heads = H // tp_count
    width = heads * HD
    ff = FF // tp_count
    rows = (rel_rows.shape[0] + 1) // 2
    tok = rows * COLS
    cotangent_own = swap_halves(cotangent)
    tokens_own = swap_halves(tokens)
    qkv_full = lax.all_gather(qkv_weight, ("shard", "ctx"), axis=1, tiled=True)
    proj_full = lax.all_gather(proj_weight, ("shard", "ctx"), axis=1, tiled=True)
    fc1_full = lax.all_gather(fc1_weight, ("shard", "ctx"), axis=0, tiled=True)
    fc2_full = lax.all_gather(fc2_weight, ("shard", "ctx"), axis=1, tiled=True)
    qv_local = lax.dynamic_slice_in_dim(qv_bias, tp_rank * width, width, 1)
    fc1_local = lax.dynamic_slice_in_dim(fc1_bias, tp_rank * ff, ff, 0)
    x = tokens_own.astype(F32)
    g = cotangent_own.astype(F32)

    def gather(block):
        return lax.all_gather(block, "tp", axis=1, tiled=True).reshape(tok, D)

    def scatter(part):
        whole = part.astype(BF16).reshape(2, tok // 2, D)
        return lax.psum_scatter(whole, "tp", scatter_dimension=1, tiled=True).astype(F32)

    unit1, inv1 = ln_stats(x)
    a1 = gather((unit1 * norm1_gain + norm1_bias).astype(BF16))
    q = (mm(a1, qkv_full[0]) + qv_local[0]).astype(BF16)
    k = mm(a1, qkv_full[1]).astype(BF16)
    v = (mm(a1, qkv_full[2]) + qv_local[1]).astype(BF16)
    tab_f, tab_b = position_tables(rel_rows, rel_cols, HD)
    hot_f, hot_b = position_hots(tok, HD, COLS, rows)
    o, o_low, lse, qa, ka = attn_fwd(q, k, v, tab_f, hot_f, heads, HD, COLS, rows)
    mid = x + scatter(mm(o_low, proj_full)) + proj_bias
    unit2, inv2 = ln_stats(mid)
    a2 = gather((unit2 * norm2_gain + norm2_bias).astype(BF16))
    cot = gather(cotangent_own)
    pre = mm(a2, fc1_full) + fc1_local
    cdf = 0.5 * (1.0 + lax.erf(pre * (2.0**-0.5)))
    act = (pre * cdf).astype(BF16)
    slope = cdf + pre * jnp.exp(-0.5 * pre * pre) * ((2.0 * math.pi) ** -0.5)
    d_pre = (mm(cot, fc2_full, NT) * slope).astype(BF16)
    d_a2 = scatter(mm(d_pre, fc1_full, NT))
    output = (mid + scatter(mm(act, fc2_full)) + fc2_bias).astype(BF16)
    fc2_grad = mm(act, cot, TN)
    fc1_grad = mm(a2, d_pre, TN)
    d_mid = g + ln_back(unit2, inv2, norm2_gain, d_a2)
    d_branch = d_mid.astype(BF16)
    d_branch_full = gather(d_branch)
    d_o = mm(d_branch_full, proj_full, NT).astype(BF16)
    proj_grad = mm(o_low, d_branch_full, TN)
    dq, dk, dv, rel_grad = attn_bwd(qa, ka, v, d_o, o, lse, tab_b, hot_b, heads, HD, COLS, rows)
    d_a1 = scatter(mm(dq, qkv_full[0], NT) + mm(dk, qkv_full[1], NT) + mm(dv, qkv_full[2], NT))
    qkv_grad = jnp.stack([mm(a1, dq, TN), mm(a1, dk, TN), mm(a1, dv, TN)])
    tokens_grad = (d_mid + ln_back(unit1, inv1, norm1_gain, d_a1)).astype(BF16)

    def reduce(part, dim):
        return lax.psum_scatter(
            part.astype(BF16), ("shard", "ctx"), scatter_dimension=dim, tiled=True
        ).astype(F32)

    def total(part):
        return jnp.sum(part.astype(F32), tuple(range(part.ndim - 1)))

    qv_part = jnp.stack([total(dq), total(dv)])
    qv_placed = lax.dynamic_update_slice_in_dim(jnp.zeros((2, D), F32), qv_part, tp_rank * width, 1)
    fc1_placed = lax.dynamic_update_slice_in_dim(jnp.zeros((FF,), F32), total(d_pre), tp_rank * ff, 0)
    small = lax.psum(
        (
            total(d_a1 * unit1),
            total(d_a1),
            qv_placed,
            rel_grad[: rel_rows.shape[0], :HD],
            rel_grad[128 : 128 + rel_cols.shape[0], :HD],
            total(d_branch),
            total(d_a2 * unit2),
            total(d_a2),
            fc1_placed,
            total(cotangent),
        ),
        ("shard", "ctx", "tp"),
    )
    return (
        swap_halves(output),
        swap_halves(tokens_grad),
        small[0],
        small[1],
        reduce(qkv_grad, 1),
        small[2],
        small[3],
        small[4],
        reduce(proj_grad, 1),
        small[5],
        small[6],
        small[7],
        reduce(fc1_grad, 0),
        small[8],
        reduce(fc2_grad, 1),
        small[9],
    )


def solution(mesh):
    in_specs = (
        P("shard", ("ctx", "tp"), None),
        P(),
        P(),
        P(None, ("shard", "ctx"), "tp"),
        P(),
        P(),
        P(),
        P("tp", ("shard", "ctx")),
        P(),
        P(),
        P(),
        P(("shard", "ctx"), "tp"),
        P(),
        P("tp", ("shard", "ctx")),
        P(),
        P("shard", ("ctx", "tp"), None),
    )
    out_specs = (
        P("shard", ("ctx", "tp"), None),
        P("shard", ("ctx", "tp"), None),
        P(),
        P(),
        P(None, ("shard", "ctx"), "tp"),
        P(),
        P(),
        P(),
        P("tp", ("shard", "ctx")),
        P(),
        P(),
        P(),
        P(("shard", "ctx"), "tp"),
        P(),
        P("tp", ("shard", "ctx")),
        P(),
    )
    def on_device(*arrays):
        rows = (arrays[5].shape[0] + 1) // 2
        fits = mesh.shape["tp"] == 4 and mesh.shape["ctx"] == 2 and HD + 2 * rows <= 128
        fits = fits and arrays[0].shape[0] == mesh.shape["ctx"] and arrays[6].shape[0] <= 128
        return (on_device_images if fits else on_device_rows)(*arrays)

    return jax.shard_map(
        on_device, mesh=mesh, in_specs=in_specs, out_specs=out_specs, check_vma=False
    )
```

```python
from functools import partial
import math

import jax
import jax.numpy as jnp
from jax import lax
from jax.experimental import pallas as pl
from jax.experimental.pallas import tpu as pltpu
from jax.sharding import PartitionSpec as P

D = 1280
H = 16
HD = 80
FF = 5120
COLS = 64
ROWS_DEV = 8


PRECISE = lax.Precision.HIGHEST
EPSILON = 1e-06
NEGATIVE = -1e30


def layer_norm(values_in, gain_vec, shift_vec):
    average = jnp.mean(values_in, -1, keepdims=True)
    centred = values_in - average
    variance = jnp.mean(centred * centred, -1, keepdims=True)
    return centred * lax.rsqrt(variance + EPSILON) * gain_vec + shift_vec


def block_size():
    return 512


def to_heads(flat_rows, heads_local):
    images, length, feat_width = flat_rows.shape
    return flat_rows.reshape(images, length, heads_local, feat_width // heads_local).transpose(
        0, 2, 1, 3
    )


def from_heads(per_head):
    images, heads_local, length, head_dim = per_head.shape
    return per_head.transpose(0, 2, 1, 3).reshape(images, length, heads_local * head_dim)


def block_scores(query_heads, key_flat, rows_bias, cols_bias, first_key, scale_factor):
    key_heads = to_heads(key_flat, query_heads.shape[1])
    key_len = key_flat.shape[1]
    key_rows = key_len // COLS
    scores = scale_factor * jnp.einsum(
        "ihqc,ihkc->ihqk", query_heads, key_heads, preferred_element_type=jnp.float32
    )
    images, heads_local, query_len, unused_len = scores.shape
    row_part = lax.dynamic_slice_in_dim(rows_bias, first_key // COLS, key_rows, 3)
    scores = scores.reshape(images, heads_local, query_len, key_rows, COLS)
    scores = scores + row_part[..., :, None] + cols_bias[..., None, :]
    return scores.reshape(images, heads_local, query_len, key_len)


def relative_terms(query_flat, rows_param, cols_param, first_row, heads_local):
    images, length, feat_width = query_flat.shape
    rows_dev = length // COLS
    grid_rows = (rows_param.shape[0] + 1) // 2
    own_rows = first_row + jnp.arange(rows_dev, dtype=jnp.int32)
    key_rows = jnp.arange(grid_rows, dtype=jnp.int32)
    row_slots = jnp.arange(rows_param.shape[0], dtype=jnp.int32)
    pick_rows = (
        row_slots[None, None, :]
        == own_rows[:, None, None] - key_rows[None, :, None] + grid_rows - 1
    ).astype(jnp.float32)
    table_rows = jnp.einsum("rkj,jc->rkc", pick_rows, rows_param, precision=PRECISE)
    col_ids = jnp.arange(COLS, dtype=jnp.int32)
    col_slots = jnp.arange(cols_param.shape[0], dtype=jnp.int32)
    pick_cols = (
        col_slots[None, None, :] == col_ids[:, None, None] - col_ids[None, :, None] + COLS - 1
    ).astype(jnp.float32)
    table_cols = jnp.einsum("wkj,jc->wkc", pick_cols, cols_param, precision=PRECISE)
    grid_form = query_flat.reshape(images, rows_dev, COLS, heads_local, feat_width // heads_local)
    along_rows = jnp.einsum("irwhc,rkc->ihrwk", grid_form, table_rows, precision=PRECISE).reshape(
        images, heads_local, length, grid_rows
    )
    along_cols = jnp.einsum("irwhc,wkc->ihrwk", grid_form, table_cols, precision=PRECISE).reshape(
        images, heads_local, length, COLS
    )
    return (along_rows, along_cols)


def on_device_rows(
    tokens,
    norm1_gain,
    norm1_bias,
    qkv_weight,
    qv_bias,
    rel_rows,
    rel_cols,
    proj_weight,
    proj_bias,
    norm2_gain,
    norm2_bias,
    fc1_weight,
    fc1_bias,
    fc2_weight,
    fc2_bias,
    cotangent,
):
    scale_factor = HD ** (-0.5)
    tp_count = lax.axis_size("tp")
    ctx_count = lax.axis_size("ctx")
    tp_rank = lax.axis_index("tp")
    ctx_rank = lax.axis_index("ctx")
    grid_rows = ROWS_DEV * ctx_count
    tok_image = grid_rows * COLS
    tok_ctx = ROWS_DEV * COLS
    heads_local = H // tp_count
    width_local = heads_local * HD
    ff_local = FF // tp_count
    images = tokens.shape[0]
    rows_table = rel_rows.astype(jnp.float32)
    cols_table = rel_cols.astype(jnp.float32)
    qkv_full, proj_full, fc1_full, fc2_full = (
        lax.all_gather(qkv_weight, ("shard", "ctx"), axis=1, tiled=True),
        lax.all_gather(proj_weight, ("shard", "ctx"), axis=1, tiled=True),
        lax.all_gather(fc1_weight, ("shard", "ctx"), axis=0, tiled=True),
        lax.all_gather(fc2_weight, ("shard", "ctx"), axis=1, tiled=True),
    )
    qv_local = lax.dynamic_slice_in_dim(qv_bias, tp_rank * width_local, width_local, 1)
    fc1_local = lax.dynamic_slice_in_dim(fc1_bias, tp_rank * ff_local, ff_local, 0)
    resid_in = tokens.astype(jnp.float32)
    normed1 = layer_norm(resid_in, norm1_gain, norm1_bias).astype(jnp.bfloat16)
    normed1_full = lax.all_gather(normed1, "tp", axis=1, tiled=True)
    projected = jnp.einsum(
        "itd,sde->itse", normed1_full, qkv_full, preferred_element_type=jnp.float32
    )
    queries = (projected[:, :, 0] + qv_local[0]).astype(jnp.bfloat16)
    keys_own = projected[:, :, 1].astype(jnp.bfloat16)
    values_own = (projected[:, :, 2] + qv_local[1]).astype(jnp.bfloat16)
    first_row = ctx_rank * ROWS_DEV
    rel_fn = partial(relative_terms, first_row=first_row, heads_local=heads_local)
    (along_rows, along_cols), rel_pull = jax.vjp(
        rel_fn, queries.astype(jnp.float32), rows_table, cols_table
    )
    query_heads = to_heads(queries, heads_local)
    start_state = (
        jnp.full((images, heads_local, tok_ctx), NEGATIVE, jnp.float32),
        jnp.zeros((images, heads_local, tok_ctx), jnp.float32),
        jnp.zeros((images, heads_local, tok_ctx, HD), jnp.float32),
        jnp.zeros((images, tok_image, width_local), jnp.bfloat16),
        jnp.zeros((images, tok_image, width_local), jnp.bfloat16),
    )
    shard_piece = (
        lax.all_gather(keys_own, "ctx", axis=1, tiled=True),
        lax.all_gather(values_own, "ctx", axis=1, tiled=True),
    )
    piece_len = shard_piece[0].shape[1]
    step_len = block_size()

    def one_step(inner, offset):
        run_max, run_sum, run_acc, keys_all, values_all = inner
        key_blk = lax.dynamic_slice_in_dim(shard_piece[0], offset, step_len, 1)
        value_blk = lax.dynamic_slice_in_dim(shard_piece[1], offset, step_len, 1)
        scores = block_scores(query_heads, key_blk, along_rows, along_cols, offset, scale_factor)
        new_max = jnp.maximum(run_max, jnp.max(scores, -1))
        factor = jnp.exp(run_max - new_max)
        weights_blk = jnp.exp(scores - new_max[..., None])
        run_sum = run_sum * factor + jnp.sum(weights_blk, -1)
        value_heads = to_heads(value_blk, heads_local)
        run_acc = run_acc * factor[..., None] + jnp.einsum(
            "ihqk,ihkc->ihqc",
            weights_blk.astype(jnp.bfloat16),
            value_heads,
            preferred_element_type=jnp.float32,
        )
        keys_all = lax.dynamic_update_slice_in_dim(keys_all, key_blk, offset, 1)
        values_all = lax.dynamic_update_slice_in_dim(values_all, value_blk, offset, 1)
        return ((new_max, run_sum, run_acc, keys_all, values_all), None)

    offsets = jnp.arange(piece_len // step_len, dtype=jnp.int32) * step_len
    result, unused = lax.scan(one_step, start_state, offsets)
    run_max, run_sum, run_acc, keys_all, values_all = result
    attn_heads = run_acc / run_sum[..., None]
    log_total = run_max + jnp.log(run_sum)
    attn_low = from_heads(attn_heads).astype(jnp.bfloat16)
    proj_part = jnp.einsum("itd,de->ite", attn_low, proj_full, preferred_element_type=jnp.float32)
    branch = lax.psum_scatter(
        proj_part.astype(jnp.bfloat16), "tp", scatter_dimension=1, tiled=True
    ).astype(jnp.float32)
    middle = resid_in + branch + proj_bias
    normed2 = layer_norm(middle, norm2_gain, norm2_bias).astype(jnp.bfloat16)
    normed2_full = lax.all_gather(normed2, "tp", axis=1, tiled=True)
    hidden_pre = (
        jnp.einsum("itd,df->itf", normed2_full, fc1_full, preferred_element_type=jnp.float32)
        + fc1_local
    )
    gelu_exact = partial(jax.nn.gelu, approximate=False)
    activated_f, gelu_pull = jax.vjp(gelu_exact, hidden_pre)
    activated = activated_f.astype(jnp.bfloat16)
    mlp_part = jnp.einsum("itf,fe->ite", activated, fc2_full, preferred_element_type=jnp.float32)
    mlp_out = lax.psum_scatter(
        mlp_part.astype(jnp.bfloat16), "tp", scatter_dimension=1, tiled=True
    ).astype(jnp.float32)
    output = (middle + mlp_out + fc2_bias).astype(jnp.bfloat16)
    cot_full = lax.all_gather(cotangent, "tp", axis=1, tiled=True)
    d_act = jnp.einsum("ite,fe->itf", cot_full, fc2_full, preferred_element_type=jnp.float32)
    d_hidden = gelu_pull(d_act)[0].astype(jnp.bfloat16)
    fc2_grad = jnp.einsum("itf,ite->fe", activated, cot_full, preferred_element_type=jnp.float32)
    fc1_grad = jnp.einsum("itd,itf->df", normed2_full, d_hidden, preferred_element_type=jnp.float32)
    fc1_bias_part = jnp.sum(d_hidden.astype(jnp.float32), (0, 1))
    fc2_bias_part = jnp.sum(cotangent.astype(jnp.float32), (0, 1))
    d_norm2_part = jnp.einsum("itf,df->itd", d_hidden, fc1_full, preferred_element_type=jnp.float32)
    d_norm2 = lax.psum_scatter(
        d_norm2_part.astype(jnp.bfloat16), "tp", scatter_dimension=1, tiled=True
    ).astype(jnp.float32)
    unused_out, norm2_pull = jax.vjp(layer_norm, middle, norm2_gain, norm2_bias)
    d_mid_part, gain2_part, bias2_part = norm2_pull(d_norm2)
    d_middle = cotangent.astype(jnp.float32) + d_mid_part
    d_branch = d_middle.astype(jnp.bfloat16)
    proj_bias_part = jnp.sum(d_branch.astype(jnp.float32), (0, 1))
    d_branch_full = lax.all_gather(d_branch, "tp", axis=1, tiled=True)
    proj_grad = jnp.einsum(
        "itd,ite->de", attn_low, d_branch_full, preferred_element_type=jnp.float32
    )
    d_attn = jnp.einsum(
        "ite,de->itd", d_branch_full, proj_full, preferred_element_type=jnp.float32
    ).astype(jnp.bfloat16)
    d_attn_heads = to_heads(d_attn, heads_local)
    delta_rows = jnp.sum(d_attn_heads.astype(jnp.float32) * attn_heads, -1)
    key_step = block_size()
    key_rows = key_step // COLS
    key_offsets = jnp.arange(tok_image // key_step, dtype=jnp.int32) * key_step

    def back_step(carried, offset):
        grad_query, grad_rows, grad_cols = carried
        key_blk = lax.dynamic_slice_in_dim(keys_all, offset, key_step, 1)
        value_blk = lax.dynamic_slice_in_dim(values_all, offset, key_step, 1)
        scores = block_scores(query_heads, key_blk, along_rows, along_cols, offset, scale_factor)
        soft_probs = jnp.exp(scores - log_total[..., None])
        value_heads = to_heads(value_blk, heads_local)
        key_heads = to_heads(key_blk, heads_local)
        d_probs = jnp.einsum(
            "ihqc,ihkc->ihqk", d_attn_heads, value_heads, preferred_element_type=jnp.float32
        )
        d_scores = (soft_probs * (d_probs - delta_rows[..., None])).astype(jnp.bfloat16)
        grad_query = grad_query + jnp.einsum(
            "ihqk,ihkc->ihqc", d_scores, key_heads, preferred_element_type=jnp.float32
        )
        grid_scores = d_scores.astype(jnp.float32).reshape(
            images, heads_local, tok_ctx, key_rows, COLS
        )
        row_sums = jnp.sum(grid_scores, 4)
        row_now = lax.dynamic_slice_in_dim(grad_rows, offset // COLS, key_rows, 3)
        grad_rows = lax.dynamic_update_slice_in_dim(
            grad_rows, row_now + row_sums, offset // COLS, 3
        )
        grad_cols = grad_cols + jnp.sum(grid_scores, 3)
        key_part = scale_factor * jnp.einsum(
            "ihqk,ihqc->ikhc", d_scores, query_heads, preferred_element_type=jnp.float32
        )
        value_part = jnp.einsum(
            "ihqk,ihqc->ikhc",
            soft_probs.astype(jnp.bfloat16),
            d_attn_heads,
            preferred_element_type=jnp.float32,
        )
        emitted = (
            key_part.reshape(images, key_step, width_local),
            value_part.reshape(images, key_step, width_local),
        )
        return ((grad_query, grad_rows, grad_cols), emitted)

    back_start = (
        jnp.zeros((images, heads_local, tok_ctx, HD), jnp.float32),
        jnp.zeros((images, heads_local, tok_ctx, grid_rows), jnp.float32),
        jnp.zeros((images, heads_local, tok_ctx, COLS), jnp.float32),
    )
    (grad_query, grad_rows, grad_cols), emitted = lax.scan(back_step, back_start, key_offsets)
    key_terms = emitted[0].transpose(1, 0, 2, 3).reshape(images, tok_image, width_local)
    value_terms = emitted[1].transpose(1, 0, 2, 3).reshape(images, tok_image, width_local)
    grad_keys, grad_values = (
        lax.psum_scatter(
            key_terms.astype(jnp.bfloat16), "ctx", scatter_dimension=1, tiled=True
        ).astype(jnp.float32),
        lax.psum_scatter(
            value_terms.astype(jnp.bfloat16), "ctx", scatter_dimension=1, tiled=True
        ).astype(jnp.float32),
    )
    d_query_rel, rows_grad_part, cols_grad_part = rel_pull((grad_rows, grad_cols))
    d_query = (scale_factor * from_heads(grad_query) + d_query_rel).astype(jnp.bfloat16)
    d_keys = grad_keys.astype(jnp.bfloat16)
    d_values = grad_values.astype(jnp.bfloat16)
    d_projected = jnp.stack((d_query, d_keys, d_values), axis=2)
    qkv_grad = jnp.einsum(
        "itd,itse->sde", normed1_full, d_projected, preferred_element_type=jnp.float32
    )
    qv_bias_part = jnp.stack(
        (
            jnp.sum(d_query.astype(jnp.float32), (0, 1)),
            jnp.sum(d_values.astype(jnp.float32), (0, 1)),
        )
    )
    d_norm1_part = jnp.einsum(
        "itse,sde->itd", d_projected, qkv_full, preferred_element_type=jnp.float32
    )
    d_norm1 = lax.psum_scatter(
        d_norm1_part.astype(jnp.bfloat16), "tp", scatter_dimension=1, tiled=True
    ).astype(jnp.float32)
    unused_in, norm1_pull = jax.vjp(layer_norm, resid_in, norm1_gain, norm1_bias)
    d_in_part, gain1_part, bias1_part = norm1_pull(d_norm1)
    tokens_grad = (d_middle + d_in_part).astype(jnp.bfloat16)
    qkv_out, proj_out, fc1_out, fc2_out = (
        lax.psum_scatter(
            qkv_grad.astype(jnp.bfloat16), ("shard", "ctx"), scatter_dimension=1, tiled=True
        ).astype(jnp.float32),
        lax.psum_scatter(
            proj_grad.astype(jnp.bfloat16), ("shard", "ctx"), scatter_dimension=1, tiled=True
        ).astype(jnp.float32),
        lax.psum_scatter(
            fc1_grad.astype(jnp.bfloat16), ("shard", "ctx"), scatter_dimension=0, tiled=True
        ).astype(jnp.float32),
        lax.psum_scatter(
            fc2_grad.astype(jnp.bfloat16), ("shard", "ctx"), scatter_dimension=1, tiled=True
        ).astype(jnp.float32),
    )
    qv_placed = lax.dynamic_update_slice_in_dim(
        jnp.zeros((2, D), jnp.float32), qv_bias_part, tp_rank * width_local, 1
    )
    fc1_placed = lax.dynamic_update_slice_in_dim(
        jnp.zeros((FF,), jnp.float32), fc1_bias_part, tp_rank * ff_local, 0
    )
    (
        gain1_sum,
        bias1_sum,
        qv_sum,
        rows_sum,
        cols_sum,
        projb_sum,
        gain2_sum,
        bias2_sum,
        fc1b_sum,
        fc2b_sum,
    ) = lax.psum(
        (
            gain1_part,
            bias1_part,
            qv_placed,
            rows_grad_part,
            cols_grad_part,
            proj_bias_part,
            gain2_part,
            bias2_part,
            fc1_placed,
            fc2_bias_part,
        ),
        ("shard", "ctx", "tp"),
    )
    return (
        output,
        tokens_grad,
        gain1_sum,
        bias1_sum,
        qkv_out,
        qv_sum,
        rows_sum,
        cols_sum,
        proj_out,
        projb_sum,
        gain2_sum,
        bias2_sum,
        fc1_out,
        fc1b_sum,
        fc2_out,
        fc2b_sum,
    )


F32 = jnp.float32
BF16 = jnp.bfloat16
NT = (((1,), (1,)), ((), ()))
NN = (((1,), (0,)), ((), ()))
TN = (((0,), (0,)), ((), ()))
VMEM_GRANT = 60 * 2**20
DMA = pltpu.SemaphoreType.DMA
ANY = pl.BlockSpec(memory_space=pl.ANY)
VM = pl.BlockSpec(memory_space=pltpu.VMEM)


def mm(left, right, dims=NN):
    return lax.dot_general(left, right, dims, preferred_element_type=F32)


def lane_ids(shape):
    return lax.broadcasted_iota(jnp.int32, shape, 1)


def place():
    return lax.axis_index("shard"), lax.axis_index("ctx"), lax.axis_index("tp")


def core_mate(t):
    return t + 1 - 2 * lax.rem(t, 2)


def far_mate(t):
    return lax.rem(t + 2, 4)


def send(src, dst, sems, k, where):
    copy = pltpu.make_async_remote_copy(
        src_ref=src,
        dst_ref=dst,
        send_sem=sems.at[0, k],
        recv_sem=sems.at[1, k],
        device_id=where,
        device_id_type=pl.DeviceIdType.MESH,
    )
    copy.start()
    return copy


def greet(shards):
    s, c, t = place()
    peers = [{"ctx": 1 - c}, {"tp": core_mate(t)}, {"tp": far_mate(t)}]
    peers += [{"shard": lax.rem(s + d, shards)} for d in range(1, shards)]
    barrier = pltpu.get_barrier_semaphore()
    for peer in peers:
        pl.semaphore_signal(barrier, inc=1, device_id=peer, device_id_type=pl.DeviceIdType.MESH)
    pl.semaphore_wait(barrier, len(peers))


class Spread:
    def __init__(self, shards, src, dst, sems, local):
        s, c, _ = place()
        self.shards, self.dst, self.sems = shards, dst, sems
        own = 2 * s + c
        self.local = pltpu.make_async_copy(src, dst.at[own], local)
        self.local.start()
        self.along = [
            send(src, dst.at[own], sems, d, {"shard": lax.rem(s + d, shards)}) for d in range(1, shards)
        ]
        self.across = [send(src, dst.at[own], sems, 0, {"ctx": 1 - c})]

    def forward(self):
        s, c, _ = place()
        for d in range(1, self.shards):
            self.along[d - 1].wait_recv()
            block = self.dst.at[2 * lax.rem(s + self.shards - d, self.shards) + c]
            self.across.append(send(block, block, self.sems, self.shards + d - 1, {"ctx": 1 - c}))

    def finish(self):
        self.local.wait()
        for copy in self.along:
            copy.wait_send()
        for copy in self.across:
            copy.wait()

    @staticmethod
    def scratch(shards):
        return [DMA((2, 2 * shards - 1)), DMA]


class Collect:
    def __init__(self, shards, src, cross, line, sems):
        s, c, _ = place()
        self.shards, self.src, self.cross, self.line, self.sems = shards, src, cross, line, sems
        self.across = []
        for d in range(shards):
            to = lax.rem(s + d + 1, shards)
            self.across.append(send(src.at[2 * to + 1 - c], cross.at[d], sems, d, {"ctx": 1 - c}))

    def forward(self):
        s, c, _ = place()
        self.along = []
        for d in range(self.shards):
            to = lax.rem(s + d + 1, self.shards)
            self.across[d].wait_recv()
            if d < self.shards - 1:
                both = self.src[2 * to + c].astype(F32) + self.cross[d].astype(F32)
                self.cross[d] = both.astype(BF16)
                self.along.append(
                    send(self.cross.at[d], self.line.at[d], self.sems, self.shards + d, {"shard": to})
                )

    def finish(self, out):
        s, c, _ = place()
        for copy in self.across:
            copy.wait_send()
        acc = self.src[2 * s + c].astype(F32) + self.cross[self.shards - 1].astype(F32)
        for d, copy in enumerate(self.along):
            copy.wait()
            acc = acc + self.line[d].astype(F32)
        out[...] = acc

    @staticmethod
    def scratch(shards, block):
        return [
            pltpu.VMEM((shards,) + block, BF16),
            pltpu.VMEM((max(shards - 1, 1),) + block, BF16),
            DMA((2, 2 * shards - 1)),
        ]


class Share:
    def __init__(self, full, sems):
        self.full, self.sems, self.copies = full, sems, {}

    def push(self, k, p, src=None):
        _, _, t = place()
        block = self.full.at[p, t]
        src = block if src is None else src
        self.copies[k] = [
            send(src, block, self.sems, 3 * k, {"tp": far_mate(t)}),
            send(src, block, self.sems, 3 * k + 1, {"tp": core_mate(t)}),
        ]

    def forward(self, k, p):
        _, _, t = place()
        self.copies[k][0].wait_recv()
        block = self.full.at[p, far_mate(t)]
        self.copies[k].append(send(block, block, self.sems, 3 * k + 2, {"tp": core_mate(t)}))

    def finish(self, k):
        first, second, third = self.copies[k]
        first.wait_send()
        second.wait()
        third.wait()


class Gather2:
    def __init__(self, part, mate, far, out, sems):
        self.part, self.mate, self.far, self.out, self.sems = part, mate, far, out, sems
        self.first, self.second = {}, {}

    def push(self, p):
        _, _, t = place()
        m = core_mate(t)
        self.first[p] = [
            send(self.part.at[p, far_mate(m)], self.mate.at[p, 1], self.sems, 3 * p, {"tp": m}),
            send(self.part.at[p, m], self.mate.at[p, 0], self.sems, 3 * p + 1, {"tp": m}),
        ]

    def forward(self, p):
        _, _, t = place()
        self.first[p][0].wait_recv()
        both = self.part[p, far_mate(t)].astype(F32) + self.mate[p, 1].astype(F32)
        self.out[p] = both.astype(BF16)
        self.second[p] = send(self.out.at[p], self.far.at[p], self.sems, 3 * p + 2, {"tp": far_mate(t)})

    def result(self, p):
        _, _, t = place()
        self.first[p][1].wait_recv()
        self.second[p].wait_recv()
        return self.part[p, t].astype(F32) + self.mate[p, 0].astype(F32) + self.far[p].astype(F32)

    def finish(self, p):
        for copy in self.first[p]:
            copy.wait_send()
        self.second[p].wait_send()

    @staticmethod
    def scratch(block):
        return [
            pltpu.VMEM((2, 2) + block, BF16),
            pltpu.VMEM((2,) + block, BF16),
            pltpu.VMEM((2,) + block, BF16),
            DMA((2, 6)),
        ]


def ln_stats(values):
    average = jnp.mean(values, -1, keepdims=True)
    centred = values - average
    inverse = lax.rsqrt(jnp.mean(centred * centred, -1, keepdims=True) + EPSILON)
    return centred * inverse, inverse


def ln_back(unit, inverse, gain, grad):
    scaled = grad * gain
    first = jnp.mean(scaled, -1, keepdims=True)
    second = jnp.mean(scaled * unit, -1, keepdims=True)
    return inverse * (scaled - first - unit * second)


def comm_call(kernel, name, ident, args, outs, scratch, hbm_in=(), hbm_out=()):
    return pl.pallas_call(
        kernel,
        out_shape=tuple(outs),
        in_specs=[ANY if i in hbm_in else VM for i in range(len(args))],
        out_specs=tuple(ANY if i in hbm_out else VM for i in range(len(outs))),
        scratch_shapes=scratch,
        compiler_params=pltpu.CompilerParams(
            vmem_limit_bytes=VMEM_GRANT, collective_id=ident, has_side_effects=True
        ),
        name=name,
    )(*args)


def front_kernel(
    shards, tok_ref, w_ref, gain_ref, bias_ref, x_ref, a_ref, wf_ref, swap_sems, share_sems, w_sems, w_local
):
    s, c, t = place()
    greet(shards)
    swap = send(tok_ref.at[1 - c], x_ref.at[c], swap_sems, 0, {"ctx": 1 - c})
    spread = Spread(shards, w_ref, wf_ref, w_sems, w_local)
    share = Share(a_ref, share_sems)

    def norm(block):
        unit, _ = ln_stats(block.astype(F32))
        return (unit * gain_ref[...] + bias_ref[...]).astype(BF16)

    own = tok_ref[c]
    x_ref[c] = own
    a_ref[c, t] = norm(own)
    share.push(0, c)
    swap.wait()
    a_ref[1 - c, t] = norm(x_ref[1 - c])
    share.push(1, 1 - c)
    share.forward(0, c)
    spread.forward()
    share.forward(1, 1 - c)
    share.finish(0)
    share.finish(1)
    spread.finish()


def fwd_kernel(
    shards, heads, hd, cols, rows, qb,
    qkv_ref, tab_ref, hot_ref, cot_ref, w_ref,
    o_ref, ob_ref, lse_ref, qa_ref, ka_ref, g_ref, cf_ref, wf_ref,
    swap_sems, share_sems, w_sems, w_local,
):
    _, me, t = place()
    greet(shards)
    swap = send(cot_ref.at[1 - me], g_ref.at[me], swap_sems, 0, {"ctx": 1 - me})
    spread = Spread(shards, w_ref, wf_ref, w_sems, w_local)
    share = Share(cf_ref, share_sems)
    own = cot_ref[me]
    g_ref[me] = own
    cf_ref[me, t] = own
    share.push(0, me, cot_ref.at[me])
    tok = qkv_ref.shape[0]
    c = hd**-0.5 * math.log2(math.e)
    up = hd**0.5
    for h in range(heads):
        sl = slice(h * hd, (h + 1) * hd)
        q_sl, k_sl, v_sl = (slice((j * heads + h) * hd, (j * heads + h + 1) * hd) for j in range(3))
        pad = jnp.zeros((tok, 128 - hd), BF16)
        qp = jnp.concatenate([qkv_ref[:, q_sl], pad], 1)
        kp = jnp.concatenate([qkv_ref[:, k_sl], pad], 1)
        vt = jnp.concatenate([qkv_ref[:, v_sl], pad], 1).T
        ka_ref[h, :, 0:128] = jnp.where(lane_ids((tok, 128)) < hd, kp, hot_ref[:, 0:128])
        ka_ref[h, :, 128:256] = hot_ref[:, 128:256]
        terms = mm(qp, tab_ref[...]) * up
        ln = lane_ids((cols, 128))
        for r in range(rows):
            rs = slice(r * cols, (r + 1) * cols)
            tr = pltpu.roll(terms[rs, 0:128], (65 + r) % 128, 1)
            tc = pltpu.roll(terms[rs, 128:256], 65, 1, stride=1, stride_axis=0)
            rh = tr.astype(BF16).astype(F32)
            rl = pltpu.roll(tr - rh, rows, 1)
            ch = tc.astype(BF16).astype(F32)
            cl = pltpu.roll(tc - ch, 64, 1)
            low = jnp.where(ln < hd + 2 * rows, rl, jnp.zeros_like(tr))
            left = jnp.where(ln < hd, qp[rs].astype(F32), jnp.where(ln < hd + rows, rh, low))
            qa_ref[h, rs, 0:128] = left.astype(BF16)
            qa_ref[h, rs, 128:256] = jnp.where(ln < 64, ch, cl).astype(BF16)

        def blk(i, _):
            at = pl.ds(pl.multiple_of(i * qb, qb), qb)
            s = mm(ka_ref[h], qa_ref[h, at, :], NT)
            m = jnp.max(s, 0, keepdims=True)
            p = jnp.exp2((s - m) * c)
            l = jnp.sum(p, 0, keepdims=True)
            o = (mm(vt, p.astype(BF16)) / l).T[:, 0:hd]
            lse_ref[h : h + 1, at] = m * c + jnp.log2(l)
            o_ref[at, sl] = o
            ob_ref[at, sl] = o.astype(BF16)
            return 0

        lax.fori_loop(0, tok // qb, blk, 0)
        if h == 0:
            swap.wait()
            cf_ref[1 - me, t] = g_ref[1 - me]
            share.push(1, 1 - me, g_ref.at[1 - me])
        if h == min(1, heads - 1):
            spread.forward()
        if h == heads - 1:
            share.forward(0, me)
            share.forward(1, 1 - me)
    share.finish(0)
    share.finish(1)
    spread.finish()


def mid_kernel(
    shards, part_ref, x_ref, pb_ref, gain_ref, bias_ref, w_ref, mid_ref, a_ref, wf_ref,
    mate, far, outb, sum_sems, share_sems, w_sems, w_local,
):
    _, _, t = place()
    greet(shards)
    gather = Gather2(part_ref, mate, far, outb, sum_sems)
    gather.push(0)
    gather.push(1)
    spread = Spread(shards, w_ref, wf_ref, w_sems, w_local)
    share = Share(a_ref, share_sems)
    gather.forward(0)
    gather.forward(1)
    for p in range(2):
        mid = x_ref[p].astype(F32) + gather.result(p) + pb_ref[...]
        mid_ref[p] = mid
        unit, _ = ln_stats(mid)
        a_ref[p, t] = (unit * gain_ref[...] + bias_ref[...]).astype(BF16)
        share.push(p, p)
    spread.forward()
    for p in range(2):
        share.forward(p, p)
    for p in range(2):
        gather.finish(p)
        share.finish(p)
    spread.finish()


def turn_kernel(
    shards, part_ref, mid_ref, g_ref, gain_ref, w_ref, dm_ref, db_ref, wg_ref, sums_ref,
    mate, far, outb, sum_sems, share_sems, w_cross, w_line, w_sems,
):
    _, _, t = place()
    greet(shards)
    gather = Gather2(part_ref, mate, far, outb, sum_sems)
    gather.push(0)
    gather.push(1)
    collect = Collect(shards, w_ref, w_cross, w_line, w_sems)
    share = Share(db_ref, share_sems)
    gather.forward(0)
    gather.forward(1)
    rows = [jnp.zeros((1, mid_ref.shape[2]), F32) for _ in range(4)]
    for p in range(2):
        unit, inverse = ln_stats(mid_ref[p])
        g = g_ref[p].astype(F32)
        da = gather.result(p)
        dm = g + ln_back(unit, inverse, gain_ref[...], da)
        dm_ref[p] = dm
        low = dm.astype(BF16)
        db_ref[p, t] = low
        share.push(p, p)
        for k, term in enumerate((da * unit, da, low.astype(F32), g)):
            rows[k] = rows[k] + jnp.sum(term, 0, keepdims=True)
    for k in range(4):
        sums_ref[k : k + 1, :] = rows[k]
    collect.forward()
    for p in range(2):
        share.forward(p, p)
    for p in range(2):
        gather.finish(p)
        share.finish(p)
    collect.finish(wg_ref)


def bwd_kernel(
    shards, heads, hd, cols, rows, qb,
    qa_ref, ka_ref, qkv_ref, do_ref, o_ref, lse_ref, tab_ref, hot_ref, part_ref, mid_ref, fb_ref, w_ref,
    dqkv_ref, rg_ref, out_ref, wg_ref,
    kt_ref, acc_k, acc_v, del_ref, res_ref, mate, far, outb, sum_sems, swap_sems, w_cross, w_line, w_sems,
):
    _, me, _ = place()
    greet(shards)
    gather = Gather2(part_ref, mate, far, outb, sum_sems)
    gather.push(0)
    gather.push(1)
    collect = Collect(shards, w_ref, w_cross, w_line, w_sems)
    gather.forward(0)
    gather.forward(1)
    tok = qkv_ref.shape[0]
    scale = hd**-0.5
    c = scale * math.log2(math.e)
    rg_ref[...] = jnp.zeros_like(rg_ref)
    for h in range(heads):
        sl = slice(h * hd, (h + 1) * hd)
        k_sl, v_sl = (slice((j * heads + h) * hd, (j * heads + h + 1) * hd) for j in (1, 2))
        pad = jnp.zeros((tok, 128 - hd), BF16)
        vp = jnp.concatenate([qkv_ref[:, v_sl], pad], 1)
        kt_ref[0:128, :] = jnp.where(lane_ids((tok, 128)) < hd, ka_ref[h, :, 0:128], hot_ref[:, 0:128]).T
        kt_ref[128:256, :] = hot_ref[:, 128:256].T
        prod = jnp.concatenate([do_ref[:, sl].astype(F32) * o_ref[:, sl], pad.astype(F32)], 1)
        del_ref[...] = lax.dot_general(
            jnp.ones((8, 128), F32), prod, NT, preferred_element_type=F32, precision=PRECISE
        )
        acc_k[...] = jnp.zeros_like(acc_k)
        acc_v[...] = jnp.zeros_like(acc_v)

        def blk(i, _):
            at = pl.ds(pl.multiple_of(i * qb, qb), qb)
            qblk = qa_ref[h, at, :]
            dob = jnp.concatenate([do_ref[at, sl], jnp.zeros((qb, 128 - hd), BF16)], 1)
            s = mm(ka_ref[h], qblk, NT)
            p = jnp.exp2(s * c - lse_ref[h : h + 1, at])
            dp = mm(vp, dob, NT)
            ds = (p * (dp - del_ref[0:1, at])).astype(BF16)
            acc_v[...] += mm(p.astype(BF16), dob)
            acc_k[...] += mm(ds, qblk[:, 0:128])
            dqa = mm(kt_ref[...], ds).T
            ln = lane_ids((cols, 128))
            parts = []
            for j in range(qb // cols):
                r = i * (qb // cols) + j
                js = slice(j * cols, (j + 1) * cols)
                dr = dqa[js, 0:128]
                dr = jnp.where((ln >= hd) & (ln < hd + rows), dr, 0.0)
                dr = pltpu.roll(dr, (48 + r) % 128, 1)
                dc = pltpu.roll(dqa[js, 128:256], 0, 1, stride=1, stride_axis=0)
                parts.append(jnp.concatenate([dr, dc], 1))
            d = jnp.concatenate(parts, 0).astype(BF16)
            rel = mm(d, tab_ref[...])
            rg_ref[...] += mm(d, qblk[:, 0:128], TN)
            dqkv_ref[at, sl] = (scale * dqa[:, 0:128] + rel)[:, 0:hd].astype(BF16)
            return 0

        lax.fori_loop(0, tok // qb, blk, 0)
        dqkv_ref[:, k_sl] = (scale * acc_k[...])[:, 0:hd].astype(BF16)
        dqkv_ref[:, v_sl] = acc_v[...][:, 0:hd].astype(BF16)
        if h == min(1, heads - 1):
            collect.forward()
        if h == min(2, heads - 1):
            for p in range(2):
                total = mid_ref[p] + gather.result(p) + fb_ref[...]
                res_ref[p] = total.astype(BF16)
            swap = send(res_ref.at[1 - me], out_ref.at[me], swap_sems, 0, {"ctx": 1 - me})
            out_ref[me] = res_ref[me]
    for p in range(2):
        gather.finish(p)
    collect.finish(wg_ref)
    swap.wait()


def end_kernel(
    shards, part_ref, x_ref, dm_ref, gain_ref, w_ref, small_ref, out_ref, wg_ref, total_ref,
    res_ref, mate, far, outb, sum_sems, swap_sems, held, got, line, small_sems, w_cross, w_line, w_sems,
):
    s, me, t = place()
    greet(shards)
    gather = Gather2(part_ref, mate, far, outb, sum_sems)
    gather.push(0)
    gather.push(1)
    collect = Collect(shards, w_ref, w_cross, w_line, w_sems)
    gather.forward(0)
    gather.forward(1)
    first = jnp.zeros((1, x_ref.shape[2]), F32)
    second = jnp.zeros((1, x_ref.shape[2]), F32)
    for p in range(2):
        unit, inverse = ln_stats(x_ref[p].astype(F32))
        da = gather.result(p)
        res_ref[p] = (dm_ref[p] + ln_back(unit, inverse, gain_ref[...], da)).astype(BF16)
        first = first + jnp.sum(da * unit, 0, keepdims=True)
        second = second + jnp.sum(da, 0, keepdims=True)
    swap = send(res_ref.at[1 - me], out_ref.at[me], swap_sems, 0, {"ctx": 1 - me})
    out_ref[me] = res_ref[me]
    held[0] = small_ref[...]
    held[0, 0:1, :] = first
    held[0, 1:2, :] = second
    waits = []
    for k, peer in enumerate(({"tp": core_mate(t)}, {"tp": far_mate(t)}, {"ctx": 1 - me})):
        copy = send(held.at[k], got.at[k], small_sems, k, peer)
        copy.wait_recv()
        waits.append(copy)
        held[k + 1] = held[k] + got[k]
    line[s] = held[3]
    for d in range(1, shards):
        waits.append(send(held.at[3], line.at[s], small_sems, 2 + d, {"shard": lax.rem(s + d, shards)}))
    collect.forward()
    for k, copy in enumerate(waits):
        if k < 3:
            copy.wait_send()
        else:
            copy.wait()
    acc = line[0]
    for k in range(1, shards):
        acc = acc + line[k]
    total_ref[...] = acc
    for p in range(2):
        gather.finish(p)
    collect.finish(wg_ref)
    swap.wait()


def position_tables(rel_rows, rel_cols, hd):
    gap = 128 - hd
    rr = jnp.pad(rel_rows, ((0, 128 - rel_rows.shape[0]), (0, gap)))
    rc = jnp.pad(rel_cols, ((0, 128 - rel_cols.shape[0]), (0, gap)))
    fr = jnp.pad(rel_rows[::-1], ((0, 128 - rel_rows.shape[0]), (0, gap)))
    fc = jnp.pad(rel_cols[::-1], ((0, 128 - rel_cols.shape[0]), (0, gap)))
    return jnp.concatenate([fr, fc], 0).T, jnp.concatenate([rr, rc], 0)


def position_hots(tok, hd, cols, rows):
    t = lax.broadcasted_iota(jnp.int32, (tok, 256), 0)
    l = lax.broadcasted_iota(jnp.int32, (tok, 256), 1)
    kr = t // cols
    kw = t % cols
    first = (l == hd + kr) | (l == hd + rows + kr) | (l == 128 + kw) | (l == 192 + kw)
    second = (l == hd + rows - 1 - kr) | (l == 128 + cols - 1 - kw)
    return first.astype(BF16), second.astype(BF16)


def on_device_images(
    tokens, norm1_gain, norm1_bias, qkv_weight, qv_bias, rel_rows, rel_cols, proj_weight, proj_bias,
    norm2_gain, norm2_bias, fc1_weight, fc1_bias, fc2_weight, fc2_bias, cotangent,
):
    S = jax.ShapeDtypeStruct
    shards = lax.axis_size("shard")
    tp_count = lax.axis_size("tp")
    tp_rank = lax.axis_index("tp")
    heads = H // tp_count
    width = heads * HD
    ff = FF // tp_count
    rows = (rel_rows.shape[0] + 1) // 2
    tok = rows * COLS
    own = tokens.shape
    piece = own[1:]
    full = (2, tp_count) + piece
    block = fc1_weight.shape
    blocks = (2 * shards,) + block
    qkv_cols = 3 * width
    w1 = jnp.concatenate([qkv_weight[0], qkv_weight[1], qkv_weight[2], proj_weight.T], 1)
    fc2_t = fc2_weight.T
    qv_local = lax.dynamic_slice_in_dim(qv_bias, tp_rank * width, width, 1)
    qkv_bias = jnp.concatenate([qv_local[0], jnp.zeros((width,), F32), qv_local[1]])
    fc1_local = lax.dynamic_slice_in_dim(fc1_bias, tp_rank * ff, ff, 0)
    tab_f, tab_b = position_tables(rel_rows, rel_cols, HD)
    hot_f, hot_b = position_hots(tok, HD, COLS, rows)
    spread = Spread.scratch(shards)
    collect = Collect.scratch(shards, block)
    gather = Gather2.scratch(piece)
    swap = [DMA((2, 1))]
    share = [DMA((2, 6))]

    def row(vec):
        return vec.reshape(1, -1)

    x, a1, w1_full = comm_call(
        partial(front_kernel, shards), "front", 0,
        (tokens, w1, row(norm1_gain), row(norm1_bias)),
        (S(own, BF16), S(full, BF16), S(blocks, BF16)),
        swap + share + spread, hbm_in=(1,), hbm_out=(2,),
    )
    a1 = a1.reshape(tok, D)
    w1_full = w1_full.reshape(D, -1)
    qkv_full = w1_full[:, :qkv_cols]
    proj_full = w1_full[:, qkv_cols:]
    qkv = (mm(a1, qkv_full) + qkv_bias).astype(BF16)
    o, o_low, lse, qa, ka, g, cot, fc1_full = comm_call(
        partial(fwd_kernel, shards, heads, HD, COLS, rows, 256), "attn_fwd", 1,
        (qkv, tab_f, hot_f, cotangent, fc1_weight),
        (
            S((tok, width), F32), S((tok, width), BF16), S((heads, tok), F32),
            S((heads, tok, 256), BF16), S((heads, tok, 256), BF16),
            S(own, BF16), S(full, BF16), S(blocks, BF16),
        ),
        swap + share + spread, hbm_in=(4,), hbm_out=(7,),
    )
    fc1_full = fc1_full.reshape(D, ff)
    cot = cot.reshape(tok, D)
    proj_part = mm(o_low, proj_full, NT).astype(BF16).reshape(full)
    mid, a2, fc2_full = comm_call(
        partial(mid_kernel, shards), "mid", 2,
        (proj_part, x, row(proj_bias), row(norm2_gain), row(norm2_bias), fc2_t),
        (S(own, F32), S(full, BF16), S(blocks, BF16)),
        gather + share + spread, hbm_in=(5,), hbm_out=(2,),
    )
    a2 = a2.reshape(tok, D)
    fc2_full = fc2_full.reshape(D, ff)
    pre = mm(a2, fc1_full) + fc1_local
    cdf = 0.5 * (1.0 + lax.erf(pre * (2.0**-0.5)))
    act = (pre * cdf).astype(BF16)
    slope = cdf + pre * jnp.exp(-0.5 * pre * pre) * ((2.0 * math.pi) ** -0.5)
    d_pre = (mm(cot, fc2_full) * slope).astype(BF16)
    d_a2 = mm(d_pre, fc1_full, NT).astype(BF16).reshape(full)
    fc2_grad = mm(cot, act, TN).astype(BF16).reshape(blocks)
    d_mid, d_branch, fc2_own, sums = comm_call(
        partial(turn_kernel, shards), "turn", 3,
        (d_a2, mid, g, row(norm2_gain), fc2_grad),
        (S(own, F32), S(full, BF16), S(block, F32), S((4, D), F32)),
        gather + share + collect,
    )
    fc1_grad = mm(a2, d_pre, TN).astype(BF16).reshape(blocks)
    mlp_part = mm(act, fc2_full, NT).astype(BF16).reshape(full)
    d_branch = d_branch.reshape(tok, D)
    d_o = mm(d_branch, proj_full).astype(BF16)
    dqkv, rel_grad, output, fc1_own = comm_call(
        partial(bwd_kernel, shards, heads, HD, COLS, rows, 256), "attn_bwd", 4,
        (qa, ka, qkv, d_o, o, lse, tab_b, hot_b, mlp_part, mid, row(fc2_bias), fc1_grad),
        (S((tok, qkv_cols), BF16), S((256, 128), F32), S(own, BF16), S(block, F32)),
        [
            pltpu.VMEM((256, tok), BF16), pltpu.VMEM((tok, 128), F32), pltpu.VMEM((tok, 128), F32),
            pltpu.VMEM((8, tok), F32), pltpu.VMEM(own, BF16),
        ] + gather + swap + collect,
    )
    d_a1 = mm(dqkv, qkv_full, NT).astype(BF16).reshape(full)
    w1_grad = jnp.concatenate([mm(a1, dqkv, TN), mm(d_branch, o_low, TN)], 1).astype(BF16).reshape(blocks)
    qkv_sum = jnp.sum(dqkv.astype(F32), 0)
    qv_part = jnp.stack([qkv_sum[:width], qkv_sum[2 * width :]])
    qv_placed = lax.dynamic_update_slice_in_dim(jnp.zeros((2, D), F32), qv_part, tp_rank * width, 1)
    fc1_sum = jnp.sum(d_pre.astype(F32), 0)
    fc1_placed = lax.dynamic_update_slice_in_dim(jnp.zeros((FF,), F32), fc1_sum, tp_rank * ff, 0)
    terms = (
        jnp.zeros((2 * D,), F32),
        qv_placed.reshape(-1),
        fc1_placed,
        sums.reshape(-1),
        rel_grad[: rel_rows.shape[0], :HD].reshape(-1),
        rel_grad[128 : 128 + rel_cols.shape[0], :HD].reshape(-1),
    )
    count = sum(term.shape[0] for term in terms)
    lines = -(-count // (8 * D)) * 8
    packed = jnp.concatenate(terms + (jnp.zeros((lines * D - count,), F32),)).reshape(lines, D)
    tokens_grad, w1_own, total = comm_call(
        partial(end_kernel, shards), "end", 5,
        (d_a1, x, d_mid, row(norm1_gain), w1_grad, packed),
        (S(own, BF16), S(block, F32), S((lines, D), F32)),
        [pltpu.VMEM(own, BF16)] + gather + swap
        + [
            pltpu.VMEM((4, lines, D), F32), pltpu.VMEM((3, lines, D), F32),
            pltpu.VMEM((shards, lines, D), F32), DMA((2, 2 + shards)),
        ]
        + collect,
    )
    flat = total.reshape(-1)
    base = 4 * D + FF
    rel_at = base + 4 * D
    rel_mid = rel_at + rel_rows.size
    return (
        output,
        tokens_grad,
        total[0],
        total[1],
        jnp.stack([w1_own[:, j * width : (j + 1) * width] for j in range(3)]),
        total[2:4],
        flat[rel_at:rel_mid].reshape(rel_rows.shape),
        flat[rel_mid : rel_mid + rel_cols.size].reshape(rel_cols.shape),
        w1_own[:, qkv_cols:].T,
        flat[base + 2 * D : base + 3 * D],
        flat[base : base + D],
        flat[base + D : base + 2 * D],
        fc1_own,
        flat[4 * D : base],
        fc2_own.T,
        flat[base + 3 * D : base + 4 * D],
    )


def solution(mesh):
    in_specs = (
        P("shard", ("ctx", "tp"), None),
        P(),
        P(),
        P(None, ("shard", "ctx"), "tp"),
        P(),
        P(),
        P(),
        P("tp", ("shard", "ctx")),
        P(),
        P(),
        P(),
        P(("shard", "ctx"), "tp"),
        P(),
        P("tp", ("shard", "ctx")),
        P(),
        P("shard", ("ctx", "tp"), None),
    )
    out_specs = (
        P("shard", ("ctx", "tp"), None),
        P("shard", ("ctx", "tp"), None),
        P(),
        P(),
        P(None, ("shard", "ctx"), "tp"),
        P(),
        P(),
        P(),
        P("tp", ("shard", "ctx")),
        P(),
        P(),
        P(),
        P(("shard", "ctx"), "tp"),
        P(),
        P("tp", ("shard", "ctx")),
        P(),
    )
    def on_device(*arrays):
        rows = (arrays[5].shape[0] + 1) // 2
        fits = mesh.shape["tp"] == 4 and mesh.shape["ctx"] == 2 and HD + 2 * rows <= 128
        fits = fits and arrays[0].shape[0] == mesh.shape["ctx"] and arrays[6].shape[0] <= 128
        return (on_device_images if fits else on_device_rows)(*arrays)

    return jax.shard_map(
        on_device, mesh=mesh, in_specs=in_specs, out_specs=out_specs, check_vma=False
    )
```

```python
from functools import partial
import math

import jax
import jax.numpy as jnp
from jax import lax
from jax.experimental import pallas as pl
from jax.experimental.pallas import tpu as pltpu
from jax.sharding import PartitionSpec as P

D = 1280
H = 16
HD = 80
FF = 5120
COLS = 64
ROWS_DEV = 8


PRECISE = lax.Precision.HIGHEST
EPSILON = 1e-06
NEGATIVE = -1e30


def layer_norm(values_in, gain_vec, shift_vec):
    average = jnp.mean(values_in, -1, keepdims=True)
    centred = values_in - average
    variance = jnp.mean(centred * centred, -1, keepdims=True)
    return centred * lax.rsqrt(variance + EPSILON) * gain_vec + shift_vec


def block_size():
    return 512


def to_heads(flat_rows, heads_local):
    images, length, feat_width = flat_rows.shape
    return flat_rows.reshape(images, length, heads_local, feat_width // heads_local).transpose(
        0, 2, 1, 3
    )


def from_heads(per_head):
    images, heads_local, length, head_dim = per_head.shape
    return per_head.transpose(0, 2, 1, 3).reshape(images, length, heads_local * head_dim)


def block_scores(query_heads, key_flat, rows_bias, cols_bias, first_key, scale_factor):
    key_heads = to_heads(key_flat, query_heads.shape[1])
    key_len = key_flat.shape[1]
    key_rows = key_len // COLS
    scores = scale_factor * jnp.einsum(
        "ihqc,ihkc->ihqk", query_heads, key_heads, preferred_element_type=jnp.float32
    )
    images, heads_local, query_len, unused_len = scores.shape
    row_part = lax.dynamic_slice_in_dim(rows_bias, first_key // COLS, key_rows, 3)
    scores = scores.reshape(images, heads_local, query_len, key_rows, COLS)
    scores = scores + row_part[..., :, None] + cols_bias[..., None, :]
    return scores.reshape(images, heads_local, query_len, key_len)


def relative_terms(query_flat, rows_param, cols_param, first_row, heads_local):
    images, length, feat_width = query_flat.shape
    rows_dev = length // COLS
    grid_rows = (rows_param.shape[0] + 1) // 2
    own_rows = first_row + jnp.arange(rows_dev, dtype=jnp.int32)
    key_rows = jnp.arange(grid_rows, dtype=jnp.int32)
    row_slots = jnp.arange(rows_param.shape[0], dtype=jnp.int32)
    pick_rows = (
        row_slots[None, None, :]
        == own_rows[:, None, None] - key_rows[None, :, None] + grid_rows - 1
    ).astype(jnp.float32)
    table_rows = jnp.einsum("rkj,jc->rkc", pick_rows, rows_param, precision=PRECISE)
    col_ids = jnp.arange(COLS, dtype=jnp.int32)
    col_slots = jnp.arange(cols_param.shape[0], dtype=jnp.int32)
    pick_cols = (
        col_slots[None, None, :] == col_ids[:, None, None] - col_ids[None, :, None] + COLS - 1
    ).astype(jnp.float32)
    table_cols = jnp.einsum("wkj,jc->wkc", pick_cols, cols_param, precision=PRECISE)
    grid_form = query_flat.reshape(images, rows_dev, COLS, heads_local, feat_width // heads_local)
    along_rows = jnp.einsum("irwhc,rkc->ihrwk", grid_form, table_rows, precision=PRECISE).reshape(
        images, heads_local, length, grid_rows
    )
    along_cols = jnp.einsum("irwhc,wkc->ihrwk", grid_form, table_cols, precision=PRECISE).reshape(
        images, heads_local, length, COLS
    )
    return (along_rows, along_cols)


def on_device_rows(
    tokens,
    norm1_gain,
    norm1_bias,
    qkv_weight,
    qv_bias,
    rel_rows,
    rel_cols,
    proj_weight,
    proj_bias,
    norm2_gain,
    norm2_bias,
    fc1_weight,
    fc1_bias,
    fc2_weight,
    fc2_bias,
    cotangent,
):
    scale_factor = HD ** (-0.5)
    tp_count = lax.axis_size("tp")
    ctx_count = lax.axis_size("ctx")
    tp_rank = lax.axis_index("tp")
    ctx_rank = lax.axis_index("ctx")
    grid_rows = ROWS_DEV * ctx_count
    tok_image = grid_rows * COLS
    tok_ctx = ROWS_DEV * COLS
    heads_local = H // tp_count
    width_local = heads_local * HD
    ff_local = FF // tp_count
    images = tokens.shape[0]
    rows_table = rel_rows.astype(jnp.float32)
    cols_table = rel_cols.astype(jnp.float32)
    qkv_full, proj_full, fc1_full, fc2_full = (
        lax.all_gather(qkv_weight, ("shard", "ctx"), axis=1, tiled=True),
        lax.all_gather(proj_weight, ("shard", "ctx"), axis=1, tiled=True),
        lax.all_gather(fc1_weight, ("shard", "ctx"), axis=0, tiled=True),
        lax.all_gather(fc2_weight, ("shard", "ctx"), axis=1, tiled=True),
    )
    qv_local = lax.dynamic_slice_in_dim(qv_bias, tp_rank * width_local, width_local, 1)
    fc1_local = lax.dynamic_slice_in_dim(fc1_bias, tp_rank * ff_local, ff_local, 0)
    resid_in = tokens.astype(jnp.float32)
    normed1 = layer_norm(resid_in, norm1_gain, norm1_bias).astype(jnp.bfloat16)
    normed1_full = lax.all_gather(normed1, "tp", axis=1, tiled=True)
    projected = jnp.einsum(
        "itd,sde->itse", normed1_full, qkv_full, preferred_element_type=jnp.float32
    )
    queries = (projected[:, :, 0] + qv_local[0]).astype(jnp.bfloat16)
    keys_own = projected[:, :, 1].astype(jnp.bfloat16)
    values_own = (projected[:, :, 2] + qv_local[1]).astype(jnp.bfloat16)
    first_row = ctx_rank * ROWS_DEV
    rel_fn = partial(relative_terms, first_row=first_row, heads_local=heads_local)
    (along_rows, along_cols), rel_pull = jax.vjp(
        rel_fn, queries.astype(jnp.float32), rows_table, cols_table
    )
    query_heads = to_heads(queries, heads_local)
    start_state = (
        jnp.full((images, heads_local, tok_ctx), NEGATIVE, jnp.float32),
        jnp.zeros((images, heads_local, tok_ctx), jnp.float32),
        jnp.zeros((images, heads_local, tok_ctx, HD), jnp.float32),
        jnp.zeros((images, tok_image, width_local), jnp.bfloat16),
        jnp.zeros((images, tok_image, width_local), jnp.bfloat16),
    )
    shard_piece = (
        lax.all_gather(keys_own, "ctx", axis=1, tiled=True),
        lax.all_gather(values_own, "ctx", axis=1, tiled=True),
    )
    piece_len = shard_piece[0].shape[1]
    step_len = block_size()

    def one_step(inner, offset):
        run_max, run_sum, run_acc, keys_all, values_all = inner
        key_blk = lax.dynamic_slice_in_dim(shard_piece[0], offset, step_len, 1)
        value_blk = lax.dynamic_slice_in_dim(shard_piece[1], offset, step_len, 1)
        scores = block_scores(query_heads, key_blk, along_rows, along_cols, offset, scale_factor)
        new_max = jnp.maximum(run_max, jnp.max(scores, -1))
        factor = jnp.exp(run_max - new_max)
        weights_blk = jnp.exp(scores - new_max[..., None])
        run_sum = run_sum * factor + jnp.sum(weights_blk, -1)
        value_heads = to_heads(value_blk, heads_local)
        run_acc = run_acc * factor[..., None] + jnp.einsum(
            "ihqk,ihkc->ihqc",
            weights_blk.astype(jnp.bfloat16),
            value_heads,
            preferred_element_type=jnp.float32,
        )
        keys_all = lax.dynamic_update_slice_in_dim(keys_all, key_blk, offset, 1)
        values_all = lax.dynamic_update_slice_in_dim(values_all, value_blk, offset, 1)
        return ((new_max, run_sum, run_acc, keys_all, values_all), None)

    offsets = jnp.arange(piece_len // step_len, dtype=jnp.int32) * step_len
    result, unused = lax.scan(one_step, start_state, offsets)
    run_max, run_sum, run_acc, keys_all, values_all = result
    attn_heads = run_acc / run_sum[..., None]
    log_total = run_max + jnp.log(run_sum)
    attn_low = from_heads(attn_heads).astype(jnp.bfloat16)
    proj_part = jnp.einsum("itd,de->ite", attn_low, proj_full, preferred_element_type=jnp.float32)
    branch = lax.psum_scatter(
        proj_part.astype(jnp.bfloat16), "tp", scatter_dimension=1, tiled=True
    ).astype(jnp.float32)
    middle = resid_in + branch + proj_bias
    normed2 = layer_norm(middle, norm2_gain, norm2_bias).astype(jnp.bfloat16)
    normed2_full = lax.all_gather(normed2, "tp", axis=1, tiled=True)
    hidden_pre = (
        jnp.einsum("itd,df->itf", normed2_full, fc1_full, preferred_element_type=jnp.float32)
        + fc1_local
    )
    gelu_exact = partial(jax.nn.gelu, approximate=False)
    activated_f, gelu_pull = jax.vjp(gelu_exact, hidden_pre)
    activated = activated_f.astype(jnp.bfloat16)
    mlp_part = jnp.einsum("itf,fe->ite", activated, fc2_full, preferred_element_type=jnp.float32)
    mlp_out = lax.psum_scatter(
        mlp_part.astype(jnp.bfloat16), "tp", scatter_dimension=1, tiled=True
    ).astype(jnp.float32)
    output = (middle + mlp_out + fc2_bias).astype(jnp.bfloat16)
    cot_full = lax.all_gather(cotangent, "tp", axis=1, tiled=True)
    d_act = jnp.einsum("ite,fe->itf", cot_full, fc2_full, preferred_element_type=jnp.float32)
    d_hidden = gelu_pull(d_act)[0].astype(jnp.bfloat16)
    fc2_grad = jnp.einsum("itf,ite->fe", activated, cot_full, preferred_element_type=jnp.float32)
    fc1_grad = jnp.einsum("itd,itf->df", normed2_full, d_hidden, preferred_element_type=jnp.float32)
    fc1_bias_part = jnp.sum(d_hidden.astype(jnp.float32), (0, 1))
    fc2_bias_part = jnp.sum(cotangent.astype(jnp.float32), (0, 1))
    d_norm2_part = jnp.einsum("itf,df->itd", d_hidden, fc1_full, preferred_element_type=jnp.float32)
    d_norm2 = lax.psum_scatter(
        d_norm2_part.astype(jnp.bfloat16), "tp", scatter_dimension=1, tiled=True
    ).astype(jnp.float32)
    unused_out, norm2_pull = jax.vjp(layer_norm, middle, norm2_gain, norm2_bias)
    d_mid_part, gain2_part, bias2_part = norm2_pull(d_norm2)
    d_middle = cotangent.astype(jnp.float32) + d_mid_part
    d_branch = d_middle.astype(jnp.bfloat16)
    proj_bias_part = jnp.sum(d_branch.astype(jnp.float32), (0, 1))
    d_branch_full = lax.all_gather(d_branch, "tp", axis=1, tiled=True)
    proj_grad = jnp.einsum(
        "itd,ite->de", attn_low, d_branch_full, preferred_element_type=jnp.float32
    )
    d_attn = jnp.einsum(
        "ite,de->itd", d_branch_full, proj_full, preferred_element_type=jnp.float32
    ).astype(jnp.bfloat16)
    d_attn_heads = to_heads(d_attn, heads_local)
    delta_rows = jnp.sum(d_attn_heads.astype(jnp.float32) * attn_heads, -1)
    key_step = block_size()
    key_rows = key_step // COLS
    key_offsets = jnp.arange(tok_image // key_step, dtype=jnp.int32) * key_step

    def back_step(carried, offset):
        grad_query, grad_rows, grad_cols = carried
        key_blk = lax.dynamic_slice_in_dim(keys_all, offset, key_step, 1)
        value_blk = lax.dynamic_slice_in_dim(values_all, offset, key_step, 1)
        scores = block_scores(query_heads, key_blk, along_rows, along_cols, offset, scale_factor)
        soft_probs = jnp.exp(scores - log_total[..., None])
        value_heads = to_heads(value_blk, heads_local)
        key_heads = to_heads(key_blk, heads_local)
        d_probs = jnp.einsum(
            "ihqc,ihkc->ihqk", d_attn_heads, value_heads, preferred_element_type=jnp.float32
        )
        d_scores = (soft_probs * (d_probs - delta_rows[..., None])).astype(jnp.bfloat16)
        grad_query = grad_query + jnp.einsum(
            "ihqk,ihkc->ihqc", d_scores, key_heads, preferred_element_type=jnp.float32
        )
        grid_scores = d_scores.astype(jnp.float32).reshape(
            images, heads_local, tok_ctx, key_rows, COLS
        )
        row_sums = jnp.sum(grid_scores, 4)
        row_now = lax.dynamic_slice_in_dim(grad_rows, offset // COLS, key_rows, 3)
        grad_rows = lax.dynamic_update_slice_in_dim(
            grad_rows, row_now + row_sums, offset // COLS, 3
        )
        grad_cols = grad_cols + jnp.sum(grid_scores, 3)
        key_part = scale_factor * jnp.einsum(
            "ihqk,ihqc->ikhc", d_scores, query_heads, preferred_element_type=jnp.float32
        )
        value_part = jnp.einsum(
            "ihqk,ihqc->ikhc",
            soft_probs.astype(jnp.bfloat16),
            d_attn_heads,
            preferred_element_type=jnp.float32,
        )
        emitted = (
            key_part.reshape(images, key_step, width_local),
            value_part.reshape(images, key_step, width_local),
        )
        return ((grad_query, grad_rows, grad_cols), emitted)

    back_start = (
        jnp.zeros((images, heads_local, tok_ctx, HD), jnp.float32),
        jnp.zeros((images, heads_local, tok_ctx, grid_rows), jnp.float32),
        jnp.zeros((images, heads_local, tok_ctx, COLS), jnp.float32),
    )
    (grad_query, grad_rows, grad_cols), emitted = lax.scan(back_step, back_start, key_offsets)
    key_terms = emitted[0].transpose(1, 0, 2, 3).reshape(images, tok_image, width_local)
    value_terms = emitted[1].transpose(1, 0, 2, 3).reshape(images, tok_image, width_local)
    grad_keys, grad_values = (
        lax.psum_scatter(
            key_terms.astype(jnp.bfloat16), "ctx", scatter_dimension=1, tiled=True
        ).astype(jnp.float32),
        lax.psum_scatter(
            value_terms.astype(jnp.bfloat16), "ctx", scatter_dimension=1, tiled=True
        ).astype(jnp.float32),
    )
    d_query_rel, rows_grad_part, cols_grad_part = rel_pull((grad_rows, grad_cols))
    d_query = (scale_factor * from_heads(grad_query) + d_query_rel).astype(jnp.bfloat16)
    d_keys = grad_keys.astype(jnp.bfloat16)
    d_values = grad_values.astype(jnp.bfloat16)
    d_projected = jnp.stack((d_query, d_keys, d_values), axis=2)
    qkv_grad = jnp.einsum(
        "itd,itse->sde", normed1_full, d_projected, preferred_element_type=jnp.float32
    )
    qv_bias_part = jnp.stack(
        (
            jnp.sum(d_query.astype(jnp.float32), (0, 1)),
            jnp.sum(d_values.astype(jnp.float32), (0, 1)),
        )
    )
    d_norm1_part = jnp.einsum(
        "itse,sde->itd", d_projected, qkv_full, preferred_element_type=jnp.float32
    )
    d_norm1 = lax.psum_scatter(
        d_norm1_part.astype(jnp.bfloat16), "tp", scatter_dimension=1, tiled=True
    ).astype(jnp.float32)
    unused_in, norm1_pull = jax.vjp(layer_norm, resid_in, norm1_gain, norm1_bias)
    d_in_part, gain1_part, bias1_part = norm1_pull(d_norm1)
    tokens_grad = (d_middle + d_in_part).astype(jnp.bfloat16)
    qkv_out, proj_out, fc1_out, fc2_out = (
        lax.psum_scatter(
            qkv_grad.astype(jnp.bfloat16), ("shard", "ctx"), scatter_dimension=1, tiled=True
        ).astype(jnp.float32),
        lax.psum_scatter(
            proj_grad.astype(jnp.bfloat16), ("shard", "ctx"), scatter_dimension=1, tiled=True
        ).astype(jnp.float32),
        lax.psum_scatter(
            fc1_grad.astype(jnp.bfloat16), ("shard", "ctx"), scatter_dimension=0, tiled=True
        ).astype(jnp.float32),
        lax.psum_scatter(
            fc2_grad.astype(jnp.bfloat16), ("shard", "ctx"), scatter_dimension=1, tiled=True
        ).astype(jnp.float32),
    )
    qv_placed = lax.dynamic_update_slice_in_dim(
        jnp.zeros((2, D), jnp.float32), qv_bias_part, tp_rank * width_local, 1
    )
    fc1_placed = lax.dynamic_update_slice_in_dim(
        jnp.zeros((FF,), jnp.float32), fc1_bias_part, tp_rank * ff_local, 0
    )
    (
        gain1_sum,
        bias1_sum,
        qv_sum,
        rows_sum,
        cols_sum,
        projb_sum,
        gain2_sum,
        bias2_sum,
        fc1b_sum,
        fc2b_sum,
    ) = lax.psum(
        (
            gain1_part,
            bias1_part,
            qv_placed,
            rows_grad_part,
            cols_grad_part,
            proj_bias_part,
            gain2_part,
            bias2_part,
            fc1_placed,
            fc2_bias_part,
        ),
        ("shard", "ctx", "tp"),
    )
    return (
        output,
        tokens_grad,
        gain1_sum,
        bias1_sum,
        qkv_out,
        qv_sum,
        rows_sum,
        cols_sum,
        proj_out,
        projb_sum,
        gain2_sum,
        bias2_sum,
        fc1_out,
        fc1b_sum,
        fc2_out,
        fc2b_sum,
    )


F32 = jnp.float32
BF16 = jnp.bfloat16
NT = (((1,), (1,)), ((), ()))
NN = (((1,), (0,)), ((), ()))
TN = (((0,), (0,)), ((), ()))
VMEM_GRANT = 60 * 2**20
DMA = pltpu.SemaphoreType.DMA
ANY = pl.BlockSpec(memory_space=pl.ANY)
VM = pl.BlockSpec(memory_space=pltpu.VMEM)


def mm(left, right, dims=NN):
    return lax.dot_general(left, right, dims, preferred_element_type=F32)


def lane_ids(shape):
    return lax.broadcasted_iota(jnp.int32, shape, 1)


def place():
    return lax.axis_index("shard"), lax.axis_index("ctx"), lax.axis_index("tp")


def core_mate(t):
    return t + 1 - 2 * lax.rem(t, 2)


def far_mate(t):
    return lax.rem(t + 2, 4)


def send(src, dst, sems, k, where):
    copy = pltpu.make_async_remote_copy(
        src_ref=src,
        dst_ref=dst,
        send_sem=sems.at[0, k],
        recv_sem=sems.at[1, k],
        device_id=where,
        device_id_type=pl.DeviceIdType.MESH,
    )
    copy.start()
    return copy


def greet(shards):
    s, c, t = place()
    peers = [{"ctx": 1 - c}, {"tp": core_mate(t)}, {"tp": far_mate(t)}]
    peers += [{"shard": lax.rem(s + d, shards)} for d in range(1, shards)]
    barrier = pltpu.get_barrier_semaphore()
    for peer in peers:
        pl.semaphore_signal(barrier, inc=1, device_id=peer, device_id_type=pl.DeviceIdType.MESH)
    pl.semaphore_wait(barrier, len(peers))


def pieces_of(rows):
    return 5 if rows % 80 == 0 else 1


class Spread:
    def __init__(self, shards, src, dst, sems, local):
        s, c, _ = place()
        self.shards, self.dst, self.sems = shards, dst, sems
        self.pieces = pieces_of(src.shape[0])
        self.rows = src.shape[0] // self.pieces
        own = 2 * s + c
        self.local = pltpu.make_async_copy(src, dst.at[own], local)
        self.local.start()
        self.along, self.across = {}, []
        for k in range(self.pieces):
            here, there = src.at[self.span(k)], dst.at[own, self.span(k)]
            for d in range(1, shards):
                self.along[d, k] = send(here, there, sems, self.slot(d, k), {"shard": lax.rem(s + d, shards)})
            self.across.append(send(here, there, sems, self.slot(0, k), {"ctx": 1 - c}))

    def span(self, k):
        return pl.ds(k * self.rows, self.rows)

    def slot(self, d, k):
        return d * self.pieces + k

    def step(self, k):
        s, c, _ = place()
        for d in range(1, self.shards):
            self.along[d, k].wait_recv()
            block = self.dst.at[2 * lax.rem(s + self.shards - d, self.shards) + c, self.span(k)]
            slot = self.slot(self.shards + d - 1, k)
            self.across.append(send(block, block, self.sems, slot, {"ctx": 1 - c}))

    def finish(self):
        self.local.wait()
        for copy in self.along.values():
            copy.wait_send()
        for copy in self.across:
            copy.wait()

    @staticmethod
    def scratch(shards, block):
        return [DMA((2, (2 * shards - 1) * pieces_of(block[0]))), DMA]


class Collect:
    def __init__(self, shards, src, cross, line, sems):
        self.shards, self.src, self.cross, self.line, self.sems = shards, src, cross, line, sems
        self.block = cross.shape[1]
        self.pieces = pieces_of(self.block)
        self.rows = self.block // self.pieces
        self.across, self.along = {}, {}
        for k in range(min(2, self.pieces)):
            self.push(k)

    def span(self, k):
        return pl.ds(k * self.rows, self.rows)

    def part(self, owner, k):
        return pl.ds(pl.multiple_of(owner * self.block + k * self.rows, self.rows), self.rows)

    def target(self, d):
        s, _, _ = place()
        return lax.rem(s + d + 1, self.shards)

    def push(self, k):
        _, c, _ = place()
        for d in range(self.shards):
            there = self.src.at[self.part(2 * self.target(d) + 1 - c, k)]
            slot = d * self.pieces + k
            self.across[d, k] = send(there, self.cross.at[d, self.span(k)], self.sems, slot, {"ctx": 1 - c})

    def step(self, k):
        _, c, _ = place()
        if k + 2 < self.pieces:
            self.push(k + 2)
        at = self.span(k)
        for d in range(self.shards):
            self.across[d, k].wait_recv()
            if d < self.shards - 1:
                both = self.src[self.part(2 * self.target(d) + c, k)].astype(F32) + self.cross[d, at].astype(F32)
                self.cross[d, at] = both.astype(BF16)
                slot = (self.shards + d) * self.pieces + k
                here, there = self.cross.at[d, at], self.line.at[d, at]
                self.along[d, k] = send(here, there, self.sems, slot, {"shard": self.target(d)})

    def finish(self, out):
        s, c, _ = place()
        for copy in self.across.values():
            copy.wait_send()
        for k in range(self.pieces):
            at = self.span(k)
            acc = self.src[self.part(2 * s + c, k)].astype(F32) + self.cross[self.shards - 1, at].astype(F32)
            for d in range(self.shards - 1):
                self.along[d, k].wait()
                acc = acc + self.line[d, at].astype(F32)
            out[at] = acc

    @staticmethod
    def scratch(shards, block):
        return [
            pltpu.VMEM((shards,) + block, BF16),
            pltpu.VMEM((max(shards - 1, 1),) + block, BF16),
            DMA((2, (2 * shards - 1) * pieces_of(block[0]))),
        ]


class Share:
    def __init__(self, full, sems):
        self.full, self.sems, self.copies = full, sems, {}

    def push(self, k, p, src=None):
        _, _, t = place()
        block = self.full.at[p, t]
        src = block if src is None else src
        self.copies[k] = [
            send(src, block, self.sems, 3 * k, {"tp": far_mate(t)}),
            send(src, block, self.sems, 3 * k + 1, {"tp": core_mate(t)}),
        ]

    def forward(self, k, p):
        _, _, t = place()
        self.copies[k][0].wait_recv()
        block = self.full.at[p, far_mate(t)]
        self.copies[k].append(send(block, block, self.sems, 3 * k + 2, {"tp": core_mate(t)}))

    def finish(self, k):
        first, second, third = self.copies[k]
        first.wait_send()
        second.wait()
        third.wait()


class Gather2:
    def __init__(self, part, mate, far, out, sems):
        self.part, self.mate, self.far, self.out, self.sems = part, mate, far, out, sems
        self.first, self.second = {}, {}

    def push(self, p):
        _, _, t = place()
        m = core_mate(t)
        self.first[p] = [
            send(self.part.at[p, far_mate(m)], self.mate.at[p, 1], self.sems, 3 * p, {"tp": m}),
            send(self.part.at[p, m], self.mate.at[p, 0], self.sems, 3 * p + 1, {"tp": m}),
        ]

    def forward(self, p):
        _, _, t = place()
        self.first[p][0].wait_recv()
        both = self.part[p, far_mate(t)].astype(F32) + self.mate[p, 1].astype(F32)
        self.out[p] = both.astype(BF16)
        self.second[p] = send(self.out.at[p], self.far.at[p], self.sems, 3 * p + 2, {"tp": far_mate(t)})

    def result(self, p):
        _, _, t = place()
        self.first[p][1].wait_recv()
        self.second[p].wait_recv()
        return self.part[p, t].astype(F32) + self.mate[p, 0].astype(F32) + self.far[p].astype(F32)

    def finish(self, p):
        for copy in self.first[p]:
            copy.wait_send()
        self.second[p].wait_send()

    @staticmethod
    def scratch(block):
        return [
            pltpu.VMEM((2, 2) + block, BF16),
            pltpu.VMEM((2,) + block, BF16),
            pltpu.VMEM((2,) + block, BF16),
            DMA((2, 6)),
        ]


def ln_stats(values):
    average = jnp.mean(values, -1, keepdims=True)
    centred = values - average
    inverse = lax.rsqrt(jnp.mean(centred * centred, -1, keepdims=True) + EPSILON)
    return centred * inverse, inverse


def ln_back(unit, inverse, gain, grad):
    scaled = grad * gain
    first = jnp.mean(scaled, -1, keepdims=True)
    second = jnp.mean(scaled * unit, -1, keepdims=True)
    return inverse * (scaled - first - unit * second)


def row_tiles(out_ref, left_ref, right_ref, dims, first, count, tile=256):
    def one(i, _):
        at = pl.ds(pl.multiple_of(i * tile, tile), tile)
        out_ref[at, :] = mm(left_ref[at, :], right_ref[...], dims).astype(out_ref.dtype)
        return 0

    lax.fori_loop(first, first + count, one, 0)


def grad_tiles(out_ref, left_ref, right_ref, first, count, cols=slice(None), tile=256):
    def one(i, _):
        at = pl.ds(pl.multiple_of(i * tile, tile), tile)
        out_ref[at, cols] = mm(left_ref[:, at], right_ref[...], TN).astype(out_ref.dtype)
        return 0

    lax.fori_loop(first, first + count, one, 0)


def comm_call(kernel, name, ident, args, outs, scratch, hbm_in=(), hbm_out=()):
    return pl.pallas_call(
        kernel,
        out_shape=tuple(outs),
        in_specs=[ANY if i in hbm_in else VM for i in range(len(args))],
        out_specs=tuple(ANY if i in hbm_out else VM for i in range(len(outs))),
        scratch_shapes=scratch,
        compiler_params=pltpu.CompilerParams(
            vmem_limit_bytes=VMEM_GRANT, collective_id=ident, has_side_effects=True
        ),
        name=name,
    )(*args)


def front_kernel(
    shards, tok_ref, w_ref, gain_ref, bias_ref, x_ref, a_ref, wf_ref, swap_sems, share_sems, w_sems, w_local
):
    s, c, t = place()
    greet(shards)
    swap = send(tok_ref.at[1 - c], x_ref.at[c], swap_sems, 0, {"ctx": 1 - c})
    spread = Spread(shards, w_ref, wf_ref, w_sems, w_local)
    share = Share(a_ref, share_sems)

    def norm(block):
        unit, _ = ln_stats(block.astype(F32))
        return (unit * gain_ref[...] + bias_ref[...]).astype(BF16)

    own = tok_ref[c]
    x_ref[c] = own
    a_ref[c, t] = norm(own)
    share.push(0, c)
    swap.wait()
    a_ref[1 - c, t] = norm(x_ref[1 - c])
    share.push(1, 1 - c)
    for k in range(spread.pieces):
        spread.step(k)
        if k == 0:
            share.forward(0, c)
        if k == min(2, spread.pieces - 1):
            share.forward(1, 1 - c)
    share.finish(0)
    share.finish(1)
    spread.finish()


def fwd_kernel(
    shards, heads, hd, cols, rows, qb,
    qkv_ref, tab_ref, hot_ref, cot_ref, w_ref, pw_ref,
    o_ref, ob_ref, lse_ref, qa_ref, ka_ref, g_ref, cf_ref, wf_ref, pp_ref,
    swap_sems, share_sems, w_sems, w_local,
):
    _, me, t = place()
    greet(shards)
    swap = send(cot_ref.at[1 - me], g_ref.at[me], swap_sems, 0, {"ctx": 1 - me})
    spread = Spread(shards, w_ref, wf_ref, w_sems, w_local)
    share = Share(cf_ref, share_sems)
    own = cot_ref[me]
    g_ref[me] = own
    cf_ref[me, t] = own
    share.push(0, me, cot_ref.at[me])
    tok = qkv_ref.shape[0]
    c = hd**-0.5 * math.log2(math.e)
    up = hd**0.5
    for h in range(heads):
        sl = slice(h * hd, (h + 1) * hd)
        q_sl, k_sl, v_sl = (slice((j * heads + h) * hd, (j * heads + h + 1) * hd) for j in range(3))
        pad = jnp.zeros((tok, 128 - hd), BF16)
        qp = jnp.concatenate([qkv_ref[:, q_sl], pad], 1)
        kp = jnp.concatenate([qkv_ref[:, k_sl], pad], 1)
        vt = jnp.concatenate([qkv_ref[:, v_sl], pad], 1).T
        ka_ref[h, :, 0:128] = jnp.where(lane_ids((tok, 128)) < hd, kp, hot_ref[:, 0:128])
        ka_ref[h, :, 128:256] = hot_ref[:, 128:256]
        terms = mm(qp, tab_ref[...]) * up
        ln = lane_ids((cols, 128))
        for r in range(rows):
            rs = slice(r * cols, (r + 1) * cols)
            tr = pltpu.roll(terms[rs, 0:128], (65 + r) % 128, 1)
            tc = pltpu.roll(terms[rs, 128:256], 65, 1, stride=1, stride_axis=0)
            rh = tr.astype(BF16).astype(F32)
            rl = pltpu.roll(tr - rh, rows, 1)
            ch = tc.astype(BF16).astype(F32)
            cl = pltpu.roll(tc - ch, 64, 1)
            low = jnp.where(ln < hd + 2 * rows, rl, jnp.zeros_like(tr))
            left = jnp.where(ln < hd, qp[rs].astype(F32), jnp.where(ln < hd + rows, rh, low))
            qa_ref[h, rs, 0:128] = left.astype(BF16)
            qa_ref[h, rs, 128:256] = jnp.where(ln < 64, ch, cl).astype(BF16)

        def blk(i, _):
            at = pl.ds(pl.multiple_of(i * qb, qb), qb)
            s = mm(ka_ref[h], qa_ref[h, at, :], NT)
            m = jnp.max(s, 0, keepdims=True)
            p = jnp.exp2((s - m) * c)
            l = jnp.sum(p, 0, keepdims=True)
            o = (mm(vt, p.astype(BF16)) / l).T[:, 0:hd]
            lse_ref[h : h + 1, at] = m * c + jnp.log2(l)
            o_ref[at, sl] = o
            ob_ref[at, sl] = o.astype(BF16)
            return 0

        lax.fori_loop(0, tok // qb, blk, 0)
        if h == 0:
            swap.wait()
            cf_ref[1 - me, t] = g_ref[1 - me]
            share.push(1, 1 - me, g_ref.at[1 - me])
        if h < spread.pieces:
            spread.step(h)
        if h == min(1, heads - 1):
            share.forward(0, me)
        if h == min(2, heads - 1):
            share.forward(1, 1 - me)
    row_tiles(pp_ref, ob_ref, pw_ref, NT, 0, tok // 256)
    for k in range(heads, spread.pieces):
        spread.step(k)
    share.finish(0)
    share.finish(1)
    spread.finish()


def mid_kernel(
    shards, part_ref, x_ref, pb_ref, gain_ref, bias_ref, w_ref, f1_ref, fb_ref,
    mid_ref, a_ref, wf_ref, act_ref, slope_ref,
    mate, far, outb, sum_sems, share_sems, w_sems, w_local,
):
    _, _, t = place()
    greet(shards)
    gather = Gather2(part_ref, mate, far, outb, sum_sems)
    gather.push(0)
    gather.push(1)
    spread = Spread(shards, w_ref, wf_ref, w_sems, w_local)
    share = Share(a_ref, share_sems)
    gather.forward(0)
    gather.forward(1)
    last = spread.pieces - 1
    for p in range(2):
        if p <= last:
            spread.step(p)
        mid = x_ref[p].astype(F32) + gather.result(p) + pb_ref[...]
        mid_ref[p] = mid
        unit, _ = ln_stats(mid)
        a_ref[p, t] = (unit * gain_ref[...] + bias_ref[...]).astype(BF16)
        share.push(p, p)
    for p in range(2):
        if p + 2 <= last:
            spread.step(p + 2)
        share.forward(p, p)
    half = a_ref.shape[1] * a_ref.shape[2]

    def hidden(p):
        def one(i, _):
            rows = a_ref[p, pl.ds(2 * i, 2)].reshape(-1, a_ref.shape[3])
            pre = mm(rows, f1_ref[...]) + fb_ref[...]
            cdf = 0.5 * (1.0 + lax.erf(pre * (2.0**-0.5)))
            bell = jnp.exp(-0.5 * pre * pre) * ((2.0 * math.pi) ** -0.5)
            at = pl.ds(pl.multiple_of(p * half + i * rows.shape[0], 128), rows.shape[0])
            act_ref[at, :] = (pre * cdf).astype(BF16)
            slope_ref[at, :] = cdf + pre * bell
            return 0

        lax.fori_loop(0, a_ref.shape[1] // 2, one, 0)

    share.finish(0)
    hidden(0)
    for k in range(4, spread.pieces):
        spread.step(k)
    share.finish(1)
    hidden(1)
    for p in range(2):
        gather.finish(p)
    spread.finish()


def turn_kernel(
    shards, part_ref, mid_ref, g_ref, gain_ref, w_ref, a2_ref, dp_ref, act_ref, f2_ref, pw_ref,
    dm_ref, db_ref, wg_ref, sums_ref, f1g_ref, mlp_ref, do_ref,
    mate, far, outb, sum_sems, share_sems, w_cross, w_line, w_sems,
):
    _, _, t = place()
    greet(shards)
    gather = Gather2(part_ref, mate, far, outb, sum_sems)
    gather.push(0)
    gather.push(1)
    collect = Collect(shards, w_ref, w_cross, w_line, w_sems)
    share = Share(db_ref, share_sems)
    gather.forward(0)
    gather.forward(1)
    rows = [jnp.zeros((1, mid_ref.shape[2]), F32) for _ in range(4)]
    last = collect.pieces - 1
    grads = f1g_ref.shape[0] // 256
    tiles = mlp_ref.shape[0] // 256
    grad_tiles(f1g_ref, a2_ref, dp_ref, 0, grads // 2)
    for p in range(2):
        if p <= last:
            collect.step(p)
        unit, inverse = ln_stats(mid_ref[p])
        g = g_ref[p].astype(F32)
        da = gather.result(p)
        dm = g + ln_back(unit, inverse, gain_ref[...], da)
        dm_ref[p] = dm
        low = dm.astype(BF16)
        db_ref[p, t] = low
        share.push(p, p)
        for k, term in enumerate((da * unit, da, low.astype(F32), g)):
            rows[k] = rows[k] + jnp.sum(term, 0, keepdims=True)
        if p == 0:
            grad_tiles(f1g_ref, a2_ref, dp_ref, grads // 2, grads - grads // 2)
    for k in range(4):
        sums_ref[k : k + 1, :] = rows[k]
    for p in range(2):
        row_tiles(mlp_ref, act_ref, f2_ref, NT, p * tiles // 2, tiles // 2)
        if p + 2 <= last:
            collect.step(p + 2)
        share.forward(p, p)
    for k in range(4, collect.pieces):
        collect.step(k)
    group = db_ref.shape[1] * db_ref.shape[2]
    for p in range(2):
        gather.finish(p)
        share.finish(p)

        def one(i, _):
            rows = db_ref[p, pl.ds(2 * i, 2)].reshape(-1, db_ref.shape[3])
            at = pl.ds(pl.multiple_of(p * group + i * rows.shape[0], 128), rows.shape[0])
            do_ref[at, :] = mm(rows, pw_ref[...]).astype(BF16)
            return 0

        lax.fori_loop(0, db_ref.shape[1] // 2, one, 0)
    collect.finish(wg_ref)


def bwd_kernel(
    shards, heads, hd, cols, rows, qb,
    qa_ref, ka_ref, qkv_ref, do_ref, o_ref, lse_ref, tab_ref, hot_ref, part_ref, mid_ref, fb_ref, w_ref,
    a1_ref, db_ref, ob_ref, w1_ref,
    rg_ref, out_ref, wg_ref, da_ref, w1g_ref, qs_ref,
    dqkv_ref,
    kt_ref, acc_k, acc_v, del_ref, res_ref, mate, far, outb, sum_sems, swap_sems, w_cross, w_line, w_sems,
):
    _, me, _ = place()
    greet(shards)
    gather = Gather2(part_ref, mate, far, outb, sum_sems)
    gather.push(0)
    gather.push(1)
    collect = Collect(shards, w_ref, w_cross, w_line, w_sems)
    gather.forward(0)
    gather.forward(1)
    tok = qkv_ref.shape[0]
    scale = hd**-0.5
    c = scale * math.log2(math.e)
    rg_ref[...] = jnp.zeros_like(rg_ref)
    for h in range(heads):
        sl = slice(h * hd, (h + 1) * hd)
        k_sl, v_sl = (slice((j * heads + h) * hd, (j * heads + h + 1) * hd) for j in (1, 2))
        pad = jnp.zeros((tok, 128 - hd), BF16)
        vp = jnp.concatenate([qkv_ref[:, v_sl], pad], 1)
        kt_ref[0:128, :] = jnp.where(lane_ids((tok, 128)) < hd, ka_ref[h, :, 0:128], hot_ref[:, 0:128]).T
        kt_ref[128:256, :] = hot_ref[:, 128:256].T
        prod = jnp.concatenate([do_ref[:, sl].astype(F32) * o_ref[:, sl], pad.astype(F32)], 1)
        del_ref[...] = lax.dot_general(
            jnp.ones((8, 128), F32), prod, NT, preferred_element_type=F32, precision=PRECISE
        )
        acc_k[...] = jnp.zeros_like(acc_k)
        acc_v[...] = jnp.zeros_like(acc_v)

        def blk(i, _):
            at = pl.ds(pl.multiple_of(i * qb, qb), qb)
            qblk = qa_ref[h, at, :]
            dob = jnp.concatenate([do_ref[at, sl], jnp.zeros((qb, 128 - hd), BF16)], 1)
            s = mm(ka_ref[h], qblk, NT)
            p = jnp.exp2(s * c - lse_ref[h : h + 1, at])
            dp = mm(vp, dob, NT)
            ds = (p * (dp - del_ref[0:1, at])).astype(BF16)
            acc_v[...] += mm(p.astype(BF16), dob)
            acc_k[...] += mm(ds, qblk[:, 0:128])
            dqa = mm(kt_ref[...], ds).T
            ln = lane_ids((cols, 128))
            parts = []
            for j in range(qb // cols):
                r = i * (qb // cols) + j
                js = slice(j * cols, (j + 1) * cols)
                dr = dqa[js, 0:128]
                dr = jnp.where((ln >= hd) & (ln < hd + rows), dr, 0.0)
                dr = pltpu.roll(dr, (48 + r) % 128, 1)
                dc = pltpu.roll(dqa[js, 128:256], 0, 1, stride=1, stride_axis=0)
                parts.append(jnp.concatenate([dr, dc], 1))
            d = jnp.concatenate(parts, 0).astype(BF16)
            rel = mm(d, tab_ref[...])
            rg_ref[...] += mm(d, qblk[:, 0:128], TN)
            dqkv_ref[at, sl] = (scale * dqa[:, 0:128] + rel)[:, 0:hd].astype(BF16)
            return 0

        lax.fori_loop(0, tok // qb, blk, 0)
        dqkv_ref[:, k_sl] = (scale * acc_k[...])[:, 0:hd].astype(BF16)
        dqkv_ref[:, v_sl] = acc_v[...][:, 0:hd].astype(BF16)
        if h < collect.pieces:
            collect.step(h)
        if h == min(2, heads - 1):
            for p in range(2):
                total = mid_ref[p] + gather.result(p) + fb_ref[...]
                res_ref[p] = total.astype(BF16)
            swap = send(res_ref.at[1 - me], out_ref.at[me], swap_sems, 0, {"ctx": 1 - me})
            out_ref[me] = res_ref[me]
    wide = dqkv_ref.shape[1]
    for i in range(tok // 256):
        at = slice(i * 256, (i + 1) * 256)
        da_ref[at, :] = mm(dqkv_ref[at, :], w1_ref[:, 0:wide], NT).astype(BF16)
    for k in range(heads, collect.pieces):
        collect.step(k)
    grads = w1g_ref.shape[0] // 256
    grad_tiles(w1g_ref, a1_ref, dqkv_ref, 0, grads, slice(0, wide))
    grad_tiles(w1g_ref, db_ref, ob_ref, 0, grads, slice(wide, w1g_ref.shape[1]))
    qs_ref[...] = jnp.sum(dqkv_ref[...].astype(F32), 0, keepdims=True)
    for p in range(2):
        gather.finish(p)
    collect.finish(wg_ref)
    swap.wait()


def end_kernel(
    shards, part_ref, x_ref, dm_ref, gain_ref, w_ref, small_ref, out_ref, wg_ref, total_ref,
    res_ref, mate, far, outb, sum_sems, swap_sems, held, got, line, small_sems, w_cross, w_line, w_sems,
):
    s, me, t = place()
    greet(shards)
    gather = Gather2(part_ref, mate, far, outb, sum_sems)
    gather.push(0)
    gather.push(1)
    collect = Collect(shards, w_ref, w_cross, w_line, w_sems)
    gather.forward(0)
    gather.forward(1)
    first = jnp.zeros((1, x_ref.shape[2]), F32)
    second = jnp.zeros((1, x_ref.shape[2]), F32)
    for p in range(2):
        if p < collect.pieces:
            collect.step(p)
        unit, inverse = ln_stats(x_ref[p].astype(F32))
        da = gather.result(p)
        res_ref[p] = (dm_ref[p] + ln_back(unit, inverse, gain_ref[...], da)).astype(BF16)
        first = first + jnp.sum(da * unit, 0, keepdims=True)
        second = second + jnp.sum(da, 0, keepdims=True)
    swap = send(res_ref.at[1 - me], out_ref.at[me], swap_sems, 0, {"ctx": 1 - me})
    out_ref[me] = res_ref[me]
    held[0] = small_ref[...]
    held[0, 0:1, :] = first
    held[0, 1:2, :] = second
    waits = []
    for k, peer in enumerate(({"tp": core_mate(t)}, {"tp": far_mate(t)}, {"ctx": 1 - me})):
        copy = send(held.at[k], got.at[k], small_sems, k, peer)
        if k + 2 < collect.pieces:
            collect.step(k + 2)
        copy.wait_recv()
        waits.append(copy)
        held[k + 1] = held[k] + got[k]
    line[s] = held[3]
    for d in range(1, shards):
        waits.append(send(held.at[3], line.at[s], small_sems, 2 + d, {"shard": lax.rem(s + d, shards)}))
    collect.finish(wg_ref)
    for k, copy in enumerate(waits):
        if k < 3:
            copy.wait_send()
        else:
            copy.wait()
    acc = line[0]
    for k in range(1, shards):
        acc = acc + line[k]
    total_ref[...] = acc
    for p in range(2):
        gather.finish(p)
    swap.wait()


def position_tables(rel_rows, rel_cols, hd):
    gap = 128 - hd
    rr = jnp.pad(rel_rows, ((0, 128 - rel_rows.shape[0]), (0, gap)))
    rc = jnp.pad(rel_cols, ((0, 128 - rel_cols.shape[0]), (0, gap)))
    fr = jnp.pad(rel_rows[::-1], ((0, 128 - rel_rows.shape[0]), (0, gap)))
    fc = jnp.pad(rel_cols[::-1], ((0, 128 - rel_cols.shape[0]), (0, gap)))
    return jnp.concatenate([fr, fc], 0).T, jnp.concatenate([rr, rc], 0)


def position_hots(tok, hd, cols, rows):
    kr = jnp.arange(rows, dtype=jnp.int32)[:, None]
    kw = jnp.arange(cols, dtype=jnp.int32)[:, None]
    l = jnp.arange(256, dtype=jnp.int32)[None, :]
    first_r = (l == hd + kr) | (l == hd + rows + kr)
    first_c = (l == 128 + kw) | (l == 192 + kw)
    second_r = l == hd + rows - 1 - kr
    second_c = l == 128 + cols - 1 - kw

    def both(r, c):
        return (r[:, None, :] | c[None, :, :]).astype(BF16).reshape(tok, 256)

    return both(first_r, first_c), both(second_r, second_c)


def on_device_images(
    tokens, norm1_gain, norm1_bias, qkv_weight, qv_bias, rel_rows, rel_cols, proj_weight, proj_bias,
    norm2_gain, norm2_bias, fc1_weight, fc1_bias, fc2_weight, fc2_bias, cotangent,
):
    S = jax.ShapeDtypeStruct
    shards = lax.axis_size("shard")
    tp_count = lax.axis_size("tp")
    tp_rank = lax.axis_index("tp")
    heads = H // tp_count
    width = heads * HD
    ff = FF // tp_count
    rows = (rel_rows.shape[0] + 1) // 2
    tok = rows * COLS
    own = tokens.shape
    piece = own[1:]
    full = (2, tp_count) + piece
    block = fc1_weight.shape
    blocks = (2 * shards,) + block
    qkv_cols = 3 * width
    w1 = jnp.concatenate([qkv_weight[0], qkv_weight[1], qkv_weight[2], proj_weight.T], 1)
    fc2_t = fc2_weight.T
    qv_local = lax.dynamic_slice_in_dim(qv_bias, tp_rank * width, width, 1)
    qkv_bias = jnp.concatenate([qv_local[0], jnp.zeros((width,), F32), qv_local[1]])
    fc1_local = lax.dynamic_slice_in_dim(fc1_bias, tp_rank * ff, ff, 0)
    tab_f, tab_b = position_tables(rel_rows, rel_cols, HD)
    hot_f, hot_b = position_hots(tok, HD, COLS, rows)
    spread = Spread.scratch(shards, block)
    collect = Collect.scratch(shards, block)
    gather = Gather2.scratch(piece)
    swap = [DMA((2, 1))]
    share = [DMA((2, 6))]

    def row(vec):
        return vec.reshape(1, -1)

    x, a1, w1_full = comm_call(
        partial(front_kernel, shards), "front", 0,
        (tokens, w1, row(norm1_gain), row(norm1_bias)),
        (S(own, BF16), S(full, BF16), S(blocks, BF16)),
        swap + share + spread, hbm_in=(1,), hbm_out=(2,),
    )
    a1 = a1.reshape(tok, D)
    w1_full = w1_full.reshape(D, -1)
    qkv_full = w1_full[:, :qkv_cols]
    proj_full = w1_full[:, qkv_cols:]
    qkv = (mm(a1, qkv_full) + qkv_bias).astype(BF16)
    o, o_low, lse, qa, ka, g, cot, fc1_full, proj_part = comm_call(
        partial(fwd_kernel, shards, heads, HD, COLS, rows, 256), "attn_fwd", 1,
        (qkv, tab_f, hot_f, cotangent, fc1_weight, proj_full),
        (
            S((tok, width), F32), S((tok, width), BF16), S((heads, tok), F32),
            S((heads, tok, 256), BF16), S((heads, tok, 256), BF16),
            S(own, BF16), S(full, BF16), S(blocks, BF16), S((tok, D), BF16),
        ),
        swap + share + spread, hbm_in=(4,), hbm_out=(7,),
    )
    fc1_full = fc1_full.reshape(D, ff)
    cot = cot.reshape(tok, D)
    proj_part = proj_part.reshape(full)
    mid, a2, fc2_full, act, slope = comm_call(
        partial(mid_kernel, shards), "mid", 2,
        (proj_part, x, row(proj_bias), row(norm2_gain), row(norm2_bias), fc2_t, fc1_full, row(fc1_local)),
        (S(own, F32), S(full, BF16), S(blocks, BF16), S((tok, ff), BF16), S((tok, ff), F32)),
        gather + share + spread, hbm_in=(5,), hbm_out=(2,),
    )
    a2 = a2.reshape(tok, D)
    fc2_full = fc2_full.reshape(D, ff)
    d_pre = (mm(cot, fc2_full) * slope).astype(BF16)
    d_a2 = mm(d_pre, fc1_full, NT).astype(BF16).reshape(full)
    fc2_grad = mm(cot, act, TN).astype(BF16)
    d_mid, d_branch, fc2_own, sums, fc1_grad, mlp_part, d_o = comm_call(
        partial(turn_kernel, shards), "turn", 3,
        (d_a2, mid, g, row(norm2_gain), fc2_grad, a2, d_pre, act, fc2_full, proj_full),
        (
            S(own, F32), S(full, BF16), S(block, F32), S((4, D), F32),
            S((D, ff), BF16), S((tok, D), BF16), S((tok, width), BF16),
        ),
        gather + share + collect,
    )
    d_branch = d_branch.reshape(tok, D)
    mlp_part = mlp_part.reshape(full)
    rel_grad, output, fc1_own, d_a1, w1_grad, qkv_sum = comm_call(
        partial(bwd_kernel, shards, heads, HD, COLS, rows, 256), "attn_bwd", 4,
        (qa, ka, qkv, d_o, o, lse, tab_b, hot_b, mlp_part, mid, row(fc2_bias), fc1_grad, a1, d_branch, o_low, w1_full),
        (
            S((256, 128), F32), S(own, BF16), S(block, F32),
            S((tok, D), BF16), S((D, qkv_cols + width), BF16), S((1, qkv_cols), F32),
        ),
        [
            pltpu.VMEM((tok, qkv_cols), BF16), pltpu.VMEM((256, tok), BF16), pltpu.VMEM((tok, 128), F32), pltpu.VMEM((tok, 128), F32),
            pltpu.VMEM((8, tok), F32), pltpu.VMEM(own, BF16),
        ] + gather + swap + collect,
    )
    d_a1 = d_a1.reshape(full)
    qkv_sum = qkv_sum[0]
    qv_part = jnp.stack([qkv_sum[:width], qkv_sum[2 * width :]])
    qv_placed = lax.dynamic_update_slice_in_dim(jnp.zeros((2, D), F32), qv_part, tp_rank * width, 1)
    fc1_sum = jnp.sum(d_pre.astype(F32), 0)
    fc1_placed = lax.dynamic_update_slice_in_dim(jnp.zeros((FF,), F32), fc1_sum, tp_rank * ff, 0)
    terms = (
        jnp.zeros((2 * D,), F32),
        qv_placed.reshape(-1),
        fc1_placed,
        sums.reshape(-1),
        rel_grad[: rel_rows.shape[0], :HD].reshape(-1),
        rel_grad[128 : 128 + rel_cols.shape[0], :HD].reshape(-1),
    )
    count = sum(term.shape[0] for term in terms)
    lines = -(-count // (8 * D)) * 8
    packed = jnp.concatenate(terms + (jnp.zeros((lines * D - count,), F32),)).reshape(lines, D)
    tokens_grad, w1_own, total = comm_call(
        partial(end_kernel, shards), "end", 5,
        (d_a1, x, d_mid, row(norm1_gain), w1_grad, packed),
        (S(own, BF16), S(block, F32), S((lines, D), F32)),
        [pltpu.VMEM(own, BF16)] + gather + swap
        + [
            pltpu.VMEM((4, lines, D), F32), pltpu.VMEM((3, lines, D), F32),
            pltpu.VMEM((shards, lines, D), F32), DMA((2, 2 + shards)),
        ]
        + collect,
    )
    flat = total.reshape(-1)
    base = 4 * D + FF
    rel_at = base + 4 * D
    rel_mid = rel_at + rel_rows.size
    return (
        output,
        tokens_grad,
        total[0],
        total[1],
        jnp.stack([w1_own[:, j * width : (j + 1) * width] for j in range(3)]),
        total[2:4],
        flat[rel_at:rel_mid].reshape(rel_rows.shape),
        flat[rel_mid : rel_mid + rel_cols.size].reshape(rel_cols.shape),
        w1_own[:, qkv_cols:].T,
        flat[base + 2 * D : base + 3 * D],
        flat[base : base + D],
        flat[base + D : base + 2 * D],
        fc1_own,
        flat[4 * D : base],
        fc2_own.T,
        flat[base + 3 * D : base + 4 * D],
    )


def solution(mesh):
    in_specs = (
        P("shard", ("ctx", "tp"), None),
        P(),
        P(),
        P(None, ("shard", "ctx"), "tp"),
        P(),
        P(),
        P(),
        P("tp", ("shard", "ctx")),
        P(),
        P(),
        P(),
        P(("shard", "ctx"), "tp"),
        P(),
        P("tp", ("shard", "ctx")),
        P(),
        P("shard", ("ctx", "tp"), None),
    )
    out_specs = (
        P("shard", ("ctx", "tp"), None),
        P("shard", ("ctx", "tp"), None),
        P(),
        P(),
        P(None, ("shard", "ctx"), "tp"),
        P(),
        P(),
        P(),
        P("tp", ("shard", "ctx")),
        P(),
        P(),
        P(),
        P(("shard", "ctx"), "tp"),
        P(),
        P("tp", ("shard", "ctx")),
        P(),
    )
    def on_device(*arrays):
        rows = (arrays[5].shape[0] + 1) // 2
        fits = mesh.shape["tp"] == 4 and mesh.shape["ctx"] == 2 and HD + 2 * rows <= 128
        fits = fits and arrays[0].shape[0] == mesh.shape["ctx"] and arrays[6].shape[0] <= 128
        return (on_device_images if fits else on_device_rows)(*arrays)

    return jax.shard_map(
        on_device, mesh=mesh, in_specs=in_specs, out_specs=out_specs, check_vma=False
    )
```

```python
from functools import partial
import math

import jax
import jax.numpy as jnp
from jax import lax
from jax.experimental import pallas as pl
from jax.experimental.pallas import tpu as pltpu
from jax.sharding import PartitionSpec as P

D = 1280
H = 16
HD = 80
FF = 5120
COLS = 64
ROWS_DEV = 8


PRECISE = lax.Precision.HIGHEST
EPSILON = 1e-06
NEGATIVE = -1e30


def layer_norm(values_in, gain_vec, shift_vec):
    average = jnp.mean(values_in, -1, keepdims=True)
    centred = values_in - average
    variance = jnp.mean(centred * centred, -1, keepdims=True)
    return centred * lax.rsqrt(variance + EPSILON) * gain_vec + shift_vec


def block_size():
    return 512


def to_heads(flat_rows, heads_local):
    images, length, feat_width = flat_rows.shape
    return flat_rows.reshape(images, length, heads_local, feat_width // heads_local).transpose(
        0, 2, 1, 3
    )


def from_heads(per_head):
    images, heads_local, length, head_dim = per_head.shape
    return per_head.transpose(0, 2, 1, 3).reshape(images, length, heads_local * head_dim)


def block_scores(query_heads, key_flat, rows_bias, cols_bias, first_key, scale_factor):
    key_heads = to_heads(key_flat, query_heads.shape[1])
    key_len = key_flat.shape[1]
    key_rows = key_len // COLS
    scores = scale_factor * jnp.einsum(
        "ihqc,ihkc->ihqk", query_heads, key_heads, preferred_element_type=jnp.float32
    )
    images, heads_local, query_len, unused_len = scores.shape
    row_part = lax.dynamic_slice_in_dim(rows_bias, first_key // COLS, key_rows, 3)
    scores = scores.reshape(images, heads_local, query_len, key_rows, COLS)
    scores = scores + row_part[..., :, None] + cols_bias[..., None, :]
    return scores.reshape(images, heads_local, query_len, key_len)


def relative_terms(query_flat, rows_param, cols_param, first_row, heads_local):
    images, length, feat_width = query_flat.shape
    rows_dev = length // COLS
    grid_rows = (rows_param.shape[0] + 1) // 2
    own_rows = first_row + jnp.arange(rows_dev, dtype=jnp.int32)
    key_rows = jnp.arange(grid_rows, dtype=jnp.int32)
    row_slots = jnp.arange(rows_param.shape[0], dtype=jnp.int32)
    pick_rows = (
        row_slots[None, None, :]
        == own_rows[:, None, None] - key_rows[None, :, None] + grid_rows - 1
    ).astype(jnp.float32)
    table_rows = jnp.einsum("rkj,jc->rkc", pick_rows, rows_param, precision=PRECISE)
    col_ids = jnp.arange(COLS, dtype=jnp.int32)
    col_slots = jnp.arange(cols_param.shape[0], dtype=jnp.int32)
    pick_cols = (
        col_slots[None, None, :] == col_ids[:, None, None] - col_ids[None, :, None] + COLS - 1
    ).astype(jnp.float32)
    table_cols = jnp.einsum("wkj,jc->wkc", pick_cols, cols_param, precision=PRECISE)
    grid_form = query_flat.reshape(images, rows_dev, COLS, heads_local, feat_width // heads_local)
    along_rows = jnp.einsum("irwhc,rkc->ihrwk", grid_form, table_rows, precision=PRECISE).reshape(
        images, heads_local, length, grid_rows
    )
    along_cols = jnp.einsum("irwhc,wkc->ihrwk", grid_form, table_cols, precision=PRECISE).reshape(
        images, heads_local, length, COLS
    )
    return (along_rows, along_cols)


def on_device_rows(
    tokens,
    norm1_gain,
    norm1_bias,
    qkv_weight,
    qv_bias,
    rel_rows,
    rel_cols,
    proj_weight,
    proj_bias,
    norm2_gain,
    norm2_bias,
    fc1_weight,
    fc1_bias,
    fc2_weight,
    fc2_bias,
    cotangent,
):
    scale_factor = HD ** (-0.5)
    tp_count = lax.axis_size("tp")
    ctx_count = lax.axis_size("ctx")
    tp_rank = lax.axis_index("tp")
    ctx_rank = lax.axis_index("ctx")
    grid_rows = ROWS_DEV * ctx_count
    tok_image = grid_rows * COLS
    tok_ctx = ROWS_DEV * COLS
    heads_local = H // tp_count
    width_local = heads_local * HD
    ff_local = FF // tp_count
    images = tokens.shape[0]
    rows_table = rel_rows.astype(jnp.float32)
    cols_table = rel_cols.astype(jnp.float32)
    qkv_full, proj_full, fc1_full, fc2_full = (
        lax.all_gather(qkv_weight, ("shard", "ctx"), axis=1, tiled=True),
        lax.all_gather(proj_weight, ("shard", "ctx"), axis=1, tiled=True),
        lax.all_gather(fc1_weight, ("shard", "ctx"), axis=0, tiled=True),
        lax.all_gather(fc2_weight, ("shard", "ctx"), axis=1, tiled=True),
    )
    qv_local = lax.dynamic_slice_in_dim(qv_bias, tp_rank * width_local, width_local, 1)
    fc1_local = lax.dynamic_slice_in_dim(fc1_bias, tp_rank * ff_local, ff_local, 0)
    resid_in = tokens.astype(jnp.float32)
    normed1 = layer_norm(resid_in, norm1_gain, norm1_bias).astype(jnp.bfloat16)
    normed1_full = lax.all_gather(normed1, "tp", axis=1, tiled=True)
    projected = jnp.einsum(
        "itd,sde->itse", normed1_full, qkv_full, preferred_element_type=jnp.float32
    )
    queries = (projected[:, :, 0] + qv_local[0]).astype(jnp.bfloat16)
    keys_own = projected[:, :, 1].astype(jnp.bfloat16)
    values_own = (projected[:, :, 2] + qv_local[1]).astype(jnp.bfloat16)
    first_row = ctx_rank * ROWS_DEV
    rel_fn = partial(relative_terms, first_row=first_row, heads_local=heads_local)
    (along_rows, along_cols), rel_pull = jax.vjp(
        rel_fn, queries.astype(jnp.float32), rows_table, cols_table
    )
    query_heads = to_heads(queries, heads_local)
    start_state = (
        jnp.full((images, heads_local, tok_ctx), NEGATIVE, jnp.float32),
        jnp.zeros((images, heads_local, tok_ctx), jnp.float32),
        jnp.zeros((images, heads_local, tok_ctx, HD), jnp.float32),
        jnp.zeros((images, tok_image, width_local), jnp.bfloat16),
        jnp.zeros((images, tok_image, width_local), jnp.bfloat16),
    )
    shard_piece = (
        lax.all_gather(keys_own, "ctx", axis=1, tiled=True),
        lax.all_gather(values_own, "ctx", axis=1, tiled=True),
    )
    piece_len = shard_piece[0].shape[1]
    step_len = block_size()

    def one_step(inner, offset):
        run_max, run_sum, run_acc, keys_all, values_all = inner
        key_blk = lax.dynamic_slice_in_dim(shard_piece[0], offset, step_len, 1)
        value_blk = lax.dynamic_slice_in_dim(shard_piece[1], offset, step_len, 1)
        scores = block_scores(query_heads, key_blk, along_rows, along_cols, offset, scale_factor)
        new_max = jnp.maximum(run_max, jnp.max(scores, -1))
        factor = jnp.exp(run_max - new_max)
        weights_blk = jnp.exp(scores - new_max[..., None])
        run_sum = run_sum * factor + jnp.sum(weights_blk, -1)
        value_heads = to_heads(value_blk, heads_local)
        run_acc = run_acc * factor[..., None] + jnp.einsum(
            "ihqk,ihkc->ihqc",
            weights_blk.astype(jnp.bfloat16),
            value_heads,
            preferred_element_type=jnp.float32,
        )
        keys_all = lax.dynamic_update_slice_in_dim(keys_all, key_blk, offset, 1)
        values_all = lax.dynamic_update_slice_in_dim(values_all, value_blk, offset, 1)
        return ((new_max, run_sum, run_acc, keys_all, values_all), None)

    offsets = jnp.arange(piece_len // step_len, dtype=jnp.int32) * step_len
    result, unused = lax.scan(one_step, start_state, offsets)
    run_max, run_sum, run_acc, keys_all, values_all = result
    attn_heads = run_acc / run_sum[..., None]
    log_total = run_max + jnp.log(run_sum)
    attn_low = from_heads(attn_heads).astype(jnp.bfloat16)
    proj_part = jnp.einsum("itd,de->ite", attn_low, proj_full, preferred_element_type=jnp.float32)
    branch = lax.psum_scatter(
        proj_part.astype(jnp.bfloat16), "tp", scatter_dimension=1, tiled=True
    ).astype(jnp.float32)
    middle = resid_in + branch + proj_bias
    normed2 = layer_norm(middle, norm2_gain, norm2_bias).astype(jnp.bfloat16)
    normed2_full = lax.all_gather(normed2, "tp", axis=1, tiled=True)
    hidden_pre = (
        jnp.einsum("itd,df->itf", normed2_full, fc1_full, preferred_element_type=jnp.float32)
        + fc1_local
    )
    gelu_exact = partial(jax.nn.gelu, approximate=False)
    activated_f, gelu_pull = jax.vjp(gelu_exact, hidden_pre)
    activated = activated_f.astype(jnp.bfloat16)
    mlp_part = jnp.einsum("itf,fe->ite", activated, fc2_full, preferred_element_type=jnp.float32)
    mlp_out = lax.psum_scatter(
        mlp_part.astype(jnp.bfloat16), "tp", scatter_dimension=1, tiled=True
    ).astype(jnp.float32)
    output = (middle + mlp_out + fc2_bias).astype(jnp.bfloat16)
    cot_full = lax.all_gather(cotangent, "tp", axis=1, tiled=True)
    d_act = jnp.einsum("ite,fe->itf", cot_full, fc2_full, preferred_element_type=jnp.float32)
    d_hidden = gelu_pull(d_act)[0].astype(jnp.bfloat16)
    fc2_grad = jnp.einsum("itf,ite->fe", activated, cot_full, preferred_element_type=jnp.float32)
    fc1_grad = jnp.einsum("itd,itf->df", normed2_full, d_hidden, preferred_element_type=jnp.float32)
    fc1_bias_part = jnp.sum(d_hidden.astype(jnp.float32), (0, 1))
    fc2_bias_part = jnp.sum(cotangent.astype(jnp.float32), (0, 1))
    d_norm2_part = jnp.einsum("itf,df->itd", d_hidden, fc1_full, preferred_element_type=jnp.float32)
    d_norm2 = lax.psum_scatter(
        d_norm2_part.astype(jnp.bfloat16), "tp", scatter_dimension=1, tiled=True
    ).astype(jnp.float32)
    unused_out, norm2_pull = jax.vjp(layer_norm, middle, norm2_gain, norm2_bias)
    d_mid_part, gain2_part, bias2_part = norm2_pull(d_norm2)
    d_middle = cotangent.astype(jnp.float32) + d_mid_part
    d_branch = d_middle.astype(jnp.bfloat16)
    proj_bias_part = jnp.sum(d_branch.astype(jnp.float32), (0, 1))
    d_branch_full = lax.all_gather(d_branch, "tp", axis=1, tiled=True)
    proj_grad = jnp.einsum(
        "itd,ite->de", attn_low, d_branch_full, preferred_element_type=jnp.float32
    )
    d_attn = jnp.einsum(
        "ite,de->itd", d_branch_full, proj_full, preferred_element_type=jnp.float32
    ).astype(jnp.bfloat16)
    d_attn_heads = to_heads(d_attn, heads_local)
    delta_rows = jnp.sum(d_attn_heads.astype(jnp.float32) * attn_heads, -1)
    key_step = block_size()
    key_rows = key_step // COLS
    key_offsets = jnp.arange(tok_image // key_step, dtype=jnp.int32) * key_step

    def back_step(carried, offset):
        grad_query, grad_rows, grad_cols = carried
        key_blk = lax.dynamic_slice_in_dim(keys_all, offset, key_step, 1)
        value_blk = lax.dynamic_slice_in_dim(values_all, offset, key_step, 1)
        scores = block_scores(query_heads, key_blk, along_rows, along_cols, offset, scale_factor)
        soft_probs = jnp.exp(scores - log_total[..., None])
        value_heads = to_heads(value_blk, heads_local)
        key_heads = to_heads(key_blk, heads_local)
        d_probs = jnp.einsum(
            "ihqc,ihkc->ihqk", d_attn_heads, value_heads, preferred_element_type=jnp.float32
        )
        d_scores = (soft_probs * (d_probs - delta_rows[..., None])).astype(jnp.bfloat16)
        grad_query = grad_query + jnp.einsum(
            "ihqk,ihkc->ihqc", d_scores, key_heads, preferred_element_type=jnp.float32
        )
        grid_scores = d_scores.astype(jnp.float32).reshape(
            images, heads_local, tok_ctx, key_rows, COLS
        )
        row_sums = jnp.sum(grid_scores, 4)
        row_now = lax.dynamic_slice_in_dim(grad_rows, offset // COLS, key_rows, 3)
        grad_rows = lax.dynamic_update_slice_in_dim(
            grad_rows, row_now + row_sums, offset // COLS, 3
        )
        grad_cols = grad_cols + jnp.sum(grid_scores, 3)
        key_part = scale_factor * jnp.einsum(
            "ihqk,ihqc->ikhc", d_scores, query_heads, preferred_element_type=jnp.float32
        )
        value_part = jnp.einsum(
            "ihqk,ihqc->ikhc",
            soft_probs.astype(jnp.bfloat16),
            d_attn_heads,
            preferred_element_type=jnp.float32,
        )
        emitted = (
            key_part.reshape(images, key_step, width_local),
            value_part.reshape(images, key_step, width_local),
        )
        return ((grad_query, grad_rows, grad_cols), emitted)

    back_start = (
        jnp.zeros((images, heads_local, tok_ctx, HD), jnp.float32),
        jnp.zeros((images, heads_local, tok_ctx, grid_rows), jnp.float32),
        jnp.zeros((images, heads_local, tok_ctx, COLS), jnp.float32),
    )
    (grad_query, grad_rows, grad_cols), emitted = lax.scan(back_step, back_start, key_offsets)
    key_terms = emitted[0].transpose(1, 0, 2, 3).reshape(images, tok_image, width_local)
    value_terms = emitted[1].transpose(1, 0, 2, 3).reshape(images, tok_image, width_local)
    grad_keys, grad_values = (
        lax.psum_scatter(
            key_terms.astype(jnp.bfloat16), "ctx", scatter_dimension=1, tiled=True
        ).astype(jnp.float32),
        lax.psum_scatter(
            value_terms.astype(jnp.bfloat16), "ctx", scatter_dimension=1, tiled=True
        ).astype(jnp.float32),
    )
    d_query_rel, rows_grad_part, cols_grad_part = rel_pull((grad_rows, grad_cols))
    d_query = (scale_factor * from_heads(grad_query) + d_query_rel).astype(jnp.bfloat16)
    d_keys = grad_keys.astype(jnp.bfloat16)
    d_values = grad_values.astype(jnp.bfloat16)
    d_projected = jnp.stack((d_query, d_keys, d_values), axis=2)
    qkv_grad = jnp.einsum(
        "itd,itse->sde", normed1_full, d_projected, preferred_element_type=jnp.float32
    )
    qv_bias_part = jnp.stack(
        (
            jnp.sum(d_query.astype(jnp.float32), (0, 1)),
            jnp.sum(d_values.astype(jnp.float32), (0, 1)),
        )
    )
    d_norm1_part = jnp.einsum(
        "itse,sde->itd", d_projected, qkv_full, preferred_element_type=jnp.float32
    )
    d_norm1 = lax.psum_scatter(
        d_norm1_part.astype(jnp.bfloat16), "tp", scatter_dimension=1, tiled=True
    ).astype(jnp.float32)
    unused_in, norm1_pull = jax.vjp(layer_norm, resid_in, norm1_gain, norm1_bias)
    d_in_part, gain1_part, bias1_part = norm1_pull(d_norm1)
    tokens_grad = (d_middle + d_in_part).astype(jnp.bfloat16)
    qkv_out, proj_out, fc1_out, fc2_out = (
        lax.psum_scatter(
            qkv_grad.astype(jnp.bfloat16), ("shard", "ctx"), scatter_dimension=1, tiled=True
        ).astype(jnp.float32),
        lax.psum_scatter(
            proj_grad.astype(jnp.bfloat16), ("shard", "ctx"), scatter_dimension=1, tiled=True
        ).astype(jnp.float32),
        lax.psum_scatter(
            fc1_grad.astype(jnp.bfloat16), ("shard", "ctx"), scatter_dimension=0, tiled=True
        ).astype(jnp.float32),
        lax.psum_scatter(
            fc2_grad.astype(jnp.bfloat16), ("shard", "ctx"), scatter_dimension=1, tiled=True
        ).astype(jnp.float32),
    )
    qv_placed = lax.dynamic_update_slice_in_dim(
        jnp.zeros((2, D), jnp.float32), qv_bias_part, tp_rank * width_local, 1
    )
    fc1_placed = lax.dynamic_update_slice_in_dim(
        jnp.zeros((FF,), jnp.float32), fc1_bias_part, tp_rank * ff_local, 0
    )
    (
        gain1_sum,
        bias1_sum,
        qv_sum,
        rows_sum,
        cols_sum,
        projb_sum,
        gain2_sum,
        bias2_sum,
        fc1b_sum,
        fc2b_sum,
    ) = lax.psum(
        (
            gain1_part,
            bias1_part,
            qv_placed,
            rows_grad_part,
            cols_grad_part,
            proj_bias_part,
            gain2_part,
            bias2_part,
            fc1_placed,
            fc2_bias_part,
        ),
        ("shard", "ctx", "tp"),
    )
    return (
        output,
        tokens_grad,
        gain1_sum,
        bias1_sum,
        qkv_out,
        qv_sum,
        rows_sum,
        cols_sum,
        proj_out,
        projb_sum,
        gain2_sum,
        bias2_sum,
        fc1_out,
        fc1b_sum,
        fc2_out,
        fc2b_sum,
    )


F32 = jnp.float32
BF16 = jnp.bfloat16
NT = (((1,), (1,)), ((), ()))
NN = (((1,), (0,)), ((), ()))
TN = (((0,), (0,)), ((), ()))
VMEM_GRANT = 60 * 2**20
DMA = pltpu.SemaphoreType.DMA
ANY = pl.BlockSpec(memory_space=pl.ANY)
VM = pl.BlockSpec(memory_space=pltpu.VMEM)


def mm(left, right, dims=NN):
    return lax.dot_general(left, right, dims, preferred_element_type=F32)


def lane_ids(shape):
    return lax.broadcasted_iota(jnp.int32, shape, 1)


def place():
    return lax.axis_index("shard"), lax.axis_index("ctx"), lax.axis_index("tp")


def core_mate(t):
    return t + 1 - 2 * lax.rem(t, 2)


def far_mate(t):
    return lax.rem(t + 2, 4)


def send(src, dst, sems, k, where):
    copy = pltpu.make_async_remote_copy(
        src_ref=src,
        dst_ref=dst,
        send_sem=sems.at[0, k],
        recv_sem=sems.at[1, k],
        device_id=where,
        device_id_type=pl.DeviceIdType.MESH,
    )
    copy.start()
    return copy


def greet(shards, line=False):
    s, c, t = place()
    size = 2 * shards
    at = s * (1 - c) + (size - 1 - s) * c
    peers = [{"ctx": 1 - c}, {"tp": core_mate(t)}, {"tp": far_mate(t)}]
    for step in (1, size - 1):
        to = lax.rem(at + step, size)
        back = to // shards
        peers.append({"shard": to * (1 - back) + (size - 1 - to) * back, "ctx": back})
    if line:
        peers += [{"shard": lax.rem(s + d, shards)} for d in range(1, shards)]
    barrier = pltpu.get_barrier_semaphore()
    for peer in peers:
        pl.semaphore_signal(barrier, inc=1, device_id=peer, device_id_type=pl.DeviceIdType.MESH)
    pl.semaphore_wait(barrier, len(peers))


class Ring:
    def __init__(self, shards, block, sems):
        s, c, _ = place()
        self.shards, self.size, self.sems = shards, 2 * shards, sems
        self.at = s * (1 - c) + (self.size - 1 - s) * c
        self.half = block // 2
        self.pieces = ring_pieces(block)
        self.rows = self.half // self.pieces
        self.first, self.end = self.pieces, self.pieces * (self.size - 1)

    def coords(self, position):
        back = position // self.shards
        return position * (1 - back) + (self.size - 1 - position) * back, back

    def peer(self, way):
        to = lax.rem(self.at + (1 if way == 0 else self.size - 1), self.size)
        shard, ctx = self.coords(to)
        return {"shard": shard, "ctx": ctx}

    def owner(self, offset):
        shard, ctx = self.coords(lax.rem(self.at + 2 * self.size + offset, self.size))
        return 2 * shard + ctx

    def split(self, event):
        if isinstance(event, int):
            return event // self.pieces, event % self.pieces
        return lax.div(event, self.pieces), lax.rem(event, self.pieces)

    def rows_of(self, way, piece):
        start = way * self.half + piece * self.rows
        return pl.ds(start if isinstance(start, int) else pl.multiple_of(start, self.rows), self.rows)

    def make(self, src, dst, way, event):
        slot = way * self.end + event
        return pltpu.make_async_remote_copy(
            src_ref=src,
            dst_ref=dst,
            send_sem=self.sems.at[0, slot],
            recv_sem=self.sems.at[1, slot],
            device_id=self.peer(way),
            device_id_type=pl.DeviceIdType.MESH,
        )

    def run(self, low, high):
        low, high = max(low, self.first), min(high, self.end)
        if low < high:
            lax.fori_loop(low, high, lambda event, _: (self.step(event), 0)[1], 0)

    def poll(self, event):
        pl.when(event < self.end)(lambda: self.step(event))


def ring_pieces(block):
    return 5 if block % 160 == 0 else 1


def ring_sems(shards, block):
    return DMA((2, 2 * ring_pieces(block) * (2 * shards - 1)))


class Spread(Ring):
    def __init__(self, shards, src, dst, sems, local):
        super().__init__(shards, src.shape[0], sems)
        self.src, self.dst = src, dst
        self.local = pltpu.make_async_copy(src, dst.at[self.owner(0)], local)
        self.local.start()
        for event in range(self.first):
            for way in range(2):
                self.hop(way, event, True).start()

    def hop(self, way, event, own=False):
        j, piece = self.split(event)
        rows = self.rows_of(way, piece)
        there = self.dst.at[self.owner(-j if way == 0 else j), rows]
        return self.make(self.src.at[rows] if own else there, there, way, event)

    def step(self, event):
        for way in range(2):
            self.hop(way, event - self.pieces).wait_recv()
            self.hop(way, event).start()

    def finish(self):
        self.local.wait()
        for way in range(2):
            for event in range(self.end - self.pieces, self.end):
                self.hop(way, event).wait_recv()

        def sent(event, _):
            for way in range(2):
                self.hop(way, event).wait_send()
            return 0

        lax.fori_loop(0, self.end, sent, 0)

    @staticmethod
    def scratch(shards, block):
        return [ring_sems(shards, block[0]), DMA]


class Collect(Ring):
    def __init__(self, shards, src, held, sems):
        super().__init__(shards, src.shape[0] // (2 * shards), sems)
        self.src, self.held, self.block = src, held, src.shape[0] // (2 * shards)
        for event in range(self.first):
            for way in range(2):
                self.hop(way, event, True).start()

    def own(self, way, j, piece):
        ahead = self.size - 1 - j
        start = self.owner(ahead if way == 0 else -ahead) * self.block + way * self.half + piece * self.rows
        return pl.ds(pl.multiple_of(start, self.rows), self.rows)

    def hop(self, way, event, own=False):
        j, piece = self.split(event)
        rows = self.rows_of(0, piece)
        there = self.held.at[way, j, rows]
        here = self.src.at[self.own(way, j, piece)] if own else self.held.at[way, j - 1, rows]
        return self.make(here, there, way, event)

    def arrived(self, way, event):
        j, piece = self.split(event)
        there = self.held.at[way, j, self.rows_of(0, piece)]
        self.make(there, there, way, event).wait_recv()

    def step(self, event):
        j, piece = self.split(event)
        rows = self.rows_of(0, piece)
        for way in range(2):
            self.arrived(way, event - self.pieces)
            both = self.held[way, j - 1, rows].astype(F32) + self.src[self.own(way, j, piece)].astype(F32)
            self.held[way, j - 1, rows] = both.astype(BF16)
            self.hop(way, event).start()

    def finish(self, out):
        for piece in range(self.pieces):
            for way in range(2):
                self.arrived(way, self.end - self.pieces + piece)
                last = self.held[way, self.size - 2, self.rows_of(0, piece)].astype(F32)
                own = self.src[self.own(way, self.size - 1, piece)].astype(F32)
                out[self.rows_of(way, piece)] = last + own

        def sent(event, _):
            for way in range(2):
                j, piece = self.split(event)
                there = self.held.at[way, j, self.rows_of(0, piece)]
                self.make(there, there, way, event).wait_send()
            return 0

        lax.fori_loop(0, self.end, sent, 0)

    @staticmethod
    def scratch(shards, block):
        return [pltpu.VMEM((2, 2 * shards - 1, block[0] // 2, block[1]), BF16), ring_sems(shards, block[0])]


class Share:
    def __init__(self, full, sems):
        self.full, self.sems, self.copies = full, sems, {}

    def push(self, k, p, src=None):
        _, _, t = place()
        block = self.full.at[p, t]
        src = block if src is None else src
        self.copies[k] = [
            send(src, block, self.sems, 3 * k, {"tp": far_mate(t)}),
            send(src, block, self.sems, 3 * k + 1, {"tp": core_mate(t)}),
        ]

    def forward(self, k, p):
        _, _, t = place()
        self.copies[k][0].wait_recv()
        block = self.full.at[p, far_mate(t)]
        self.copies[k].append(send(block, block, self.sems, 3 * k + 2, {"tp": core_mate(t)}))

    def finish(self, k):
        first, second, third = self.copies[k]
        first.wait_send()
        second.wait()
        third.wait()


class Gather2:
    def __init__(self, part, mate, far, out, sems):
        self.part, self.mate, self.far, self.out, self.sems = part, mate, far, out, sems
        self.first, self.second = {}, {}

    def push(self, p):
        _, _, t = place()
        m = core_mate(t)
        self.first[p] = [
            send(self.part.at[p, far_mate(m)], self.mate.at[p, 1], self.sems, 3 * p, {"tp": m}),
            send(self.part.at[p, m], self.mate.at[p, 0], self.sems, 3 * p + 1, {"tp": m}),
        ]

    def forward(self, p):
        _, _, t = place()
        self.first[p][0].wait_recv()
        both = self.part[p, far_mate(t)].astype(F32) + self.mate[p, 1].astype(F32)
        self.out[p] = both.astype(BF16)
        self.second[p] = send(self.out.at[p], self.far.at[p], self.sems, 3 * p + 2, {"tp": far_mate(t)})

    def result(self, p):
        _, _, t = place()
        self.first[p][1].wait_recv()
        self.second[p].wait_recv()
        return self.part[p, t].astype(F32) + self.mate[p, 0].astype(F32) + self.far[p].astype(F32)

    def finish(self, p):
        for copy in self.first[p]:
            copy.wait_send()
        self.second[p].wait_send()

    @staticmethod
    def scratch(block):
        return [
            pltpu.VMEM((2, 2) + block, BF16),
            pltpu.VMEM((2,) + block, BF16),
            pltpu.VMEM((2,) + block, BF16),
            DMA((2, 6)),
        ]


def ln_stats(values):
    average = jnp.mean(values, -1, keepdims=True)
    centred = values - average
    inverse = lax.rsqrt(jnp.mean(centred * centred, -1, keepdims=True) + EPSILON)
    return centred * inverse, inverse


def ln_back(unit, inverse, gain, grad):
    scaled = grad * gain
    first = jnp.mean(scaled, -1, keepdims=True)
    second = jnp.mean(scaled * unit, -1, keepdims=True)
    return inverse * (scaled - first - unit * second)


def row_tiles(out_ref, left_ref, right_ref, dims, first, count, tile=256):
    def one(i, _):
        at = pl.ds(pl.multiple_of(i * tile, tile), tile)
        out_ref[at, :] = mm(left_ref[at, :], right_ref[...], dims).astype(out_ref.dtype)
        return 0

    lax.fori_loop(first, first + count, one, 0)


def grad_tiles(out_ref, left_ref, right_ref, first, count, cols=slice(None), tile=256):
    def one(i, _):
        at = pl.ds(pl.multiple_of(i * tile, tile), tile)
        out_ref[at, cols] = mm(left_ref[:, at], right_ref[...], TN).astype(out_ref.dtype)
        return 0

    lax.fori_loop(first, first + count, one, 0)


def comm_call(kernel, name, ident, args, outs, scratch, hbm_in=(), hbm_out=()):
    return pl.pallas_call(
        kernel,
        out_shape=tuple(outs),
        in_specs=[ANY if i in hbm_in else VM for i in range(len(args))],
        out_specs=tuple(ANY if i in hbm_out else VM for i in range(len(outs))),
        scratch_shapes=scratch,
        compiler_params=pltpu.CompilerParams(
            vmem_limit_bytes=VMEM_GRANT, collective_id=ident, has_side_effects=True
        ),
        name=name,
    )(*args)


def front_kernel(
    shards, tok_ref, w_ref, gain_ref, bias_ref, x_ref, a_ref, wf_ref, swap_sems, share_sems, w_sems, w_local
):
    s, c, t = place()
    greet(shards)
    swap = send(tok_ref.at[1 - c], x_ref.at[c], swap_sems, 0, {"ctx": 1 - c})
    spread = Spread(shards, w_ref, wf_ref, w_sems, w_local)
    share = Share(a_ref, share_sems)

    def norm(block):
        unit, _ = ln_stats(block.astype(F32))
        return (unit * gain_ref[...] + bias_ref[...]).astype(BF16)

    own = tok_ref[c]
    x_ref[c] = own
    a_ref[c, t] = norm(own)
    share.push(0, c)
    swap.wait()
    a_ref[1 - c, t] = norm(x_ref[1 - c])
    share.push(1, 1 - c)
    spread.run(0, 10)
    share.forward(0, c)
    spread.run(10, 18)
    share.forward(1, 1 - c)
    spread.run(18, spread.end)
    share.finish(0)
    share.finish(1)
    spread.finish()


def fwd_kernel(
    shards, heads, hd, cols, rows, qb,
    qkv_ref, tab_ref, hot_ref, cot_ref, w_ref, pw_ref,
    o_ref, ob_ref, lse_ref, qa_ref, ka_ref, g_ref, cf_ref, wf_ref, pp_ref,
    swap_sems, share_sems, w_sems, w_local,
):
    _, me, t = place()
    greet(shards)
    swap = send(cot_ref.at[1 - me], g_ref.at[me], swap_sems, 0, {"ctx": 1 - me})
    spread = Spread(shards, w_ref, wf_ref, w_sems, w_local)
    share = Share(cf_ref, share_sems)
    own = cot_ref[me]
    g_ref[me] = own
    cf_ref[me, t] = own
    share.push(0, me, cot_ref.at[me])
    tok = qkv_ref.shape[0]
    c = hd**-0.5 * math.log2(math.e)
    up = hd**0.5
    for h in range(heads):
        sl = slice(h * hd, (h + 1) * hd)
        q_sl, k_sl, v_sl = (slice((j * heads + h) * hd, (j * heads + h + 1) * hd) for j in range(3))
        pad = jnp.zeros((tok, 128 - hd), BF16)
        qp = jnp.concatenate([qkv_ref[:, q_sl], pad], 1)
        kp = jnp.concatenate([qkv_ref[:, k_sl], pad], 1)
        vt = jnp.concatenate([qkv_ref[:, v_sl], pad], 1).T
        ka_ref[h, :, 0:128] = jnp.where(lane_ids((tok, 128)) < hd, kp, hot_ref[:, 0:128])
        ka_ref[h, :, 128:256] = hot_ref[:, 128:256]
        terms = mm(qp, tab_ref[...]) * up
        ln = lane_ids((cols, 128))
        for r in range(rows):
            rs = slice(r * cols, (r + 1) * cols)
            tr = pltpu.roll(terms[rs, 0:128], (65 + r) % 128, 1)
            tc = pltpu.roll(terms[rs, 128:256], 65, 1, stride=1, stride_axis=0)
            rh = tr.astype(BF16).astype(F32)
            rl = pltpu.roll(tr - rh, rows, 1)
            ch = tc.astype(BF16).astype(F32)
            cl = pltpu.roll(tc - ch, 64, 1)
            low = jnp.where(ln < hd + 2 * rows, rl, jnp.zeros_like(tr))
            left = jnp.where(ln < hd, qp[rs].astype(F32), jnp.where(ln < hd + rows, rh, low))
            qa_ref[h, rs, 0:128] = left.astype(BF16)
            qa_ref[h, rs, 128:256] = jnp.where(ln < 64, ch, cl).astype(BF16)

        def blk(i, _):
            at = pl.ds(pl.multiple_of(i * qb, qb), qb)
            s = mm(ka_ref[h], qa_ref[h, at, :], NT)
            m = jnp.max(s, 0, keepdims=True)
            p = jnp.exp2((s - m) * c)
            l = jnp.sum(p, 0, keepdims=True)
            o = (mm(vt, p.astype(BF16)) / l).T[:, 0:hd]
            lse_ref[h : h + 1, at] = m * c + jnp.log2(l)
            o_ref[at, sl] = o
            ob_ref[at, sl] = o.astype(BF16)
            for k in range(2):
                spread.poll(spread.first + 2 * (h * (tok // qb) + i) + k)
            return 0

        lax.fori_loop(0, tok // qb, blk, 0)
        if h == 0:
            swap.wait()
            cf_ref[1 - me, t] = g_ref[1 - me]
            share.push(1, 1 - me, g_ref.at[1 - me])
        if h == min(1, heads - 1):
            share.forward(0, me)
        if h == min(2, heads - 1):
            share.forward(1, 1 - me)
    row_tiles(pp_ref, ob_ref, pw_ref, NT, 0, tok // 256)
    spread.run(spread.first + 2 * heads * (tok // qb), spread.end)
    share.finish(0)
    share.finish(1)
    spread.finish()


def mid_kernel(
    shards, part_ref, x_ref, pb_ref, gain_ref, bias_ref, w_ref, f1_ref, fb_ref,
    mid_ref, a_ref, wf_ref, act_ref, slope_ref,
    mate, far, outb, sum_sems, share_sems, w_sems, w_local,
):
    _, _, t = place()
    greet(shards)
    gather = Gather2(part_ref, mate, far, outb, sum_sems)
    gather.push(0)
    gather.push(1)
    spread = Spread(shards, w_ref, wf_ref, w_sems, w_local)
    share = Share(a_ref, share_sems)
    gather.forward(0)
    gather.forward(1)
    for p in range(2):
        spread.run(8 * p, 8 * p + 8)
        mid = x_ref[p].astype(F32) + gather.result(p) + pb_ref[...]
        mid_ref[p] = mid
        unit, _ = ln_stats(mid)
        a_ref[p, t] = (unit * gain_ref[...] + bias_ref[...]).astype(BF16)
        share.push(p, p)
    for p in range(2):
        spread.run(16 + 7 * p, 23 + 7 * p)
        share.forward(p, p)
    half = a_ref.shape[1] * a_ref.shape[2]

    def hidden(p):
        def one(i, _):
            rows = a_ref[p, pl.ds(2 * i, 2)].reshape(-1, a_ref.shape[3])
            pre = mm(rows, f1_ref[...]) + fb_ref[...]
            cdf = 0.5 * (1.0 + lax.erf(pre * (2.0**-0.5)))
            bell = jnp.exp(-0.5 * pre * pre) * ((2.0 * math.pi) ** -0.5)
            at = pl.ds(pl.multiple_of(p * half + i * rows.shape[0], 128), rows.shape[0])
            act_ref[at, :] = (pre * cdf).astype(BF16)
            slope_ref[at, :] = cdf + pre * bell
            return 0

        lax.fori_loop(0, a_ref.shape[1] // 2, one, 0)

    share.finish(0)
    hidden(0)
    spread.run(30, spread.end)
    share.finish(1)
    hidden(1)
    for p in range(2):
        gather.finish(p)
    spread.finish()


def turn_kernel(
    shards, part_ref, mid_ref, g_ref, gain_ref, w_ref, a2_ref, dp_ref, act_ref, f2_ref, pw_ref,
    dm_ref, db_ref, wg_ref, sums_ref, f1g_ref, mlp_ref, do_ref,
    mate, far, outb, sum_sems, share_sems, w_held, w_sems,
):
    _, _, t = place()
    greet(shards)
    gather = Gather2(part_ref, mate, far, outb, sum_sems)
    gather.push(0)
    gather.push(1)
    collect = Collect(shards, w_ref, w_held, w_sems)
    share = Share(db_ref, share_sems)
    gather.forward(0)
    gather.forward(1)
    rows = [jnp.zeros((1, mid_ref.shape[2]), F32) for _ in range(4)]
    grads = f1g_ref.shape[0] // 256
    tiles = mlp_ref.shape[0] // 256
    grad_tiles(f1g_ref, a2_ref, dp_ref, 0, grads // 2)
    for p in range(2):
        collect.run(8 * p, 8 * p + 8)
        unit, inverse = ln_stats(mid_ref[p])
        g = g_ref[p].astype(F32)
        da = gather.result(p)
        dm = g + ln_back(unit, inverse, gain_ref[...], da)
        dm_ref[p] = dm
        low = dm.astype(BF16)
        db_ref[p, t] = low
        share.push(p, p)
        for k, term in enumerate((da * unit, da, low.astype(F32), g)):
            rows[k] = rows[k] + jnp.sum(term, 0, keepdims=True)
        if p == 0:
            grad_tiles(f1g_ref, a2_ref, dp_ref, grads // 2, grads - grads // 2)
    for k in range(4):
        sums_ref[k : k + 1, :] = rows[k]
    for p in range(2):
        row_tiles(mlp_ref, act_ref, f2_ref, NT, p * tiles // 2, tiles // 2)
        collect.run(16 + 7 * p, 23 + 7 * p)
        share.forward(p, p)
    collect.run(30, collect.end)
    group = db_ref.shape[1] * db_ref.shape[2]
    for p in range(2):
        gather.finish(p)
        share.finish(p)

        def one(i, _):
            rows = db_ref[p, pl.ds(2 * i, 2)].reshape(-1, db_ref.shape[3])
            at = pl.ds(pl.multiple_of(p * group + i * rows.shape[0], 128), rows.shape[0])
            do_ref[at, :] = mm(rows, pw_ref[...]).astype(BF16)
            return 0

        lax.fori_loop(0, db_ref.shape[1] // 2, one, 0)
    collect.finish(wg_ref)


def bwd_kernel(
    shards, heads, hd, cols, rows, qb,
    qa_ref, ka_ref, qkv_ref, do_ref, o_ref, lse_ref, tab_ref, hot_ref, part_ref, mid_ref, fb_ref, w_ref,
    a1_ref, db_ref, ob_ref, w1_ref,
    rg_ref, out_ref, wg_ref, da_ref, w1g_ref, qs_ref,
    dqkv_ref,
    kt_ref, acc_k, acc_v, del_ref, res_ref, mate, far, outb, sum_sems, swap_sems, w_held, w_sems,
):
    _, me, _ = place()
    greet(shards)
    gather = Gather2(part_ref, mate, far, outb, sum_sems)
    gather.push(0)
    gather.push(1)
    collect = Collect(shards, w_ref, w_held, w_sems)
    gather.forward(0)
    gather.forward(1)
    tok = qkv_ref.shape[0]
    scale = hd**-0.5
    c = scale * math.log2(math.e)
    rg_ref[...] = jnp.zeros_like(rg_ref)
    for h in range(heads):
        sl = slice(h * hd, (h + 1) * hd)
        k_sl, v_sl = (slice((j * heads + h) * hd, (j * heads + h + 1) * hd) for j in (1, 2))
        pad = jnp.zeros((tok, 128 - hd), BF16)
        vp = jnp.concatenate([qkv_ref[:, v_sl], pad], 1)
        kt_ref[0:128, :] = jnp.where(lane_ids((tok, 128)) < hd, ka_ref[h, :, 0:128], hot_ref[:, 0:128]).T
        kt_ref[128:256, :] = hot_ref[:, 128:256].T
        prod = jnp.concatenate([do_ref[:, sl].astype(F32) * o_ref[:, sl], pad.astype(F32)], 1)
        del_ref[...] = lax.dot_general(
            jnp.ones((8, 128), F32), prod, NT, preferred_element_type=F32, precision=PRECISE
        )
        acc_k[...] = jnp.zeros_like(acc_k)
        acc_v[...] = jnp.zeros_like(acc_v)

        def blk(i, _):
            at = pl.ds(pl.multiple_of(i * qb, qb), qb)
            qblk = qa_ref[h, at, :]
            dob = jnp.concatenate([do_ref[at, sl], jnp.zeros((qb, 128 - hd), BF16)], 1)
            s = mm(ka_ref[h], qblk, NT)
            p = jnp.exp2(s * c - lse_ref[h : h + 1, at])
            dp = mm(vp, dob, NT)
            ds = (p * (dp - del_ref[0:1, at])).astype(BF16)
            acc_v[...] += mm(p.astype(BF16), dob)
            acc_k[...] += mm(ds, qblk[:, 0:128])
            dqa = mm(kt_ref[...], ds).T
            ln = lane_ids((cols, 128))
            parts = []
            for j in range(qb // cols):
                r = i * (qb // cols) + j
                js = slice(j * cols, (j + 1) * cols)
                dr = dqa[js, 0:128]
                dr = jnp.where((ln >= hd) & (ln < hd + rows), dr, 0.0)
                dr = pltpu.roll(dr, (48 + r) % 128, 1)
                dc = pltpu.roll(dqa[js, 128:256], 0, 1, stride=1, stride_axis=0)
                parts.append(jnp.concatenate([dr, dc], 1))
            d = jnp.concatenate(parts, 0).astype(BF16)
            rel = mm(d, tab_ref[...])
            rg_ref[...] += mm(d, qblk[:, 0:128], TN)
            dqkv_ref[at, sl] = (scale * dqa[:, 0:128] + rel)[:, 0:hd].astype(BF16)
            for k in range(2):
                collect.poll(collect.first + 2 * (h * (tok // qb) + i) + k)
            return 0

        lax.fori_loop(0, tok // qb, blk, 0)
        dqkv_ref[:, k_sl] = (scale * acc_k[...])[:, 0:hd].astype(BF16)
        dqkv_ref[:, v_sl] = acc_v[...][:, 0:hd].astype(BF16)
        if h == min(2, heads - 1):
            for p in range(2):
                total = mid_ref[p] + gather.result(p) + fb_ref[...]
                res_ref[p] = total.astype(BF16)
            swap = send(res_ref.at[1 - me], out_ref.at[me], swap_sems, 0, {"ctx": 1 - me})
            out_ref[me] = res_ref[me]
    wide = dqkv_ref.shape[1]
    for i in range(tok // 256):
        at = slice(i * 256, (i + 1) * 256)
        da_ref[at, :] = mm(dqkv_ref[at, :], w1_ref[:, 0:wide], NT).astype(BF16)
    collect.run(collect.first + 2 * heads * (tok // qb), collect.end)
    grads = w1g_ref.shape[0] // 256
    grad_tiles(w1g_ref, a1_ref, dqkv_ref, 0, grads, slice(0, wide))
    grad_tiles(w1g_ref, db_ref, ob_ref, 0, grads, slice(wide, w1g_ref.shape[1]))
    qs_ref[...] = jnp.sum(dqkv_ref[...].astype(F32), 0, keepdims=True)
    for p in range(2):
        gather.finish(p)
    collect.finish(wg_ref)
    swap.wait()


def end_kernel(
    shards, part_ref, x_ref, dm_ref, gain_ref, w_ref, small_ref, out_ref, wg_ref, total_ref,
    res_ref, mate, far, outb, sum_sems, swap_sems, held, got, line, small_sems, w_held, w_sems,
):
    s, me, t = place()
    greet(shards, True)
    gather = Gather2(part_ref, mate, far, outb, sum_sems)
    gather.push(0)
    gather.push(1)
    collect = Collect(shards, w_ref, w_held, w_sems)
    gather.forward(0)
    gather.forward(1)
    first = jnp.zeros((1, x_ref.shape[2]), F32)
    second = jnp.zeros((1, x_ref.shape[2]), F32)
    for p in range(2):
        collect.run(8 * p, 8 * p + 8)
        unit, inverse = ln_stats(x_ref[p].astype(F32))
        da = gather.result(p)
        res_ref[p] = (dm_ref[p] + ln_back(unit, inverse, gain_ref[...], da)).astype(BF16)
        first = first + jnp.sum(da * unit, 0, keepdims=True)
        second = second + jnp.sum(da, 0, keepdims=True)
    swap = send(res_ref.at[1 - me], out_ref.at[me], swap_sems, 0, {"ctx": 1 - me})
    out_ref[me] = res_ref[me]
    held[0] = small_ref[...]
    held[0, 0:1, :] = first
    held[0, 1:2, :] = second
    waits = []
    for k, peer in enumerate(({"tp": core_mate(t)}, {"tp": far_mate(t)}, {"ctx": 1 - me})):
        copy = send(held.at[k], got.at[k], small_sems, k, peer)
        collect.run(16 + 4 * k, 20 + 4 * k)
        copy.wait_recv()
        waits.append(copy)
        held[k + 1] = held[k] + got[k]
    line[s] = held[3]
    for d in range(1, shards):
        waits.append(send(held.at[3], line.at[s], small_sems, 2 + d, {"shard": lax.rem(s + d, shards)}))
    collect.run(28, collect.end)
    collect.finish(wg_ref)
    for k, copy in enumerate(waits):
        if k < 3:
            copy.wait_send()
        else:
            copy.wait()
    acc = line[0]
    for k in range(1, shards):
        acc = acc + line[k]
    total_ref[...] = acc
    for p in range(2):
        gather.finish(p)
    swap.wait()


def position_tables(rel_rows, rel_cols, hd):
    gap = 128 - hd
    rr = jnp.pad(rel_rows, ((0, 128 - rel_rows.shape[0]), (0, gap)))
    rc = jnp.pad(rel_cols, ((0, 128 - rel_cols.shape[0]), (0, gap)))
    fr = jnp.pad(rel_rows[::-1], ((0, 128 - rel_rows.shape[0]), (0, gap)))
    fc = jnp.pad(rel_cols[::-1], ((0, 128 - rel_cols.shape[0]), (0, gap)))
    return jnp.concatenate([fr, fc], 0).T, jnp.concatenate([rr, rc], 0)


def position_hots(tok, hd, cols, rows):
    kr = jnp.arange(rows, dtype=jnp.int32)[:, None]
    kw = jnp.arange(cols, dtype=jnp.int32)[:, None]
    l = jnp.arange(256, dtype=jnp.int32)[None, :]
    first_r = (l == hd + kr) | (l == hd + rows + kr)
    first_c = (l == 128 + kw) | (l == 192 + kw)
    second_r = l == hd + rows - 1 - kr
    second_c = l == 128 + cols - 1 - kw

    def both(r, c):
        return (r[:, None, :] | c[None, :, :]).astype(BF16).reshape(tok, 256)

    return both(first_r, first_c), both(second_r, second_c)


def on_device_images(
    tokens, norm1_gain, norm1_bias, qkv_weight, qv_bias, rel_rows, rel_cols, proj_weight, proj_bias,
    norm2_gain, norm2_bias, fc1_weight, fc1_bias, fc2_weight, fc2_bias, cotangent,
):
    S = jax.ShapeDtypeStruct
    shards = lax.axis_size("shard")
    tp_count = lax.axis_size("tp")
    tp_rank = lax.axis_index("tp")
    heads = H // tp_count
    width = heads * HD
    ff = FF // tp_count
    rows = (rel_rows.shape[0] + 1) // 2
    tok = rows * COLS
    own = tokens.shape
    piece = own[1:]
    full = (2, tp_count) + piece
    block = fc1_weight.shape
    blocks = (2 * shards,) + block
    qkv_cols = 3 * width
    w1 = jnp.concatenate([qkv_weight[0], qkv_weight[1], qkv_weight[2], proj_weight.T], 1)
    fc2_t = fc2_weight.T
    qv_local = lax.dynamic_slice_in_dim(qv_bias, tp_rank * width, width, 1)
    qkv_bias = jnp.concatenate([qv_local[0], jnp.zeros((width,), F32), qv_local[1]])
    fc1_local = lax.dynamic_slice_in_dim(fc1_bias, tp_rank * ff, ff, 0)
    tab_f, tab_b = position_tables(rel_rows, rel_cols, HD)
    hot_f, hot_b = position_hots(tok, HD, COLS, rows)
    spread = Spread.scratch(shards, block)
    collect = Collect.scratch(shards, block)
    gather = Gather2.scratch(piece)
    swap = [DMA((2, 1))]
    share = [DMA((2, 6))]

    def row(vec):
        return vec.reshape(1, -1)

    x, a1, w1_full = comm_call(
        partial(front_kernel, shards), "front", 0,
        (tokens, w1, row(norm1_gain), row(norm1_bias)),
        (S(own, BF16), S(full, BF16), S(blocks, BF16)),
        swap + share + spread, hbm_in=(1,), hbm_out=(2,),
    )
    a1 = a1.reshape(tok, D)
    w1_full = w1_full.reshape(D, -1)
    qkv_full = w1_full[:, :qkv_cols]
    proj_full = w1_full[:, qkv_cols:]
    qkv = (mm(a1, qkv_full) + qkv_bias).astype(BF16)
    o, o_low, lse, qa, ka, g, cot, fc1_full, proj_part = comm_call(
        partial(fwd_kernel, shards, heads, HD, COLS, rows, 256), "attn_fwd", 1,
        (qkv, tab_f, hot_f, cotangent, fc1_weight, proj_full),
        (
            S((tok, width), F32), S((tok, width), BF16), S((heads, tok), F32),
            S((heads, tok, 256), BF16), S((heads, tok, 256), BF16),
            S(own, BF16), S(full, BF16), S(blocks, BF16), S((tok, D), BF16),
        ),
        swap + share + spread, hbm_in=(4,), hbm_out=(7,),
    )
    fc1_full = fc1_full.reshape(D, ff)
    cot = cot.reshape(tok, D)
    proj_part = proj_part.reshape(full)
    mid, a2, fc2_full, act, slope = comm_call(
        partial(mid_kernel, shards), "mid", 2,
        (proj_part, x, row(proj_bias), row(norm2_gain), row(norm2_bias), fc2_t, fc1_full, row(fc1_local)),
        (S(own, F32), S(full, BF16), S(blocks, BF16), S((tok, ff), BF16), S((tok, ff), F32)),
        gather + share + spread, hbm_in=(5,), hbm_out=(2,),
    )
    a2 = a2.reshape(tok, D)
    fc2_full = fc2_full.reshape(D, ff)
    d_pre = (mm(cot, fc2_full) * slope).astype(BF16)
    d_a2 = mm(d_pre, fc1_full, NT).astype(BF16).reshape(full)
    fc2_grad = mm(cot, act, TN).astype(BF16)
    d_mid, d_branch, fc2_own, sums, fc1_grad, mlp_part, d_o = comm_call(
        partial(turn_kernel, shards), "turn", 3,
        (d_a2, mid, g, row(norm2_gain), fc2_grad, a2, d_pre, act, fc2_full, proj_full),
        (
            S(own, F32), S(full, BF16), S(block, F32), S((4, D), F32),
            S((D, ff), BF16), S((tok, D), BF16), S((tok, width), BF16),
        ),
        gather + share + collect,
    )
    d_branch = d_branch.reshape(tok, D)
    mlp_part = mlp_part.reshape(full)
    rel_grad, output, fc1_own, d_a1, w1_grad, qkv_sum = comm_call(
        partial(bwd_kernel, shards, heads, HD, COLS, rows, 256), "attn_bwd", 4,
        (qa, ka, qkv, d_o, o, lse, tab_b, hot_b, mlp_part, mid, row(fc2_bias), fc1_grad, a1, d_branch, o_low, w1_full),
        (
            S((256, 128), F32), S(own, BF16), S(block, F32),
            S((tok, D), BF16), S((D, qkv_cols + width), BF16), S((1, qkv_cols), F32),
        ),
        [
            pltpu.VMEM((tok, qkv_cols), BF16), pltpu.VMEM((256, tok), BF16), pltpu.VMEM((tok, 128), F32), pltpu.VMEM((tok, 128), F32),
            pltpu.VMEM((8, tok), F32), pltpu.VMEM(own, BF16),
        ] + gather + swap + collect,
    )
    d_a1 = d_a1.reshape(full)
    qkv_sum = qkv_sum[0]
    qv_part = jnp.stack([qkv_sum[:width], qkv_sum[2 * width :]])
    qv_placed = lax.dynamic_update_slice_in_dim(jnp.zeros((2, D), F32), qv_part, tp_rank * width, 1)
    fc1_sum = jnp.sum(d_pre.astype(F32), 0)
    fc1_placed = lax.dynamic_update_slice_in_dim(jnp.zeros((FF,), F32), fc1_sum, tp_rank * ff, 0)
    terms = (
        jnp.zeros((2 * D,), F32),
        qv_placed.reshape(-1),
        fc1_placed,
        sums.reshape(-1),
        rel_grad[: rel_rows.shape[0], :HD].reshape(-1),
        rel_grad[128 : 128 + rel_cols.shape[0], :HD].reshape(-1),
    )
    count = sum(term.shape[0] for term in terms)
    lines = -(-count // (8 * D)) * 8
    packed = jnp.concatenate(terms + (jnp.zeros((lines * D - count,), F32),)).reshape(lines, D)
    tokens_grad, w1_own, total = comm_call(
        partial(end_kernel, shards), "end", 5,
        (d_a1, x, d_mid, row(norm1_gain), w1_grad, packed),
        (S(own, BF16), S(block, F32), S((lines, D), F32)),
        [pltpu.VMEM(own, BF16)] + gather + swap
        + [
            pltpu.VMEM((4, lines, D), F32), pltpu.VMEM((3, lines, D), F32),
            pltpu.VMEM((shards, lines, D), F32), DMA((2, 2 + shards)),
        ]
        + collect,
    )
    flat = total.reshape(-1)
    base = 4 * D + FF
    rel_at = base + 4 * D
    rel_mid = rel_at + rel_rows.size
    return (
        output,
        tokens_grad,
        total[0],
        total[1],
        jnp.stack([w1_own[:, j * width : (j + 1) * width] for j in range(3)]),
        total[2:4],
        flat[rel_at:rel_mid].reshape(rel_rows.shape),
        flat[rel_mid : rel_mid + rel_cols.size].reshape(rel_cols.shape),
        w1_own[:, qkv_cols:].T,
        flat[base + 2 * D : base + 3 * D],
        flat[base : base + D],
        flat[base + D : base + 2 * D],
        fc1_own,
        flat[4 * D : base],
        fc2_own.T,
        flat[base + 3 * D : base + 4 * D],
    )


def solution(mesh):
    in_specs = (
        P("shard", ("ctx", "tp"), None),
        P(),
        P(),
        P(None, ("shard", "ctx"), "tp"),
        P(),
        P(),
        P(),
        P("tp", ("shard", "ctx")),
        P(),
        P(),
        P(),
        P(("shard", "ctx"), "tp"),
        P(),
        P("tp", ("shard", "ctx")),
        P(),
        P("shard", ("ctx", "tp"), None),
    )
    out_specs = (
        P("shard", ("ctx", "tp"), None),
        P("shard", ("ctx", "tp"), None),
        P(),
        P(),
        P(None, ("shard", "ctx"), "tp"),
        P(),
        P(),
        P(),
        P("tp", ("shard", "ctx")),
        P(),
        P(),
        P(),
        P(("shard", "ctx"), "tp"),
        P(),
        P("tp", ("shard", "ctx")),
        P(),
    )
    def on_device(*arrays):
        rows = (arrays[5].shape[0] + 1) // 2
        fits = mesh.shape["tp"] == 4 and mesh.shape["ctx"] == 2 and HD + 2 * rows <= 128
        fits = fits and arrays[0].shape[0] == mesh.shape["ctx"] and arrays[6].shape[0] <= 128
        return (on_device_images if fits else on_device_rows)(*arrays)

    return jax.shard_map(
        on_device, mesh=mesh, in_specs=in_specs, out_specs=out_specs, check_vma=False
    )
```

```python
from functools import partial
import math

import jax
import jax.numpy as jnp
from jax import lax
from jax.experimental import pallas as pl
from jax.experimental.pallas import tpu as pltpu
from jax.sharding import PartitionSpec as P

D = 1280
H = 16
HD = 80
FF = 5120
COLS = 64
ROWS_DEV = 8


PRECISE = lax.Precision.HIGHEST
EPSILON = 1e-06
NEGATIVE = -1e30


def layer_norm(values_in, gain_vec, shift_vec):
    average = jnp.mean(values_in, -1, keepdims=True)
    centred = values_in - average
    variance = jnp.mean(centred * centred, -1, keepdims=True)
    return centred * lax.rsqrt(variance + EPSILON) * gain_vec + shift_vec


def block_size():
    return 512


def to_heads(flat_rows, heads_local):
    images, length, feat_width = flat_rows.shape
    return flat_rows.reshape(images, length, heads_local, feat_width // heads_local).transpose(
        0, 2, 1, 3
    )


def from_heads(per_head):
    images, heads_local, length, head_dim = per_head.shape
    return per_head.transpose(0, 2, 1, 3).reshape(images, length, heads_local * head_dim)


def block_scores(query_heads, key_flat, rows_bias, cols_bias, first_key, scale_factor):
    key_heads = to_heads(key_flat, query_heads.shape[1])
    key_len = key_flat.shape[1]
    key_rows = key_len // COLS
    scores = scale_factor * jnp.einsum(
        "ihqc,ihkc->ihqk", query_heads, key_heads, preferred_element_type=jnp.float32
    )
    images, heads_local, query_len, unused_len = scores.shape
    row_part = lax.dynamic_slice_in_dim(rows_bias, first_key // COLS, key_rows, 3)
    scores = scores.reshape(images, heads_local, query_len, key_rows, COLS)
    scores = scores + row_part[..., :, None] + cols_bias[..., None, :]
    return scores.reshape(images, heads_local, query_len, key_len)


def relative_terms(query_flat, rows_param, cols_param, first_row, heads_local):
    images, length, feat_width = query_flat.shape
    rows_dev = length // COLS
    grid_rows = (rows_param.shape[0] + 1) // 2
    own_rows = first_row + jnp.arange(rows_dev, dtype=jnp.int32)
    key_rows = jnp.arange(grid_rows, dtype=jnp.int32)
    row_slots = jnp.arange(rows_param.shape[0], dtype=jnp.int32)
    pick_rows = (
        row_slots[None, None, :]
        == own_rows[:, None, None] - key_rows[None, :, None] + grid_rows - 1
    ).astype(jnp.float32)
    table_rows = jnp.einsum("rkj,jc->rkc", pick_rows, rows_param, precision=PRECISE)
    col_ids = jnp.arange(COLS, dtype=jnp.int32)
    col_slots = jnp.arange(cols_param.shape[0], dtype=jnp.int32)
    pick_cols = (
        col_slots[None, None, :] == col_ids[:, None, None] - col_ids[None, :, None] + COLS - 1
    ).astype(jnp.float32)
    table_cols = jnp.einsum("wkj,jc->wkc", pick_cols, cols_param, precision=PRECISE)
    grid_form = query_flat.reshape(images, rows_dev, COLS, heads_local, feat_width // heads_local)
    along_rows = jnp.einsum("irwhc,rkc->ihrwk", grid_form, table_rows, precision=PRECISE).reshape(
        images, heads_local, length, grid_rows
    )
    along_cols = jnp.einsum("irwhc,wkc->ihrwk", grid_form, table_cols, precision=PRECISE).reshape(
        images, heads_local, length, COLS
    )
    return (along_rows, along_cols)


def on_device_rows(
    tokens,
    norm1_gain,
    norm1_bias,
    qkv_weight,
    qv_bias,
    rel_rows,
    rel_cols,
    proj_weight,
    proj_bias,
    norm2_gain,
    norm2_bias,
    fc1_weight,
    fc1_bias,
    fc2_weight,
    fc2_bias,
    cotangent,
):
    scale_factor = HD ** (-0.5)
    tp_count = lax.axis_size("tp")
    ctx_count = lax.axis_size("ctx")
    tp_rank = lax.axis_index("tp")
    ctx_rank = lax.axis_index("ctx")
    grid_rows = ROWS_DEV * ctx_count
    tok_image = grid_rows * COLS
    tok_ctx = ROWS_DEV * COLS
    heads_local = H // tp_count
    width_local = heads_local * HD
    ff_local = FF // tp_count
    images = tokens.shape[0]
    rows_table = rel_rows.astype(jnp.float32)
    cols_table = rel_cols.astype(jnp.float32)
    qkv_full, proj_full, fc1_full, fc2_full = (
        lax.all_gather(qkv_weight, ("shard", "ctx"), axis=1, tiled=True),
        lax.all_gather(proj_weight, ("shard", "ctx"), axis=1, tiled=True),
        lax.all_gather(fc1_weight, ("shard", "ctx"), axis=0, tiled=True),
        lax.all_gather(fc2_weight, ("shard", "ctx"), axis=1, tiled=True),
    )
    qv_local = lax.dynamic_slice_in_dim(qv_bias, tp_rank * width_local, width_local, 1)
    fc1_local = lax.dynamic_slice_in_dim(fc1_bias, tp_rank * ff_local, ff_local, 0)
    resid_in = tokens.astype(jnp.float32)
    normed1 = layer_norm(resid_in, norm1_gain, norm1_bias).astype(jnp.bfloat16)
    normed1_full = lax.all_gather(normed1, "tp", axis=1, tiled=True)
    projected = jnp.einsum(
        "itd,sde->itse", normed1_full, qkv_full, preferred_element_type=jnp.float32
    )
    queries = (projected[:, :, 0] + qv_local[0]).astype(jnp.bfloat16)
    keys_own = projected[:, :, 1].astype(jnp.bfloat16)
    values_own = (projected[:, :, 2] + qv_local[1]).astype(jnp.bfloat16)
    first_row = ctx_rank * ROWS_DEV
    rel_fn = partial(relative_terms, first_row=first_row, heads_local=heads_local)
    (along_rows, along_cols), rel_pull = jax.vjp(
        rel_fn, queries.astype(jnp.float32), rows_table, cols_table
    )
    query_heads = to_heads(queries, heads_local)
    start_state = (
        jnp.full((images, heads_local, tok_ctx), NEGATIVE, jnp.float32),
        jnp.zeros((images, heads_local, tok_ctx), jnp.float32),
        jnp.zeros((images, heads_local, tok_ctx, HD), jnp.float32),
        jnp.zeros((images, tok_image, width_local), jnp.bfloat16),
        jnp.zeros((images, tok_image, width_local), jnp.bfloat16),
    )
    shard_piece = (
        lax.all_gather(keys_own, "ctx", axis=1, tiled=True),
        lax.all_gather(values_own, "ctx", axis=1, tiled=True),
    )
    piece_len = shard_piece[0].shape[1]
    step_len = block_size()

    def one_step(inner, offset):
        run_max, run_sum, run_acc, keys_all, values_all = inner
        key_blk = lax.dynamic_slice_in_dim(shard_piece[0], offset, step_len, 1)
        value_blk = lax.dynamic_slice_in_dim(shard_piece[1], offset, step_len, 1)
        scores = block_scores(query_heads, key_blk, along_rows, along_cols, offset, scale_factor)
        new_max = jnp.maximum(run_max, jnp.max(scores, -1))
        factor = jnp.exp(run_max - new_max)
        weights_blk = jnp.exp(scores - new_max[..., None])
        run_sum = run_sum * factor + jnp.sum(weights_blk, -1)
        value_heads = to_heads(value_blk, heads_local)
        run_acc = run_acc * factor[..., None] + jnp.einsum(
            "ihqk,ihkc->ihqc",
            weights_blk.astype(jnp.bfloat16),
            value_heads,
            preferred_element_type=jnp.float32,
        )
        keys_all = lax.dynamic_update_slice_in_dim(keys_all, key_blk, offset, 1)
        values_all = lax.dynamic_update_slice_in_dim(values_all, value_blk, offset, 1)
        return ((new_max, run_sum, run_acc, keys_all, values_all), None)

    offsets = jnp.arange(piece_len // step_len, dtype=jnp.int32) * step_len
    result, unused = lax.scan(one_step, start_state, offsets)
    run_max, run_sum, run_acc, keys_all, values_all = result
    attn_heads = run_acc / run_sum[..., None]
    log_total = run_max + jnp.log(run_sum)
    attn_low = from_heads(attn_heads).astype(jnp.bfloat16)
    proj_part = jnp.einsum("itd,de->ite", attn_low, proj_full, preferred_element_type=jnp.float32)
    branch = lax.psum_scatter(
        proj_part.astype(jnp.bfloat16), "tp", scatter_dimension=1, tiled=True
    ).astype(jnp.float32)
    middle = resid_in + branch + proj_bias
    normed2 = layer_norm(middle, norm2_gain, norm2_bias).astype(jnp.bfloat16)
    normed2_full = lax.all_gather(normed2, "tp", axis=1, tiled=True)
    hidden_pre = (
        jnp.einsum("itd,df->itf", normed2_full, fc1_full, preferred_element_type=jnp.float32)
        + fc1_local
    )
    gelu_exact = partial(jax.nn.gelu, approximate=False)
    activated_f, gelu_pull = jax.vjp(gelu_exact, hidden_pre)
    activated = activated_f.astype(jnp.bfloat16)
    mlp_part = jnp.einsum("itf,fe->ite", activated, fc2_full, preferred_element_type=jnp.float32)
    mlp_out = lax.psum_scatter(
        mlp_part.astype(jnp.bfloat16), "tp", scatter_dimension=1, tiled=True
    ).astype(jnp.float32)
    output = (middle + mlp_out + fc2_bias).astype(jnp.bfloat16)
    cot_full = lax.all_gather(cotangent, "tp", axis=1, tiled=True)
    d_act = jnp.einsum("ite,fe->itf", cot_full, fc2_full, preferred_element_type=jnp.float32)
    d_hidden = gelu_pull(d_act)[0].astype(jnp.bfloat16)
    fc2_grad = jnp.einsum("itf,ite->fe", activated, cot_full, preferred_element_type=jnp.float32)
    fc1_grad = jnp.einsum("itd,itf->df", normed2_full, d_hidden, preferred_element_type=jnp.float32)
    fc1_bias_part = jnp.sum(d_hidden.astype(jnp.float32), (0, 1))
    fc2_bias_part = jnp.sum(cotangent.astype(jnp.float32), (0, 1))
    d_norm2_part = jnp.einsum("itf,df->itd", d_hidden, fc1_full, preferred_element_type=jnp.float32)
    d_norm2 = lax.psum_scatter(
        d_norm2_part.astype(jnp.bfloat16), "tp", scatter_dimension=1, tiled=True
    ).astype(jnp.float32)
    unused_out, norm2_pull = jax.vjp(layer_norm, middle, norm2_gain, norm2_bias)
    d_mid_part, gain2_part, bias2_part = norm2_pull(d_norm2)
    d_middle = cotangent.astype(jnp.float32) + d_mid_part
    d_branch = d_middle.astype(jnp.bfloat16)
    proj_bias_part = jnp.sum(d_branch.astype(jnp.float32), (0, 1))
    d_branch_full = lax.all_gather(d_branch, "tp", axis=1, tiled=True)
    proj_grad = jnp.einsum(
        "itd,ite->de", attn_low, d_branch_full, preferred_element_type=jnp.float32
    )
    d_attn = jnp.einsum(
        "ite,de->itd", d_branch_full, proj_full, preferred_element_type=jnp.float32
    ).astype(jnp.bfloat16)
    d_attn_heads = to_heads(d_attn, heads_local)
    delta_rows = jnp.sum(d_attn_heads.astype(jnp.float32) * attn_heads, -1)
    key_step = block_size()
    key_rows = key_step // COLS
    key_offsets = jnp.arange(tok_image // key_step, dtype=jnp.int32) * key_step

    def back_step(carried, offset):
        grad_query, grad_rows, grad_cols = carried
        key_blk = lax.dynamic_slice_in_dim(keys_all, offset, key_step, 1)
        value_blk = lax.dynamic_slice_in_dim(values_all, offset, key_step, 1)
        scores = block_scores(query_heads, key_blk, along_rows, along_cols, offset, scale_factor)
        soft_probs = jnp.exp(scores - log_total[..., None])
        value_heads = to_heads(value_blk, heads_local)
        key_heads = to_heads(key_blk, heads_local)
        d_probs = jnp.einsum(
            "ihqc,ihkc->ihqk", d_attn_heads, value_heads, preferred_element_type=jnp.float32
        )
        d_scores = (soft_probs * (d_probs - delta_rows[..., None])).astype(jnp.bfloat16)
        grad_query = grad_query + jnp.einsum(
            "ihqk,ihkc->ihqc", d_scores, key_heads, preferred_element_type=jnp.float32
        )
        grid_scores = d_scores.astype(jnp.float32).reshape(
            images, heads_local, tok_ctx, key_rows, COLS
        )
        row_sums = jnp.sum(grid_scores, 4)
        row_now = lax.dynamic_slice_in_dim(grad_rows, offset // COLS, key_rows, 3)
        grad_rows = lax.dynamic_update_slice_in_dim(
            grad_rows, row_now + row_sums, offset // COLS, 3
        )
        grad_cols = grad_cols + jnp.sum(grid_scores, 3)
        key_part = scale_factor * jnp.einsum(
            "ihqk,ihqc->ikhc", d_scores, query_heads, preferred_element_type=jnp.float32
        )
        value_part = jnp.einsum(
            "ihqk,ihqc->ikhc",
            soft_probs.astype(jnp.bfloat16),
            d_attn_heads,
            preferred_element_type=jnp.float32,
        )
        emitted = (
            key_part.reshape(images, key_step, width_local),
            value_part.reshape(images, key_step, width_local),
        )
        return ((grad_query, grad_rows, grad_cols), emitted)

    back_start = (
        jnp.zeros((images, heads_local, tok_ctx, HD), jnp.float32),
        jnp.zeros((images, heads_local, tok_ctx, grid_rows), jnp.float32),
        jnp.zeros((images, heads_local, tok_ctx, COLS), jnp.float32),
    )
    (grad_query, grad_rows, grad_cols), emitted = lax.scan(back_step, back_start, key_offsets)
    key_terms = emitted[0].transpose(1, 0, 2, 3).reshape(images, tok_image, width_local)
    value_terms = emitted[1].transpose(1, 0, 2, 3).reshape(images, tok_image, width_local)
    grad_keys, grad_values = (
        lax.psum_scatter(
            key_terms.astype(jnp.bfloat16), "ctx", scatter_dimension=1, tiled=True
        ).astype(jnp.float32),
        lax.psum_scatter(
            value_terms.astype(jnp.bfloat16), "ctx", scatter_dimension=1, tiled=True
        ).astype(jnp.float32),
    )
    d_query_rel, rows_grad_part, cols_grad_part = rel_pull((grad_rows, grad_cols))
    d_query = (scale_factor * from_heads(grad_query) + d_query_rel).astype(jnp.bfloat16)
    d_keys = grad_keys.astype(jnp.bfloat16)
    d_values = grad_values.astype(jnp.bfloat16)
    d_projected = jnp.stack((d_query, d_keys, d_values), axis=2)
    qkv_grad = jnp.einsum(
        "itd,itse->sde", normed1_full, d_projected, preferred_element_type=jnp.float32
    )
    qv_bias_part = jnp.stack(
        (
            jnp.sum(d_query.astype(jnp.float32), (0, 1)),
            jnp.sum(d_values.astype(jnp.float32), (0, 1)),
        )
    )
    d_norm1_part = jnp.einsum(
        "itse,sde->itd", d_projected, qkv_full, preferred_element_type=jnp.float32
    )
    d_norm1 = lax.psum_scatter(
        d_norm1_part.astype(jnp.bfloat16), "tp", scatter_dimension=1, tiled=True
    ).astype(jnp.float32)
    unused_in, norm1_pull = jax.vjp(layer_norm, resid_in, norm1_gain, norm1_bias)
    d_in_part, gain1_part, bias1_part = norm1_pull(d_norm1)
    tokens_grad = (d_middle + d_in_part).astype(jnp.bfloat16)
    qkv_out, proj_out, fc1_out, fc2_out = (
        lax.psum_scatter(
            qkv_grad.astype(jnp.bfloat16), ("shard", "ctx"), scatter_dimension=1, tiled=True
        ).astype(jnp.float32),
        lax.psum_scatter(
            proj_grad.astype(jnp.bfloat16), ("shard", "ctx"), scatter_dimension=1, tiled=True
        ).astype(jnp.float32),
        lax.psum_scatter(
            fc1_grad.astype(jnp.bfloat16), ("shard", "ctx"), scatter_dimension=0, tiled=True
        ).astype(jnp.float32),
        lax.psum_scatter(
            fc2_grad.astype(jnp.bfloat16), ("shard", "ctx"), scatter_dimension=1, tiled=True
        ).astype(jnp.float32),
    )
    qv_placed = lax.dynamic_update_slice_in_dim(
        jnp.zeros((2, D), jnp.float32), qv_bias_part, tp_rank * width_local, 1
    )
    fc1_placed = lax.dynamic_update_slice_in_dim(
        jnp.zeros((FF,), jnp.float32), fc1_bias_part, tp_rank * ff_local, 0
    )
    (
        gain1_sum,
        bias1_sum,
        qv_sum,
        rows_sum,
        cols_sum,
        projb_sum,
        gain2_sum,
        bias2_sum,
        fc1b_sum,
        fc2b_sum,
    ) = lax.psum(
        (
            gain1_part,
            bias1_part,
            qv_placed,
            rows_grad_part,
            cols_grad_part,
            proj_bias_part,
            gain2_part,
            bias2_part,
            fc1_placed,
            fc2_bias_part,
        ),
        ("shard", "ctx", "tp"),
    )
    return (
        output,
        tokens_grad,
        gain1_sum,
        bias1_sum,
        qkv_out,
        qv_sum,
        rows_sum,
        cols_sum,
        proj_out,
        projb_sum,
        gain2_sum,
        bias2_sum,
        fc1_out,
        fc1b_sum,
        fc2_out,
        fc2b_sum,
    )


F32 = jnp.float32
BF16 = jnp.bfloat16
NT = (((1,), (1,)), ((), ()))
NN = (((1,), (0,)), ((), ()))
TN = (((0,), (0,)), ((), ()))
VMEM_GRANT = 60 * 2**20
DMA = pltpu.SemaphoreType.DMA
ANY = pl.BlockSpec(memory_space=pl.ANY)
VM = pl.BlockSpec(memory_space=pltpu.VMEM)


def mm(left, right, dims=NN):
    return lax.dot_general(left, right, dims, preferred_element_type=F32)


def lane_ids(shape):
    return lax.broadcasted_iota(jnp.int32, shape, 1)


def place():
    return lax.axis_index("shard"), lax.axis_index("ctx"), lax.axis_index("tp")


def core_mate(t):
    return t + 1 - 2 * lax.rem(t, 2)


def far_mate(t):
    return lax.rem(t + 2, 4)


def send(src, dst, sems, k, where):
    copy = pltpu.make_async_remote_copy(
        src_ref=src,
        dst_ref=dst,
        send_sem=sems.at[0, k],
        recv_sem=sems.at[1, k],
        device_id=where,
        device_id_type=pl.DeviceIdType.MESH,
    )
    copy.start()
    return copy


def swap_copy(src, dst, sems):
    _, c, _ = place()
    return pltpu.make_async_remote_copy(
        src_ref=src,
        dst_ref=dst,
        send_sem=sems.at[0, 0],
        recv_sem=sems.at[1, 0],
        device_id={"ctx": 1 - c},
        device_id_type=pl.DeviceIdType.MESH,
    )


def reverser(top):
    down = lax.broadcasted_iota(jnp.int32, (128, 128), 0)
    return jnp.where(down + lane_ids((128, 128)) == top, 1.0, 0.0).astype(BF16)


def greet(shards, line=False):
    s, c, t = place()
    size = 2 * shards
    at = s * (1 - c) + (size - 1 - s) * c
    peers = [{"ctx": 1 - c}, {"tp": core_mate(t)}, {"tp": far_mate(t)}]
    for step in (1, size - 1):
        to = lax.rem(at + step, size)
        back = to // shards
        peers.append({"shard": to * (1 - back) + (size - 1 - to) * back, "ctx": back})
    if line:
        peers += [{"shard": lax.rem(s + d, shards)} for d in range(1, shards)]
    barrier = pltpu.get_barrier_semaphore()
    for peer in peers:
        pl.semaphore_signal(barrier, inc=1, device_id=peer, device_id_type=pl.DeviceIdType.MESH)
    pl.semaphore_wait(barrier, len(peers))


class Ring:
    def __init__(self, shards, block, sems):
        s, c, _ = place()
        self.shards, self.size, self.sems = shards, 2 * shards, sems
        self.at = s * (1 - c) + (self.size - 1 - s) * c
        self.half = block // 2
        self.pieces = ring_pieces(block)
        self.rows = self.half // self.pieces
        self.first, self.end = self.pieces, self.pieces * (self.size - 1)
        self.now = self.first

    def coords(self, position):
        back = position // self.shards
        return position * (1 - back) + (self.size - 1 - position) * back, back

    def peer(self, way):
        to = lax.rem(self.at + (1 if way == 0 else self.size - 1), self.size)
        shard, ctx = self.coords(to)
        return {"shard": shard, "ctx": ctx}

    def owner(self, offset):
        shard, ctx = self.coords(lax.rem(self.at + 2 * self.size + offset, self.size))
        return 2 * shard + ctx

    def split(self, event):
        if isinstance(event, int):
            return event // self.pieces, event % self.pieces
        return lax.div(event, self.pieces), lax.rem(event, self.pieces)

    def rows_of(self, way, piece):
        start = way * self.half + piece * self.rows
        return pl.ds(start if isinstance(start, int) else pl.multiple_of(start, self.rows), self.rows)

    def make(self, src, dst, way, event):
        slot = way * self.end + event
        return pltpu.make_async_remote_copy(
            src_ref=src,
            dst_ref=dst,
            send_sem=self.sems.at[0, slot],
            recv_sem=self.sems.at[1, slot],
            device_id=self.peer(way),
            device_id_type=pl.DeviceIdType.MESH,
        )

    def run(self, low, high):
        low, high = max(low, self.first), min(high, self.end)
        if low < high:
            lax.fori_loop(low, high, lambda event, _: (self.step(event), 0)[1], 0)

    def tick(self, count):
        self.run(self.now, self.now + count)
        self.now += count

    def poll(self, event):
        pl.when(event < self.end)(lambda: self.step(event))


def ring_pieces(block):
    return 5 if block % 160 == 0 else 1


def ring_sems(shards, block):
    return DMA((2, 2 * ring_pieces(block) * (2 * shards - 1)))


class Spread(Ring):
    def __init__(self, shards, src, dst, sems, local):
        super().__init__(shards, src.shape[0], sems)
        self.src, self.dst = src, dst
        self.local = pltpu.make_async_copy(src, dst.at[self.owner(0)], local)
        self.local.start()
        for event in range(self.first):
            for way in range(2):
                self.hop(way, event, True).start()

    def hop(self, way, event, own=False):
        j, piece = self.split(event)
        rows = self.rows_of(way, piece)
        there = self.dst.at[self.owner(-j if way == 0 else j), rows]
        return self.make(self.src.at[rows] if own else there, there, way, event)

    def step(self, event):
        for way in range(2):
            self.hop(way, event - self.pieces).wait_recv()
            self.hop(way, event).start()

    def finish(self):
        self.local.wait()
        for way in range(2):
            for event in range(self.end - self.pieces, self.end):
                self.hop(way, event).wait_recv()

        def sent(event, _):
            for way in range(2):
                self.hop(way, event).wait_send()
            return 0

        lax.fori_loop(0, self.end, sent, 0)

    @staticmethod
    def scratch(shards, block):
        return [ring_sems(shards, block[0]), DMA]


class Collect(Ring):
    def __init__(self, shards, src, held, sems):
        super().__init__(shards, src.shape[0] // (2 * shards), sems)
        self.src, self.held, self.block = src, held, src.shape[0] // (2 * shards)

    def begin(self):
        for event in range(self.first):
            for way in range(2):
                self.hop(way, event, True).start()

    def block_rows(self, offset):
        return pl.ds(pl.multiple_of(self.owner(offset) * self.block, self.rows), self.block)

    def order(self):
        near = [(-k, k) for k in range(1, self.size // 2)]
        return near + [(self.size // 2, 0)]

    def own(self, way, j, piece):
        ahead = self.size - 1 - j
        start = self.owner(ahead if way == 0 else -ahead) * self.block + way * self.half + piece * self.rows
        return pl.ds(pl.multiple_of(start, self.rows), self.rows)

    def hop(self, way, event, own=False):
        j, piece = self.split(event)
        rows = self.rows_of(0, piece)
        there = self.held.at[way, j, rows]
        here = self.src.at[self.own(way, j, piece)] if own else self.held.at[way, j - 1, rows]
        return self.make(here, there, way, event)

    def arrived(self, way, event):
        j, piece = self.split(event)
        there = self.held.at[way, j, self.rows_of(0, piece)]
        self.make(there, there, way, event).wait_recv()

    def step(self, event):
        j, piece = self.split(event)
        rows = self.rows_of(0, piece)
        for way in range(2):
            self.arrived(way, event - self.pieces)
            both = self.held[way, j - 1, rows].astype(F32) + self.src[self.own(way, j, piece)].astype(F32)
            self.held[way, j - 1, rows] = both.astype(BF16)
            self.hop(way, event).start()

    def finish(self, out):
        for piece in range(self.pieces):
            for way in range(2):
                self.arrived(way, self.end - self.pieces + piece)
                last = self.held[way, self.size - 2, self.rows_of(0, piece)].astype(F32)
                own = self.src[self.own(way, self.size - 1, piece)].astype(F32)
                out[self.rows_of(way, piece)] = last + own

        def sent(event, _):
            for way in range(2):
                j, piece = self.split(event)
                there = self.held.at[way, j, self.rows_of(0, piece)]
                self.make(there, there, way, event).wait_send()
            return 0

        lax.fori_loop(0, self.end, sent, 0)

    @staticmethod
    def scratch(shards, block):
        return [pltpu.VMEM((2, 2 * shards - 1, block[0] // 2, block[1]), BF16), ring_sems(shards, block[0])]


class Share:
    def __init__(self, full, sems):
        self.full, self.sems, self.copies = full, sems, {}

    def push(self, k, p, src=None):
        _, _, t = place()
        block = self.full.at[p, t]
        src = block if src is None else src
        passed = self.full.at[p, far_mate(t)]
        self.copies[k] = [
            send(src, block, self.sems, 3 * k, {"tp": far_mate(t)}),
            send(src, block, self.sems, 3 * k + 1, {"tp": core_mate(t)}),
            pltpu.make_async_remote_copy(
                src_ref=passed,
                dst_ref=passed,
                send_sem=self.sems.at[0, 3 * k + 2],
                recv_sem=self.sems.at[1, 3 * k + 2],
                device_id={"tp": core_mate(t)},
                device_id_type=pl.DeviceIdType.MESH,
            ),
        ]

    def forward(self, k, p):
        self.copies[k][0].wait_recv()
        self.copies[k][2].start()

    def finish(self, k):
        first, second, third = self.copies[k]
        first.wait_send()
        second.wait()
        third.wait()


class Gather2:
    def __init__(self, part, mate, far, out, sems):
        self.part, self.mate, self.far, self.out, self.sems = part, mate, far, out, sems
        self.first, self.second = {}, {}

    def push(self, p):
        _, _, t = place()
        m = core_mate(t)
        self.first[p] = [
            send(self.part.at[p, far_mate(m)], self.mate.at[p, 1], self.sems, 3 * p, {"tp": m}),
            send(self.part.at[p, m], self.mate.at[p, 0], self.sems, 3 * p + 1, {"tp": m}),
        ]

    def forward(self, p):
        _, _, t = place()
        self.first[p][0].wait_recv()
        both = self.part[p, far_mate(t)].astype(F32) + self.mate[p, 1].astype(F32)
        self.out[p] = both.astype(BF16)
        self.second[p] = send(self.out.at[p], self.far.at[p], self.sems, 3 * p + 2, {"tp": far_mate(t)})

    def result(self, p):
        _, _, t = place()
        self.first[p][1].wait_recv()
        self.second[p].wait_recv()
        return self.part[p, t].astype(F32) + self.mate[p, 0].astype(F32) + self.far[p].astype(F32)

    def finish(self, p):
        for copy in self.first[p]:
            copy.wait_send()
        self.second[p].wait_send()

    @staticmethod
    def scratch(block):
        return [
            pltpu.VMEM((2, 2) + block, BF16),
            pltpu.VMEM((2,) + block, BF16),
            pltpu.VMEM((2,) + block, BF16),
            DMA((2, 6)),
        ]


def ln_stats(values):
    average = jnp.mean(values, -1, keepdims=True)
    centred = values - average
    inverse = lax.rsqrt(jnp.mean(centred * centred, -1, keepdims=True) + EPSILON)
    return centred * inverse, inverse


def ln_back(unit, inverse, gain, grad):
    scaled = grad * gain
    first = jnp.mean(scaled, -1, keepdims=True)
    second = jnp.mean(scaled * unit, -1, keepdims=True)
    return inverse * (scaled - first - unit * second)


def row_tiles(out_ref, left_ref, right_ref, dims, first, count, tile=256):
    def one(i, _):
        at = pl.ds(pl.multiple_of(i * tile, tile), tile)
        out_ref[at, :] = mm(left_ref[at, :], right_ref[...], dims).astype(out_ref.dtype)
        return 0

    lax.fori_loop(first, first + count, one, 0)


def grad_tiles(out_ref, left_ref, right_ref, first, count, cols=slice(None), tile=256):
    def one(i, _):
        at = pl.ds(pl.multiple_of(i * tile, tile), tile)
        out_ref[at, cols] = mm(left_ref[:, at], right_ref[...], TN).astype(out_ref.dtype)
        return 0

    lax.fori_loop(first, first + count, one, 0)


def comm_call(kernel, name, ident, args, outs, scratch, hbm_in=(), hbm_out=()):
    return pl.pallas_call(
        kernel,
        out_shape=tuple(outs),
        in_specs=[ANY if i in hbm_in else VM for i in range(len(args))],
        out_specs=tuple(ANY if i in hbm_out else VM for i in range(len(outs))),
        scratch_shapes=scratch,
        compiler_params=pltpu.CompilerParams(
            vmem_limit_bytes=VMEM_GRANT, collective_id=ident, has_side_effects=True
        ),
        name=name,
    )(*args)


def turned(out_ref, full_ref, p, ring=None):
    count, length = full_ref.shape[1:3]
    for i in range(count):
        start = (p * count + i) * length
        out_ref[:, pl.ds(start if isinstance(start, int) else pl.multiple_of(start, 128), length)] = full_ref[p, i].T
        if ring is not None and i % 2 == 1:
            ring.tick(1)


def front_kernel(
    shards, tok_ref, qkvw_ref, pw_ref, vec_ref, x_ref, a_ref, wf_ref, at_ref,
    w1_ref, swap_sems, share_sems, w_sems, w_local,
):
    s, c, t = place()
    wide = qkvw_ref.shape[2]
    for j in range(3):
        w1_ref[:, j * wide : (j + 1) * wide] = qkvw_ref[j]
    w1_ref[:, 3 * wide : 4 * wide] = pw_ref[...]
    greet(shards)
    swap = send(tok_ref.at[1 - c], x_ref.at[c], swap_sems, 0, {"ctx": 1 - c})
    spread = Spread(shards, w1_ref, wf_ref, w_sems, w_local)
    share = Share(a_ref, share_sems)

    def norm(block):
        unit, _ = ln_stats(block.astype(F32))
        return (unit * vec_ref[0:1, :] + vec_ref[1:2, :]).astype(BF16)

    own = tok_ref[c]
    x_ref[c] = own
    a_ref[c, t] = norm(own)
    share.push(0, c)
    swap.wait()
    a_ref[1 - c, t] = norm(x_ref[1 - c])
    share.push(1, 1 - c)
    share.forward(0, c)
    spread.tick(9)
    share.forward(1, 1 - c)
    spread.tick(6)
    share.finish(0)
    share.finish(1)
    turned(at_ref, a_ref, 0, spread)
    spread.tick(4)
    turned(at_ref, a_ref, 1, spread)
    spread.tick(spread.end)
    spread.finish()


def fwd_kernel(
    shards, heads, hd, cols, rows, qb,
    a1_ref, w1_ref, vec_ref, tab_ref, hot_ref, cot_ref, w_ref,
    vh_ref, oh_ref, ob_ref, lse_ref, qa_ref, ka_ref, g_ref, cf_ref, wf_ref, pp_ref,
    qh_ref, vt_ref, rt_ref, swap_sems, share_sems, w_sems, w_local,
):
    _, me, t = place()
    tok, width = ob_ref.shape
    wide = 3 * width
    blocks = tok // qb
    rt_ref[0:128, :] = mm(reverser(2 * rows - 2), tab_ref[0:128, :]).astype(BF16)
    rt_ref[128:256, :] = mm(reverser(2 * cols - 2), tab_ref[128:256, :]).astype(BF16)
    greet(shards)
    spread = Spread(shards, w_ref, wf_ref, w_sems, w_local)
    share = Share(cf_ref, share_sems)
    own = cot_ref[me]
    g_ref[me] = own
    cf_ref[0, t] = own
    share.push(0, 0, cot_ref.at[me])
    swap = swap_copy(cot_ref.at[1 - me], g_ref.at[me], swap_sems)

    def project(i, _):
        at = pl.ds(pl.multiple_of(i * qb, qb), qb)
        tile = (mm(a1_ref[at, :], w1_ref[:, 0:wide]) + vec_ref[7:8, 0:wide]).astype(BF16)
        pad = jnp.zeros((qb, 128 - hd), BF16)
        front = lane_ids((qb, 128)) < hd
        for h in range(heads):
            part = [tile[:, (j * heads + h) * hd : (j * heads + h + 1) * hd] for j in range(3)]
            part = [jnp.concatenate([x, pad], 1) for x in part]
            qh_ref[h, at, :] = part[0]
            ka_ref[h, at, 0:128] = jnp.where(front, part[1], hot_ref[at, 0:128])
            ka_ref[h, at, 128:256] = hot_ref[at, 128:256]
            vh_ref[h, at, :] = part[2]
        for k in range(2):
            spread.poll(spread.first + 2 * i + k)
        return 0

    lax.fori_loop(0, blocks, project, 0)
    c = hd**-0.5 * math.log2(math.e)
    up = hd**0.5

    def head(h, _):
        vt_ref[...] = vh_ref[h].T
        terms = mm(qh_ref[h], rt_ref[...], NT) * up
        ln = lane_ids((cols, 128))
        for r in range(rows):
            rs = slice(r * cols, (r + 1) * cols)
            tr = pltpu.roll(terms[rs, 0:128], (65 + r) % 128, 1)
            tc = pltpu.roll(terms[rs, 128:256], 65, 1, stride=1, stride_axis=0)
            rh = tr.astype(BF16).astype(F32)
            rl = pltpu.roll(tr - rh, rows, 1)
            ch = tc.astype(BF16).astype(F32)
            cl = pltpu.roll(tc - ch, 64, 1)
            low = jnp.where(ln < hd + 2 * rows, rl, jnp.zeros_like(tr))
            left = jnp.where(ln < hd, qh_ref[h, rs, :].astype(F32), jnp.where(ln < hd + rows, rh, low))
            qa_ref[h, rs, 0:128] = left.astype(BF16)
            qa_ref[h, rs, 128:256] = jnp.where(ln < 64, ch, cl).astype(BF16)

        def blk(i, _):
            at = pl.ds(pl.multiple_of(i * qb, qb), qb)
            s = mm(ka_ref[h], qa_ref[h, at, :], NT)
            m = jnp.max(s, 0, keepdims=True)
            p = jnp.exp2((s - m) * c)
            l = jnp.sum(p, 0, keepdims=True)
            lse_ref[h, :, at] = m * c + jnp.log2(l)
            oh_ref[h, at, :] = (mm(vt_ref[...], p.astype(BF16)) / l).T
            for k in range(2):
                spread.poll(spread.first + 2 * ((h + 1) * blocks + i) + k)
            return 0

        lax.fori_loop(0, blocks, blk, 0)
        pl.when(h == 1)(lambda: share.forward(0, 0))
        pl.when(h == min(2, heads - 1))(swap.start)
        return 0

    lax.fori_loop(0, heads, head, 0)
    for h in range(heads):
        ob_ref[:, h * hd : (h + 1) * hd] = oh_ref[h, :, 0:hd].astype(BF16)
    for i in range(tok // 256):
        at = slice(i * 256, (i + 1) * 256)
        pp_ref[at, :] = mm(ob_ref[at, :], w1_ref[:, wide:], NT).astype(BF16)
    spread.run(spread.first + 2 * (heads + 1) * blocks, spread.end)
    share.finish(0)
    spread.finish()
    swap.wait()


def mid_kernel(
    shards, part_ref, x_ref, vec_ref, w_ref, f1_ref, g_ref, c0_ref,
    mid_ref, a_ref, wf_ref, act_ref, slope_ref, cf_ref, ct_ref,
    mate, far, outb, sum_sems, share_sems, cot_sems, cot_local, w_sems, w_local,
):
    _, me, t = place()
    greet(shards)
    gather = Gather2(part_ref, mate, far, outb, sum_sems)
    gather.push(0)
    gather.push(1)
    spread = Spread(shards, w_ref, wf_ref, w_sems, w_local)
    share = Share(a_ref, share_sems)
    kept = pltpu.make_async_copy(c0_ref.at[0], cf_ref.at[me], cot_local)
    kept.start()
    cots = Share(cf_ref, cot_sems)
    gather.forward(0)
    gather.forward(1)
    cf_ref[1 - me, t] = g_ref[1 - me]
    kept.wait()
    turned(ct_ref, cf_ref, me, spread)
    spread.tick(6)
    for p in range(2):
        mid = x_ref[p].astype(F32) + gather.result(p) + vec_ref[2:3, :]
        mid_ref[p] = mid
        unit, _ = ln_stats(mid)
        a_ref[p, t] = (unit * vec_ref[3:4, :] + vec_ref[4:5, :]).astype(BF16)
        share.push(p, p)
        if p == 1:
            cots.push(0, 1 - me, g_ref.at[1 - me])
        spread.tick(7)
    share.forward(0, 0)
    half = a_ref.shape[1] * a_ref.shape[2]

    def hidden(p):
        def one(i, _):
            rows = a_ref[p, pl.ds(2 * i, 2)].reshape(-1, a_ref.shape[3])
            pre = mm(rows, f1_ref[...]) + vec_ref[6:7, :]
            cdf = 0.5 * (1.0 + lax.erf(pre * (2.0**-0.5)))
            bell = jnp.exp(-0.5 * pre * pre) * ((2.0 * math.pi) ** -0.5)
            at = pl.ds(pl.multiple_of(p * half + i * rows.shape[0], 128), rows.shape[0])
            act_ref[at, :] = (pre * cdf).astype(BF16)
            slope_ref[at, :] = cdf + pre * bell
            for k in range(2):
                spread.poll(base + 2 * i + k)
            return 0

        base = spread.now
        lax.fori_loop(0, a_ref.shape[1] // 2, one, 0)
        spread.now += a_ref.shape[1]

    share.finish(0)
    hidden(0)
    spread.tick(spread.end)
    share.forward(1, 1)
    share.finish(1)
    hidden(1)
    cots.forward(0, 1 - me)
    cots.finish(0)
    turned(ct_ref, cf_ref, 1 - me)
    for p in range(2):
        gather.finish(p)
    spread.finish()


def turn_kernel(
    shards, ct_ref, act_ref, slope_ref, cot_ref, f2_ref, f1_ref, a2_ref, mid_ref, g_ref, vec_ref, w1_ref,
    dm_ref, db_ref, dbt_ref, wg_ref, sums_ref, f1g_ref, mlp_ref, do_ref,
    w2g_ref, part_ref, dp_ref, mate, far, outb, sum_sems, share_sems, w_held, w_sems,
):
    _, _, t = place()
    greet(shards)
    collect = Collect(shards, w2g_ref, w_held, w_sems)

    def grad_blocks(pair):
        for offset in pair:
            at = collect.block_rows(offset)
            w2g_ref[at, :] = mm(ct_ref[at, :], act_ref[...]).astype(BF16)

    order = collect.order()
    grad_blocks(order[0])
    collect.begin()
    gather = Gather2(part_ref, mate, far, outb, sum_sems)
    share = Share(db_ref, share_sems)
    group = db_ref.shape[1] * db_ref.shape[2]
    tile = 2 * db_ref.shape[2]
    sums_ref[...] = jnp.zeros_like(sums_ref)
    left = list(order[1:])
    halves = db_ref.shape[1] // 2

    def back(n, base):
        p, i = n // halves, n % halves
        at = pl.ds(pl.multiple_of(n * tile, tile), tile)
        d_pre = (mm(cot_ref[at, :], f2_ref[...]) * slope_ref[at, :]).astype(BF16)
        dp_ref[at, :] = d_pre
        sums_ref[4:5, :] += jnp.sum(d_pre.astype(F32), 0, keepdims=True)
        collect.poll(base + 2 * n)
        d_a2 = mm(d_pre, f1_ref[...], NT).astype(BF16)
        part_ref[p, pl.ds(2 * i, 2)] = d_a2.reshape(2, tile // 2, -1)
        collect.poll(base + 2 * n + 1)
        return base

    for n in range(2 * halves):
        if left:
            grad_blocks(left.pop(0))
        lax.fori_loop(n, n + 1, back, jnp.int32(collect.now - 2 * n))
        collect.now += 2
        collect.tick(1)
        if n == halves - 1:
            gather.push(0)
        if n == halves:
            gather.forward(0)
    for pair in left:
        grad_blocks(pair)
    gather.push(1)
    collect.tick(2)
    gather.forward(1)
    grads = f1g_ref.shape[0] // 256
    tiles = mlp_ref.shape[0] // 256
    for p in range(2):
        low, high = (0, grads // 2) if p == 0 else (grads // 2, grads)
        for i in range(low, high):
            grad_tiles(f1g_ref, a2_ref, dp_ref, i, 1)
            collect.tick(1)
        if p == 1:
            collect.tick(2)
        unit, inverse = ln_stats(mid_ref[p])
        g = g_ref[p].astype(F32)
        da = gather.result(p)
        dm = g + ln_back(unit, inverse, vec_ref[3:4, :], da)
        dm_ref[p] = dm
        low_dm = dm.astype(BF16)
        db_ref[p, t] = low_dm
        share.push(p, p)
        for k, term in enumerate((da * unit, da, low_dm.astype(F32), g)):
            sums_ref[k : k + 1, :] += jnp.sum(term, 0, keepdims=True)
        collect.tick(1)
    for p in range(2):
        for i in range(tiles // 2):
            row_tiles(mlp_ref, act_ref, f2_ref, NT, p * tiles // 2 + i, 1)
            collect.tick(2)
        if p == 1:
            collect.tick(collect.end)
        share.forward(p, p)
    wide = do_ref.shape[1]
    for p in range(2):
        gather.finish(p)
        share.finish(p)
        turned(dbt_ref, db_ref, p)
        for i in range(db_ref.shape[1] // 2):
            rows = db_ref[p, 2 * i : 2 * i + 2].reshape(tile, -1)
            at = slice(p * group + i * tile, p * group + (i + 1) * tile)
            do_ref[at, :] = mm(rows, w1_ref[:, 3 * wide :]).astype(BF16)
    collect.finish(wg_ref)


def bwd_kernel(
    shards, heads, hd, cols, rows, qb,
    qa_ref, ka_ref, vh_ref, do_ref, oh_ref, lse_ref, tab_ref, hot_ref, part_ref, mid_ref, vec_ref, w_ref, w1_ref,
    dqkv_ref, rg_ref, out_ref, wg_ref, da_ref, qs_ref,
    doh_ref, dh_ref, kt_ref, acc_k, acc_v, del_ref, res_ref,
    mate, far, outb, sum_sems, swap_sems, w_held, w_sems,
):
    _, me, _ = place()
    greet(shards)
    gather = Gather2(part_ref, mate, far, outb, sum_sems)
    gather.push(0)
    gather.push(1)
    collect = Collect(shards, w_ref, w_held, w_sems)
    collect.begin()
    tok, wide = dqkv_ref.shape
    blocks = tok // qb
    for h in range(heads):
        pad = jnp.zeros((tok, 128 - hd), BF16)
        doh_ref[h] = jnp.concatenate([do_ref[:, h * hd : (h + 1) * hd], pad], 1)
    gather.forward(0)
    gather.forward(1)
    swap = swap_copy(res_ref.at[1 - me], out_ref.at[me], swap_sems)
    scale = hd**-0.5
    c = scale * math.log2(math.e)
    rg_ref[...] = jnp.zeros_like(rg_ref)

    def head(h, _):
        kt_ref[0:128, :] = jnp.where(lane_ids((tok, 128)) < hd, ka_ref[h, :, 0:128], hot_ref[:, 0:128]).T
        kt_ref[128:256, :] = hot_ref[:, 128:256].T
        del_ref[...] = lax.dot_general(
            jnp.ones((8, 128), F32), doh_ref[h].astype(F32) * oh_ref[h], NT,
            preferred_element_type=F32, precision=PRECISE,
        )
        acc_k[...] = jnp.zeros_like(acc_k)
        acc_v[...] = jnp.zeros_like(acc_v)

        def blk(i, _):
            at = pl.ds(pl.multiple_of(i * qb, qb), qb)
            qblk = qa_ref[h, at, :]
            dob = doh_ref[h, at, :]
            s = mm(ka_ref[h], qblk, NT)
            p = jnp.exp2(s * c - lse_ref[h, :, at])
            dp = mm(vh_ref[h], dob, NT)
            ds = (p * (dp - del_ref[0:1, at])).astype(BF16)
            acc_v[...] += mm(p.astype(BF16), dob)
            acc_k[...] += mm(ds, qblk[:, 0:128])
            dqa = mm(kt_ref[...], ds).T
            ln = lane_ids((cols, 128))
            parts = []
            for j in range(qb // cols):
                r = i * (qb // cols) + j
                js = slice(j * cols, (j + 1) * cols)
                dr = dqa[js, 0:128]
                dr = jnp.where((ln >= hd) & (ln < hd + rows), dr, 0.0)
                dr = pltpu.roll(dr, lax.rem(48 + r, 128), 1)
                dc = pltpu.roll(dqa[js, 128:256], 0, 1, stride=1, stride_axis=0)
                parts.append(jnp.concatenate([dr, dc], 1))
            d = jnp.concatenate(parts, 0).astype(BF16)
            rel = mm(d, tab_ref[...])
            rg_ref[...] += mm(d, qblk[:, 0:128], TN)
            dh_ref[h, at, :] = (scale * dqa[:, 0:128] + rel).astype(BF16)
            for k in range(2):
                collect.poll(collect.first + 2 * (h * blocks + i) + k)
            return 0

        lax.fori_loop(0, blocks, blk, 0)
        dh_ref[heads + h] = (scale * acc_k[...]).astype(BF16)
        dh_ref[2 * heads + h] = acc_v[...].astype(BF16)

        @pl.when(h == min(2, heads - 1))
        def _():
            for p in range(2):
                total = mid_ref[p] + gather.result(p) + vec_ref[5:6, :]
                res_ref[p] = total.astype(BF16)
            swap.start()

        return 0

    lax.fori_loop(0, heads, head, 0)
    out_ref[me] = res_ref[me]
    for j in range(3 * heads):
        dqkv_ref[:, j * hd : (j + 1) * hd] = dh_ref[j, :, 0:hd]
    for i in range(tok // 256):
        at = slice(i * 256, (i + 1) * 256)
        da_ref[at, :] = mm(dqkv_ref[at, :], w1_ref[:, 0:wide], NT).astype(BF16)
    collect.run(collect.first + 2 * heads * blocks, collect.end)
    qs_ref[...] = jnp.sum(dqkv_ref[...].astype(F32), 0, keepdims=True)
    for p in range(2):
        gather.finish(p)
    collect.finish(wg_ref)
    swap.wait()


def end_kernel(
    shards, part_ref, x_ref, dm_ref, vec_ref, at_ref, dqkv_ref, dbt_ref, ob_ref, small_ref,
    out_ref, wg_ref, total_ref,
    w1g_ref, res_ref, mate, far, outb, sum_sems, swap_sems, held, got, line, small_sems, w_held, w_sems,
):
    s, me, t = place()
    greet(shards, True)
    gather = Gather2(part_ref, mate, far, outb, sum_sems)
    gather.push(0)
    gather.push(1)
    collect = Collect(shards, w1g_ref, w_held, w_sems)
    wide = dqkv_ref.shape[1]

    def grad_blocks(pair):
        for offset in pair:
            at = collect.block_rows(offset)
            w1g_ref[at, 0:wide] = mm(at_ref[at, :], dqkv_ref[...]).astype(BF16)
            w1g_ref[at, wide:] = mm(dbt_ref[at, :], ob_ref[...]).astype(BF16)

    order = collect.order()
    grad_blocks(order[0])
    collect.begin()
    gather.forward(0)
    gather.forward(1)
    for pair in order[1:]:
        grad_blocks(pair)
        collect.tick(2)
    first = jnp.zeros((1, x_ref.shape[2]), F32)
    second = jnp.zeros((1, x_ref.shape[2]), F32)
    for p in range(2):
        collect.tick(3 + 3 * p)
        unit, inverse = ln_stats(x_ref[p].astype(F32))
        da = gather.result(p)
        res_ref[p] = (dm_ref[p] + ln_back(unit, inverse, vec_ref[0:1, :], da)).astype(BF16)
        first = first + jnp.sum(da * unit, 0, keepdims=True)
        second = second + jnp.sum(da, 0, keepdims=True)
    swap = send(res_ref.at[1 - me], out_ref.at[me], swap_sems, 0, {"ctx": 1 - me})
    out_ref[me] = res_ref[me]
    held[0] = small_ref[...]
    held[0, 0:1, :] = first
    held[0, 1:2, :] = second
    waits = []
    for k, peer in enumerate(({"tp": core_mate(t)}, {"tp": far_mate(t)}, {"ctx": 1 - me})):
        copy = send(held.at[k], got.at[k], small_sems, k, peer)
        collect.tick(3)
        copy.wait_recv()
        waits.append(copy)
        held[k + 1] = held[k] + got[k]
    line[s] = held[3]
    for d in range(1, shards):
        waits.append(send(held.at[3], line.at[s], small_sems, 2 + d, {"shard": lax.rem(s + d, shards)}))
    collect.tick(collect.end)
    collect.finish(wg_ref)
    for k, copy in enumerate(waits):
        if k < 3:
            copy.wait_send()
        else:
            copy.wait()
    acc = line[0]
    for k in range(1, shards):
        acc = acc + line[k]
    total_ref[...] = acc
    for p in range(2):
        gather.finish(p)
    swap.wait()


def position_table(rel_rows, rel_cols, hd):
    rr = jnp.pad(rel_rows, ((0, 128 - rel_rows.shape[0]), (0, 128 - hd)))
    rc = jnp.pad(rel_cols, ((0, 128 - rel_cols.shape[0]), (0, 128 - hd)))
    return jnp.concatenate([rr, rc], 0)


def position_hots(tok, hd, cols, rows):
    kr = jnp.arange(rows, dtype=jnp.int32)[:, None]
    kw = jnp.arange(cols, dtype=jnp.int32)[:, None]
    l = jnp.arange(256, dtype=jnp.int32)[None, :]
    first_r = (l == hd + kr) | (l == hd + rows + kr)
    first_c = (l == 128 + kw) | (l == 192 + kw)
    second_r = l == hd + rows - 1 - kr
    second_c = l == 128 + cols - 1 - kw

    def both(r, c):
        return (r[:, None, :] | c[None, :, :]).astype(BF16).reshape(tok, 256)

    return both(first_r, first_c), both(second_r, second_c)


def on_device_images(
    tokens, norm1_gain, norm1_bias, qkv_weight, qv_bias, rel_rows, rel_cols, proj_weight, proj_bias,
    norm2_gain, norm2_bias, fc1_weight, fc1_bias, fc2_weight, fc2_bias, cotangent,
):
    S = jax.ShapeDtypeStruct
    shards = lax.axis_size("shard")
    tp_count = lax.axis_size("tp")
    tp_rank = lax.axis_index("tp")
    heads = H // tp_count
    width = heads * HD
    ff = FF // tp_count
    rows = (rel_rows.shape[0] + 1) // 2
    tok = rows * COLS
    own = tokens.shape
    piece = own[1:]
    full = (2, tp_count) + piece
    block = fc1_weight.shape
    blocks = (2 * shards,) + block
    qkv_cols = 3 * width
    fc2_t = fc2_weight.T
    qv_local = lax.dynamic_slice_in_dim(qv_bias, tp_rank * width, width, 1)
    qkv_bias = jnp.concatenate([qv_local[0], jnp.zeros((width,), F32), qv_local[1]])
    fc1_local = lax.dynamic_slice_in_dim(fc1_bias, tp_rank * ff, ff, 0)
    vec = jnp.concatenate(
        [
            norm1_gain, norm1_bias, proj_bias, norm2_gain, norm2_bias, fc2_bias, fc1_local,
            qkv_bias, jnp.zeros((D - qkv_cols,), F32),
        ]
    ).reshape(8, D)
    tab = position_table(rel_rows, rel_cols, HD)
    hot_f, hot_b = position_hots(tok, HD, COLS, rows)
    spread = Spread.scratch(shards, block)
    collect = Collect.scratch(shards, block)
    gather = Gather2.scratch(piece)
    swap = [DMA((2, 1))]
    share = [DMA((2, 6))]

    x, a1, w1_full, a1_turned = comm_call(
        partial(front_kernel, shards), "front", 0,
        (tokens, qkv_weight, proj_weight.T, vec),
        (S(own, BF16), S(full, BF16), S(blocks, BF16), S((D, tok), BF16)),
        [pltpu.VMEM(block, BF16)] + swap + share + spread, hbm_out=(2,),
    )
    w1_full = w1_full.reshape(D, -1)
    vh, oh, o_low, lse, qa, ka, g, cot_first, fc1_full, proj_part = comm_call(
        partial(fwd_kernel, shards, heads, HD, COLS, rows, 256), "attn_fwd", 1,
        (a1.reshape(tok, D), w1_full, vec, tab, hot_f, cotangent, fc1_weight),
        (
            S((heads, tok, 128), BF16), S((heads, tok, 128), F32), S((tok, width), BF16), S((heads, 1, tok), F32),
            S((heads, tok, 256), BF16), S((heads, tok, 256), BF16),
            S(own, BF16), S((1,) + full[1:], BF16), S(blocks, BF16), S((tok, D), BF16),
        ),
        [pltpu.VMEM((heads, tok, 128), BF16), pltpu.VMEM((128, tok), BF16), pltpu.VMEM((256, 128), BF16)]
        + swap + share + spread, hbm_in=(6,), hbm_out=(8,),
    )
    fc1_full = fc1_full.reshape(D, ff)
    mid, a2, fc2_full, act, slope, cot, cot_turned = comm_call(
        partial(mid_kernel, shards), "mid", 2,
        (proj_part.reshape(full), x, vec, fc2_t, fc1_full, g, cot_first),
        (
            S(own, F32), S(full, BF16), S(blocks, BF16), S((tok, ff), BF16), S((tok, ff), F32),
            S(full, BF16), S((D, tok), BF16),
        ),
        gather + share + share + [DMA] + spread, hbm_in=(3,), hbm_out=(2,),
    )
    fc2_full = fc2_full.reshape(D, ff)
    d_mid, _, d_branch_turned, fc2_own, sums, fc1_grad, mlp_part, d_o = comm_call(
        partial(turn_kernel, shards), "turn", 3,
        (
            cot_turned, act, slope, cot.reshape(tok, D), fc2_full, fc1_full, a2.reshape(tok, D), mid, g, vec,
            w1_full,
        ),
        (
            S(own, F32), S(full, BF16), S((D, tok), BF16), S(block, F32), S((8, D), F32),
            S((D, ff), BF16), S((tok, D), BF16), S((tok, width), BF16),
        ),
        [pltpu.VMEM((D, ff), BF16), pltpu.VMEM(full, BF16), pltpu.VMEM((tok, ff), BF16)]
        + gather + share + collect,
    )
    dqkv, rel_grad, output, fc1_own, d_a1, qkv_sum = comm_call(
        partial(bwd_kernel, shards, heads, HD, COLS, rows, 256), "attn_bwd", 4,
        (qa, ka, vh, d_o, oh, lse, tab, hot_b, mlp_part.reshape(full), mid, vec, fc1_grad, w1_full),
        (
            S((tok, qkv_cols), BF16), S((256, 128), F32), S(own, BF16), S(block, F32),
            S((tok, D), BF16), S((1, qkv_cols), F32),
        ),
        [
            pltpu.VMEM((heads, tok, 128), BF16), pltpu.VMEM((3 * heads, tok, 128), BF16),
            pltpu.VMEM((256, tok), BF16), pltpu.VMEM((tok, 128), F32), pltpu.VMEM((tok, 128), F32),
            pltpu.VMEM((8, tok), F32), pltpu.VMEM(own, BF16),
        ] + gather + swap + collect,
    )
    qkv_sum = qkv_sum[0]
    qv_part = jnp.stack([qkv_sum[:width], qkv_sum[2 * width :]])
    qv_placed = lax.dynamic_update_slice_in_dim(jnp.zeros((2, D), F32), qv_part, tp_rank * width, 1)
    fc1_placed = lax.dynamic_update_slice_in_dim(jnp.zeros((FF,), F32), sums[4], tp_rank * ff, 0)
    terms = (
        jnp.zeros((2 * D,), F32),
        qv_placed.reshape(-1),
        fc1_placed,
        sums[:4].reshape(-1),
        rel_grad[: rel_rows.shape[0], :HD].reshape(-1),
        rel_grad[128 : 128 + rel_cols.shape[0], :HD].reshape(-1),
    )
    count = sum(term.shape[0] for term in terms)
    lines = -(-count // (8 * D)) * 8
    packed = jnp.concatenate(terms + (jnp.zeros((lines * D - count,), F32),)).reshape(lines, D)
    tokens_grad, w1_own, total = comm_call(
        partial(end_kernel, shards), "end", 5,
        (d_a1.reshape(full), x, d_mid, vec, a1_turned, dqkv, d_branch_turned, o_low, packed),
        (S(own, BF16), S(block, F32), S((lines, D), F32)),
        [pltpu.VMEM((D, ff), BF16), pltpu.VMEM(own, BF16)] + gather + swap
        + [
            pltpu.VMEM((4, lines, D), F32), pltpu.VMEM((3, lines, D), F32),
            pltpu.VMEM((shards, lines, D), F32), DMA((2, 2 + shards)),
        ]
        + collect,
    )
    flat = total.reshape(-1)
    base = 4 * D + FF
    rel_at = base + 4 * D
    rel_mid = rel_at + rel_rows.size
    return (
        output,
        tokens_grad,
        total[0],
        total[1],
        jnp.stack([w1_own[:, j * width : (j + 1) * width] for j in range(3)]),
        total[2:4],
        flat[rel_at:rel_mid].reshape(rel_rows.shape),
        flat[rel_mid : rel_mid + rel_cols.size].reshape(rel_cols.shape),
        w1_own[:, qkv_cols:].T,
        flat[base + 2 * D : base + 3 * D],
        flat[base : base + D],
        flat[base + D : base + 2 * D],
        fc1_own,
        flat[4 * D : base],
        fc2_own.T,
        flat[base + 3 * D : base + 4 * D],
    )


def solution(mesh):
    in_specs = (
        P("shard", ("ctx", "tp"), None),
        P(),
        P(),
        P(None, ("shard", "ctx"), "tp"),
        P(),
        P(),
        P(),
        P("tp", ("shard", "ctx")),
        P(),
        P(),
        P(),
        P(("shard", "ctx"), "tp"),
        P(),
        P("tp", ("shard", "ctx")),
        P(),
        P("shard", ("ctx", "tp"), None),
    )
    out_specs = (
        P("shard", ("ctx", "tp"), None),
        P("shard", ("ctx", "tp"), None),
        P(),
        P(),
        P(None, ("shard", "ctx"), "tp"),
        P(),
        P(),
        P(),
        P("tp", ("shard", "ctx")),
        P(),
        P(),
        P(),
        P(("shard", "ctx"), "tp"),
        P(),
        P("tp", ("shard", "ctx")),
        P(),
    )
    def on_device(*arrays):
        rows = (arrays[5].shape[0] + 1) // 2
        fits = mesh.shape["tp"] == 4 and mesh.shape["ctx"] == 2 and HD + 2 * rows <= 128
        fits = fits and arrays[0].shape[0] == mesh.shape["ctx"] and arrays[6].shape[0] <= 128
        return (on_device_images if fits else on_device_rows)(*arrays)

    return jax.shard_map(
        on_device, mesh=mesh, in_specs=in_specs, out_specs=out_specs, check_vma=False
    )
```

```python
from functools import partial
import math

import jax
import jax.numpy as jnp
from jax import lax
from jax.experimental import pallas as pl
from jax.experimental.pallas import tpu as pltpu
from jax.sharding import PartitionSpec as P

D = 1280
H = 16
HD = 80
FF = 5120
COLS = 64
ROWS_DEV = 8


PRECISE = lax.Precision.HIGHEST
EPSILON = 1e-06
NEGATIVE = -1e30


def layer_norm(values_in, gain_vec, shift_vec):
    average = jnp.mean(values_in, -1, keepdims=True)
    centred = values_in - average
    variance = jnp.mean(centred * centred, -1, keepdims=True)
    return centred * lax.rsqrt(variance + EPSILON) * gain_vec + shift_vec


def block_size():
    return 512


def to_heads(flat_rows, heads_local):
    images, length, feat_width = flat_rows.shape
    return flat_rows.reshape(images, length, heads_local, feat_width // heads_local).transpose(
        0, 2, 1, 3
    )


def from_heads(per_head):
    images, heads_local, length, head_dim = per_head.shape
    return per_head.transpose(0, 2, 1, 3).reshape(images, length, heads_local * head_dim)


def block_scores(query_heads, key_flat, rows_bias, cols_bias, first_key, scale_factor):
    key_heads = to_heads(key_flat, query_heads.shape[1])
    key_len = key_flat.shape[1]
    key_rows = key_len // COLS
    scores = scale_factor * jnp.einsum(
        "ihqc,ihkc->ihqk", query_heads, key_heads, preferred_element_type=jnp.float32
    )
    images, heads_local, query_len, unused_len = scores.shape
    row_part = lax.dynamic_slice_in_dim(rows_bias, first_key // COLS, key_rows, 3)
    scores = scores.reshape(images, heads_local, query_len, key_rows, COLS)
    scores = scores + row_part[..., :, None] + cols_bias[..., None, :]
    return scores.reshape(images, heads_local, query_len, key_len)


def relative_terms(query_flat, rows_param, cols_param, first_row, heads_local):
    images, length, feat_width = query_flat.shape
    rows_dev = length // COLS
    grid_rows = (rows_param.shape[0] + 1) // 2
    own_rows = first_row + jnp.arange(rows_dev, dtype=jnp.int32)
    key_rows = jnp.arange(grid_rows, dtype=jnp.int32)
    row_slots = jnp.arange(rows_param.shape[0], dtype=jnp.int32)
    pick_rows = (
        row_slots[None, None, :]
        == own_rows[:, None, None] - key_rows[None, :, None] + grid_rows - 1
    ).astype(jnp.float32)
    table_rows = jnp.einsum("rkj,jc->rkc", pick_rows, rows_param, precision=PRECISE)
    col_ids = jnp.arange(COLS, dtype=jnp.int32)
    col_slots = jnp.arange(cols_param.shape[0], dtype=jnp.int32)
    pick_cols = (
        col_slots[None, None, :] == col_ids[:, None, None] - col_ids[None, :, None] + COLS - 1
    ).astype(jnp.float32)
    table_cols = jnp.einsum("wkj,jc->wkc", pick_cols, cols_param, precision=PRECISE)
    grid_form = query_flat.reshape(images, rows_dev, COLS, heads_local, feat_width // heads_local)
    along_rows = jnp.einsum("irwhc,rkc->ihrwk", grid_form, table_rows, precision=PRECISE).reshape(
        images, heads_local, length, grid_rows
    )
    along_cols = jnp.einsum("irwhc,wkc->ihrwk", grid_form, table_cols, precision=PRECISE).reshape(
        images, heads_local, length, COLS
    )
    return (along_rows, along_cols)


def on_device_rows(
    tokens,
    norm1_gain,
    norm1_bias,
    qkv_weight,
    qv_bias,
    rel_rows,
    rel_cols,
    proj_weight,
    proj_bias,
    norm2_gain,
    norm2_bias,
    fc1_weight,
    fc1_bias,
    fc2_weight,
    fc2_bias,
    cotangent,
):
    scale_factor = HD ** (-0.5)
    tp_count = lax.axis_size("tp")
    ctx_count = lax.axis_size("ctx")
    tp_rank = lax.axis_index("tp")
    ctx_rank = lax.axis_index("ctx")
    grid_rows = ROWS_DEV * ctx_count
    tok_image = grid_rows * COLS
    tok_ctx = ROWS_DEV * COLS
    heads_local = H // tp_count
    width_local = heads_local * HD
    ff_local = FF // tp_count
    images = tokens.shape[0]
    rows_table = rel_rows.astype(jnp.float32)
    cols_table = rel_cols.astype(jnp.float32)
    qkv_full, proj_full, fc1_full, fc2_full = (
        lax.all_gather(qkv_weight, ("shard", "ctx"), axis=1, tiled=True),
        lax.all_gather(proj_weight, ("shard", "ctx"), axis=1, tiled=True),
        lax.all_gather(fc1_weight, ("shard", "ctx"), axis=0, tiled=True),
        lax.all_gather(fc2_weight, ("shard", "ctx"), axis=1, tiled=True),
    )
    qv_local = lax.dynamic_slice_in_dim(qv_bias, tp_rank * width_local, width_local, 1)
    fc1_local = lax.dynamic_slice_in_dim(fc1_bias, tp_rank * ff_local, ff_local, 0)
    resid_in = tokens.astype(jnp.float32)
    normed1 = layer_norm(resid_in, norm1_gain, norm1_bias).astype(jnp.bfloat16)
    normed1_full = lax.all_gather(normed1, "tp", axis=1, tiled=True)
    projected = jnp.einsum(
        "itd,sde->itse", normed1_full, qkv_full, preferred_element_type=jnp.float32
    )
    queries = (projected[:, :, 0] + qv_local[0]).astype(jnp.bfloat16)
    keys_own = projected[:, :, 1].astype(jnp.bfloat16)
    values_own = (projected[:, :, 2] + qv_local[1]).astype(jnp.bfloat16)
    first_row = ctx_rank * ROWS_DEV
    rel_fn = partial(relative_terms, first_row=first_row, heads_local=heads_local)
    (along_rows, along_cols), rel_pull = jax.vjp(
        rel_fn, queries.astype(jnp.float32), rows_table, cols_table
    )
    query_heads = to_heads(queries, heads_local)
    start_state = (
        jnp.full((images, heads_local, tok_ctx), NEGATIVE, jnp.float32),
        jnp.zeros((images, heads_local, tok_ctx), jnp.float32),
        jnp.zeros((images, heads_local, tok_ctx, HD), jnp.float32),
        jnp.zeros((images, tok_image, width_local), jnp.bfloat16),
        jnp.zeros((images, tok_image, width_local), jnp.bfloat16),
    )
    shard_piece = (
        lax.all_gather(keys_own, "ctx", axis=1, tiled=True),
        lax.all_gather(values_own, "ctx", axis=1, tiled=True),
    )
    piece_len = shard_piece[0].shape[1]
    step_len = block_size()

    def one_step(inner, offset):
        run_max, run_sum, run_acc, keys_all, values_all = inner
        key_blk = lax.dynamic_slice_in_dim(shard_piece[0], offset, step_len, 1)
        value_blk = lax.dynamic_slice_in_dim(shard_piece[1], offset, step_len, 1)
        scores = block_scores(query_heads, key_blk, along_rows, along_cols, offset, scale_factor)
        new_max = jnp.maximum(run_max, jnp.max(scores, -1))
        factor = jnp.exp(run_max - new_max)
        weights_blk = jnp.exp(scores - new_max[..., None])
        run_sum = run_sum * factor + jnp.sum(weights_blk, -1)
        value_heads = to_heads(value_blk, heads_local)
        run_acc = run_acc * factor[..., None] + jnp.einsum(
            "ihqk,ihkc->ihqc",
            weights_blk.astype(jnp.bfloat16),
            value_heads,
            preferred_element_type=jnp.float32,
        )
        keys_all = lax.dynamic_update_slice_in_dim(keys_all, key_blk, offset, 1)
        values_all = lax.dynamic_update_slice_in_dim(values_all, value_blk, offset, 1)
        return ((new_max, run_sum, run_acc, keys_all, values_all), None)

    offsets = jnp.arange(piece_len // step_len, dtype=jnp.int32) * step_len
    result, unused = lax.scan(one_step, start_state, offsets)
    run_max, run_sum, run_acc, keys_all, values_all = result
    attn_heads = run_acc / run_sum[..., None]
    log_total = run_max + jnp.log(run_sum)
    attn_low = from_heads(attn_heads).astype(jnp.bfloat16)
    proj_part = jnp.einsum("itd,de->ite", attn_low, proj_full, preferred_element_type=jnp.float32)
    branch = lax.psum_scatter(
        proj_part.astype(jnp.bfloat16), "tp", scatter_dimension=1, tiled=True
    ).astype(jnp.float32)
    middle = resid_in + branch + proj_bias
    normed2 = layer_norm(middle, norm2_gain, norm2_bias).astype(jnp.bfloat16)
    normed2_full = lax.all_gather(normed2, "tp", axis=1, tiled=True)
    hidden_pre = (
        jnp.einsum("itd,df->itf", normed2_full, fc1_full, preferred_element_type=jnp.float32)
        + fc1_local
    )
    gelu_exact = partial(jax.nn.gelu, approximate=False)
    activated_f, gelu_pull = jax.vjp(gelu_exact, hidden_pre)
    activated = activated_f.astype(jnp.bfloat16)
    mlp_part = jnp.einsum("itf,fe->ite", activated, fc2_full, preferred_element_type=jnp.float32)
    mlp_out = lax.psum_scatter(
        mlp_part.astype(jnp.bfloat16), "tp", scatter_dimension=1, tiled=True
    ).astype(jnp.float32)
    output = (middle + mlp_out + fc2_bias).astype(jnp.bfloat16)
    cot_full = lax.all_gather(cotangent, "tp", axis=1, tiled=True)
    d_act = jnp.einsum("ite,fe->itf", cot_full, fc2_full, preferred_element_type=jnp.float32)
    d_hidden = gelu_pull(d_act)[0].astype(jnp.bfloat16)
    fc2_grad = jnp.einsum("itf,ite->fe", activated, cot_full, preferred_element_type=jnp.float32)
    fc1_grad = jnp.einsum("itd,itf->df", normed2_full, d_hidden, preferred_element_type=jnp.float32)
    fc1_bias_part = jnp.sum(d_hidden.astype(jnp.float32), (0, 1))
    fc2_bias_part = jnp.sum(cotangent.astype(jnp.float32), (0, 1))
    d_norm2_part = jnp.einsum("itf,df->itd", d_hidden, fc1_full, preferred_element_type=jnp.float32)
    d_norm2 = lax.psum_scatter(
        d_norm2_part.astype(jnp.bfloat16), "tp", scatter_dimension=1, tiled=True
    ).astype(jnp.float32)
    unused_out, norm2_pull = jax.vjp(layer_norm, middle, norm2_gain, norm2_bias)
    d_mid_part, gain2_part, bias2_part = norm2_pull(d_norm2)
    d_middle = cotangent.astype(jnp.float32) + d_mid_part
    d_branch = d_middle.astype(jnp.bfloat16)
    proj_bias_part = jnp.sum(d_branch.astype(jnp.float32), (0, 1))
    d_branch_full = lax.all_gather(d_branch, "tp", axis=1, tiled=True)
    proj_grad = jnp.einsum(
        "itd,ite->de", attn_low, d_branch_full, preferred_element_type=jnp.float32
    )
    d_attn = jnp.einsum(
        "ite,de->itd", d_branch_full, proj_full, preferred_element_type=jnp.float32
    ).astype(jnp.bfloat16)
    d_attn_heads = to_heads(d_attn, heads_local)
    delta_rows = jnp.sum(d_attn_heads.astype(jnp.float32) * attn_heads, -1)
    key_step = block_size()
    key_rows = key_step // COLS
    key_offsets = jnp.arange(tok_image // key_step, dtype=jnp.int32) * key_step

    def back_step(carried, offset):
        grad_query, grad_rows, grad_cols = carried
        key_blk = lax.dynamic_slice_in_dim(keys_all, offset, key_step, 1)
        value_blk = lax.dynamic_slice_in_dim(values_all, offset, key_step, 1)
        scores = block_scores(query_heads, key_blk, along_rows, along_cols, offset, scale_factor)
        soft_probs = jnp.exp(scores - log_total[..., None])
        value_heads = to_heads(value_blk, heads_local)
        key_heads = to_heads(key_blk, heads_local)
        d_probs = jnp.einsum(
            "ihqc,ihkc->ihqk", d_attn_heads, value_heads, preferred_element_type=jnp.float32
        )
        d_scores = (soft_probs * (d_probs - delta_rows[..., None])).astype(jnp.bfloat16)
        grad_query = grad_query + jnp.einsum(
            "ihqk,ihkc->ihqc", d_scores, key_heads, preferred_element_type=jnp.float32
        )
        grid_scores = d_scores.astype(jnp.float32).reshape(
            images, heads_local, tok_ctx, key_rows, COLS
        )
        row_sums = jnp.sum(grid_scores, 4)
        row_now = lax.dynamic_slice_in_dim(grad_rows, offset // COLS, key_rows, 3)
        grad_rows = lax.dynamic_update_slice_in_dim(
            grad_rows, row_now + row_sums, offset // COLS, 3
        )
        grad_cols = grad_cols + jnp.sum(grid_scores, 3)
        key_part = scale_factor * jnp.einsum(
            "ihqk,ihqc->ikhc", d_scores, query_heads, preferred_element_type=jnp.float32
        )
        value_part = jnp.einsum(
            "ihqk,ihqc->ikhc",
            soft_probs.astype(jnp.bfloat16),
            d_attn_heads,
            preferred_element_type=jnp.float32,
        )
        emitted = (
            key_part.reshape(images, key_step, width_local),
            value_part.reshape(images, key_step, width_local),
        )
        return ((grad_query, grad_rows, grad_cols), emitted)

    back_start = (
        jnp.zeros((images, heads_local, tok_ctx, HD), jnp.float32),
        jnp.zeros((images, heads_local, tok_ctx, grid_rows), jnp.float32),
        jnp.zeros((images, heads_local, tok_ctx, COLS), jnp.float32),
    )
    (grad_query, grad_rows, grad_cols), emitted = lax.scan(back_step, back_start, key_offsets)
    key_terms = emitted[0].transpose(1, 0, 2, 3).reshape(images, tok_image, width_local)
    value_terms = emitted[1].transpose(1, 0, 2, 3).reshape(images, tok_image, width_local)
    grad_keys, grad_values = (
        lax.psum_scatter(
            key_terms.astype(jnp.bfloat16), "ctx", scatter_dimension=1, tiled=True
        ).astype(jnp.float32),
        lax.psum_scatter(
            value_terms.astype(jnp.bfloat16), "ctx", scatter_dimension=1, tiled=True
        ).astype(jnp.float32),
    )
    d_query_rel, rows_grad_part, cols_grad_part = rel_pull((grad_rows, grad_cols))
    d_query = (scale_factor * from_heads(grad_query) + d_query_rel).astype(jnp.bfloat16)
    d_keys = grad_keys.astype(jnp.bfloat16)
    d_values = grad_values.astype(jnp.bfloat16)
    d_projected = jnp.stack((d_query, d_keys, d_values), axis=2)
    qkv_grad = jnp.einsum(
        "itd,itse->sde", normed1_full, d_projected, preferred_element_type=jnp.float32
    )
    qv_bias_part = jnp.stack(
        (
            jnp.sum(d_query.astype(jnp.float32), (0, 1)),
            jnp.sum(d_values.astype(jnp.float32), (0, 1)),
        )
    )
    d_norm1_part = jnp.einsum(
        "itse,sde->itd", d_projected, qkv_full, preferred_element_type=jnp.float32
    )
    d_norm1 = lax.psum_scatter(
        d_norm1_part.astype(jnp.bfloat16), "tp", scatter_dimension=1, tiled=True
    ).astype(jnp.float32)
    unused_in, norm1_pull = jax.vjp(layer_norm, resid_in, norm1_gain, norm1_bias)
    d_in_part, gain1_part, bias1_part = norm1_pull(d_norm1)
    tokens_grad = (d_middle + d_in_part).astype(jnp.bfloat16)
    qkv_out, proj_out, fc1_out, fc2_out = (
        lax.psum_scatter(
            qkv_grad.astype(jnp.bfloat16), ("shard", "ctx"), scatter_dimension=1, tiled=True
        ).astype(jnp.float32),
        lax.psum_scatter(
            proj_grad.astype(jnp.bfloat16), ("shard", "ctx"), scatter_dimension=1, tiled=True
        ).astype(jnp.float32),
        lax.psum_scatter(
            fc1_grad.astype(jnp.bfloat16), ("shard", "ctx"), scatter_dimension=0, tiled=True
        ).astype(jnp.float32),
        lax.psum_scatter(
            fc2_grad.astype(jnp.bfloat16), ("shard", "ctx"), scatter_dimension=1, tiled=True
        ).astype(jnp.float32),
    )
    qv_placed = lax.dynamic_update_slice_in_dim(
        jnp.zeros((2, D), jnp.float32), qv_bias_part, tp_rank * width_local, 1
    )
    fc1_placed = lax.dynamic_update_slice_in_dim(
        jnp.zeros((FF,), jnp.float32), fc1_bias_part, tp_rank * ff_local, 0
    )
    (
        gain1_sum,
        bias1_sum,
        qv_sum,
        rows_sum,
        cols_sum,
        projb_sum,
        gain2_sum,
        bias2_sum,
        fc1b_sum,
        fc2b_sum,
    ) = lax.psum(
        (
            gain1_part,
            bias1_part,
            qv_placed,
            rows_grad_part,
            cols_grad_part,
            proj_bias_part,
            gain2_part,
            bias2_part,
            fc1_placed,
            fc2_bias_part,
        ),
        ("shard", "ctx", "tp"),
    )
    return (
        output,
        tokens_grad,
        gain1_sum,
        bias1_sum,
        qkv_out,
        qv_sum,
        rows_sum,
        cols_sum,
        proj_out,
        projb_sum,
        gain2_sum,
        bias2_sum,
        fc1_out,
        fc1b_sum,
        fc2_out,
        fc2b_sum,
    )


F32 = jnp.float32
BF16 = jnp.bfloat16
NT = (((1,), (1,)), ((), ()))
NN = (((1,), (0,)), ((), ()))
TN = (((0,), (0,)), ((), ()))
VMEM_GRANT = 60 * 2**20
DMA = pltpu.SemaphoreType.DMA
ANY = pl.BlockSpec(memory_space=pl.ANY)
VM = pl.BlockSpec(memory_space=pltpu.VMEM)


def mm(left, right, dims=NN):
    return lax.dot_general(left, right, dims, preferred_element_type=F32)


def lane_ids(shape):
    return lax.broadcasted_iota(jnp.int32, shape, 1)


def place():
    return lax.axis_index("shard"), lax.axis_index("ctx"), lax.axis_index("tp")


def core_mate(t):
    return t + 1 - 2 * lax.rem(t, 2)


def far_mate(t):
    return lax.rem(t + 2, 4)


def aim(src, dst, sems, k, where):
    return pltpu.make_async_remote_copy(
        src_ref=src,
        dst_ref=dst,
        send_sem=sems.at[0, k],
        recv_sem=sems.at[1, k],
        device_id=where,
        device_id_type=pl.DeviceIdType.MESH,
    )


def send(src, dst, sems, k, where):
    copy = aim(src, dst, sems, k, where)
    copy.start()
    return copy


def swap_copy(src, dst, sems):
    _, c, _ = place()
    return pltpu.make_async_remote_copy(
        src_ref=src,
        dst_ref=dst,
        send_sem=sems.at[0, 0],
        recv_sem=sems.at[1, 0],
        device_id={"ctx": 1 - c},
        device_id_type=pl.DeviceIdType.MESH,
    )


def fill_tables(tab_ref, rr_ref, rc_ref):
    tab_ref[...] = jnp.zeros_like(tab_ref)
    tab_ref[0 : rr_ref.shape[0], 0 : rr_ref.shape[1]] = rr_ref[...]
    tab_ref[128 : 128 + rc_ref.shape[0], 0 : rc_ref.shape[1]] = rc_ref[...]


def fill_hots(hot_ref, hd, cols, rows, second):
    shift = cols.bit_length() - 1
    down = lax.broadcasted_iota(jnp.int32, hot_ref.shape, 0)
    kr = lax.shift_right_logical(down, shift)
    kw = down & (cols - 1)
    l = lane_ids(hot_ref.shape)
    if second:
        hit = (l == hd + rows - 1 - kr) | (l == 128 + cols - 1 - kw)
    else:
        hit = (l == hd + kr) | (l == hd + rows + kr) | (l == 128 + kw) | (l == 192 + kw)
    hot_ref[...] = jnp.where(hit, 1.0, 0.0).astype(BF16)


def reverser(top):
    down = lax.broadcasted_iota(jnp.int32, (128, 128), 0)
    return jnp.where(down + lane_ids((128, 128)) == top, 1.0, 0.0).astype(BF16)


def greet(shards, line=False):
    s, c, t = place()
    size = 2 * shards
    at = s * (1 - c) + (size - 1 - s) * c
    peers = [{"ctx": 1 - c}, {"tp": core_mate(t)}, {"tp": far_mate(t)}]
    for step in (1, size - 1):
        to = lax.rem(at + step, size)
        back = to // shards
        peers.append({"shard": to * (1 - back) + (size - 1 - to) * back, "ctx": back})
    if line:
        peers += [{"shard": lax.rem(s + d, shards)} for d in range(1, shards)]
    barrier = pltpu.get_barrier_semaphore()
    for peer in peers:
        pl.semaphore_signal(barrier, inc=1, device_id=peer, device_id_type=pl.DeviceIdType.MESH)
    pl.semaphore_wait(barrier, len(peers))


class Ring:
    def __init__(self, shards, block, sems):
        s, c, _ = place()
        self.shards, self.size, self.sems = shards, 2 * shards, sems
        self.at = s * (1 - c) + (self.size - 1 - s) * c
        self.half = block // 2
        self.pieces = ring_pieces(block)
        self.rows = self.half // self.pieces
        self.first, self.end = self.pieces, self.pieces * (self.size - 1)
        self.now = self.first

    def coords(self, position):
        back = position // self.shards
        return position * (1 - back) + (self.size - 1 - position) * back, back

    def peer(self, way):
        to = lax.rem(self.at + (1 if way == 0 else self.size - 1), self.size)
        shard, ctx = self.coords(to)
        return {"shard": shard, "ctx": ctx}

    def owner(self, offset):
        shard, ctx = self.coords(lax.rem(self.at + 2 * self.size + offset, self.size))
        return 2 * shard + ctx

    def split(self, event):
        if isinstance(event, int):
            return event // self.pieces, event % self.pieces
        return lax.div(event, self.pieces), lax.rem(event, self.pieces)

    def rows_of(self, way, piece):
        start = way * self.half + piece * self.rows
        return pl.ds(start if isinstance(start, int) else pl.multiple_of(start, self.rows), self.rows)

    def make(self, src, dst, way, event):
        slot = way * self.end + event
        return pltpu.make_async_remote_copy(
            src_ref=src,
            dst_ref=dst,
            send_sem=self.sems.at[0, slot],
            recv_sem=self.sems.at[1, slot],
            device_id=self.peer(way),
            device_id_type=pl.DeviceIdType.MESH,
        )

    def run(self, low, high):
        low, high = max(low, self.first), min(high, self.end)
        if low < high:
            lax.fori_loop(low, high, lambda event, _: (self.step(event), 0)[1], 0)

    def tick(self, count):
        self.run(self.now, self.now + count)
        self.now += count

    def poll(self, event):
        pl.when((event >= self.first) & (event < self.end))(lambda: self.step(event))


def ring_pieces(block):
    return 5 if block % 160 == 0 else 1


def ring_sems(shards, block):
    return DMA((2, 2 * ring_pieces(block) * (2 * shards - 1)))


class Spread(Ring):
    def __init__(self, shards, src, dst, sems, local):
        super().__init__(shards, src.shape[0], sems)
        self.src, self.dst = src, dst
        self.local = pltpu.make_async_copy(src, dst.at[self.owner(0)], local)
        self.local.start()
        for event in range(self.first):
            for way in range(2):
                self.hop(way, event, True).start()

    def hop(self, way, event, own=False):
        j, piece = self.split(event)
        rows = self.rows_of(way, piece)
        there = self.dst.at[self.owner(-j if way == 0 else j), rows]
        return self.make(self.src.at[rows] if own else there, there, way, event)

    def step(self, event):
        for way in range(2):
            self.hop(way, event - self.pieces).wait_recv()
            self.hop(way, event).start()

    def finish(self):
        self.local.wait()
        for way in range(2):
            for event in range(self.end - self.pieces, self.end):
                self.hop(way, event).wait_recv()

        def sent(event, _):
            for way in range(2):
                self.hop(way, event).wait_send()
            return 0

        lax.fori_loop(0, self.end, sent, 0)

    @staticmethod
    def scratch(shards, block):
        return [ring_sems(shards, block[0]), DMA]


class Collect(Ring):
    def __init__(self, shards, src, held, sems):
        super().__init__(shards, src.shape[0] // (2 * shards), sems)
        self.src, self.held, self.block = src, held, src.shape[0] // (2 * shards)

    def begin(self):
        for event in range(self.first):
            for way in range(2):
                self.hop(way, event, True).start()

    def pair_rows(self, n, j):
        offset = (n + 1) * (2 * j - 1)
        last = (2 * n + j + 1) // self.size
        return pl.ds(pl.multiple_of(self.owner(offset * (1 - last)) * self.block, self.rows), self.block)

    def own(self, way, j, piece):
        ahead = self.size - 1 - j
        start = self.owner(ahead if way == 0 else -ahead) * self.block + way * self.half + piece * self.rows
        return pl.ds(pl.multiple_of(start, self.rows), self.rows)

    def hop(self, way, event, own=False):
        j, piece = self.split(event)
        rows = self.rows_of(0, piece)
        there = self.held.at[way, j, rows]
        here = self.src.at[self.own(way, j, piece)] if own else self.held.at[way, j - 1, rows]
        return self.make(here, there, way, event)

    def arrived(self, way, event):
        j, piece = self.split(event)
        there = self.held.at[way, j, self.rows_of(0, piece)]
        self.make(there, there, way, event).wait_recv()

    def step(self, event):
        j, piece = self.split(event)
        rows = self.rows_of(0, piece)
        for way in range(2):
            self.arrived(way, event - self.pieces)
            both = self.held[way, j - 1, rows].astype(F32) + self.src[self.own(way, j, piece)].astype(F32)
            self.held[way, j - 1, rows] = both.astype(BF16)
            self.hop(way, event).start()

    def finish(self, out):
        for piece in range(self.pieces):
            for way in range(2):
                self.arrived(way, self.end - self.pieces + piece)
                last = self.held[way, self.size - 2, self.rows_of(0, piece)].astype(F32)
                own = self.src[self.own(way, self.size - 1, piece)].astype(F32)
                out[self.rows_of(way, piece)] = last + own

        def sent(event, _):
            for way in range(2):
                j, piece = self.split(event)
                there = self.held.at[way, j, self.rows_of(0, piece)]
                self.make(there, there, way, event).wait_send()
            return 0

        lax.fori_loop(0, self.end, sent, 0)

    @staticmethod
    def scratch(shards, block):
        return [pltpu.VMEM((2, 2 * shards - 1, block[0] // 2, block[1]), BF16), ring_sems(shards, block[0])]


class Share:
    def __init__(self, full, sems):
        self.full, self.sems = full, sems

    def copies(self, k, p, src=None):
        _, _, t = place()
        block, passed = self.full.at[p, t], self.full.at[p, far_mate(t)]
        src = block if src is None else src
        return (
            partial(aim, src, block, self.sems, 3 * k, {"tp": far_mate(t)}),
            partial(aim, src, block, self.sems, 3 * k + 1, {"tp": core_mate(t)}),
            partial(aim, passed, passed, self.sems, 3 * k + 2, {"tp": core_mate(t)}),
        )

    def push(self, k, p, src=None):
        for copy in self.copies(k, p, src)[:2]:
            copy().start()

    def forward(self, k, p):
        far, _, third = self.copies(k, p)
        far().wait_recv()
        third().start()

    def finish(self, k, p):
        far, core, third = self.copies(k, p)
        far().wait_send()
        core().wait()
        third().wait()


class Gather2:
    def __init__(self, part, mate, far, out, sems):
        self.part, self.mate, self.far, self.out, self.sems = part, mate, far, out, sems

    def copies(self, p):
        _, _, t = place()
        m = core_mate(t)
        return (
            partial(aim, self.part.at[p, far_mate(m)], self.mate.at[p, 1], self.sems, 3 * p, {"tp": m}),
            partial(aim, self.part.at[p, m], self.mate.at[p, 0], self.sems, 3 * p + 1, {"tp": m}),
            partial(aim, self.out.at[p], self.far.at[p], self.sems, 3 * p + 2, {"tp": far_mate(t)}),
        )

    def push(self, p):
        for copy in self.copies(p)[:2]:
            copy().start()

    def forward(self, p):
        _, _, t = place()
        passing, _, onward = self.copies(p)
        passing().wait_recv()
        both = self.part[p, far_mate(t)].astype(F32) + self.mate[p, 1].astype(F32)
        self.out[p] = both.astype(BF16)
        onward().start()

    def result(self, p):
        _, _, t = place()
        _, own, onward = self.copies(p)
        own().wait_recv()
        onward().wait_recv()
        return self.part[p, t].astype(F32) + self.mate[p, 0].astype(F32) + self.far[p].astype(F32)

    def finish(self, p):
        for copy in self.copies(p):
            copy().wait_send()

    @staticmethod
    def scratch(block):
        return [
            pltpu.VMEM((2, 2) + block, BF16),
            pltpu.VMEM((2,) + block, BF16),
            pltpu.VMEM((2,) + block, BF16),
            DMA((2, 6)),
        ]


def ln_stats(values):
    average = jnp.mean(values, -1, keepdims=True)
    centred = values - average
    inverse = lax.rsqrt(jnp.mean(centred * centred, -1, keepdims=True) + EPSILON)
    return centred * inverse, inverse


def ln_back(unit, inverse, gain, grad):
    scaled = grad * gain
    first = jnp.mean(scaled, -1, keepdims=True)
    second = jnp.mean(scaled * unit, -1, keepdims=True)
    return inverse * (scaled - first - unit * second)


def row_tiles(out_ref, left_ref, right_ref, dims, first, count, tile=256):
    def one(i, _):
        at = pl.ds(pl.multiple_of(i * tile, tile), tile)
        out_ref[at, :] = mm(left_ref[at, :], right_ref[...], dims).astype(out_ref.dtype)
        return 0

    lax.fori_loop(first, first + count, one, 0)


def grad_tiles(out_ref, left_ref, right_ref, first, count, cols=slice(None), tile=256):
    def one(i, _):
        at = pl.ds(pl.multiple_of(i * tile, tile), tile)
        out_ref[at, cols] = mm(left_ref[:, at], right_ref[...], TN).astype(out_ref.dtype)
        return 0

    lax.fori_loop(first, first + count, one, 0)


def comm_call(kernel, name, ident, args, outs, scratch, hbm_in=(), hbm_out=()):
    return pl.pallas_call(
        kernel,
        out_shape=tuple(outs),
        in_specs=[ANY if i in hbm_in else VM for i in range(len(args))],
        out_specs=tuple(ANY if i in hbm_out else VM for i in range(len(outs))),
        scratch_shapes=scratch,
        compiler_params=pltpu.CompilerParams(
            vmem_limit_bytes=VMEM_GRANT, collective_id=ident, has_side_effects=True
        ),
        name=name,
    )(*args)


def turned(out_ref, full_ref, p):
    count, length = full_ref.shape[1:3]

    def one(i, _):
        start = pl.multiple_of((p * count + i) * length, 128)
        out_ref[:, pl.ds(start, length)] = full_ref[p, i].T
        return 0

    lax.fori_loop(0, count, one, 0)


def front_kernel(
    shards, tok_ref, qkvw_ref, pw_ref, vec_ref, x_ref, a_ref, wf_ref, at_ref,
    w1_ref, swap_sems, share_sems, w_sems, w_local,
):
    s, c, t = place()
    wide = qkvw_ref.shape[2]
    for j in range(3):
        w1_ref[:, j * wide : (j + 1) * wide] = qkvw_ref[j]
    w1_ref[:, 3 * wide : 4 * wide] = pw_ref[...]
    greet(shards)
    swap = send(tok_ref.at[1 - c], x_ref.at[c], swap_sems, 0, {"ctx": 1 - c})
    spread = Spread(shards, w1_ref, wf_ref, w_sems, w_local)
    share = Share(a_ref, share_sems)

    def norm(block):
        unit, _ = ln_stats(block.astype(F32))
        return (unit * vec_ref[0:1, :] + vec_ref[1:2, :]).astype(BF16)

    own = tok_ref[c]
    x_ref[c] = own
    a_ref[c, t] = norm(own)
    share.push(0, c)
    swap.wait()
    a_ref[1 - c, t] = norm(x_ref[1 - c])
    share.push(1, 1 - c)
    share.forward(0, c)
    spread.tick(9)
    share.forward(1, 1 - c)
    spread.tick(6)
    share.finish(0, c)
    share.finish(1, 1 - c)
    turned(at_ref, a_ref, 0)
    spread.tick(2)
    spread.tick(4)
    turned(at_ref, a_ref, 1)
    spread.tick(2)
    spread.tick(spread.end)
    spread.finish()


def fwd_kernel(
    shards, heads, hd, cols, rows, qb,
    a1_ref, w1_ref, vec_ref, rr_ref, rc_ref, cot_ref, w_ref,
    vh_ref, oh_ref, ob_ref, lse_ref, qa_ref, ka_ref, g_ref, cf_ref, wf_ref, pp_ref,
    qh_ref, vt_ref, rt_ref, tab_ref, hot_ref, swap_sems, share_sems, w_sems, w_local,
):
    _, me, t = place()
    tok, width = ob_ref.shape
    wide = 3 * width
    blocks = tok // qb
    fill_tables(tab_ref, rr_ref, rc_ref)
    fill_hots(hot_ref, hd, cols, rows, False)
    rt_ref[0:128, :] = mm(reverser(2 * rows - 2), tab_ref[0:128, :]).astype(BF16)
    rt_ref[128:256, :] = mm(reverser(2 * cols - 2), tab_ref[128:256, :]).astype(BF16)
    greet(shards)
    swap = swap_copy(cot_ref.at[1 - me], g_ref.at[me], swap_sems)
    swap.start()
    spread = Spread(shards, w_ref, wf_ref, w_sems, w_local)
    share = Share(cf_ref, share_sems)
    own = cot_ref[me]
    g_ref[me] = own
    cf_ref[me, t] = own
    share.push(0, me, cot_ref.at[me])

    def project(i, _):
        at = pl.ds(pl.multiple_of(i * qb, qb), qb)
        tile = (mm(a1_ref[at, :], w1_ref[:, 0:wide]) + vec_ref[7:8, 0:wide]).astype(BF16)
        pad = jnp.zeros((qb, 128 - hd), BF16)
        front = lane_ids((qb, 128)) < hd
        for h in range(heads):
            part = [tile[:, (j * heads + h) * hd : (j * heads + h + 1) * hd] for j in range(3)]
            part = [jnp.concatenate([x, pad], 1) for x in part]
            qh_ref[h, at, :] = part[0]
            ka_ref[h, at, 0:128] = jnp.where(front, part[1], hot_ref[at, 0:128])
            ka_ref[h, at, 128:256] = hot_ref[at, 128:256]
            vh_ref[h, at, :] = part[2]
        return 0

    lax.fori_loop(0, blocks, project, 0)
    swap.wait()
    cf_ref[1 - me, t] = g_ref[1 - me]
    share.push(1, 1 - me, g_ref.at[1 - me])
    c = hd**-0.5 * math.log2(math.e)
    up = hd**0.5

    def head(h, _):
        vt_ref[...] = vh_ref[h].T
        terms = mm(qh_ref[h], rt_ref[...], NT) * up
        ln = lane_ids((cols, 128))
        for r in range(rows):
            rs = slice(r * cols, (r + 1) * cols)
            tr = pltpu.roll(terms[rs, 0:128], (65 + r) % 128, 1)
            tc = pltpu.roll(terms[rs, 128:256], 65, 1, stride=1, stride_axis=0)
            rh = tr.astype(BF16).astype(F32)
            rl = pltpu.roll(tr - rh, rows, 1)
            ch = tc.astype(BF16).astype(F32)
            cl = pltpu.roll(tc - ch, 64, 1)
            low = jnp.where(ln < hd + 2 * rows, rl, jnp.zeros_like(tr))
            left = jnp.where(ln < hd, qh_ref[h, rs, :].astype(F32), jnp.where(ln < hd + rows, rh, low))
            qa_ref[h, rs, 0:128] = left.astype(BF16)
            qa_ref[h, rs, 128:256] = jnp.where(ln < 64, ch, cl).astype(BF16)

        def blk(i, _):
            at = pl.ds(pl.multiple_of(i * qb, qb), qb)
            s = mm(ka_ref[h], qa_ref[h, at, :], NT)
            m = jnp.max(s, 0, keepdims=True)
            p = jnp.exp2((s - m) * c)
            l = jnp.sum(p, 0, keepdims=True)
            lse_ref[h, :, at] = m * c + jnp.log2(l)
            oh_ref[h, at, :] = (mm(vt_ref[...], p.astype(BF16)) / l).T
            for k in range(2):
                spread.poll(spread.first + 2 * (h * blocks + i) + k)
            return 0

        lax.fori_loop(0, blocks, blk, 0)
        pl.when(h == 0)(lambda: share.forward(0, me))
        pl.when(h == min(1, heads - 1))(lambda: share.forward(1, 1 - me))
        return 0

    lax.fori_loop(0, heads, head, 0)
    for h in range(heads):
        ob_ref[:, h * hd : (h + 1) * hd] = oh_ref[h, :, 0:hd].astype(BF16)

    def out_rows(i, _):
        at = pl.ds(pl.multiple_of(i * qb, qb), qb)
        pp_ref[at, :] = mm(ob_ref[at, :], w1_ref[:, wide:], NT).astype(BF16)
        return 0

    lax.fori_loop(0, blocks, out_rows, 0)
    spread.run(spread.first + 2 * heads * blocks, spread.end)
    share.finish(0, me)
    share.finish(1, 1 - me)
    spread.finish()


def mid_kernel(
    shards, part_ref, x_ref, vec_ref, w_ref, f1_ref, cf_ref,
    mid_ref, a_ref, wf_ref, act_ref, slope_ref, ct_ref,
    mate, far, outb, sum_sems, share_sems, w_sems, w_local,
):
    _, _, t = place()
    greet(shards)
    gather = Gather2(part_ref, mate, far, outb, sum_sems)
    gather.push(0)
    gather.push(1)
    spread = Spread(shards, w_ref, wf_ref, w_sems, w_local)
    share = Share(a_ref, share_sems)
    gather.forward(0)
    gather.forward(1)
    turned(ct_ref, cf_ref, 0)
    spread.tick(8)
    for p in range(2):
        mid = x_ref[p].astype(F32) + gather.result(p) + vec_ref[2:3, :]
        mid_ref[p] = mid
        unit, _ = ln_stats(mid)
        a_ref[p, t] = (unit * vec_ref[3:4, :] + vec_ref[4:5, :]).astype(BF16)
        share.push(p, p)
        if p == 1:
            turned(ct_ref, cf_ref, 1)
        spread.tick(7)
    share.forward(0, 0)
    half = a_ref.shape[1] * a_ref.shape[2]

    def hidden(p):
        def one(i, _):
            rows = a_ref[p, pl.ds(2 * i, 2)].reshape(-1, a_ref.shape[3])
            pre = mm(rows, f1_ref[...]) + vec_ref[6:7, :]
            cdf = 0.5 * (1.0 + lax.erf(pre * (2.0**-0.5)))
            bell = jnp.exp(-0.5 * pre * pre) * ((2.0 * math.pi) ** -0.5)
            at = pl.ds(pl.multiple_of(p * half + i * rows.shape[0], 128), rows.shape[0])
            act_ref[at, :] = (pre * cdf).astype(BF16)
            slope_ref[at, :] = cdf + pre * bell
            for k in range(2):
                spread.poll(base + 2 * i + k)
            return 0

        base = spread.now
        lax.fori_loop(0, a_ref.shape[1] // 2, one, 0)
        spread.now += a_ref.shape[1]

    share.finish(0, 0)
    hidden(0)
    spread.tick(spread.end)
    share.forward(1, 1)
    share.finish(1, 1)
    hidden(1)
    for p in range(2):
        gather.finish(p)
    spread.finish()


def turn_kernel(
    shards, ct_ref, act_ref, slope_ref, cot_ref, f2_ref, f1_ref, a2_ref, mid_ref, g_ref, vec_ref, w1_ref,
    dm_ref, db_ref, dbt_ref, wg_ref, sums_ref, f1g_ref, mlp_ref, do_ref,
    w2g_ref, part_ref, dp_ref, mate, far, outb, sum_sems, share_sems, w_held, w_sems,
):
    _, _, t = place()
    greet(shards)
    collect = Collect(shards, w2g_ref, w_held, w_sems)
    gather = Gather2(part_ref, mate, far, outb, sum_sems)
    share = Share(db_ref, share_sems)
    tile = 2 * db_ref.shape[2]
    halves = db_ref.shape[1] // 2
    sums_ref[...] = jnp.zeros_like(sums_ref)
    step = collect.pieces

    def back(n, _):
        def block(j, _):
            at = collect.pair_rows(n, j)
            w2g_ref[at, :] = mm(ct_ref[at, :], act_ref[...]).astype(BF16)
            return 0

        lax.fori_loop(0, 2, block, 0)
        pl.when(n == 0)(collect.begin)
        pl.when(n == halves)(lambda: gather.forward(0))
        p, i = n // halves, n % halves
        at = pl.ds(pl.multiple_of(n * tile, tile), tile)
        d_pre = (mm(cot_ref[at, :], f2_ref[...]) * slope_ref[at, :]).astype(BF16)
        dp_ref[at, :] = d_pre
        sums_ref[4:5, :] += jnp.sum(d_pre.astype(F32), 0, keepdims=True)
        for k in range(2):
            collect.poll(step * n + k)
        d_a2 = mm(d_pre, f1_ref[...], NT).astype(BF16)
        part_ref[p, pl.ds(2 * i, 2)] = d_a2.reshape(2, tile // 2, -1)
        pl.when(n == halves - 1)(lambda: gather.push(0))
        for k in range(2, step):
            collect.poll(step * n + k)
        return 0

    lax.fori_loop(0, 2 * halves, back, 0)
    gather.push(1)
    base = 2 * halves * step

    def hidden_grad(i, _):
        at = pl.ds(pl.multiple_of(i * 256, 256), 256)
        f1g_ref[at, :] = mm(a2_ref[:, at], dp_ref[...], TN).astype(BF16)
        collect.poll(base + i)
        pl.when(i == 0)(lambda: gather.forward(1))

        @pl.when((i == 1) | (i == count - 1))
        def _():
            p = lax.div(i, count - 1)
            unit, inverse = ln_stats(mid_ref[p])
            g = g_ref[p].astype(F32)
            da = gather.result(p)
            dm = g + ln_back(unit, inverse, vec_ref[3:4, :], da)
            dm_ref[p] = dm
            low_dm = dm.astype(BF16)
            db_ref[p, t] = low_dm
            share.push(p, p)
            for k, term in enumerate((da * unit, da, low_dm.astype(F32), g)):
                sums_ref[k : k + 1, :] += jnp.sum(term, 0, keepdims=True)

        return 0

    count = f1g_ref.shape[0] // 256
    lax.fori_loop(0, count, hidden_grad, 0)
    base2 = base + count

    def mlp(n, _):
        at = pl.ds(pl.multiple_of(n * tile, tile), tile)
        mlp_ref[at, :] = mm(act_ref[at, :], f2_ref[...], NT).astype(BF16)
        for k in range(2):
            collect.poll(base2 + 2 * n + k)
        pl.when(n == 2 * halves - 1)(lambda: share.forward(0, 0))
        return 0

    lax.fori_loop(0, 2 * halves, mlp, 0)
    collect.run(base2 + 4 * halves, collect.end)
    share.forward(1, 1)
    wide = do_ref.shape[1]

    def d_o(n, _):
        p, i = n // halves, n % halves
        pl.when(i == 0)(lambda: share.finish(p, p))
        rows = db_ref[p, pl.ds(2 * i, 2)].reshape(tile, -1)
        at = pl.ds(pl.multiple_of(n * tile, tile), tile)
        do_ref[at, :] = mm(rows, w1_ref[:, 3 * wide :]).astype(BF16)
        dbt_ref[:, at] = rows.T
        return 0

    lax.fori_loop(0, 2 * halves, d_o, 0)
    for p in range(2):
        gather.finish(p)
    collect.finish(wg_ref)


def bwd_kernel(
    shards, heads, hd, cols, rows, qb,
    qa_ref, ka_ref, vh_ref, do_ref, oh_ref, lse_ref, rr_ref, rc_ref, w_ref, part_ref, mid_ref, vec_ref,
    dqkv_ref, rg_ref, wg_ref, qs_ref, out_ref,
    doh_ref, dh_ref, kt_ref, acc_k, acc_v, del_ref, tab_ref, hot_ref, res_ref,
    mate, far, outb, sum_sems, swap_sems, w_held, w_sems,
):
    fill_tables(tab_ref, rr_ref, rc_ref)
    fill_hots(hot_ref, hd, cols, rows, True)
    _, me, _ = place()
    greet(shards)
    gather = Gather2(part_ref, mate, far, outb, sum_sems)
    gather.push(0)
    gather.push(1)
    swap = swap_copy(res_ref.at[1 - me], out_ref.at[me], swap_sems)
    collect = Collect(shards, w_ref, w_held, w_sems)
    collect.begin()
    tok, wide = dqkv_ref.shape
    blocks = tok // qb
    for h in range(heads):
        pad = jnp.zeros((tok, 128 - hd), BF16)
        doh_ref[h] = jnp.concatenate([do_ref[:, h * hd : (h + 1) * hd], pad], 1)
    gather.forward(0)
    gather.forward(1)
    scale = hd**-0.5
    c = scale * math.log2(math.e)
    rg_ref[...] = jnp.zeros_like(rg_ref)

    def head(h, _):
        kt_ref[0:128, :] = jnp.where(lane_ids((tok, 128)) < hd, ka_ref[h, :, 0:128], hot_ref[:, 0:128]).T
        kt_ref[128:256, :] = hot_ref[:, 128:256].T
        del_ref[...] = lax.dot_general(
            jnp.ones((8, 128), F32), doh_ref[h].astype(F32) * oh_ref[h], NT,
            preferred_element_type=F32, precision=PRECISE,
        )
        acc_k[...] = jnp.zeros_like(acc_k)
        acc_v[...] = jnp.zeros_like(acc_v)

        def blk(i, _):
            at = pl.ds(pl.multiple_of(i * qb, qb), qb)
            qblk = qa_ref[h, at, :]
            dob = doh_ref[h, at, :]
            s = mm(ka_ref[h], qblk, NT)
            p = jnp.exp2(s * c - lse_ref[h, :, at])
            dp = mm(vh_ref[h], dob, NT)
            ds = (p * (dp - del_ref[0:1, at])).astype(BF16)
            acc_v[...] += mm(p.astype(BF16), dob)
            acc_k[...] += mm(ds, qblk[:, 0:128])
            dqa = mm(kt_ref[...], ds).T
            ln = lane_ids((cols, 128))
            parts = []
            for j in range(qb // cols):
                r = i * (qb // cols) + j
                js = slice(j * cols, (j + 1) * cols)
                dr = dqa[js, 0:128]
                dr = jnp.where((ln >= hd) & (ln < hd + rows), dr, 0.0)
                dr = pltpu.roll(dr, lax.rem(48 + r, 128), 1)
                dc = pltpu.roll(dqa[js, 128:256], 0, 1, stride=1, stride_axis=0)
                parts.append(jnp.concatenate([dr, dc], 1))
            d = jnp.concatenate(parts, 0).astype(BF16)
            rel = mm(d, tab_ref[...])
            rg_ref[...] += mm(d, qblk[:, 0:128], TN)
            dh_ref[h, at, :] = (scale * dqa[:, 0:128] + rel).astype(BF16)
            for k in range(2):
                collect.poll(collect.first + 2 * (h * blocks + i) + k)
            return 0

        lax.fori_loop(0, blocks, blk, 0)
        dh_ref[heads + h] = (scale * acc_k[...]).astype(BF16)
        dh_ref[2 * heads + h] = acc_v[...].astype(BF16)

        @pl.when(h == min(2, heads - 1))
        def _():
            for p in range(2):
                total = mid_ref[p] + gather.result(p) + vec_ref[5:6, :]
                res_ref[p] = total.astype(BF16)

        return 0

    lax.fori_loop(0, heads, head, 0)
    swap.start()
    out_ref[me] = res_ref[me]
    for j in range(3 * heads):
        dqkv_ref[:, j * hd : (j + 1) * hd] = dh_ref[j, :, 0:hd]
    collect.run(collect.first + 2 * heads * blocks, collect.end)
    qs_ref[...] = mm(jnp.ones((8, tok), BF16), dqkv_ref[...])
    for p in range(2):
        gather.finish(p)
    collect.finish(wg_ref)
    swap.wait()


def end_kernel(
    shards, x_ref, dm_ref, vec_ref, at_ref, dqkv_ref, dbt_ref, ob_ref, small_ref, w1_ref,
    grad_ref, qg_ref, pg_ref, total_ref,
    w1g_ref, wg_ref, part_ref, gres_ref, mate, far, outb, sum_sems, swap_sems,
    held, got, line, small_sems, w_held, w_sems,
):
    s, me, t = place()
    greet(shards, True)
    gather = Gather2(part_ref, mate, far, outb, sum_sems)
    collect = Collect(shards, w1g_ref, w_held, w_sems)
    wide = dqkv_ref.shape[1]
    tile = 2 * part_ref.shape[2]
    halves = part_ref.shape[1] // 2
    step = collect.pieces

    def back(n, _):
        p, i = n // halves, n % halves
        rows = pl.ds(pl.multiple_of(n * tile, tile), tile)
        d_a1 = mm(dqkv_ref[rows, :], w1_ref[:, 0:wide], NT).astype(BF16)
        part_ref[p, pl.ds(2 * i, 2)] = d_a1.reshape(2, tile // 2, -1)
        pl.when(n == halves - 1)(lambda: gather.push(0))
        for k in range(step):
            collect.poll(step * (n - 1) + k)

        def block(j, _):
            at = collect.pair_rows(n, j)
            w1g_ref[at, 0:wide] = mm(at_ref[at, :], dqkv_ref[...]).astype(BF16)
            w1g_ref[at, wide:] = mm(dbt_ref[at, :], ob_ref[...]).astype(BF16)
            return 0

        lax.fori_loop(0, 2, block, 0)
        pl.when(n == 0)(collect.begin)
        pl.when(n == halves)(lambda: gather.forward(0))
        return 0

    lax.fori_loop(0, 2 * halves, back, 0)
    gather.push(1)
    collect.now = step * (2 * halves - 1)
    collect.tick(2)
    gather.forward(1)
    collect.tick(2)
    held[0] = small_ref[...]
    for p in range(2):
        unit, inverse = ln_stats(x_ref[p].astype(F32))
        collect.tick(2)
        da = gather.result(p)
        gres_ref[p] = (dm_ref[p] + ln_back(unit, inverse, vec_ref[0:1, :], da)).astype(BF16)
        held[0, 0:1, :] += jnp.sum(da * unit, 0, keepdims=True)
        held[0, 1:2, :] += jnp.sum(da, 0, keepdims=True)
        collect.tick(3)
    grad_ref[me] = gres_ref[me]
    swap = swap_copy(gres_ref.at[1 - me], grad_ref.at[me], swap_sems)
    waits = []
    for k, peer in enumerate(({"tp": core_mate(t)}, {"tp": far_mate(t)}, {"ctx": 1 - me})):
        copy = send(held.at[k], got.at[k], small_sems, k, peer)
        if k == 2:
            swap.start()
        collect.tick(2)
        copy.wait_recv()
        waits.append(copy)
        held[k + 1] = held[k] + got[k]
    line[s] = held[3]
    for d in range(1, shards):
        waits.append(send(held.at[3], line.at[s], small_sems, 2 + d, {"shard": lax.rem(s + d, shards)}))
    collect.tick(collect.end)
    collect.finish(wg_ref)
    part = wide // 3
    for j in range(3):
        qg_ref[j] = wg_ref[:, j * part : (j + 1) * part]
    pg_ref[...] = wg_ref[:, wide:]
    for k, copy in enumerate(waits):
        if k < 3:
            copy.wait_send()
        else:
            copy.wait()
    acc = line[0]
    for k in range(1, shards):
        acc = acc + line[k]
    total_ref[...] = acc
    for p in range(2):
        gather.finish(p)
    swap.wait()


def on_device_images(
    tokens, norm1_gain, norm1_bias, qkv_weight, qv_bias, rel_rows, rel_cols, proj_weight, proj_bias,
    norm2_gain, norm2_bias, fc1_weight, fc1_bias, fc2_weight, fc2_bias, cotangent,
):
    S = jax.ShapeDtypeStruct
    shards = lax.axis_size("shard")
    tp_count = lax.axis_size("tp")
    tp_rank = lax.axis_index("tp")
    heads = H // tp_count
    width = heads * HD
    ff = FF // tp_count
    rows = (rel_rows.shape[0] + 1) // 2
    tok = rows * COLS
    own = tokens.shape
    piece = own[1:]
    full = (2, tp_count) + piece
    block = fc1_weight.shape
    blocks = (2 * shards,) + block
    qkv_cols = 3 * width
    fc2_t = fc2_weight.T
    qv_local = lax.dynamic_slice_in_dim(qv_bias, tp_rank * width, width, 1)
    qkv_bias = jnp.concatenate([qv_local[0], jnp.zeros((width,), F32), qv_local[1]])
    fc1_local = lax.dynamic_slice_in_dim(fc1_bias, tp_rank * ff, ff, 0)
    vec = jnp.concatenate(
        [
            norm1_gain, norm1_bias, proj_bias, norm2_gain, norm2_bias, fc2_bias, fc1_local,
            qkv_bias, jnp.zeros((D - qkv_cols,), F32),
        ]
    ).reshape(8, D)
    spread = Spread.scratch(shards, block)
    collect = Collect.scratch(shards, block)
    gather = Gather2.scratch(piece)
    swap = [DMA((2, 1))]
    share = [DMA((2, 6))]

    x, a1, w1_full, a1_turned = comm_call(
        partial(front_kernel, shards), "front", 0,
        (tokens, qkv_weight, proj_weight.T, vec),
        (S(own, BF16), S(full, BF16), S(blocks, BF16), S((D, tok), BF16)),
        [pltpu.VMEM(block, BF16)] + swap + share + spread, hbm_out=(2,),
    )
    w1_full = w1_full.reshape(D, -1)
    vh, oh, o_low, lse, qa, ka, g, cot, fc1_full, proj_part = comm_call(
        partial(fwd_kernel, shards, heads, HD, COLS, rows, 256), "attn_fwd", 1,
        (a1.reshape(tok, D), w1_full, vec, rel_rows, rel_cols, cotangent, fc1_weight),
        (
            S((heads, tok, 128), BF16), S((heads, tok, 128), F32), S((tok, width), BF16), S((heads, 1, tok), F32),
            S((heads, tok, 256), BF16), S((heads, tok, 256), BF16),
            S(own, BF16), S(full, BF16), S(blocks, BF16), S((tok, D), BF16),
        ),
        [
            pltpu.VMEM((heads, tok, 128), BF16), pltpu.VMEM((128, tok), BF16), pltpu.VMEM((256, 128), BF16),
            pltpu.VMEM((256, 128), BF16), pltpu.VMEM((tok, 256), BF16),
        ]
        + swap + share + spread, hbm_in=(6,), hbm_out=(8,),
    )
    fc1_full = fc1_full.reshape(D, ff)
    mid, a2, fc2_full, act, slope, cot_turned = comm_call(
        partial(mid_kernel, shards), "mid", 2,
        (proj_part.reshape(full), x, vec, fc2_t, fc1_full, cot),
        (
            S(own, F32), S(full, BF16), S(blocks, BF16), S((tok, ff), BF16), S((tok, ff), F32),
            S((D, tok), BF16),
        ),
        gather + share + spread, hbm_in=(3,), hbm_out=(2,),
    )
    fc2_full = fc2_full.reshape(D, ff)
    d_mid, _, d_branch_turned, fc2_own, sums, fc1_grad, mlp_part, d_o = comm_call(
        partial(turn_kernel, shards), "turn", 3,
        (
            cot_turned, act, slope, cot.reshape(tok, D), fc2_full, fc1_full, a2.reshape(tok, D), mid, g, vec,
            w1_full,
        ),
        (
            S(own, F32), S(full, BF16), S((D, tok), BF16), S(block, F32), S((8, D), F32),
            S((D, ff), BF16), S((tok, D), BF16), S((tok, width), BF16),
        ),
        [pltpu.VMEM((D, ff), BF16), pltpu.VMEM(full, BF16), pltpu.VMEM((tok, ff), BF16)]
        + gather + share + collect,
    )
    dqkv, rel_grad, fc1_own, qkv_sum, output = comm_call(
        partial(bwd_kernel, shards, heads, HD, COLS, rows, 256), "attn_bwd", 4,
        (qa, ka, vh, d_o, oh, lse, rel_rows, rel_cols, fc1_grad, mlp_part.reshape(full), mid, vec),
        (S((tok, qkv_cols), BF16), S((256, 128), F32), S(block, F32), S((8, qkv_cols), F32), S(own, BF16)),
        [
            pltpu.VMEM((heads, tok, 128), BF16), pltpu.VMEM((3 * heads, tok, 128), BF16),
            pltpu.VMEM((256, tok), BF16), pltpu.VMEM((tok, 128), F32), pltpu.VMEM((tok, 128), F32),
            pltpu.VMEM((8, tok), F32), pltpu.VMEM((256, 128), BF16), pltpu.VMEM((tok, 256), BF16),
            pltpu.VMEM(own, BF16),
        ] + gather + swap + collect,
    )
    qkv_sum = qkv_sum[0]
    qv_part = jnp.stack([qkv_sum[:width], qkv_sum[2 * width :]])
    qv_placed = lax.dynamic_update_slice_in_dim(jnp.zeros((2, D), F32), qv_part, tp_rank * width, 1)
    fc1_placed = lax.dynamic_update_slice_in_dim(jnp.zeros((FF,), F32), sums[4], tp_rank * ff, 0)
    terms = (
        jnp.zeros((2 * D,), F32),
        qv_placed.reshape(-1),
        fc1_placed,
        sums[:4].reshape(-1),
        rel_grad[: rel_rows.shape[0], :HD].reshape(-1),
        rel_grad[128 : 128 + rel_cols.shape[0], :HD].reshape(-1),
    )
    count = sum(term.shape[0] for term in terms)
    lines = -(-count // (8 * D)) * 8
    packed = jnp.concatenate(terms + (jnp.zeros((lines * D - count,), F32),)).reshape(lines, D)
    tokens_grad, qkv_own, proj_own, total = comm_call(
        partial(end_kernel, shards), "end", 5,
        (x, d_mid, vec, a1_turned, dqkv, d_branch_turned, o_low, packed, w1_full),
        (S(own, BF16), S((3, block[0], width), F32), S((block[0], width), F32), S((lines, D), F32)),
        [pltpu.VMEM((D, ff), BF16), pltpu.VMEM(block, F32), pltpu.VMEM(full, BF16), pltpu.VMEM(own, BF16)]
        + gather + swap
        + [
            pltpu.VMEM((4, lines, D), F32), pltpu.VMEM((3, lines, D), F32),
            pltpu.VMEM((shards, lines, D), F32), DMA((2, 2 + shards)),
        ]
        + collect,
    )
    flat = total.reshape(-1)
    base = 4 * D + FF
    rel_at = base + 4 * D
    rel_mid = rel_at + rel_rows.size
    return (
        output,
        tokens_grad,
        total[0],
        total[1],
        qkv_own,
        total[2:4],
        flat[rel_at:rel_mid].reshape(rel_rows.shape),
        flat[rel_mid : rel_mid + rel_cols.size].reshape(rel_cols.shape),
        proj_own.T,
        flat[base + 2 * D : base + 3 * D],
        flat[base : base + D],
        flat[base + D : base + 2 * D],
        fc1_own,
        flat[4 * D : base],
        fc2_own.T,
        flat[base + 3 * D : base + 4 * D],
    )


def solution(mesh):
    in_specs = (
        P("shard", ("ctx", "tp"), None),
        P(),
        P(),
        P(None, ("shard", "ctx"), "tp"),
        P(),
        P(),
        P(),
        P("tp", ("shard", "ctx")),
        P(),
        P(),
        P(),
        P(("shard", "ctx"), "tp"),
        P(),
        P("tp", ("shard", "ctx")),
        P(),
        P("shard", ("ctx", "tp"), None),
    )
    out_specs = (
        P("shard", ("ctx", "tp"), None),
        P("shard", ("ctx", "tp"), None),
        P(),
        P(),
        P(None, ("shard", "ctx"), "tp"),
        P(),
        P(),
        P(),
        P("tp", ("shard", "ctx")),
        P(),
        P(),
        P(),
        P(("shard", "ctx"), "tp"),
        P(),
        P("tp", ("shard", "ctx")),
        P(),
    )
    def on_device(*arrays):
        rows = (arrays[5].shape[0] + 1) // 2
        fits = mesh.shape["tp"] == 4 and mesh.shape["ctx"] == 2 and HD + 2 * rows <= 128
        fits = fits and arrays[0].shape[0] == mesh.shape["ctx"] and arrays[6].shape[0] <= 128
        return (on_device_images if fits else on_device_rows)(*arrays)

    return jax.shard_map(
        on_device, mesh=mesh, in_specs=in_specs, out_specs=out_specs, check_vma=False
    )
```

```python
from functools import partial
import math

import jax
import jax.numpy as jnp
from jax import lax
from jax.experimental import pallas as pl
from jax.experimental.pallas import tpu as pltpu
from jax.sharding import PartitionSpec as P

D = 1280
H = 16
HD = 80
FF = 5120
COLS = 64
ROWS_DEV = 8


PRECISE = lax.Precision.HIGHEST
EPSILON = 1e-06
NEGATIVE = -1e30


def layer_norm(values_in, gain_vec, shift_vec):
    average = jnp.mean(values_in, -1, keepdims=True)
    centred = values_in - average
    variance = jnp.mean(centred * centred, -1, keepdims=True)
    return centred * lax.rsqrt(variance + EPSILON) * gain_vec + shift_vec


def block_size():
    return 512


def to_heads(flat_rows, heads_local):
    images, length, feat_width = flat_rows.shape
    return flat_rows.reshape(images, length, heads_local, feat_width // heads_local).transpose(
        0, 2, 1, 3
    )


def from_heads(per_head):
    images, heads_local, length, head_dim = per_head.shape
    return per_head.transpose(0, 2, 1, 3).reshape(images, length, heads_local * head_dim)


def block_scores(query_heads, key_flat, rows_bias, cols_bias, first_key, scale_factor):
    key_heads = to_heads(key_flat, query_heads.shape[1])
    key_len = key_flat.shape[1]
    key_rows = key_len // COLS
    scores = scale_factor * jnp.einsum(
        "ihqc,ihkc->ihqk", query_heads, key_heads, preferred_element_type=jnp.float32
    )
    images, heads_local, query_len, unused_len = scores.shape
    row_part = lax.dynamic_slice_in_dim(rows_bias, first_key // COLS, key_rows, 3)
    scores = scores.reshape(images, heads_local, query_len, key_rows, COLS)
    scores = scores + row_part[..., :, None] + cols_bias[..., None, :]
    return scores.reshape(images, heads_local, query_len, key_len)


def relative_terms(query_flat, rows_param, cols_param, first_row, heads_local):
    images, length, feat_width = query_flat.shape
    rows_dev = length // COLS
    grid_rows = (rows_param.shape[0] + 1) // 2
    own_rows = first_row + jnp.arange(rows_dev, dtype=jnp.int32)
    key_rows = jnp.arange(grid_rows, dtype=jnp.int32)
    row_slots = jnp.arange(rows_param.shape[0], dtype=jnp.int32)
    pick_rows = (
        row_slots[None, None, :]
        == own_rows[:, None, None] - key_rows[None, :, None] + grid_rows - 1
    ).astype(jnp.float32)
    table_rows = jnp.einsum("rkj,jc->rkc", pick_rows, rows_param, precision=PRECISE)
    col_ids = jnp.arange(COLS, dtype=jnp.int32)
    col_slots = jnp.arange(cols_param.shape[0], dtype=jnp.int32)
    pick_cols = (
        col_slots[None, None, :] == col_ids[:, None, None] - col_ids[None, :, None] + COLS - 1
    ).astype(jnp.float32)
    table_cols = jnp.einsum("wkj,jc->wkc", pick_cols, cols_param, precision=PRECISE)
    grid_form = query_flat.reshape(images, rows_dev, COLS, heads_local, feat_width // heads_local)
    along_rows = jnp.einsum("irwhc,rkc->ihrwk", grid_form, table_rows, precision=PRECISE).reshape(
        images, heads_local, length, grid_rows
    )
    along_cols = jnp.einsum("irwhc,wkc->ihrwk", grid_form, table_cols, precision=PRECISE).reshape(
        images, heads_local, length, COLS
    )
    return (along_rows, along_cols)


def on_device_rows(
    tokens,
    norm1_gain,
    norm1_bias,
    qkv_weight,
    qv_bias,
    rel_rows,
    rel_cols,
    proj_weight,
    proj_bias,
    norm2_gain,
    norm2_bias,
    fc1_weight,
    fc1_bias,
    fc2_weight,
    fc2_bias,
    cotangent,
):
    scale_factor = HD ** (-0.5)
    tp_count = lax.axis_size("tp")
    ctx_count = lax.axis_size("ctx")
    tp_rank = lax.axis_index("tp")
    ctx_rank = lax.axis_index("ctx")
    grid_rows = ROWS_DEV * ctx_count
    tok_image = grid_rows * COLS
    tok_ctx = ROWS_DEV * COLS
    heads_local = H // tp_count
    width_local = heads_local * HD
    ff_local = FF // tp_count
    images = tokens.shape[0]
    rows_table = rel_rows.astype(jnp.float32)
    cols_table = rel_cols.astype(jnp.float32)
    qkv_full, proj_full, fc1_full, fc2_full = (
        lax.all_gather(qkv_weight, ("shard", "ctx"), axis=1, tiled=True),
        lax.all_gather(proj_weight, ("shard", "ctx"), axis=1, tiled=True),
        lax.all_gather(fc1_weight, ("shard", "ctx"), axis=0, tiled=True),
        lax.all_gather(fc2_weight, ("shard", "ctx"), axis=1, tiled=True),
    )
    qv_local = lax.dynamic_slice_in_dim(qv_bias, tp_rank * width_local, width_local, 1)
    fc1_local = lax.dynamic_slice_in_dim(fc1_bias, tp_rank * ff_local, ff_local, 0)
    resid_in = tokens.astype(jnp.float32)
    normed1 = layer_norm(resid_in, norm1_gain, norm1_bias).astype(jnp.bfloat16)
    normed1_full = lax.all_gather(normed1, "tp", axis=1, tiled=True)
    projected = jnp.einsum(
        "itd,sde->itse", normed1_full, qkv_full, preferred_element_type=jnp.float32
    )
    queries = (projected[:, :, 0] + qv_local[0]).astype(jnp.bfloat16)
    keys_own = projected[:, :, 1].astype(jnp.bfloat16)
    values_own = (projected[:, :, 2] + qv_local[1]).astype(jnp.bfloat16)
    first_row = ctx_rank * ROWS_DEV
    rel_fn = partial(relative_terms, first_row=first_row, heads_local=heads_local)
    (along_rows, along_cols), rel_pull = jax.vjp(
        rel_fn, queries.astype(jnp.float32), rows_table, cols_table
    )
    query_heads = to_heads(queries, heads_local)
    start_state = (
        jnp.full((images, heads_local, tok_ctx), NEGATIVE, jnp.float32),
        jnp.zeros((images, heads_local, tok_ctx), jnp.float32),
        jnp.zeros((images, heads_local, tok_ctx, HD), jnp.float32),
        jnp.zeros((images, tok_image, width_local), jnp.bfloat16),
        jnp.zeros((images, tok_image, width_local), jnp.bfloat16),
    )
    shard_piece = (
        lax.all_gather(keys_own, "ctx", axis=1, tiled=True),
        lax.all_gather(values_own, "ctx", axis=1, tiled=True),
    )
    piece_len = shard_piece[0].shape[1]
    step_len = block_size()

    def one_step(inner, offset):
        run_max, run_sum, run_acc, keys_all, values_all = inner
        key_blk = lax.dynamic_slice_in_dim(shard_piece[0], offset, step_len, 1)
        value_blk = lax.dynamic_slice_in_dim(shard_piece[1], offset, step_len, 1)
        scores = block_scores(query_heads, key_blk, along_rows, along_cols, offset, scale_factor)
        new_max = jnp.maximum(run_max, jnp.max(scores, -1))
        factor = jnp.exp(run_max - new_max)
        weights_blk = jnp.exp(scores - new_max[..., None])
        run_sum = run_sum * factor + jnp.sum(weights_blk, -1)
        value_heads = to_heads(value_blk, heads_local)
        run_acc = run_acc * factor[..., None] + jnp.einsum(
            "ihqk,ihkc->ihqc",
            weights_blk.astype(jnp.bfloat16),
            value_heads,
            preferred_element_type=jnp.float32,
        )
        keys_all = lax.dynamic_update_slice_in_dim(keys_all, key_blk, offset, 1)
        values_all = lax.dynamic_update_slice_in_dim(values_all, value_blk, offset, 1)
        return ((new_max, run_sum, run_acc, keys_all, values_all), None)

    offsets = jnp.arange(piece_len // step_len, dtype=jnp.int32) * step_len
    result, unused = lax.scan(one_step, start_state, offsets)
    run_max, run_sum, run_acc, keys_all, values_all = result
    attn_heads = run_acc / run_sum[..., None]
    log_total = run_max + jnp.log(run_sum)
    attn_low = from_heads(attn_heads).astype(jnp.bfloat16)
    proj_part = jnp.einsum("itd,de->ite", attn_low, proj_full, preferred_element_type=jnp.float32)
    branch = lax.psum_scatter(
        proj_part.astype(jnp.bfloat16), "tp", scatter_dimension=1, tiled=True
    ).astype(jnp.float32)
    middle = resid_in + branch + proj_bias
    normed2 = layer_norm(middle, norm2_gain, norm2_bias).astype(jnp.bfloat16)
    normed2_full = lax.all_gather(normed2, "tp", axis=1, tiled=True)
    hidden_pre = (
        jnp.einsum("itd,df->itf", normed2_full, fc1_full, preferred_element_type=jnp.float32)
        + fc1_local
    )
    gelu_exact = partial(jax.nn.gelu, approximate=False)
    activated_f, gelu_pull = jax.vjp(gelu_exact, hidden_pre)
    activated = activated_f.astype(jnp.bfloat16)
    mlp_part = jnp.einsum("itf,fe->ite", activated, fc2_full, preferred_element_type=jnp.float32)
    mlp_out = lax.psum_scatter(
        mlp_part.astype(jnp.bfloat16), "tp", scatter_dimension=1, tiled=True
    ).astype(jnp.float32)
    output = (middle + mlp_out + fc2_bias).astype(jnp.bfloat16)
    cot_full = lax.all_gather(cotangent, "tp", axis=1, tiled=True)
    d_act = jnp.einsum("ite,fe->itf", cot_full, fc2_full, preferred_element_type=jnp.float32)
    d_hidden = gelu_pull(d_act)[0].astype(jnp.bfloat16)
    fc2_grad = jnp.einsum("itf,ite->fe", activated, cot_full, preferred_element_type=jnp.float32)
    fc1_grad = jnp.einsum("itd,itf->df", normed2_full, d_hidden, preferred_element_type=jnp.float32)
    fc1_bias_part = jnp.sum(d_hidden.astype(jnp.float32), (0, 1))
    fc2_bias_part = jnp.sum(cotangent.astype(jnp.float32), (0, 1))
    d_norm2_part = jnp.einsum("itf,df->itd", d_hidden, fc1_full, preferred_element_type=jnp.float32)
    d_norm2 = lax.psum_scatter(
        d_norm2_part.astype(jnp.bfloat16), "tp", scatter_dimension=1, tiled=True
    ).astype(jnp.float32)
    unused_out, norm2_pull = jax.vjp(layer_norm, middle, norm2_gain, norm2_bias)
    d_mid_part, gain2_part, bias2_part = norm2_pull(d_norm2)
    d_middle = cotangent.astype(jnp.float32) + d_mid_part
    d_branch = d_middle.astype(jnp.bfloat16)
    proj_bias_part = jnp.sum(d_branch.astype(jnp.float32), (0, 1))
    d_branch_full = lax.all_gather(d_branch, "tp", axis=1, tiled=True)
    proj_grad = jnp.einsum(
        "itd,ite->de", attn_low, d_branch_full, preferred_element_type=jnp.float32
    )
    d_attn = jnp.einsum(
        "ite,de->itd", d_branch_full, proj_full, preferred_element_type=jnp.float32
    ).astype(jnp.bfloat16)
    d_attn_heads = to_heads(d_attn, heads_local)
    delta_rows = jnp.sum(d_attn_heads.astype(jnp.float32) * attn_heads, -1)
    key_step = block_size()
    key_rows = key_step // COLS
    key_offsets = jnp.arange(tok_image // key_step, dtype=jnp.int32) * key_step

    def back_step(carried, offset):
        grad_query, grad_rows, grad_cols = carried
        key_blk = lax.dynamic_slice_in_dim(keys_all, offset, key_step, 1)
        value_blk = lax.dynamic_slice_in_dim(values_all, offset, key_step, 1)
        scores = block_scores(query_heads, key_blk, along_rows, along_cols, offset, scale_factor)
        soft_probs = jnp.exp(scores - log_total[..., None])
        value_heads = to_heads(value_blk, heads_local)
        key_heads = to_heads(key_blk, heads_local)
        d_probs = jnp.einsum(
            "ihqc,ihkc->ihqk", d_attn_heads, value_heads, preferred_element_type=jnp.float32
        )
        d_scores = (soft_probs * (d_probs - delta_rows[..., None])).astype(jnp.bfloat16)
        grad_query = grad_query + jnp.einsum(
            "ihqk,ihkc->ihqc", d_scores, key_heads, preferred_element_type=jnp.float32
        )
        grid_scores = d_scores.astype(jnp.float32).reshape(
            images, heads_local, tok_ctx, key_rows, COLS
        )
        row_sums = jnp.sum(grid_scores, 4)
        row_now = lax.dynamic_slice_in_dim(grad_rows, offset // COLS, key_rows, 3)
        grad_rows = lax.dynamic_update_slice_in_dim(
            grad_rows, row_now + row_sums, offset // COLS, 3
        )
        grad_cols = grad_cols + jnp.sum(grid_scores, 3)
        key_part = scale_factor * jnp.einsum(
            "ihqk,ihqc->ikhc", d_scores, query_heads, preferred_element_type=jnp.float32
        )
        value_part = jnp.einsum(
            "ihqk,ihqc->ikhc",
            soft_probs.astype(jnp.bfloat16),
            d_attn_heads,
            preferred_element_type=jnp.float32,
        )
        emitted = (
            key_part.reshape(images, key_step, width_local),
            value_part.reshape(images, key_step, width_local),
        )
        return ((grad_query, grad_rows, grad_cols), emitted)

    back_start = (
        jnp.zeros((images, heads_local, tok_ctx, HD), jnp.float32),
        jnp.zeros((images, heads_local, tok_ctx, grid_rows), jnp.float32),
        jnp.zeros((images, heads_local, tok_ctx, COLS), jnp.float32),
    )
    (grad_query, grad_rows, grad_cols), emitted = lax.scan(back_step, back_start, key_offsets)
    key_terms = emitted[0].transpose(1, 0, 2, 3).reshape(images, tok_image, width_local)
    value_terms = emitted[1].transpose(1, 0, 2, 3).reshape(images, tok_image, width_local)
    grad_keys, grad_values = (
        lax.psum_scatter(
            key_terms.astype(jnp.bfloat16), "ctx", scatter_dimension=1, tiled=True
        ).astype(jnp.float32),
        lax.psum_scatter(
            value_terms.astype(jnp.bfloat16), "ctx", scatter_dimension=1, tiled=True
        ).astype(jnp.float32),
    )
    d_query_rel, rows_grad_part, cols_grad_part = rel_pull((grad_rows, grad_cols))
    d_query = (scale_factor * from_heads(grad_query) + d_query_rel).astype(jnp.bfloat16)
    d_keys = grad_keys.astype(jnp.bfloat16)
    d_values = grad_values.astype(jnp.bfloat16)
    d_projected = jnp.stack((d_query, d_keys, d_values), axis=2)
    qkv_grad = jnp.einsum(
        "itd,itse->sde", normed1_full, d_projected, preferred_element_type=jnp.float32
    )
    qv_bias_part = jnp.stack(
        (
            jnp.sum(d_query.astype(jnp.float32), (0, 1)),
            jnp.sum(d_values.astype(jnp.float32), (0, 1)),
        )
    )
    d_norm1_part = jnp.einsum(
        "itse,sde->itd", d_projected, qkv_full, preferred_element_type=jnp.float32
    )
    d_norm1 = lax.psum_scatter(
        d_norm1_part.astype(jnp.bfloat16), "tp", scatter_dimension=1, tiled=True
    ).astype(jnp.float32)
    unused_in, norm1_pull = jax.vjp(layer_norm, resid_in, norm1_gain, norm1_bias)
    d_in_part, gain1_part, bias1_part = norm1_pull(d_norm1)
    tokens_grad = (d_middle + d_in_part).astype(jnp.bfloat16)
    qkv_out, proj_out, fc1_out, fc2_out = (
        lax.psum_scatter(
            qkv_grad.astype(jnp.bfloat16), ("shard", "ctx"), scatter_dimension=1, tiled=True
        ).astype(jnp.float32),
        lax.psum_scatter(
            proj_grad.astype(jnp.bfloat16), ("shard", "ctx"), scatter_dimension=1, tiled=True
        ).astype(jnp.float32),
        lax.psum_scatter(
            fc1_grad.astype(jnp.bfloat16), ("shard", "ctx"), scatter_dimension=0, tiled=True
        ).astype(jnp.float32),
        lax.psum_scatter(
            fc2_grad.astype(jnp.bfloat16), ("shard", "ctx"), scatter_dimension=1, tiled=True
        ).astype(jnp.float32),
    )
    qv_placed = lax.dynamic_update_slice_in_dim(
        jnp.zeros((2, D), jnp.float32), qv_bias_part, tp_rank * width_local, 1
    )
    fc1_placed = lax.dynamic_update_slice_in_dim(
        jnp.zeros((FF,), jnp.float32), fc1_bias_part, tp_rank * ff_local, 0
    )
    (
        gain1_sum,
        bias1_sum,
        qv_sum,
        rows_sum,
        cols_sum,
        projb_sum,
        gain2_sum,
        bias2_sum,
        fc1b_sum,
        fc2b_sum,
    ) = lax.psum(
        (
            gain1_part,
            bias1_part,
            qv_placed,
            rows_grad_part,
            cols_grad_part,
            proj_bias_part,
            gain2_part,
            bias2_part,
            fc1_placed,
            fc2_bias_part,
        ),
        ("shard", "ctx", "tp"),
    )
    return (
        output,
        tokens_grad,
        gain1_sum,
        bias1_sum,
        qkv_out,
        qv_sum,
        rows_sum,
        cols_sum,
        proj_out,
        projb_sum,
        gain2_sum,
        bias2_sum,
        fc1_out,
        fc1b_sum,
        fc2_out,
        fc2b_sum,
    )


F32 = jnp.float32
BF16 = jnp.bfloat16
NT = (((1,), (1,)), ((), ()))
NN = (((1,), (0,)), ((), ()))
TN = (((0,), (0,)), ((), ()))
VMEM_GRANT = 60 * 2**20
DMA = pltpu.SemaphoreType.DMA
ANY = pl.BlockSpec(memory_space=pl.ANY)
VM = pl.BlockSpec(memory_space=pltpu.VMEM)


def mm(left, right, dims=NN):
    return lax.dot_general(left, right, dims, preferred_element_type=F32)


def lane_ids(shape):
    return lax.broadcasted_iota(jnp.int32, shape, 1)


def place():
    return lax.axis_index("shard"), lax.axis_index("ctx"), lax.axis_index("tp")


def core_mate(t):
    return t + 1 - 2 * lax.rem(t, 2)


def far_mate(t):
    return lax.rem(t + 2, 4)


def aim(src, dst, sems, k, where):
    return pltpu.make_async_remote_copy(
        src_ref=src,
        dst_ref=dst,
        send_sem=sems.at[0, k],
        recv_sem=sems.at[1, k],
        device_id=where,
        device_id_type=pl.DeviceIdType.MESH,
    )


def send(src, dst, sems, k, where):
    copy = aim(src, dst, sems, k, where)
    copy.start()
    return copy


def swap_copy(src, dst, sems):
    _, c, _ = place()
    return pltpu.make_async_remote_copy(
        src_ref=src,
        dst_ref=dst,
        send_sem=sems.at[0, 0],
        recv_sem=sems.at[1, 0],
        device_id={"ctx": 1 - c},
        device_id_type=pl.DeviceIdType.MESH,
    )


def fill_tables(tab_ref, rr_ref, rc_ref):
    tab_ref[...] = jnp.zeros_like(tab_ref)
    tab_ref[0 : rr_ref.shape[0], 0 : rr_ref.shape[1]] = rr_ref[...]
    tab_ref[128 : 128 + rc_ref.shape[0], 0 : rc_ref.shape[1]] = rc_ref[...]


def fill_hots(hot_ref, hd, cols, rows, second):
    shift = cols.bit_length() - 1
    down = lax.broadcasted_iota(jnp.int32, hot_ref.shape, 0)
    kr = lax.shift_right_logical(down, shift)
    kw = down & (cols - 1)
    l = lane_ids(hot_ref.shape)
    if second:
        hit = (l == hd + rows - 1 - kr) | (l == 128 + cols - 1 - kw)
    else:
        hit = (l == hd + kr) | (l == hd + rows + kr) | (l == 128 + kw) | (l == 192 + kw)
    hot_ref[...] = jnp.where(hit, 1.0, 0.0).astype(BF16)


def reverser(top):
    down = lax.broadcasted_iota(jnp.int32, (128, 128), 0)
    return jnp.where(down + lane_ids((128, 128)) == top, 1.0, 0.0).astype(BF16)


def greet(shards, line=False):
    s, c, t = place()
    size = 2 * shards
    at = s * (1 - c) + (size - 1 - s) * c
    peers = [{"ctx": 1 - c}, {"tp": core_mate(t)}, {"tp": far_mate(t)}]
    for step in (1, size - 1):
        to = lax.rem(at + step, size)
        back = to // shards
        peers.append({"shard": to * (1 - back) + (size - 1 - to) * back, "ctx": back})
    if line:
        peers += [{"shard": lax.rem(s + d, shards)} for d in range(1, shards)]
    barrier = pltpu.get_barrier_semaphore()
    for peer in peers:
        pl.semaphore_signal(barrier, inc=1, device_id=peer, device_id_type=pl.DeviceIdType.MESH)
    pl.semaphore_wait(barrier, len(peers))


class Ring:
    def __init__(self, shards, block, sems):
        s, c, _ = place()
        self.shards, self.size, self.sems = shards, 2 * shards, sems
        self.at = s * (1 - c) + (self.size - 1 - s) * c
        self.half = block // 2
        self.pieces = ring_pieces(block)
        self.rows = self.half // self.pieces
        self.first, self.end = self.pieces, self.pieces * (self.size - 1)
        self.now = self.first

    def coords(self, position):
        back = position // self.shards
        return position * (1 - back) + (self.size - 1 - position) * back, back

    def peer(self, way):
        to = lax.rem(self.at + (1 if way == 0 else self.size - 1), self.size)
        shard, ctx = self.coords(to)
        return {"shard": shard, "ctx": ctx}

    def owner(self, offset):
        shard, ctx = self.coords(lax.rem(self.at + 2 * self.size + offset, self.size))
        return 2 * shard + ctx

    def split(self, event):
        if isinstance(event, int):
            return event // self.pieces, event % self.pieces
        return lax.div(event, self.pieces), lax.rem(event, self.pieces)

    def rows_of(self, way, piece):
        start = way * self.half + piece * self.rows
        return pl.ds(start if isinstance(start, int) else pl.multiple_of(start, self.rows), self.rows)

    def make(self, src, dst, way, event):
        slot = way * self.end + event
        return pltpu.make_async_remote_copy(
            src_ref=src,
            dst_ref=dst,
            send_sem=self.sems.at[0, slot],
            recv_sem=self.sems.at[1, slot],
            device_id=self.peer(way),
            device_id_type=pl.DeviceIdType.MESH,
        )

    def run(self, low, high):
        low, high = max(low, self.first), min(high, self.end)
        if low < high:
            lax.fori_loop(low, high, lambda event, _: (self.step(event), 0)[1], 0)

    def tick(self, count):
        self.run(self.now, self.now + count)
        self.now += count

    def poll(self, event):
        pl.when((event >= self.first) & (event < self.end))(lambda: self.step(event))


def ring_pieces(block):
    return 5 if block % 160 == 0 else 1


def ring_sems(shards, block):
    return DMA((2, 2 * ring_pieces(block) * (2 * shards - 1)))


class Spread(Ring):
    def __init__(self, shards, src, dst, sems, local):
        super().__init__(shards, src.shape[0], sems)
        self.src, self.dst = src, dst
        self.local = pltpu.make_async_copy(src, dst.at[self.owner(0)], local)
        self.local.start()
        for event in range(self.first):
            for way in range(2):
                self.hop(way, event, True).start()

    def hop(self, way, event, own=False):
        j, piece = self.split(event)
        rows = self.rows_of(way, piece)
        there = self.dst.at[self.owner(-j if way == 0 else j), rows]
        return self.make(self.src.at[rows] if own else there, there, way, event)

    def step(self, event):
        for way in range(2):
            self.hop(way, event - self.pieces).wait_recv()
            self.hop(way, event).start()

    def finish(self):
        self.local.wait()
        for way in range(2):
            for event in range(self.end - self.pieces, self.end):
                self.hop(way, event).wait_recv()

        def sent(event, _):
            for way in range(2):
                self.hop(way, event).wait_send()
            return 0

        lax.fori_loop(0, self.end, sent, 0)

    @staticmethod
    def scratch(shards, block):
        return [ring_sems(shards, block[0]), DMA]


class Collect(Ring):
    def __init__(self, shards, src, held, sems):
        super().__init__(shards, src.shape[0] // (2 * shards), sems)
        self.src, self.held, self.block = src, held, src.shape[0] // (2 * shards)

    def begin(self):
        for event in range(self.first):
            for way in range(2):
                self.hop(way, event, True).start()

    def pair_rows(self, n, j):
        offset = (n + 1) * (2 * j - 1)
        last = (2 * n + j + 1) // self.size
        return pl.ds(pl.multiple_of(self.owner(offset * (1 - last)) * self.block, self.rows), self.block)

    def own(self, way, j, piece):
        ahead = self.size - 1 - j
        start = self.owner(ahead if way == 0 else -ahead) * self.block + way * self.half + piece * self.rows
        return pl.ds(pl.multiple_of(start, self.rows), self.rows)

    def hop(self, way, event, own=False):
        j, piece = self.split(event)
        rows = self.rows_of(0, piece)
        there = self.held.at[way, j, rows]
        here = self.src.at[self.own(way, j, piece)] if own else self.held.at[way, j - 1, rows]
        return self.make(here, there, way, event)

    def arrived(self, way, event):
        j, piece = self.split(event)
        there = self.held.at[way, j, self.rows_of(0, piece)]
        self.make(there, there, way, event).wait_recv()

    def step(self, event):
        j, piece = self.split(event)
        rows = self.rows_of(0, piece)
        for way in range(2):
            self.arrived(way, event - self.pieces)
            both = self.held[way, j - 1, rows].astype(F32) + self.src[self.own(way, j, piece)].astype(F32)
            self.held[way, j - 1, rows] = both.astype(BF16)
            self.hop(way, event).start()

    def finish(self, out):
        for piece in range(self.pieces):
            for way in range(2):
                self.arrived(way, self.end - self.pieces + piece)
                last = self.held[way, self.size - 2, self.rows_of(0, piece)].astype(F32)
                own = self.src[self.own(way, self.size - 1, piece)].astype(F32)
                out[self.rows_of(way, piece)] = last + own

        def sent(event, _):
            for way in range(2):
                j, piece = self.split(event)
                there = self.held.at[way, j, self.rows_of(0, piece)]
                self.make(there, there, way, event).wait_send()
            return 0

        lax.fori_loop(0, self.end, sent, 0)

    @staticmethod
    def scratch(shards, block):
        return [pltpu.VMEM((2, 2 * shards - 1, block[0] // 2, block[1]), BF16), ring_sems(shards, block[0])]


class Share:
    def __init__(self, full, sems):
        self.full, self.sems = full, sems

    def copies(self, k, p, src=None):
        _, _, t = place()
        block, passed = self.full.at[p, t], self.full.at[p, far_mate(t)]
        src = block if src is None else src
        return (
            partial(aim, src, block, self.sems, 3 * k, {"tp": far_mate(t)}),
            partial(aim, src, block, self.sems, 3 * k + 1, {"tp": core_mate(t)}),
            partial(aim, passed, passed, self.sems, 3 * k + 2, {"tp": core_mate(t)}),
        )

    def push(self, k, p, src=None):
        for copy in self.copies(k, p, src)[:2]:
            copy().start()

    def forward(self, k, p):
        far, _, third = self.copies(k, p)
        far().wait_recv()
        third().start()

    def finish(self, k, p):
        far, core, third = self.copies(k, p)
        far().wait_send()
        core().wait()
        third().wait()


class Gather2:
    def __init__(self, part, mate, far, out, sems):
        self.part, self.mate, self.far, self.out, self.sems = part, mate, far, out, sems

    def copies(self, p):
        _, _, t = place()
        m = core_mate(t)
        return (
            partial(aim, self.part.at[p, far_mate(m)], self.mate.at[p, 1], self.sems, 3 * p, {"tp": m}),
            partial(aim, self.part.at[p, m], self.mate.at[p, 0], self.sems, 3 * p + 1, {"tp": m}),
            partial(aim, self.out.at[p], self.far.at[p], self.sems, 3 * p + 2, {"tp": far_mate(t)}),
        )

    def push(self, p):
        for copy in self.copies(p)[:2]:
            copy().start()

    def forward(self, p):
        _, _, t = place()
        passing, _, onward = self.copies(p)
        passing().wait_recv()
        both = self.part[p, far_mate(t)].astype(F32) + self.mate[p, 1].astype(F32)
        self.out[p] = both.astype(BF16)
        onward().start()

    def result(self, p):
        _, _, t = place()
        _, own, onward = self.copies(p)
        own().wait_recv()
        onward().wait_recv()
        return self.part[p, t].astype(F32) + self.mate[p, 0].astype(F32) + self.far[p].astype(F32)

    def finish(self, p):
        for copy in self.copies(p):
            copy().wait_send()

    @staticmethod
    def scratch(block):
        return [
            pltpu.VMEM((2, 2) + block, BF16),
            pltpu.VMEM((2,) + block, BF16),
            pltpu.VMEM((2,) + block, BF16),
            DMA((2, 6)),
        ]


def ln_stats(values):
    average = jnp.mean(values, -1, keepdims=True)
    centred = values - average
    inverse = lax.rsqrt(jnp.mean(centred * centred, -1, keepdims=True) + EPSILON)
    return centred * inverse, inverse


def ln_back(unit, inverse, gain, grad):
    scaled = grad * gain
    first = jnp.mean(scaled, -1, keepdims=True)
    second = jnp.mean(scaled * unit, -1, keepdims=True)
    return inverse * (scaled - first - unit * second)


class Stream:
    def __init__(self, loads, stores, sems):
        self.loads, self.stores, self.sems, self.flying = loads, stores, sems, []

    def need(self, *operands):
        for i in operands:
            if i in self.loads:
                self.loads.pop(i).wait()

    def put(self, j, half=None):
        src, dst, q = self.stores[j]
        if half is not None:
            size = src.shape[0] // 2
            src, dst = src.at[half * size : (half + 1) * size], dst.at[half * size : (half + 1) * size]
        copy = pltpu.make_async_copy(src, dst, self.sems.at[2 * q + (half or 0)])
        copy.start()
        self.flying.append((j, copy))

    def close(self):
        self.need(*list(self.loads))
        done = [j for j, _ in self.flying]
        for j in self.stores:
            if j not in done:
                self.put(j)
        for _, copy in self.flying:
            copy.wait()


def comm_call(kernel, name, ident, args, outs, scratch, hbm_in=(), hbm_out=(), late=(), early=()):
    count, results, own = len(args), len(outs), len(scratch)

    def body(*refs):
        ins, out = list(refs[:count]), list(refs[count : count + results])
        inner = refs[count + results : count + results + own]
        extra = refs[count + results + own :]
        buffers, load_sems, store_sems = extra[:-2], extra[-2], extra[-1]
        loads, stores = {}, {}
        for q, i in enumerate(late):
            loads[i] = pltpu.make_async_copy(ins[i], buffers[q], load_sems.at[q])
            loads[i].start()
            ins[i] = buffers[q]
        for q, j in enumerate(early):
            held = buffers[len(late) + q]
            stores[j] = (held, out[j], q)
            out[j] = held
        stream = Stream(loads, stores, store_sems)
        kernel(stream, *ins, *out, *inner)
        stream.close()

    return pl.pallas_call(
        body,
        out_shape=tuple(outs),
        in_specs=[ANY if i in hbm_in or i in late else VM for i in range(count)],
        out_specs=tuple(ANY if j in hbm_out or j in early else VM for j in range(results)),
        scratch_shapes=list(scratch)
        + [pltpu.VMEM(args[i].shape, args[i].dtype) for i in late]
        + [pltpu.VMEM(outs[j].shape, outs[j].dtype) for j in early]
        + [DMA((max(len(late), 1),)), DMA((max(2 * len(early), 1),))],
        compiler_params=pltpu.CompilerParams(
            vmem_limit_bytes=VMEM_GRANT, collective_id=ident, has_side_effects=True
        ),
        name=name,
    )(*args)


def turned(out_ref, full_ref, p):
    count, length = full_ref.shape[1:3]

    def one(i, _):
        start = pl.multiple_of((p * count + i) * length, 128)
        out_ref[:, pl.ds(start, length)] = full_ref[p, i].T
        return 0

    lax.fori_loop(0, count, one, 0)


def front_kernel(
    shards, io, tok_ref, qkvw_ref, pw_ref, vec_ref, x_ref, a_ref, wf_ref, at_ref,
    w1_ref, swap_sems, share_sems, w_sems, w_local,
):
    s, c, t = place()
    wide = qkvw_ref.shape[2]
    for j in range(3):
        w1_ref[:, j * wide : (j + 1) * wide] = qkvw_ref[j]
    w1_ref[:, 3 * wide : 4 * wide] = pw_ref[...]
    greet(shards)
    swap = send(tok_ref.at[1 - c], x_ref.at[c], swap_sems, 0, {"ctx": 1 - c})
    spread = Spread(shards, w1_ref, wf_ref, w_sems, w_local)
    share = Share(a_ref, share_sems)

    def norm(block):
        unit, _ = ln_stats(block.astype(F32))
        return (unit * vec_ref[0:1, :] + vec_ref[1:2, :]).astype(BF16)

    own = tok_ref[c]
    x_ref[c] = own
    a_ref[c, t] = norm(own)
    share.push(0, c)
    swap.wait()
    a_ref[1 - c, t] = norm(x_ref[1 - c])
    share.push(1, 1 - c)
    share.forward(0, c)
    spread.tick(9)
    share.forward(1, 1 - c)
    spread.tick(6)
    share.finish(0, c)
    share.finish(1, 1 - c)
    io.put(0)
    io.put(1)
    turned(at_ref, a_ref, 0)
    spread.tick(2)
    spread.tick(4)
    turned(at_ref, a_ref, 1)
    io.put(3)
    spread.tick(2)
    spread.tick(spread.end)
    spread.finish()


def fwd_kernel(
    shards, heads, hd, cols, rows, qb, io,
    a1_ref, w1_ref, vec_ref, rr_ref, rc_ref, cot_ref, w_ref,
    vh_ref, oh_ref, ob_ref, lse_ref, qa_ref, ka_ref, g_ref, cf_ref, wf_ref, pp_ref,
    qh_ref, vt_ref, rt_ref, tab_ref, hot_ref, swap_sems, share_sems, w_sems, w_local,
):
    _, me, t = place()
    tok, width = ob_ref.shape
    wide = 3 * width
    blocks = tok // qb
    fill_tables(tab_ref, rr_ref, rc_ref)
    fill_hots(hot_ref, hd, cols, rows, False)
    rt_ref[0:128, :] = mm(reverser(2 * rows - 2), tab_ref[0:128, :]).astype(BF16)
    rt_ref[128:256, :] = mm(reverser(2 * cols - 2), tab_ref[128:256, :]).astype(BF16)
    greet(shards)
    swap = swap_copy(cot_ref.at[1 - me], g_ref.at[me], swap_sems)
    swap.start()
    spread = Spread(shards, w_ref, wf_ref, w_sems, w_local)
    share = Share(cf_ref, share_sems)
    own = cot_ref[me]
    g_ref[me] = own
    cf_ref[me, t] = own
    share.push(0, me, cot_ref.at[me])

    io.need(0, 1)

    def project(i, _):
        at = pl.ds(pl.multiple_of(i * qb, qb), qb)
        tile = (mm(a1_ref[at, :], w1_ref[:, 0:wide]) + vec_ref[7:8, 0:wide]).astype(BF16)
        pad = jnp.zeros((qb, 128 - hd), BF16)
        front = lane_ids((qb, 128)) < hd
        for h in range(heads):
            part = [tile[:, (j * heads + h) * hd : (j * heads + h + 1) * hd] for j in range(3)]
            part = [jnp.concatenate([x, pad], 1) for x in part]
            qh_ref[h, at, :] = part[0]
            ka_ref[h, at, 0:128] = jnp.where(front, part[1], hot_ref[at, 0:128])
            ka_ref[h, at, 128:256] = hot_ref[at, 128:256]
            vh_ref[h, at, :] = part[2]
        return 0

    lax.fori_loop(0, blocks, project, 0)
    io.put(0)
    io.put(5)
    swap.wait()
    cf_ref[1 - me, t] = g_ref[1 - me]
    share.push(1, 1 - me, g_ref.at[1 - me])
    c = hd**-0.5 * math.log2(math.e)
    up = hd**0.5

    def head(h, _):
        vt_ref[...] = vh_ref[h].T
        terms = mm(qh_ref[h], rt_ref[...], NT) * up
        ln = lane_ids((cols, 128))
        for r in range(rows):
            rs = slice(r * cols, (r + 1) * cols)
            tr = pltpu.roll(terms[rs, 0:128], (65 + r) % 128, 1)
            tc = pltpu.roll(terms[rs, 128:256], 65, 1, stride=1, stride_axis=0)
            rh = tr.astype(BF16).astype(F32)
            rl = pltpu.roll(tr - rh, rows, 1)
            ch = tc.astype(BF16).astype(F32)
            cl = pltpu.roll(tc - ch, 64, 1)
            low = jnp.where(ln < hd + 2 * rows, rl, jnp.zeros_like(tr))
            left = jnp.where(ln < hd, qh_ref[h, rs, :].astype(F32), jnp.where(ln < hd + rows, rh, low))
            qa_ref[h, rs, 0:128] = left.astype(BF16)
            qa_ref[h, rs, 128:256] = jnp.where(ln < 64, ch, cl).astype(BF16)

        def blk(i, _):
            at = pl.ds(pl.multiple_of(i * qb, qb), qb)
            s = mm(ka_ref[h], qa_ref[h, at, :], NT)
            m = jnp.max(s, 0, keepdims=True)
            p = jnp.exp2((s - m) * c)
            l = jnp.sum(p, 0, keepdims=True)
            lse_ref[h, :, at] = m * c + jnp.log2(l)
            oh_ref[h, at, :] = (mm(vt_ref[...], p.astype(BF16)) / l).T
            turn = h * blocks + i
            event = spread.first + turn + (turn + 1) // 2
            spread.poll(event)
            pl.when(turn % 2 == 0)(lambda: spread.poll(event + 1))
            return 0

        lax.fori_loop(0, blocks, blk, 0)
        pl.when(h == 0)(lambda: share.forward(0, me))
        pl.when(h == min(1, heads - 1))(lambda: share.forward(1, 1 - me))
        return 0

    lax.fori_loop(0, heads, head, 0)
    io.put(1)
    io.put(4)
    for h in range(heads):
        ob_ref[:, h * hd : (h + 1) * hd] = oh_ref[h, :, 0:hd].astype(BF16)

    io.put(2)
    done = spread.first + heads * blocks * 3 // 2

    def out_rows(i, _):
        at = pl.ds(pl.multiple_of(i * qb, qb), qb)
        pp_ref[at, :] = mm(ob_ref[at, :], w1_ref[:, wide:], NT).astype(BF16)
        for k in range(2):
            spread.poll(done + 2 * i + k)
        return 0

    lax.fori_loop(0, blocks, out_rows, 0)
    io.put(9)
    spread.run(done + 2 * blocks, spread.end)
    share.finish(0, me)
    share.finish(1, 1 - me)
    io.put(7)
    spread.finish()


def mid_kernel(
    shards, io, part_ref, x_ref, vec_ref, w_ref, f1_ref, cf_ref,
    mid_ref, a_ref, wf_ref, act_ref, slope_ref, ct_ref,
    mate, far, outb, sum_sems, share_sems, w_sems, w_local,
):
    _, _, t = place()
    greet(shards)
    gather = Gather2(part_ref, mate, far, outb, sum_sems)
    io.need(0)
    gather.push(0)
    gather.push(1)
    spread = Spread(shards, w_ref, wf_ref, w_sems, w_local)
    share = Share(a_ref, share_sems)
    gather.forward(0)
    gather.forward(1)
    io.need(5, 1)
    turned(ct_ref, cf_ref, 0)
    spread.tick(8)
    for p in range(2):
        mid = x_ref[p].astype(F32) + gather.result(p) + vec_ref[2:3, :]
        mid_ref[p] = mid
        unit, _ = ln_stats(mid)
        a_ref[p, t] = (unit * vec_ref[3:4, :] + vec_ref[4:5, :]).astype(BF16)
        share.push(p, p)
        if p == 1:
            turned(ct_ref, cf_ref, 1)
            io.put(0)
            io.put(5)
        spread.tick(7)
    share.forward(0, 0)
    half = a_ref.shape[1] * a_ref.shape[2]

    def hidden(p):
        def one(i, _):
            rows = a_ref[p, pl.ds(2 * i, 2)].reshape(-1, a_ref.shape[3])
            pre = mm(rows, f1_ref[...]) + vec_ref[6:7, :]
            cdf = 0.5 * (1.0 + lax.erf(pre * (2.0**-0.5)))
            bell = jnp.exp(-0.5 * pre * pre) * ((2.0 * math.pi) ** -0.5)
            at = pl.ds(pl.multiple_of(p * half + i * rows.shape[0], 128), rows.shape[0])
            act_ref[at, :] = (pre * cdf).astype(BF16)
            slope_ref[at, :] = cdf + pre * bell
            for k in range(2):
                spread.poll(base + 2 * i + k)
            return 0

        base = spread.now
        lax.fori_loop(0, a_ref.shape[1] // 2, one, 0)
        spread.now += a_ref.shape[1]

    share.finish(0, 0)
    io.need(4)
    hidden(0)
    io.put(3, 0)
    io.put(4, 0)
    spread.tick(spread.end)
    share.forward(1, 1)
    share.finish(1, 1)
    io.put(1)
    hidden(1)
    io.put(4, 1)
    io.put(3, 1)
    for p in range(2):
        gather.finish(p)
    spread.finish()


def turn_kernel(
    shards, io, ct_ref, act_ref, slope_ref, cot_ref, f2_ref, f1_ref, a2_ref, mid_ref, g_ref, vec_ref, w1_ref,
    dm_ref, dbt_ref, wg_ref, sums_ref, f1g_ref, mlp_ref, do_ref,
    db_ref, w2g_ref, part_ref, dp_ref, mate, far, outb, sum_sems, share_sems, w_held, w_sems,
):
    _, _, t = place()
    greet(shards)
    collect = Collect(shards, w2g_ref, w_held, w_sems)
    gather = Gather2(part_ref, mate, far, outb, sum_sems)
    share = Share(db_ref, share_sems)
    tile = 2 * db_ref.shape[2]
    halves = db_ref.shape[1] // 2
    sums_ref[...] = jnp.zeros_like(sums_ref)
    step = collect.pieces

    io.need(0, 1, 2, 3, 4, 5)

    def back(n, _):
        def block(j, _):
            at = collect.pair_rows(n, j)
            w2g_ref[at, :] = mm(ct_ref[at, :], act_ref[...]).astype(BF16)
            return 0

        def blocks():
            lax.fori_loop(0, 2, block, 0)

        pl.when(n < halves)(lambda: blocks())
        pl.when(n == 0)(collect.begin)
        p, i = n // halves, n % halves
        at = pl.ds(pl.multiple_of(n * tile, tile), tile)
        d_pre = (mm(cot_ref[at, :], f2_ref[...]) * slope_ref[at, :]).astype(BF16)
        dp_ref[at, :] = d_pre
        sums_ref[4:5, :] += jnp.sum(d_pre.astype(F32), 0, keepdims=True)
        for k in range(2):
            collect.poll(step * n - 2 + k)
        pl.when(n == halves)(lambda: gather.forward(0))
        d_a2 = mm(d_pre, f1_ref[...], NT).astype(BF16)
        part_ref[p, pl.ds(2 * i, 2)] = d_a2.reshape(2, tile // 2, -1)
        pl.when(n == halves - 1)(lambda: gather.push(0))
        pl.when(n == 2 * halves - 1)(lambda: gather.push(1))
        pl.when(n >= halves)(lambda: blocks())
        for k in range(2, step):
            collect.poll(step * n - 2 + k)
        return 0

    lax.fori_loop(0, 2 * halves, back, 0)
    base = 2 * halves * step - 2

    def hidden_grad(i, _):
        at = pl.ds(pl.multiple_of(i * 256, 256), 256)
        f1g_ref[at, :] = mm(a2_ref[:, at], dp_ref[...], TN).astype(BF16)
        collect.poll(base + i)
        pl.when(i == 0)(lambda: gather.forward(1))

        @pl.when((i == 1) | (i == count - 1))
        def _():
            p = lax.div(i, count - 1)
            unit, inverse = ln_stats(mid_ref[p])
            g = g_ref[p].astype(F32)
            da = gather.result(p)
            dm = g + ln_back(unit, inverse, vec_ref[3:4, :], da)
            dm_ref[p] = dm
            low_dm = dm.astype(BF16)
            db_ref[p, t] = low_dm
            share.push(p, p)
            for k, term in enumerate((da * unit, da, low_dm.astype(F32), g)):
                sums_ref[k : k + 1, :] += jnp.sum(term, 0, keepdims=True)

        return 0

    count = f1g_ref.shape[0] // 256
    io.need(6, 7, 8)
    lax.fori_loop(0, count, hidden_grad, 0)
    io.put(0)
    io.put(4)
    base2 = base + count

    def mlp(n, _):
        at = pl.ds(pl.multiple_of(n * tile, tile), tile)
        mlp_ref[at, :] = mm(act_ref[at, :], f2_ref[...], NT).astype(BF16)
        for k in range(2):
            collect.poll(base2 + 2 * n + k)
        pl.when(n == 2 * halves - 1)(lambda: share.forward(0, 0))
        return 0

    lax.fori_loop(0, 2 * halves, mlp, 0)
    io.put(5)
    collect.run(base2 + 4 * halves, collect.end)
    share.forward(1, 1)
    wide = do_ref.shape[1]
    io.need(10)

    def d_o(n, _):
        p, i = n // halves, n % halves
        pl.when(i == 0)(lambda: share.finish(p, p))
        rows = db_ref[p, pl.ds(2 * i, 2)].reshape(tile, -1)
        at = pl.ds(pl.multiple_of(n * tile, tile), tile)
        do_ref[at, :] = mm(rows, w1_ref[:, 3 * wide :]).astype(BF16)
        dbt_ref[:, at] = rows.T
        return 0

    lax.fori_loop(0, 2 * halves, d_o, 0)
    io.put(1)
    io.put(6)
    for p in range(2):
        gather.finish(p)
    collect.finish(wg_ref)


def bwd_kernel(
    shards, heads, hd, cols, rows, qb, io,
    qa_ref, ka_ref, vh_ref, do_ref, oh_ref, lse_ref, rr_ref, rc_ref, w_ref, part_ref, mid_ref, vec_ref,
    dqkv_ref, rg_ref, wg_ref, qs_ref, out_ref,
    doh_ref, dh_ref, kt_ref, acc_k, acc_v, del_ref, tab_ref, hot_ref, res_ref,
    mate, far, outb, sum_sems, swap_sems, w_held, w_sems,
):
    fill_tables(tab_ref, rr_ref, rc_ref)
    fill_hots(hot_ref, hd, cols, rows, True)
    _, me, _ = place()
    greet(shards)
    gather = Gather2(part_ref, mate, far, outb, sum_sems)
    io.need(9)
    gather.push(0)
    gather.push(1)
    swap = swap_copy(res_ref.at[1 - me], out_ref.at[me], swap_sems)
    collect = Collect(shards, w_ref, w_held, w_sems)
    io.need(8)
    collect.begin()
    io.need(3)
    tok, wide = dqkv_ref.shape
    blocks = tok // qb
    for h in range(heads):
        pad = jnp.zeros((tok, 128 - hd), BF16)
        doh_ref[h] = jnp.concatenate([do_ref[:, h * hd : (h + 1) * hd], pad], 1)
    gather.forward(0)
    gather.forward(1)
    scale = hd**-0.5
    c = scale * math.log2(math.e)
    rg_ref[...] = jnp.zeros_like(rg_ref)

    io.need(0, 1, 2, 4, 10)

    def head(h, _):
        kt_ref[0:128, :] = jnp.where(lane_ids((tok, 128)) < hd, ka_ref[h, :, 0:128], hot_ref[:, 0:128]).T
        kt_ref[128:256, :] = hot_ref[:, 128:256].T
        del_ref[...] = lax.dot_general(
            jnp.ones((8, 128), F32), doh_ref[h].astype(F32) * oh_ref[h], NT,
            preferred_element_type=F32, precision=PRECISE,
        )
        acc_k[...] = jnp.zeros_like(acc_k)
        acc_v[...] = jnp.zeros_like(acc_v)

        def blk(i, _):
            at = pl.ds(pl.multiple_of(i * qb, qb), qb)
            qblk = qa_ref[h, at, :]
            dob = doh_ref[h, at, :]
            s = mm(ka_ref[h], qblk, NT)
            p = jnp.exp2(s * c - lse_ref[h, :, at])
            dp = mm(vh_ref[h], dob, NT)
            ds = (p * (dp - del_ref[0:1, at])).astype(BF16)
            acc_v[...] += mm(p.astype(BF16), dob)
            acc_k[...] += mm(ds, qblk[:, 0:128])
            dqa = mm(kt_ref[...], ds).T
            ln = lane_ids((cols, 128))
            parts = []
            for j in range(qb // cols):
                r = i * (qb // cols) + j
                js = slice(j * cols, (j + 1) * cols)
                dr = dqa[js, 0:128]
                dr = jnp.where((ln >= hd) & (ln < hd + rows), dr, 0.0)
                dr = pltpu.roll(dr, lax.rem(48 + r, 128), 1)
                dc = pltpu.roll(dqa[js, 128:256], 0, 1, stride=1, stride_axis=0)
                parts.append(jnp.concatenate([dr, dc], 1))
            d = jnp.concatenate(parts, 0).astype(BF16)
            rel = mm(d, tab_ref[...])
            rg_ref[...] += mm(d, qblk[:, 0:128], TN)
            dh_ref[h, at, :] = (scale * dqa[:, 0:128] + rel).astype(BF16)
            for k in range(2):
                collect.poll(collect.first + 2 * (h * blocks + i) + k)
            return 0

        lax.fori_loop(0, blocks, blk, 0)
        dh_ref[heads + h] = (scale * acc_k[...]).astype(BF16)
        dh_ref[2 * heads + h] = acc_v[...].astype(BF16)

        @pl.when(h == min(2, heads - 1))
        def _():
            for p in range(2):
                total = mid_ref[p] + gather.result(p) + vec_ref[5:6, :]
                res_ref[p] = total.astype(BF16)

        return 0

    lax.fori_loop(0, heads, head, 0)
    swap.start()
    out_ref[me] = res_ref[me]
    for j in range(3 * heads):
        dqkv_ref[:, j * hd : (j + 1) * hd] = dh_ref[j, :, 0:hd]
    io.put(0)
    collect.run(collect.first + 2 * heads * blocks, collect.end)
    qs_ref[...] = mm(jnp.ones((8, tok), BF16), dqkv_ref[...])
    for p in range(2):
        gather.finish(p)
    collect.finish(wg_ref)
    swap.wait()


def end_kernel(
    shards, io, x_ref, dm_ref, vec_ref, at_ref, dqkv_ref, dbt_ref, ob_ref, small_ref, w1_ref,
    grad_ref, qg_ref, pg_ref, total_ref,
    w1g_ref, wg_ref, part_ref, gres_ref, mate, far, outb, sum_sems, swap_sems,
    held, got, line, small_sems, w_held, w_sems,
):
    s, me, t = place()
    greet(shards, True)
    gather = Gather2(part_ref, mate, far, outb, sum_sems)
    collect = Collect(shards, w1g_ref, w_held, w_sems)
    wide = dqkv_ref.shape[1]
    tile = 2 * part_ref.shape[2]
    halves = part_ref.shape[1] // 2
    step = collect.pieces

    io.need(4, 8, 3, 5, 6)

    def back(n, _):
        def block(j, _):
            at = collect.pair_rows(n, j)
            w1g_ref[at, 0:wide] = mm(at_ref[at, :], dqkv_ref[...]).astype(BF16)
            w1g_ref[at, wide:] = mm(dbt_ref[at, :], ob_ref[...]).astype(BF16)
            return 0

        lax.fori_loop(0, 2, block, 0)
        pl.when(n == 0)(collect.begin)
        for k in range(2):
            collect.poll(step * n + k)
        pl.when(n == 2)(lambda: gather.forward(1))

        def rows_of(i, _):
            rows = pl.ds(pl.multiple_of((n * halves + i) * tile, tile), tile)
            d_a1 = mm(dqkv_ref[rows, :], w1_ref[:, 0:wide], NT).astype(BF16)
            part_ref[n, pl.ds(2 * i, 2)] = d_a1.reshape(2, tile // 2, -1)
            return 0

        @pl.when(n < 2)
        def _():
            lax.fori_loop(0, halves, rows_of, 0)
            gather.push(n)

        for k in range(2, step):
            collect.poll(step * n + k)
        pl.when(n == 1)(lambda: gather.forward(0))
        return 0

    lax.fori_loop(0, 2 * halves, back, 0)
    collect.now = step * 2 * halves
    held[0] = small_ref[...]
    io.need(0, 1)
    for p in range(2):
        unit, inverse = ln_stats(x_ref[p].astype(F32))
        collect.tick(1)
        da = gather.result(p)
        gres_ref[p] = (dm_ref[p] + ln_back(unit, inverse, vec_ref[0:1, :], da)).astype(BF16)
        held[0, 0:1, :] += jnp.sum(da * unit, 0, keepdims=True)
        held[0, 1:2, :] += jnp.sum(da, 0, keepdims=True)
        collect.tick(1)
    grad_ref[me] = gres_ref[me]
    swap = swap_copy(gres_ref.at[1 - me], grad_ref.at[me], swap_sems)
    waits = []
    for k, peer in enumerate(({"tp": core_mate(t)}, {"tp": far_mate(t)}, {"ctx": 1 - me})):
        copy = send(held.at[k], got.at[k], small_sems, k, peer)
        if k == 2:
            swap.start()
        collect.tick(2)
        copy.wait_recv()
        waits.append(copy)
        held[k + 1] = held[k] + got[k]
    line[s] = held[3]
    for d in range(1, shards):
        waits.append(send(held.at[3], line.at[s], small_sems, 2 + d, {"shard": lax.rem(s + d, shards)}))
    collect.tick(collect.end)
    collect.finish(wg_ref)
    part = wide // 3
    for j in range(3):
        qg_ref[j] = wg_ref[:, j * part : (j + 1) * part]
    pg_ref[...] = wg_ref[:, wide:]
    for k, copy in enumerate(waits):
        if k < 3:
            copy.wait_send()
        else:
            copy.wait()
    acc = line[0]
    for k in range(1, shards):
        acc = acc + line[k]
    total_ref[...] = acc
    for p in range(2):
        gather.finish(p)
    swap.wait()


def settle_kernel(rows, *refs):
    count = (len(refs) - 1 - len(rows)) // 2
    total_ref = refs[count]
    outs = refs[count + 1 :]
    for k in range(count):
        outs[k][...] = refs[k][...]
    for k, (row, size) in enumerate(rows):
        if size == 1:
            outs[count + k][...] = total_ref[row, :]
        else:
            outs[count + k][...] = total_ref[row : row + size, :]


def on_device_images(
    tokens, norm1_gain, norm1_bias, qkv_weight, qv_bias, rel_rows, rel_cols, proj_weight, proj_bias,
    norm2_gain, norm2_bias, fc1_weight, fc1_bias, fc2_weight, fc2_bias, cotangent,
):
    S = jax.ShapeDtypeStruct
    shards = lax.axis_size("shard")
    tp_count = lax.axis_size("tp")
    tp_rank = lax.axis_index("tp")
    heads = H // tp_count
    width = heads * HD
    ff = FF // tp_count
    rows = (rel_rows.shape[0] + 1) // 2
    tok = rows * COLS
    own = tokens.shape
    piece = own[1:]
    full = (2, tp_count) + piece
    block = fc1_weight.shape
    blocks = (2 * shards,) + block
    qkv_cols = 3 * width
    fc2_t = fc2_weight.T
    qv_local = lax.dynamic_slice_in_dim(qv_bias, tp_rank * width, width, 1)
    qkv_bias = jnp.concatenate([qv_local[0], jnp.zeros((width,), F32), qv_local[1]])
    fc1_local = lax.dynamic_slice_in_dim(fc1_bias, tp_rank * ff, ff, 0)
    vec = jnp.concatenate(
        [
            norm1_gain, norm1_bias, proj_bias, norm2_gain, norm2_bias, fc2_bias, fc1_local,
            qkv_bias, jnp.zeros((D - qkv_cols,), F32),
        ]
    ).reshape(8, D)
    spread = Spread.scratch(shards, block)
    collect = Collect.scratch(shards, block)
    gather = Gather2.scratch(piece)
    swap = [DMA((2, 1))]
    share = [DMA((2, 6))]

    x, a1, w1_full, a1_turned = comm_call(
        partial(front_kernel, shards), "front", 0,
        (tokens, qkv_weight, proj_weight.T, vec),
        (S(own, BF16), S(full, BF16), S(blocks, BF16), S((D, tok), BF16)),
        [pltpu.VMEM(block, BF16)] + swap + share + spread, hbm_out=(2,), early=(0, 1, 3),
    )
    w1_full = w1_full.reshape(D, -1)
    vh, oh, o_low, lse, qa, ka, g, cot, fc1_full, proj_part = comm_call(
        partial(fwd_kernel, shards, heads, HD, COLS, rows, 256), "attn_fwd", 1,
        (a1.reshape(tok, D), w1_full, vec, rel_rows, rel_cols, cotangent, fc1_weight),
        (
            S((heads, tok, 128), BF16), S((heads, tok, 128), F32), S((tok, width), BF16), S((heads, 1, tok), F32),
            S((heads, tok, 256), BF16), S((heads, tok, 256), BF16),
            S(own, BF16), S(full, BF16), S(blocks, BF16), S((tok, D), BF16),
        ),
        [
            pltpu.VMEM((heads, tok, 128), BF16), pltpu.VMEM((128, tok), BF16), pltpu.VMEM((256, 128), BF16),
            pltpu.VMEM((256, 128), BF16), pltpu.VMEM((tok, 256), BF16),
        ]
        + swap + share + spread, hbm_in=(6,), hbm_out=(8,), late=(1, 0), early=(0, 1, 2, 4, 5, 7, 9),
    )
    fc1_full = fc1_full.reshape(D, ff)
    mid, a2, fc2_full, act, slope, cot_turned = comm_call(
        partial(mid_kernel, shards), "mid", 2,
        (proj_part.reshape(full), x, vec, fc2_t, fc1_full, cot),
        (
            S(own, F32), S(full, BF16), S(blocks, BF16), S((tok, ff), BF16), S((tok, ff), F32),
            S((D, tok), BF16),
        ),
        gather + share + spread, hbm_in=(3,), hbm_out=(2,), late=(0, 5, 1, 4), early=(0, 1, 3, 4, 5),
    )
    fc2_full = fc2_full.reshape(D, ff)
    d_mid, d_branch_turned, fc2_own, sums, fc1_grad, mlp_part, d_o = comm_call(
        partial(turn_kernel, shards), "turn", 3,
        (
            cot_turned, act, slope, cot.reshape(tok, D), fc2_full, fc1_full, a2.reshape(tok, D), mid, g, vec,
            w1_full,
        ),
        (
            S(own, F32), S((D, tok), BF16), S(block, F32), S((8, D), F32),
            S((D, ff), BF16), S((tok, D), BF16), S((tok, width), BF16),
        ),
        [pltpu.VMEM(full, BF16), pltpu.VMEM((D, ff), BF16), pltpu.VMEM(full, BF16), pltpu.VMEM((tok, ff), BF16)]
        + gather + share + collect,
        late=(0, 1, 2, 3, 4, 5, 6, 7, 8, 10), early=(0, 1, 4, 5, 6),
    )
    dqkv, rel_grad, fc1_own, qkv_sum, output = comm_call(
        partial(bwd_kernel, shards, heads, HD, COLS, rows, 256), "attn_bwd", 4,
        (qa, ka, vh, d_o, oh, lse, rel_rows, rel_cols, fc1_grad, mlp_part.reshape(full), mid, vec),
        (S((tok, qkv_cols), BF16), S((256, 128), F32), S(block, F32), S((8, qkv_cols), F32), S(own, BF16)),
        [
            pltpu.VMEM((heads, tok, 128), BF16), pltpu.VMEM((3 * heads, tok, 128), BF16),
            pltpu.VMEM((256, tok), BF16), pltpu.VMEM((tok, 128), F32), pltpu.VMEM((tok, 128), F32),
            pltpu.VMEM((8, tok), F32), pltpu.VMEM((256, 128), BF16), pltpu.VMEM((tok, 256), BF16),
            pltpu.VMEM(own, BF16),
        ] + gather + swap + collect,
        late=(8, 9, 3, 2, 4, 1, 0, 10), early=(0,),
    )
    qkv_sum = qkv_sum[0]
    qv_part = jnp.stack([qkv_sum[:width], qkv_sum[2 * width :]])
    qv_placed = lax.dynamic_update_slice_in_dim(jnp.zeros((2, D), F32), qv_part, tp_rank * width, 1)
    fc1_placed = lax.dynamic_update_slice_in_dim(jnp.zeros((FF,), F32), sums[4], tp_rank * ff, 0)
    terms = (
        jnp.zeros((2 * D,), F32),
        qv_placed.reshape(-1),
        fc1_placed,
        sums[:4].reshape(-1),
        rel_grad[: rel_rows.shape[0], :HD].reshape(-1),
        rel_grad[128 : 128 + rel_cols.shape[0], :HD].reshape(-1),
    )
    count = sum(term.shape[0] for term in terms)
    lines = -(-count // (8 * D)) * 8
    packed = jnp.concatenate(terms + (jnp.zeros((lines * D - count,), F32),)).reshape(lines, D)
    tokens_grad, qkv_own, proj_own, total = comm_call(
        partial(end_kernel, shards), "end", 5,
        (x, d_mid, vec, a1_turned, dqkv, d_branch_turned, o_low, packed, w1_full),
        (S(own, BF16), S((3, block[0], width), F32), S((block[0], width), F32), S((lines, D), F32)),
        [pltpu.VMEM((D, ff), BF16), pltpu.VMEM(block, F32), pltpu.VMEM(full, BF16), pltpu.VMEM(own, BF16)]
        + gather + swap
        + [
            pltpu.VMEM((4, lines, D), F32), pltpu.VMEM((3, lines, D), F32),
            pltpu.VMEM((shards, lines, D), F32), DMA((2, 2 + shards)),
        ]
        + collect,
        late=(4, 8, 3, 5, 6, 0, 1),
    )
    rows_out = 4 + FF // D
    places = ((0, 1), (1, 1), (2, 2), (rows_out + 2, 1), (rows_out, 1), (rows_out + 1, 1), (rows_out + 3, 1))
    big = (output, tokens_grad, qkv_own, proj_own, fc1_own, fc2_own)
    final = pl.pallas_call(
        partial(settle_kernel, places),
        out_shape=tuple(S(b.shape, b.dtype) for b in big)
        + tuple(S((D,) if size == 1 else (size, D), F32) for _, size in places),
        compiler_params=pltpu.CompilerParams(vmem_limit_bytes=VMEM_GRANT),
        name="settle",
    )(*big, total)
    output, tokens_grad, qkv_own, proj_own, fc1_own, fc2_own = final[:6]
    gain1, bias1, qv_grad, projb, gain2, bias2, fc2b = final[6:]
    flat = total.reshape(-1)
    base = 4 * D + FF
    rel_at = base + 4 * D
    rel_mid = rel_at + rel_rows.size
    return (
        output,
        tokens_grad,
        gain1,
        bias1,
        qkv_own,
        qv_grad,
        flat[rel_at:rel_mid].reshape(rel_rows.shape),
        flat[rel_mid : rel_mid + rel_cols.size].reshape(rel_cols.shape),
        proj_own.T,
        projb,
        gain2,
        bias2,
        fc1_own,
        flat[4 * D : base],
        fc2_own.T,
        fc2b,
    )


def solution(mesh):
    in_specs = (
        P("shard", ("ctx", "tp"), None),
        P(),
        P(),
        P(None, ("shard", "ctx"), "tp"),
        P(),
        P(),
        P(),
        P("tp", ("shard", "ctx")),
        P(),
        P(),
        P(),
        P(("shard", "ctx"), "tp"),
        P(),
        P("tp", ("shard", "ctx")),
        P(),
        P("shard", ("ctx", "tp"), None),
    )
    out_specs = (
        P("shard", ("ctx", "tp"), None),
        P("shard", ("ctx", "tp"), None),
        P(),
        P(),
        P(None, ("shard", "ctx"), "tp"),
        P(),
        P(),
        P(),
        P("tp", ("shard", "ctx")),
        P(),
        P(),
        P(),
        P(("shard", "ctx"), "tp"),
        P(),
        P("tp", ("shard", "ctx")),
        P(),
    )
    def on_device(*arrays):
        rows = (arrays[5].shape[0] + 1) // 2
        fits = mesh.shape["tp"] == 4 and mesh.shape["ctx"] == 2 and HD + 2 * rows <= 128
        fits = fits and arrays[0].shape[0] == mesh.shape["ctx"] and arrays[6].shape[0] <= 128
        return (on_device_images if fits else on_device_rows)(*arrays)

    return jax.shard_map(
        on_device, mesh=mesh, in_specs=in_specs, out_specs=out_specs, check_vma=False
    )
```

```python
from functools import partial
import math

import jax
import jax.numpy as jnp
from jax import lax
from jax.experimental import pallas as pl
from jax.experimental.pallas import tpu as pltpu
from jax.sharding import PartitionSpec as P

D = 1280
H = 16
HD = 80
FF = 5120
COLS = 64
ROWS_DEV = 8


PRECISE = lax.Precision.HIGHEST
EPSILON = 1e-06
NEGATIVE = -1e30


def layer_norm(values_in, gain_vec, shift_vec):
    average = jnp.mean(values_in, -1, keepdims=True)
    centred = values_in - average
    variance = jnp.mean(centred * centred, -1, keepdims=True)
    return centred * lax.rsqrt(variance + EPSILON) * gain_vec + shift_vec


def block_size():
    return 512


def to_heads(flat_rows, heads_local):
    images, length, feat_width = flat_rows.shape
    return flat_rows.reshape(images, length, heads_local, feat_width // heads_local).transpose(
        0, 2, 1, 3
    )


def from_heads(per_head):
    images, heads_local, length, head_dim = per_head.shape
    return per_head.transpose(0, 2, 1, 3).reshape(images, length, heads_local * head_dim)


def block_scores(query_heads, key_flat, rows_bias, cols_bias, first_key, scale_factor):
    key_heads = to_heads(key_flat, query_heads.shape[1])
    key_len = key_flat.shape[1]
    key_rows = key_len // COLS
    scores = scale_factor * jnp.einsum(
        "ihqc,ihkc->ihqk", query_heads, key_heads, preferred_element_type=jnp.float32
    )
    images, heads_local, query_len, unused_len = scores.shape
    row_part = lax.dynamic_slice_in_dim(rows_bias, first_key // COLS, key_rows, 3)
    scores = scores.reshape(images, heads_local, query_len, key_rows, COLS)
    scores = scores + row_part[..., :, None] + cols_bias[..., None, :]
    return scores.reshape(images, heads_local, query_len, key_len)


def relative_terms(query_flat, rows_param, cols_param, first_row, heads_local):
    images, length, feat_width = query_flat.shape
    rows_dev = length // COLS
    grid_rows = (rows_param.shape[0] + 1) // 2
    own_rows = first_row + jnp.arange(rows_dev, dtype=jnp.int32)
    key_rows = jnp.arange(grid_rows, dtype=jnp.int32)
    row_slots = jnp.arange(rows_param.shape[0], dtype=jnp.int32)
    pick_rows = (
        row_slots[None, None, :]
        == own_rows[:, None, None] - key_rows[None, :, None] + grid_rows - 1
    ).astype(jnp.float32)
    table_rows = jnp.einsum("rkj,jc->rkc", pick_rows, rows_param, precision=PRECISE)
    col_ids = jnp.arange(COLS, dtype=jnp.int32)
    col_slots = jnp.arange(cols_param.shape[0], dtype=jnp.int32)
    pick_cols = (
        col_slots[None, None, :] == col_ids[:, None, None] - col_ids[None, :, None] + COLS - 1
    ).astype(jnp.float32)
    table_cols = jnp.einsum("wkj,jc->wkc", pick_cols, cols_param, precision=PRECISE)
    grid_form = query_flat.reshape(images, rows_dev, COLS, heads_local, feat_width // heads_local)
    along_rows = jnp.einsum("irwhc,rkc->ihrwk", grid_form, table_rows, precision=PRECISE).reshape(
        images, heads_local, length, grid_rows
    )
    along_cols = jnp.einsum("irwhc,wkc->ihrwk", grid_form, table_cols, precision=PRECISE).reshape(
        images, heads_local, length, COLS
    )
    return (along_rows, along_cols)


def on_device_rows(
    tokens,
    norm1_gain,
    norm1_bias,
    qkv_weight,
    qv_bias,
    rel_rows,
    rel_cols,
    proj_weight,
    proj_bias,
    norm2_gain,
    norm2_bias,
    fc1_weight,
    fc1_bias,
    fc2_weight,
    fc2_bias,
    cotangent,
):
    scale_factor = HD ** (-0.5)
    tp_count = lax.axis_size("tp")
    ctx_count = lax.axis_size("ctx")
    tp_rank = lax.axis_index("tp")
    ctx_rank = lax.axis_index("ctx")
    grid_rows = ROWS_DEV * ctx_count
    tok_image = grid_rows * COLS
    tok_ctx = ROWS_DEV * COLS
    heads_local = H // tp_count
    width_local = heads_local * HD
    ff_local = FF // tp_count
    images = tokens.shape[0]
    rows_table = rel_rows.astype(jnp.float32)
    cols_table = rel_cols.astype(jnp.float32)
    qkv_full, proj_full, fc1_full, fc2_full = (
        lax.all_gather(qkv_weight, ("shard", "ctx"), axis=1, tiled=True),
        lax.all_gather(proj_weight, ("shard", "ctx"), axis=1, tiled=True),
        lax.all_gather(fc1_weight, ("shard", "ctx"), axis=0, tiled=True),
        lax.all_gather(fc2_weight, ("shard", "ctx"), axis=1, tiled=True),
    )
    qv_local = lax.dynamic_slice_in_dim(qv_bias, tp_rank * width_local, width_local, 1)
    fc1_local = lax.dynamic_slice_in_dim(fc1_bias, tp_rank * ff_local, ff_local, 0)
    resid_in = tokens.astype(jnp.float32)
    normed1 = layer_norm(resid_in, norm1_gain, norm1_bias).astype(jnp.bfloat16)
    normed1_full = lax.all_gather(normed1, "tp", axis=1, tiled=True)
    projected = jnp.einsum(
        "itd,sde->itse", normed1_full, qkv_full, preferred_element_type=jnp.float32
    )
    queries = (projected[:, :, 0] + qv_local[0]).astype(jnp.bfloat16)
    keys_own = projected[:, :, 1].astype(jnp.bfloat16)
    values_own = (projected[:, :, 2] + qv_local[1]).astype(jnp.bfloat16)
    first_row = ctx_rank * ROWS_DEV
    rel_fn = partial(relative_terms, first_row=first_row, heads_local=heads_local)
    (along_rows, along_cols), rel_pull = jax.vjp(
        rel_fn, queries.astype(jnp.float32), rows_table, cols_table
    )
    query_heads = to_heads(queries, heads_local)
    start_state = (
        jnp.full((images, heads_local, tok_ctx), NEGATIVE, jnp.float32),
        jnp.zeros((images, heads_local, tok_ctx), jnp.float32),
        jnp.zeros((images, heads_local, tok_ctx, HD), jnp.float32),
        jnp.zeros((images, tok_image, width_local), jnp.bfloat16),
        jnp.zeros((images, tok_image, width_local), jnp.bfloat16),
    )
    shard_piece = (
        lax.all_gather(keys_own, "ctx", axis=1, tiled=True),
        lax.all_gather(values_own, "ctx", axis=1, tiled=True),
    )
    piece_len = shard_piece[0].shape[1]
    step_len = block_size()

    def one_step(inner, offset):
        run_max, run_sum, run_acc, keys_all, values_all = inner
        key_blk = lax.dynamic_slice_in_dim(shard_piece[0], offset, step_len, 1)
        value_blk = lax.dynamic_slice_in_dim(shard_piece[1], offset, step_len, 1)
        scores = block_scores(query_heads, key_blk, along_rows, along_cols, offset, scale_factor)
        new_max = jnp.maximum(run_max, jnp.max(scores, -1))
        factor = jnp.exp(run_max - new_max)
        weights_blk = jnp.exp(scores - new_max[..., None])
        run_sum = run_sum * factor + jnp.sum(weights_blk, -1)
        value_heads = to_heads(value_blk, heads_local)
        run_acc = run_acc * factor[..., None] + jnp.einsum(
            "ihqk,ihkc->ihqc",
            weights_blk.astype(jnp.bfloat16),
            value_heads,
            preferred_element_type=jnp.float32,
        )
        keys_all = lax.dynamic_update_slice_in_dim(keys_all, key_blk, offset, 1)
        values_all = lax.dynamic_update_slice_in_dim(values_all, value_blk, offset, 1)
        return ((new_max, run_sum, run_acc, keys_all, values_all), None)

    offsets = jnp.arange(piece_len // step_len, dtype=jnp.int32) * step_len
    result, unused = lax.scan(one_step, start_state, offsets)
    run_max, run_sum, run_acc, keys_all, values_all = result
    attn_heads = run_acc / run_sum[..., None]
    log_total = run_max + jnp.log(run_sum)
    attn_low = from_heads(attn_heads).astype(jnp.bfloat16)
    proj_part = jnp.einsum("itd,de->ite", attn_low, proj_full, preferred_element_type=jnp.float32)
    branch = lax.psum_scatter(
        proj_part.astype(jnp.bfloat16), "tp", scatter_dimension=1, tiled=True
    ).astype(jnp.float32)
    middle = resid_in + branch + proj_bias
    normed2 = layer_norm(middle, norm2_gain, norm2_bias).astype(jnp.bfloat16)
    normed2_full = lax.all_gather(normed2, "tp", axis=1, tiled=True)
    hidden_pre = (
        jnp.einsum("itd,df->itf", normed2_full, fc1_full, preferred_element_type=jnp.float32)
        + fc1_local
    )
    gelu_exact = partial(jax.nn.gelu, approximate=False)
    activated_f, gelu_pull = jax.vjp(gelu_exact, hidden_pre)
    activated = activated_f.astype(jnp.bfloat16)
    mlp_part = jnp.einsum("itf,fe->ite", activated, fc2_full, preferred_element_type=jnp.float32)
    mlp_out = lax.psum_scatter(
        mlp_part.astype(jnp.bfloat16), "tp", scatter_dimension=1, tiled=True
    ).astype(jnp.float32)
    output = (middle + mlp_out + fc2_bias).astype(jnp.bfloat16)
    cot_full = lax.all_gather(cotangent, "tp", axis=1, tiled=True)
    d_act = jnp.einsum("ite,fe->itf", cot_full, fc2_full, preferred_element_type=jnp.float32)
    d_hidden = gelu_pull(d_act)[0].astype(jnp.bfloat16)
    fc2_grad = jnp.einsum("itf,ite->fe", activated, cot_full, preferred_element_type=jnp.float32)
    fc1_grad = jnp.einsum("itd,itf->df", normed2_full, d_hidden, preferred_element_type=jnp.float32)
    fc1_bias_part = jnp.sum(d_hidden.astype(jnp.float32), (0, 1))
    fc2_bias_part = jnp.sum(cotangent.astype(jnp.float32), (0, 1))
    d_norm2_part = jnp.einsum("itf,df->itd", d_hidden, fc1_full, preferred_element_type=jnp.float32)
    d_norm2 = lax.psum_scatter(
        d_norm2_part.astype(jnp.bfloat16), "tp", scatter_dimension=1, tiled=True
    ).astype(jnp.float32)
    unused_out, norm2_pull = jax.vjp(layer_norm, middle, norm2_gain, norm2_bias)
    d_mid_part, gain2_part, bias2_part = norm2_pull(d_norm2)
    d_middle = cotangent.astype(jnp.float32) + d_mid_part
    d_branch = d_middle.astype(jnp.bfloat16)
    proj_bias_part = jnp.sum(d_branch.astype(jnp.float32), (0, 1))
    d_branch_full = lax.all_gather(d_branch, "tp", axis=1, tiled=True)
    proj_grad = jnp.einsum(
        "itd,ite->de", attn_low, d_branch_full, preferred_element_type=jnp.float32
    )
    d_attn = jnp.einsum(
        "ite,de->itd", d_branch_full, proj_full, preferred_element_type=jnp.float32
    ).astype(jnp.bfloat16)
    d_attn_heads = to_heads(d_attn, heads_local)
    delta_rows = jnp.sum(d_attn_heads.astype(jnp.float32) * attn_heads, -1)
    key_step = block_size()
    key_rows = key_step // COLS
    key_offsets = jnp.arange(tok_image // key_step, dtype=jnp.int32) * key_step

    def back_step(carried, offset):
        grad_query, grad_rows, grad_cols = carried
        key_blk = lax.dynamic_slice_in_dim(keys_all, offset, key_step, 1)
        value_blk = lax.dynamic_slice_in_dim(values_all, offset, key_step, 1)
        scores = block_scores(query_heads, key_blk, along_rows, along_cols, offset, scale_factor)
        soft_probs = jnp.exp(scores - log_total[..., None])
        value_heads = to_heads(value_blk, heads_local)
        key_heads = to_heads(key_blk, heads_local)
        d_probs = jnp.einsum(
            "ihqc,ihkc->ihqk", d_attn_heads, value_heads, preferred_element_type=jnp.float32
        )
        d_scores = (soft_probs * (d_probs - delta_rows[..., None])).astype(jnp.bfloat16)
        grad_query = grad_query + jnp.einsum(
            "ihqk,ihkc->ihqc", d_scores, key_heads, preferred_element_type=jnp.float32
        )
        grid_scores = d_scores.astype(jnp.float32).reshape(
            images, heads_local, tok_ctx, key_rows, COLS
        )
        row_sums = jnp.sum(grid_scores, 4)
        row_now = lax.dynamic_slice_in_dim(grad_rows, offset // COLS, key_rows, 3)
        grad_rows = lax.dynamic_update_slice_in_dim(
            grad_rows, row_now + row_sums, offset // COLS, 3
        )
        grad_cols = grad_cols + jnp.sum(grid_scores, 3)
        key_part = scale_factor * jnp.einsum(
            "ihqk,ihqc->ikhc", d_scores, query_heads, preferred_element_type=jnp.float32
        )
        value_part = jnp.einsum(
            "ihqk,ihqc->ikhc",
            soft_probs.astype(jnp.bfloat16),
            d_attn_heads,
            preferred_element_type=jnp.float32,
        )
        emitted = (
            key_part.reshape(images, key_step, width_local),
            value_part.reshape(images, key_step, width_local),
        )
        return ((grad_query, grad_rows, grad_cols), emitted)

    back_start = (
        jnp.zeros((images, heads_local, tok_ctx, HD), jnp.float32),
        jnp.zeros((images, heads_local, tok_ctx, grid_rows), jnp.float32),
        jnp.zeros((images, heads_local, tok_ctx, COLS), jnp.float32),
    )
    (grad_query, grad_rows, grad_cols), emitted = lax.scan(back_step, back_start, key_offsets)
    key_terms = emitted[0].transpose(1, 0, 2, 3).reshape(images, tok_image, width_local)
    value_terms = emitted[1].transpose(1, 0, 2, 3).reshape(images, tok_image, width_local)
    grad_keys, grad_values = (
        lax.psum_scatter(
            key_terms.astype(jnp.bfloat16), "ctx", scatter_dimension=1, tiled=True
        ).astype(jnp.float32),
        lax.psum_scatter(
            value_terms.astype(jnp.bfloat16), "ctx", scatter_dimension=1, tiled=True
        ).astype(jnp.float32),
    )
    d_query_rel, rows_grad_part, cols_grad_part = rel_pull((grad_rows, grad_cols))
    d_query = (scale_factor * from_heads(grad_query) + d_query_rel).astype(jnp.bfloat16)
    d_keys = grad_keys.astype(jnp.bfloat16)
    d_values = grad_values.astype(jnp.bfloat16)
    d_projected = jnp.stack((d_query, d_keys, d_values), axis=2)
    qkv_grad = jnp.einsum(
        "itd,itse->sde", normed1_full, d_projected, preferred_element_type=jnp.float32
    )
    qv_bias_part = jnp.stack(
        (
            jnp.sum(d_query.astype(jnp.float32), (0, 1)),
            jnp.sum(d_values.astype(jnp.float32), (0, 1)),
        )
    )
    d_norm1_part = jnp.einsum(
        "itse,sde->itd", d_projected, qkv_full, preferred_element_type=jnp.float32
    )
    d_norm1 = lax.psum_scatter(
        d_norm1_part.astype(jnp.bfloat16), "tp", scatter_dimension=1, tiled=True
    ).astype(jnp.float32)
    unused_in, norm1_pull = jax.vjp(layer_norm, resid_in, norm1_gain, norm1_bias)
    d_in_part, gain1_part, bias1_part = norm1_pull(d_norm1)
    tokens_grad = (d_middle + d_in_part).astype(jnp.bfloat16)
    qkv_out, proj_out, fc1_out, fc2_out = (
        lax.psum_scatter(
            qkv_grad.astype(jnp.bfloat16), ("shard", "ctx"), scatter_dimension=1, tiled=True
        ).astype(jnp.float32),
        lax.psum_scatter(
            proj_grad.astype(jnp.bfloat16), ("shard", "ctx"), scatter_dimension=1, tiled=True
        ).astype(jnp.float32),
        lax.psum_scatter(
            fc1_grad.astype(jnp.bfloat16), ("shard", "ctx"), scatter_dimension=0, tiled=True
        ).astype(jnp.float32),
        lax.psum_scatter(
            fc2_grad.astype(jnp.bfloat16), ("shard", "ctx"), scatter_dimension=1, tiled=True
        ).astype(jnp.float32),
    )
    qv_placed = lax.dynamic_update_slice_in_dim(
        jnp.zeros((2, D), jnp.float32), qv_bias_part, tp_rank * width_local, 1
    )
    fc1_placed = lax.dynamic_update_slice_in_dim(
        jnp.zeros((FF,), jnp.float32), fc1_bias_part, tp_rank * ff_local, 0
    )
    (
        gain1_sum,
        bias1_sum,
        qv_sum,
        rows_sum,
        cols_sum,
        projb_sum,
        gain2_sum,
        bias2_sum,
        fc1b_sum,
        fc2b_sum,
    ) = lax.psum(
        (
            gain1_part,
            bias1_part,
            qv_placed,
            rows_grad_part,
            cols_grad_part,
            proj_bias_part,
            gain2_part,
            bias2_part,
            fc1_placed,
            fc2_bias_part,
        ),
        ("shard", "ctx", "tp"),
    )
    return (
        output,
        tokens_grad,
        gain1_sum,
        bias1_sum,
        qkv_out,
        qv_sum,
        rows_sum,
        cols_sum,
        proj_out,
        projb_sum,
        gain2_sum,
        bias2_sum,
        fc1_out,
        fc1b_sum,
        fc2_out,
        fc2b_sum,
    )


F32 = jnp.float32
BF16 = jnp.bfloat16
NT = (((1,), (1,)), ((), ()))
NN = (((1,), (0,)), ((), ()))
TN = (((0,), (0,)), ((), ()))
VMEM_GRANT = 60 * 2**20
DMA = pltpu.SemaphoreType.DMA
ANY = pl.BlockSpec(memory_space=pl.ANY)
VM = pl.BlockSpec(memory_space=pltpu.VMEM)


def mm(left, right, dims=NN):
    return lax.dot_general(left, right, dims, preferred_element_type=F32)


def lane_ids(shape):
    return lax.broadcasted_iota(jnp.int32, shape, 1)


def place():
    return lax.axis_index("shard"), lax.axis_index("ctx"), lax.axis_index("tp")


def core_mate(t):
    return t + 1 - 2 * lax.rem(t, 2)


def far_mate(t):
    return lax.rem(t + 2, 4)


def aim(src, dst, sems, k, where):
    return pltpu.make_async_remote_copy(
        src_ref=src,
        dst_ref=dst,
        send_sem=sems.at[0, k],
        recv_sem=sems.at[1, k],
        device_id=where,
        device_id_type=pl.DeviceIdType.MESH,
    )


def send(src, dst, sems, k, where):
    copy = aim(src, dst, sems, k, where)
    copy.start()
    return copy


def swap_copy(src, dst, sems):
    _, c, _ = place()
    return pltpu.make_async_remote_copy(
        src_ref=src,
        dst_ref=dst,
        send_sem=sems.at[0, 0],
        recv_sem=sems.at[1, 0],
        device_id={"ctx": 1 - c},
        device_id_type=pl.DeviceIdType.MESH,
    )


def fill_tables(tab_ref, rr_ref, rc_ref):
    tab_ref[...] = jnp.zeros_like(tab_ref)
    tab_ref[0 : rr_ref.shape[0], 0 : rr_ref.shape[1]] = rr_ref[...]
    tab_ref[128 : 128 + rc_ref.shape[0], 0 : rc_ref.shape[1]] = rc_ref[...]


def fill_hots(hot_ref, hd, cols, rows, second):
    shift = cols.bit_length() - 1
    down = lax.broadcasted_iota(jnp.int32, hot_ref.shape, 0)
    kr = lax.shift_right_logical(down, shift)
    kw = down & (cols - 1)
    l = lane_ids(hot_ref.shape)
    if second:
        hit = (l == hd + rows - 1 - kr) | (l == 128 + cols - 1 - kw)
    else:
        hit = (l == hd + kr) | (l == hd + rows + kr) | (l == 128 + kw) | (l == 192 + kw)
    hot_ref[...] = jnp.where(hit, 1.0, 0.0).astype(BF16)


def reverser(top):
    down = lax.broadcasted_iota(jnp.int32, (128, 128), 0)
    return jnp.where(down + lane_ids((128, 128)) == top, 1.0, 0.0).astype(BF16)


def greet(shards, line=False):
    s, c, t = place()
    size = 2 * shards
    at = s * (1 - c) + (size - 1 - s) * c
    peers = [{"ctx": 1 - c}, {"tp": core_mate(t)}, {"tp": far_mate(t)}]
    for step in (1, size - 1):
        to = lax.rem(at + step, size)
        back = to // shards
        peers.append({"shard": to * (1 - back) + (size - 1 - to) * back, "ctx": back})
    if line:
        peers.append({"tp": core_mate(far_mate(t))})
        for d in range(1, shards):
            peers.append({"shard": lax.rem(s + d, shards)})
            peers.append({"shard": lax.rem(s + d, shards), "ctx": 1 - c})
    barrier = pltpu.get_barrier_semaphore()
    for peer in peers:
        pl.semaphore_signal(barrier, inc=1, device_id=peer, device_id_type=pl.DeviceIdType.MESH)
    pl.semaphore_wait(barrier, len(peers))


class Ring:
    def __init__(self, shards, block, sems):
        s, c, _ = place()
        self.shards, self.size, self.sems = shards, 2 * shards, sems
        self.at = s * (1 - c) + (self.size - 1 - s) * c
        self.half = block // 2
        self.pieces = ring_pieces(block)
        self.rows = self.half // self.pieces
        self.first, self.end = self.pieces, self.pieces * (self.size - 1)
        self.now = self.first

    def coords(self, position):
        back = position // self.shards
        return position * (1 - back) + (self.size - 1 - position) * back, back

    def peer(self, way):
        to = lax.rem(self.at + (1 if way == 0 else self.size - 1), self.size)
        shard, ctx = self.coords(to)
        return {"shard": shard, "ctx": ctx}

    def owner(self, offset):
        shard, ctx = self.coords(lax.rem(self.at + 2 * self.size + offset, self.size))
        return 2 * shard + ctx

    def split(self, event):
        if isinstance(event, int):
            return event // self.pieces, event % self.pieces
        return lax.div(event, self.pieces), lax.rem(event, self.pieces)

    def rows_of(self, way, piece):
        start = way * self.half + piece * self.rows
        return pl.ds(start if isinstance(start, int) else pl.multiple_of(start, self.rows), self.rows)

    def make(self, src, dst, way, event):
        slot = way * self.end + event
        return pltpu.make_async_remote_copy(
            src_ref=src,
            dst_ref=dst,
            send_sem=self.sems.at[0, slot],
            recv_sem=self.sems.at[1, slot],
            device_id=self.peer(way),
            device_id_type=pl.DeviceIdType.MESH,
        )

    def run(self, low, high):
        low, high = max(low, self.first), min(high, self.end)
        if low < high:
            lax.fori_loop(low, high, lambda event, _: (self.step(event), 0)[1], 0)

    def tick(self, count):
        self.run(self.now, self.now + count)
        self.now += count

    def poll(self, event):
        pl.when((event >= self.first) & (event < self.end))(lambda: self.step(event))


def ring_pieces(block):
    return 5 if block % 160 == 0 else 1


def ring_sems(shards, block):
    return DMA((2, 2 * ring_pieces(block) * (2 * shards - 1)))


class Spread(Ring):
    def __init__(self, shards, src, dst, sems, local):
        super().__init__(shards, src.shape[0], sems)
        self.src, self.dst = src, dst
        self.local = pltpu.make_async_copy(src, dst.at[self.owner(0)], local)
        self.local.start()
        for event in range(self.first):
            for way in range(2):
                self.hop(way, event, True).start()

    def hop(self, way, event, own=False):
        j, piece = self.split(event)
        rows = self.rows_of(way, piece)
        there = self.dst.at[self.owner(-j if way == 0 else j), rows]
        return self.make(self.src.at[rows] if own else there, there, way, event)

    def step(self, event):
        for way in range(2):
            self.hop(way, event - self.pieces).wait_recv()
            self.hop(way, event).start()

    def finish(self):
        self.local.wait()
        for way in range(2):
            for event in range(self.end - self.pieces, self.end):
                self.hop(way, event).wait_recv()

        def sent(event, _):
            for way in range(2):
                self.hop(way, event).wait_send()
            return 0

        lax.fori_loop(0, self.end, sent, 0)

    @staticmethod
    def scratch(shards, block):
        return [ring_sems(shards, block[0]), DMA]


class Collect(Ring):
    def __init__(self, shards, src, held, sems):
        super().__init__(shards, src.shape[0] // (2 * shards), sems)
        self.src, self.held, self.block = src, held, src.shape[0] // (2 * shards)

    def begin(self):
        for event in range(self.first):
            for way in range(2):
                self.hop(way, event, True).start()

    def pair_rows(self, n, j):
        offset = (n + 1) * (2 * j - 1)
        last = (2 * n + j + 1) // self.size
        return pl.ds(pl.multiple_of(self.owner(offset * (1 - last)) * self.block, self.rows), self.block)

    def own(self, way, j, piece):
        ahead = self.size - 1 - j
        start = self.owner(ahead if way == 0 else -ahead) * self.block + way * self.half + piece * self.rows
        return pl.ds(pl.multiple_of(start, self.rows), self.rows)

    def hop(self, way, event, own=False):
        j, piece = self.split(event)
        rows = self.rows_of(0, piece)
        there = self.held.at[way, j, rows]
        here = self.src.at[self.own(way, j, piece)] if own else self.held.at[way, j - 1, rows]
        return self.make(here, there, way, event)

    def arrived(self, way, event):
        j, piece = self.split(event)
        there = self.held.at[way, j, self.rows_of(0, piece)]
        self.make(there, there, way, event).wait_recv()

    def step(self, event):
        j, piece = self.split(event)
        rows = self.rows_of(0, piece)
        for way in range(2):
            self.arrived(way, event - self.pieces)
            both = self.held[way, j - 1, rows].astype(F32) + self.src[self.own(way, j, piece)].astype(F32)
            self.held[way, j - 1, rows] = both.astype(BF16)
            self.hop(way, event).start()

    def finish(self, out):
        for piece in range(self.pieces):
            for way in range(2):
                self.arrived(way, self.end - self.pieces + piece)
                last = self.held[way, self.size - 2, self.rows_of(0, piece)].astype(F32)
                own = self.src[self.own(way, self.size - 1, piece)].astype(F32)
                out[self.rows_of(way, piece)] = last + own

        def sent(event, _):
            for way in range(2):
                j, piece = self.split(event)
                there = self.held.at[way, j, self.rows_of(0, piece)]
                self.make(there, there, way, event).wait_send()
            return 0

        lax.fori_loop(0, self.end, sent, 0)

    @staticmethod
    def scratch(shards, block):
        return [pltpu.VMEM((2, 2 * shards - 1, block[0] // 2, block[1]), BF16), ring_sems(shards, block[0])]


class Share:
    def __init__(self, full, sems):
        self.full, self.sems = full, sems

    def copies(self, k, p, src=None):
        _, _, t = place()
        block, passed = self.full.at[p, t], self.full.at[p, far_mate(t)]
        src = block if src is None else src
        return (
            partial(aim, src, block, self.sems, 3 * k, {"tp": far_mate(t)}),
            partial(aim, src, block, self.sems, 3 * k + 1, {"tp": core_mate(t)}),
            partial(aim, passed, passed, self.sems, 3 * k + 2, {"tp": core_mate(t)}),
        )

    def push(self, k, p, src=None):
        for copy in self.copies(k, p, src)[:2]:
            copy().start()

    def forward(self, k, p):
        far, _, third = self.copies(k, p)
        far().wait_recv()
        third().start()

    def finish(self, k, p):
        far, core, third = self.copies(k, p)
        far().wait_send()
        core().wait()
        third().wait()


class Gather2:
    def __init__(self, part, mate, far, out, sems):
        self.part, self.mate, self.far, self.out, self.sems = part, mate, far, out, sems

    def copies(self, p):
        _, _, t = place()
        m = core_mate(t)
        return (
            partial(aim, self.part.at[p, far_mate(m)], self.mate.at[p, 1], self.sems, 3 * p, {"tp": m}),
            partial(aim, self.part.at[p, m], self.mate.at[p, 0], self.sems, 3 * p + 1, {"tp": m}),
            partial(aim, self.out.at[p], self.far.at[p], self.sems, 3 * p + 2, {"tp": far_mate(t)}),
        )

    def push(self, p):
        for copy in self.copies(p)[:2]:
            copy().start()

    def forward(self, p):
        _, _, t = place()
        passing, _, onward = self.copies(p)
        passing().wait_recv()
        both = self.part[p, far_mate(t)].astype(F32) + self.mate[p, 1].astype(F32)
        self.out[p] = both.astype(BF16)
        onward().start()

    def result(self, p):
        _, _, t = place()
        _, own, onward = self.copies(p)
        own().wait_recv()
        onward().wait_recv()
        return self.part[p, t].astype(F32) + self.mate[p, 0].astype(F32) + self.far[p].astype(F32)

    def finish(self, p):
        for copy in self.copies(p):
            copy().wait_send()

    @staticmethod
    def scratch(block):
        return [
            pltpu.VMEM((2, 2) + block, BF16),
            pltpu.VMEM((2,) + block, BF16),
            pltpu.VMEM((2,) + block, BF16),
            DMA((2, 6)),
        ]


def ln_stats(values):
    average = jnp.mean(values, -1, keepdims=True)
    centred = values - average
    inverse = lax.rsqrt(jnp.mean(centred * centred, -1, keepdims=True) + EPSILON)
    return centred * inverse, inverse


def ln_back(unit, inverse, gain, grad):
    scaled = grad * gain
    first = jnp.mean(scaled, -1, keepdims=True)
    second = jnp.mean(scaled * unit, -1, keepdims=True)
    return inverse * (scaled - first - unit * second)


class Stream:
    def __init__(self, loads, stores, sems):
        self.loads, self.stores, self.sems, self.flying = loads, stores, sems, []

    def need(self, *operands):
        for i in operands:
            if i in self.loads:
                self.loads.pop(i).wait()

    def put(self, j, half=None):
        src, dst, q = self.stores[j]
        if half is not None:
            size = src.shape[0] // 2
            src, dst = src.at[half * size : (half + 1) * size], dst.at[half * size : (half + 1) * size]
        copy = pltpu.make_async_copy(src, dst, self.sems.at[2 * q + (half or 0)])
        copy.start()
        self.flying.append((j, copy))

    def close(self):
        self.need(*list(self.loads))
        done = [j for j, _ in self.flying]
        for j in self.stores:
            if j not in done:
                self.put(j)
        for _, copy in self.flying:
            copy.wait()


def comm_call(kernel, name, ident, args, outs, scratch, hbm_in=(), hbm_out=(), late=(), early=()):
    count, results, own = len(args), len(outs), len(scratch)

    def body(*refs):
        ins, out = list(refs[:count]), list(refs[count : count + results])
        inner = refs[count + results : count + results + own]
        extra = refs[count + results + own :]
        buffers, load_sems, store_sems = extra[:-2], extra[-2], extra[-1]
        loads, stores = {}, {}
        for q, i in enumerate(late):
            loads[i] = pltpu.make_async_copy(ins[i], buffers[q], load_sems.at[q])
            loads[i].start()
            ins[i] = buffers[q]
        for q, j in enumerate(early):
            held = buffers[len(late) + q]
            stores[j] = (held, out[j], q)
            out[j] = held
        stream = Stream(loads, stores, store_sems)
        kernel(stream, *ins, *out, *inner)
        stream.close()

    return pl.pallas_call(
        body,
        out_shape=tuple(outs),
        in_specs=[ANY if i in hbm_in or i in late else VM for i in range(count)],
        out_specs=tuple(ANY if j in hbm_out or j in early else VM for j in range(results)),
        scratch_shapes=list(scratch)
        + [pltpu.VMEM(args[i].shape, args[i].dtype) for i in late]
        + [pltpu.VMEM(outs[j].shape, outs[j].dtype) for j in early]
        + [DMA((max(len(late), 1),)), DMA((max(2 * len(early), 1),))],
        compiler_params=pltpu.CompilerParams(
            vmem_limit_bytes=VMEM_GRANT, collective_id=ident, has_side_effects=True
        ),
        name=name,
    )(*args)


def turned(out_ref, full_ref, p):
    count, length = full_ref.shape[1:3]

    def one(i, _):
        start = pl.multiple_of((p * count + i) * length, 128)
        out_ref[:, pl.ds(start, length)] = full_ref[p, i].T
        return 0

    lax.fori_loop(0, count, one, 0)


def front_kernel(
    shards, io, tok_ref, qkvw_ref, pw_ref, vec_ref, x_ref, a_ref, wf_ref, at_ref,
    w1_ref, swap_sems, share_sems, w_sems, w_local,
):
    s, c, t = place()
    wide = qkvw_ref.shape[2]
    for j in range(3):
        w1_ref[:, j * wide : (j + 1) * wide] = qkvw_ref[j]
    w1_ref[:, 3 * wide : 4 * wide] = pw_ref[...]
    greet(shards)
    swap = send(tok_ref.at[1 - c], x_ref.at[c], swap_sems, 0, {"ctx": 1 - c})
    spread = Spread(shards, w1_ref, wf_ref, w_sems, w_local)
    share = Share(a_ref, share_sems)

    def norm(block):
        unit, _ = ln_stats(block.astype(F32))
        return (unit * vec_ref[0:1, :] + vec_ref[1:2, :]).astype(BF16)

    own = tok_ref[c]
    x_ref[c] = own
    a_ref[c, t] = norm(own)
    share.push(0, c)
    swap.wait()
    a_ref[1 - c, t] = norm(x_ref[1 - c])
    share.push(1, 1 - c)
    share.forward(0, c)
    spread.tick(9)
    share.forward(1, 1 - c)
    spread.tick(6)
    share.finish(0, c)
    share.finish(1, 1 - c)
    io.put(0)
    io.put(1)
    turned(at_ref, a_ref, 0)
    spread.tick(2)
    spread.tick(4)
    turned(at_ref, a_ref, 1)
    io.put(3)
    spread.tick(2)
    spread.tick(spread.end)
    spread.finish()


def fwd_kernel(
    shards, heads, hd, cols, rows, qb, io,
    a1_ref, w1_ref, vec_ref, rr_ref, rc_ref, cot_ref, w_ref,
    vh_ref, oh_ref, ob_ref, lse_ref, qa_ref, ka_ref, g_ref, cf_ref, wf_ref, pp_ref,
    qh_ref, vt_ref, rt_ref, tab_ref, hot_ref, swap_sems, share_sems, w_sems, w_local,
):
    _, me, t = place()
    tok, width = ob_ref.shape
    wide = 3 * width
    blocks = tok // qb
    fill_tables(tab_ref, rr_ref, rc_ref)
    fill_hots(hot_ref, hd, cols, rows, False)
    rt_ref[0:128, :] = mm(reverser(2 * rows - 2), tab_ref[0:128, :]).astype(BF16)
    rt_ref[128:256, :] = mm(reverser(2 * cols - 2), tab_ref[128:256, :]).astype(BF16)
    greet(shards)
    swap = swap_copy(cot_ref.at[1 - me], g_ref.at[me], swap_sems)
    swap.start()
    spread = Spread(shards, w_ref, wf_ref, w_sems, w_local)
    share = Share(cf_ref, share_sems)
    own = cot_ref[me]
    g_ref[me] = own
    cf_ref[me, t] = own
    share.push(0, me, cot_ref.at[me])

    io.need(0, 1)

    def project(i, _):
        at = pl.ds(pl.multiple_of(i * qb, qb), qb)
        tile = (mm(a1_ref[at, :], w1_ref[:, 0:wide]) + vec_ref[7:8, 0:wide]).astype(BF16)
        pad = jnp.zeros((qb, 128 - hd), BF16)
        front = lane_ids((qb, 128)) < hd
        for h in range(heads):
            part = [tile[:, (j * heads + h) * hd : (j * heads + h + 1) * hd] for j in range(3)]
            part = [jnp.concatenate([x, pad], 1) for x in part]
            qh_ref[h, at, :] = part[0]
            ka_ref[h, at, 0:128] = jnp.where(front, part[1], hot_ref[at, 0:128])
            ka_ref[h, at, 128:256] = hot_ref[at, 128:256]
            vh_ref[h, at, :] = part[2]
        return 0

    lax.fori_loop(0, blocks, project, 0)
    io.put(0)
    io.put(5)
    swap.wait()
    cf_ref[1 - me, t] = g_ref[1 - me]
    share.push(1, 1 - me, g_ref.at[1 - me])
    c = hd**-0.5 * math.log2(math.e)
    up = hd**0.5

    def head(h, _):
        vt_ref[...] = vh_ref[h].T
        terms = mm(qh_ref[h], rt_ref[...], NT) * up
        ln = lane_ids((cols, 128))
        for r in range(rows):
            rs = slice(r * cols, (r + 1) * cols)
            tr = pltpu.roll(terms[rs, 0:128], (65 + r) % 128, 1)
            tc = pltpu.roll(terms[rs, 128:256], 65, 1, stride=1, stride_axis=0)
            rh = tr.astype(BF16).astype(F32)
            rl = pltpu.roll(tr - rh, rows, 1)
            ch = tc.astype(BF16).astype(F32)
            cl = pltpu.roll(tc - ch, 64, 1)
            low = jnp.where(ln < hd + 2 * rows, rl, jnp.zeros_like(tr))
            left = jnp.where(ln < hd, qh_ref[h, rs, :].astype(F32), jnp.where(ln < hd + rows, rh, low))
            qa_ref[h, rs, 0:128] = left.astype(BF16)
            qa_ref[h, rs, 128:256] = jnp.where(ln < 64, ch, cl).astype(BF16)

        def blk(i, _):
            at = pl.ds(pl.multiple_of(i * qb, qb), qb)
            s = mm(ka_ref[h], qa_ref[h, at, :], NT)
            m = jnp.max(s, 0, keepdims=True)
            p = jnp.exp2((s - m) * c)
            l = jnp.sum(p, 0, keepdims=True)
            lse_ref[h, :, at] = m * c + jnp.log2(l)
            oh_ref[h, at, :] = (mm(vt_ref[...], p.astype(BF16)) / l).T
            turn = h * blocks + i
            event = spread.first + turn + (turn + 1) // 2
            spread.poll(event)
            pl.when(turn % 2 == 0)(lambda: spread.poll(event + 1))
            return 0

        lax.fori_loop(0, blocks, blk, 0)
        pl.when(h == 0)(lambda: share.forward(0, me))
        pl.when(h == min(1, heads - 1))(lambda: share.forward(1, 1 - me))
        return 0

    lax.fori_loop(0, heads, head, 0)
    io.put(1)
    io.put(4)
    for h in range(heads):
        ob_ref[:, h * hd : (h + 1) * hd] = oh_ref[h, :, 0:hd].astype(BF16)

    io.put(2)
    done = spread.first + heads * blocks * 3 // 2

    def out_rows(i, _):
        at = pl.ds(pl.multiple_of(i * qb, qb), qb)
        pp_ref[at, :] = mm(ob_ref[at, :], w1_ref[:, wide:], NT).astype(BF16)
        for k in range(2):
            spread.poll(done + 2 * i + k)
        return 0

    lax.fori_loop(0, blocks, out_rows, 0)
    io.put(9)
    spread.run(done + 2 * blocks, spread.end)
    share.finish(0, me)
    share.finish(1, 1 - me)
    io.put(7)
    spread.finish()


def mid_kernel(
    shards, io, part_ref, x_ref, vec_ref, w_ref, f1_ref, cf_ref,
    mid_ref, a_ref, wf_ref, act_ref, slope_ref, ct_ref,
    mate, far, outb, sum_sems, share_sems, w_sems, w_local,
):
    _, _, t = place()
    greet(shards)
    gather = Gather2(part_ref, mate, far, outb, sum_sems)
    io.need(0)
    gather.push(0)
    gather.push(1)
    spread = Spread(shards, w_ref, wf_ref, w_sems, w_local)
    share = Share(a_ref, share_sems)
    gather.forward(0)
    gather.forward(1)
    io.need(5, 1)
    turned(ct_ref, cf_ref, 0)
    spread.tick(8)
    for p in range(2):
        mid = x_ref[p].astype(F32) + gather.result(p) + vec_ref[2:3, :]
        mid_ref[p] = mid
        unit, _ = ln_stats(mid)
        a_ref[p, t] = (unit * vec_ref[3:4, :] + vec_ref[4:5, :]).astype(BF16)
        share.push(p, p)
        if p == 1:
            turned(ct_ref, cf_ref, 1)
            io.put(0)
            io.put(5)
        spread.tick(7)
    share.forward(0, 0)
    half = a_ref.shape[1] * a_ref.shape[2]

    def hidden(p):
        def one(i, _):
            rows = a_ref[p, pl.ds(2 * i, 2)].reshape(-1, a_ref.shape[3])
            pre = mm(rows, f1_ref[...]) + vec_ref[6:7, :]
            cdf = 0.5 * (1.0 + lax.erf(pre * (2.0**-0.5)))
            bell = jnp.exp(-0.5 * pre * pre) * ((2.0 * math.pi) ** -0.5)
            at = pl.ds(pl.multiple_of(p * half + i * rows.shape[0], 128), rows.shape[0])
            act_ref[at, :] = (pre * cdf).astype(BF16)
            slope_ref[at, :] = cdf + pre * bell
            for k in range(2):
                spread.poll(base + 2 * i + k)
            return 0

        base = spread.now
        lax.fori_loop(0, a_ref.shape[1] // 2, one, 0)
        spread.now += a_ref.shape[1]

    share.finish(0, 0)
    io.need(4)
    hidden(0)
    io.put(3, 0)
    io.put(4, 0)
    spread.tick(spread.end)
    share.forward(1, 1)
    share.finish(1, 1)
    io.put(1)
    hidden(1)
    io.put(4, 1)
    io.put(3, 1)
    for p in range(2):
        gather.finish(p)
    spread.finish()


def turn_kernel(
    shards, io, ct_ref, act_ref, slope_ref, cot_ref, f2_ref, f1_ref, a2_ref, mid_ref, g_ref, vec_ref, w1_ref,
    dm_ref, dbt_ref, wg_ref, sums_ref, f1g_ref, mlp_ref, do_ref,
    db_ref, w2g_ref, part_ref, dp_ref, mate, far, outb, sum_sems, share_sems, w_held, w_sems,
):
    _, _, t = place()
    greet(shards)
    collect = Collect(shards, w2g_ref, w_held, w_sems)
    gather = Gather2(part_ref, mate, far, outb, sum_sems)
    share = Share(db_ref, share_sems)
    tile = 2 * db_ref.shape[2]
    halves = db_ref.shape[1] // 2
    sums_ref[...] = jnp.zeros_like(sums_ref)
    step = collect.pieces

    io.need(0, 1, 2, 3, 4, 5)

    def back(n, _):
        def block(j, _):
            at = collect.pair_rows(n, j)
            w2g_ref[at, :] = mm(ct_ref[at, :], act_ref[...]).astype(BF16)
            return 0

        def blocks():
            lax.fori_loop(0, 2, block, 0)

        pl.when(n < halves)(lambda: blocks())
        pl.when(n == 0)(collect.begin)
        p, i = n // halves, n % halves
        at = pl.ds(pl.multiple_of(n * tile, tile), tile)
        d_pre = (mm(cot_ref[at, :], f2_ref[...]) * slope_ref[at, :]).astype(BF16)
        dp_ref[at, :] = d_pre
        sums_ref[4:5, :] += jnp.sum(d_pre.astype(F32), 0, keepdims=True)
        for k in range(2):
            collect.poll(step * n - 2 + k)
        pl.when(n == halves)(lambda: gather.forward(0))
        d_a2 = mm(d_pre, f1_ref[...], NT).astype(BF16)
        part_ref[p, pl.ds(2 * i, 2)] = d_a2.reshape(2, tile // 2, -1)
        pl.when(n == halves - 1)(lambda: gather.push(0))
        pl.when(n == 2 * halves - 1)(lambda: gather.push(1))
        pl.when(n >= halves)(lambda: blocks())
        for k in range(2, step):
            collect.poll(step * n - 2 + k)
        return 0

    lax.fori_loop(0, 2 * halves, back, 0)
    base = 2 * halves * step - 2

    def hidden_grad(i, _):
        at = pl.ds(pl.multiple_of(i * 256, 256), 256)
        f1g_ref[at, :] = mm(a2_ref[:, at], dp_ref[...], TN).astype(BF16)
        collect.poll(base + i)
        pl.when(i == 0)(lambda: gather.forward(1))

        @pl.when((i == 1) | (i == count - 1))
        def _():
            p = lax.div(i, count - 1)
            unit, inverse = ln_stats(mid_ref[p])
            g = g_ref[p].astype(F32)
            da = gather.result(p)
            dm = g + ln_back(unit, inverse, vec_ref[3:4, :], da)
            dm_ref[p] = dm
            low_dm = dm.astype(BF16)
            db_ref[p, t] = low_dm
            share.push(p, p)
            for k, term in enumerate((da * unit, da, low_dm.astype(F32), g)):
                sums_ref[k : k + 1, :] += jnp.sum(term, 0, keepdims=True)

        return 0

    count = f1g_ref.shape[0] // 256
    io.need(6, 7, 8)
    lax.fori_loop(0, count, hidden_grad, 0)
    io.put(0)
    io.put(4)
    base2 = base + count

    def mlp(n, _):
        at = pl.ds(pl.multiple_of(n * tile, tile), tile)
        mlp_ref[at, :] = mm(act_ref[at, :], f2_ref[...], NT).astype(BF16)
        for k in range(2):
            collect.poll(base2 + 2 * n + k)
        pl.when(n == 2 * halves - 1)(lambda: share.forward(0, 0))
        return 0

    lax.fori_loop(0, 2 * halves, mlp, 0)
    io.put(5)
    collect.run(base2 + 4 * halves, collect.end)
    share.forward(1, 1)
    wide = do_ref.shape[1]
    io.need(10)

    def d_o(n, _):
        p, i = n // halves, n % halves
        pl.when(i == 0)(lambda: share.finish(p, p))
        rows = db_ref[p, pl.ds(2 * i, 2)].reshape(tile, -1)
        at = pl.ds(pl.multiple_of(n * tile, tile), tile)
        do_ref[at, :] = mm(rows, w1_ref[:, 3 * wide :]).astype(BF16)
        dbt_ref[:, at] = rows.T
        return 0

    lax.fori_loop(0, 2 * halves, d_o, 0)
    io.put(1)
    io.put(6)
    for p in range(2):
        gather.finish(p)
    collect.finish(wg_ref)


def bwd_kernel(
    shards, heads, hd, cols, rows, qb, io,
    qa_ref, ka_ref, vh_ref, do_ref, oh_ref, lse_ref, rr_ref, rc_ref, w_ref, part_ref, mid_ref, vec_ref,
    dqkv_ref, rg_ref, wg_ref, qs_ref, out_ref,
    doh_ref, dh_ref, kt_ref, acc_k, acc_v, del_ref, tab_ref, hot_ref, res_ref,
    mate, far, outb, sum_sems, swap_sems, w_held, w_sems,
):
    fill_tables(tab_ref, rr_ref, rc_ref)
    fill_hots(hot_ref, hd, cols, rows, True)
    _, me, _ = place()
    greet(shards)
    gather = Gather2(part_ref, mate, far, outb, sum_sems)
    io.need(9)
    gather.push(0)
    gather.push(1)
    swap = swap_copy(res_ref.at[1 - me], out_ref.at[me], swap_sems)
    collect = Collect(shards, w_ref, w_held, w_sems)
    io.need(8)
    collect.begin()
    io.need(3)
    tok, wide = dqkv_ref.shape
    blocks = tok // qb
    for h in range(heads):
        pad = jnp.zeros((tok, 128 - hd), BF16)
        doh_ref[h] = jnp.concatenate([do_ref[:, h * hd : (h + 1) * hd], pad], 1)
    gather.forward(0)
    gather.forward(1)
    scale = hd**-0.5
    c = scale * math.log2(math.e)
    rg_ref[...] = jnp.zeros_like(rg_ref)

    io.need(0, 1, 2, 4, 10)

    def head(h, _):
        kt_ref[0:128, :] = jnp.where(lane_ids((tok, 128)) < hd, ka_ref[h, :, 0:128], hot_ref[:, 0:128]).T
        kt_ref[128:256, :] = hot_ref[:, 128:256].T
        del_ref[...] = lax.dot_general(
            jnp.ones((8, 128), F32), doh_ref[h].astype(F32) * oh_ref[h], NT,
            preferred_element_type=F32, precision=PRECISE,
        )
        acc_k[...] = jnp.zeros_like(acc_k)
        acc_v[...] = jnp.zeros_like(acc_v)

        def blk(i, _):
            at = pl.ds(pl.multiple_of(i * qb, qb), qb)
            qblk = qa_ref[h, at, :]
            dob = doh_ref[h, at, :]
            s = mm(ka_ref[h], qblk, NT)
            p = jnp.exp2(s * c - lse_ref[h, :, at])
            dp = mm(vh_ref[h], dob, NT)
            ds = (p * (dp - del_ref[0:1, at])).astype(BF16)
            acc_v[...] += mm(p.astype(BF16), dob)
            acc_k[...] += mm(ds, qblk[:, 0:128])
            dqa = mm(kt_ref[...], ds).T
            ln = lane_ids((cols, 128))
            parts = []
            for j in range(qb // cols):
                r = i * (qb // cols) + j
                js = slice(j * cols, (j + 1) * cols)
                dr = dqa[js, 0:128]
                dr = jnp.where((ln >= hd) & (ln < hd + rows), dr, 0.0)
                dr = pltpu.roll(dr, lax.rem(48 + r, 128), 1)
                dc = pltpu.roll(dqa[js, 128:256], 0, 1, stride=1, stride_axis=0)
                parts.append(jnp.concatenate([dr, dc], 1))
            d = jnp.concatenate(parts, 0).astype(BF16)
            rel = mm(d, tab_ref[...])
            rg_ref[...] += mm(d, qblk[:, 0:128], TN)
            dh_ref[h, at, :] = (scale * dqa[:, 0:128] + rel).astype(BF16)
            for k in range(2):
                collect.poll(collect.first + 2 * (h * blocks + i) + k)
            return 0

        lax.fori_loop(0, blocks, blk, 0)
        dh_ref[heads + h] = (scale * acc_k[...]).astype(BF16)
        dh_ref[2 * heads + h] = acc_v[...].astype(BF16)

        @pl.when(h == min(2, heads - 1))
        def _():
            for p in range(2):
                total = mid_ref[p] + gather.result(p) + vec_ref[5:6, :]
                res_ref[p] = total.astype(BF16)

        return 0

    lax.fori_loop(0, heads, head, 0)
    swap.start()
    out_ref[me] = res_ref[me]
    for j in range(3 * heads):
        dqkv_ref[:, j * hd : (j + 1) * hd] = dh_ref[j, :, 0:hd]
    io.put(0)
    collect.run(collect.first + 2 * heads * blocks, collect.end)
    qs_ref[...] = mm(jnp.ones((8, tok), BF16), dqkv_ref[...])
    for p in range(2):
        gather.finish(p)
    collect.finish(wg_ref)
    swap.wait()


def end_kernel(
    shards, io, x_ref, dm_ref, vec_ref, at_ref, dqkv_ref, dbt_ref, ob_ref, sums_ref, w1_ref, rg_ref, qs_ref,
    grad_ref, qg_ref, pg_ref, total_ref, late_ref,
    w1g_ref, wg_ref, part_ref, gres_ref, mate, far, outb, sum_sems, swap_sems,
    held, got, line, small_sems, near, wide_all, late_sems, w_held, w_sems,
):
    s, me, t = place()
    half = held.shape[2] // 2
    held[0] = jnp.zeros_like(held[0])
    held[0, :, 0:128] = rg_ref[0:32, :]
    for k in range(4):
        held[0, :, 128 * (k + 1) : 128 * (k + 2)] = rg_ref[128 + 32 * k : 160 + 32 * k, :]
    for k in range(4):
        for u in range(2):
            held[0, 2 * k + u : 2 * k + u + 1, half:] = sums_ref[k : k + 1, u * half : (u + 1) * half]
    for u in range(2):
        held[0, pl.ds(8 + 2 * t + u, 1), half:] = sums_ref[4:5, u * half : (u + 1) * half]
    span = dqkv_ref.shape[1] // 3
    pair = jnp.concatenate([qs_ref[0:1, 0:span], qs_ref[0:1, 2 * span :]], 1)
    held[0, pl.ds(16 + t, 1), half:] = pair
    mine = pl.ds(pl.multiple_of(8 * t, 8), 8)
    mates = ({"tp": core_mate(t)}, {"tp": far_mate(t)}, {"tp": core_mate(far_mate(t))})

    def whole(k):
        return aim(held.at[k], got.at[k], small_sems, k, mates[k])

    def cross():
        return aim(held.at[2, mine], got.at[2, mine], small_sems, 2, {"ctx": 1 - me})

    def along(d):
        return aim(held.at[3, mine], line.at[s], small_sems, 2 + d, {"shard": lax.rem(s + d, shards)})

    def spread_sum(k):
        return aim(total_ref.at[mine], total_ref.at[mine], small_sems, 2 + shards + k, mates[k])

    def close_by(k):
        return aim(near.at[t], near.at[t], late_sems, k, mates[k])

    def far_off(d, flip):
        there = {"shard": lax.rem(s + d, shards), "ctx": 1 - me if flip else me}
        own = wide_all.at[2 * s + me]
        return aim(own, own, late_sems, 3 + 2 * d + flip, there)

    others = [(d, flip) for d in range(shards) for flip in range(2) if d + flip > 0]
    greet(shards, True)
    whole(0).start()
    gather = Gather2(part_ref, mate, far, outb, sum_sems)
    collect = Collect(shards, w1g_ref, w_held, w_sems)
    wide = dqkv_ref.shape[1]
    tile = 2 * part_ref.shape[2]
    halves = part_ref.shape[1] // 2
    step = collect.pieces

    io.need(4, 8, 3, 5, 6)

    def back(n, _):
        def block(j, _):
            at = collect.pair_rows(n, j)
            w1g_ref[at, 0:wide] = mm(at_ref[at, :], dqkv_ref[...]).astype(BF16)
            w1g_ref[at, wide:] = mm(dbt_ref[at, :], ob_ref[...]).astype(BF16)
            return 0

        lax.fori_loop(0, 2, block, 0)
        pl.when(n == 0)(collect.begin)
        for k in range(2):
            collect.poll(step * n + k)
        pl.when(n == 2)(lambda: gather.forward(1))

        def rows_of(i, _):
            rows = pl.ds(pl.multiple_of((n * halves + i) * tile, tile), tile)
            d_a1 = mm(dqkv_ref[rows, :], w1_ref[:, 0:wide], NT).astype(BF16)
            part_ref[n, pl.ds(2 * i, 2)] = d_a1.reshape(2, tile // 2, -1)
            return 0

        @pl.when(n < 2)
        def _():
            lax.fori_loop(0, halves, rows_of, 0)
            gather.push(n)

        for k in range(2, step):
            collect.poll(step * n + k)
        pl.when(n == 1)(lambda: gather.forward(0))

        @pl.when(n == 0)
        def _():
            whole(0).wait_recv()
            held[1] = held[0] + got[0]
            whole(1).start()

        @pl.when(n == 1)
        def _():
            whole(1).wait_recv()
            held[2] = held[1] + got[1]
            cross().start()

        @pl.when(n == 2)
        def _():
            cross().wait_recv()
            held[3, mine] = held[2, mine] + got[2, mine]
            line[s] = held[3, mine]
            for d in range(1, shards):
                along(d).start()

        return 0

    lax.fori_loop(0, 2 * halves, back, 0)
    collect.now = step * 2 * halves
    io.need(0, 1)
    first = jnp.zeros((1, x_ref.shape[2]), F32)
    second = jnp.zeros((1, x_ref.shape[2]), F32)
    for p in range(2):
        unit, inverse = ln_stats(x_ref[p].astype(F32))
        collect.tick(1)
        da = gather.result(p)
        gres_ref[p] = (dm_ref[p] + ln_back(unit, inverse, vec_ref[0:1, :], da)).astype(BF16)
        first = first + jnp.sum(da * unit, 0, keepdims=True)
        second = second + jnp.sum(da, 0, keepdims=True)
        collect.tick(1)
    for k in range(4):
        near[t, k : k + 1, :] = first[:, k * span : (k + 1) * span]
        near[t, 4 + k : 5 + k, :] = second[:, k * span : (k + 1) * span]
    for k in range(3):
        close_by(k).start()
    grad_ref[me] = gres_ref[me]
    swap = swap_copy(gres_ref.at[1 - me], grad_ref.at[me], swap_sems)
    for d in range(1, shards):
        along(d).wait_recv()
    acc = line[0]
    for k in range(1, shards):
        acc = acc + line[k]
    total_ref[mine] = acc
    for k in range(3):
        spread_sum(k).start()
    collect.tick(2)
    for k in range(3):
        close_by(k).wait_recv()
    wide_all[2 * s + me] = near[0] + near[1] + near[2] + near[3]
    for d, flip in others:
        far_off(d, flip).start()
    swap.start()
    collect.tick(collect.end)
    collect.finish(wg_ref)
    part = wide // 3
    for j in range(3):
        qg_ref[j] = wg_ref[:, j * part : (j + 1) * part]
    pg_ref[...] = wg_ref[:, wide:]
    for d, flip in others:
        far_off(d, flip).wait()
    acc = wide_all[0]
    for k in range(1, 2 * shards):
        acc = acc + wide_all[k]
    late_ref[...] = acc
    for k in range(3):
        spread_sum(k).wait()
        close_by(k).wait_send()
    for k in range(2):
        whole(k).wait_send()
    cross().wait_send()
    for d in range(1, shards):
        along(d).wait_send()
    for p in range(2):
        gather.finish(p)
    swap.wait()


def settle_kernel(
    total_ref, late_ref, out_ref, grad_ref, qg_ref, pg_ref, f1_ref, f2_ref,
    out_to, grad_to, qg_to, pg_to, f1_to, f2_to,
    gain1_to, bias1_to, qv_to, rr_to, rc_to, gain2_to, bias2_to, projb_to, fc2b_to, fc1b_to,
):
    for here, there in (
        (out_ref, out_to), (grad_ref, grad_to), (qg_ref, qg_to), (pg_ref, pg_to), (f1_ref, f1_to), (f2_ref, f2_to)
    ):
        there[...] = here[...]
    half = total_ref.shape[1] // 2
    span = late_ref.shape[1]

    def side(parts):
        return jnp.concatenate(parts, 1)

    gain1_to[...] = side([late_ref[k : k + 1, :] for k in range(4)])[0, :]
    bias1_to[...] = side([late_ref[4 + k : 5 + k, :] for k in range(4)])[0, :]
    for u in range(2):
        at = slice(half + u * span, half + (u + 1) * span)
        qv_to[u : u + 1, :] = side([total_ref[16 + k : 17 + k, at] for k in range(4)])
    rr_to[...] = total_ref[0 : rr_to.shape[0], 0 : rr_to.shape[1]]
    for k in range(4):
        size = min(32, rc_to.shape[0] - 32 * k)
        rc_to[32 * k : 32 * k + size, :] = total_ref[0:size, 128 * (k + 1) : 128 * (k + 1) + rc_to.shape[1]]
    for k, there in enumerate((gain2_to, bias2_to, projb_to, fc2b_to)):
        there[...] = side([total_ref[2 * k + u : 2 * k + u + 1, half:] for u in range(2)])[0, :]
    for k in range(4):
        fc1b_to[k : k + 1, :] = side([total_ref[8 + 2 * k + u : 9 + 2 * k + u, half:] for u in range(2)])


def on_device_images(
    tokens, norm1_gain, norm1_bias, qkv_weight, qv_bias, rel_rows, rel_cols, proj_weight, proj_bias,
    norm2_gain, norm2_bias, fc1_weight, fc1_bias, fc2_weight, fc2_bias, cotangent,
):
    S = jax.ShapeDtypeStruct
    shards = lax.axis_size("shard")
    tp_count = lax.axis_size("tp")
    tp_rank = lax.axis_index("tp")
    heads = H // tp_count
    width = heads * HD
    ff = FF // tp_count
    rows = (rel_rows.shape[0] + 1) // 2
    tok = rows * COLS
    own = tokens.shape
    piece = own[1:]
    full = (2, tp_count) + piece
    block = fc1_weight.shape
    blocks = (2 * shards,) + block
    qkv_cols = 3 * width
    fc2_t = fc2_weight.T
    qv_local = lax.dynamic_slice_in_dim(qv_bias, tp_rank * width, width, 1)
    qkv_bias = jnp.concatenate([qv_local[0], jnp.zeros((width,), F32), qv_local[1]])
    fc1_local = lax.dynamic_slice_in_dim(fc1_bias, tp_rank * ff, ff, 0)
    vec = jnp.concatenate(
        [
            norm1_gain, norm1_bias, proj_bias, norm2_gain, norm2_bias, fc2_bias, fc1_local,
            qkv_bias, jnp.zeros((D - qkv_cols,), F32),
        ]
    ).reshape(8, D)
    spread = Spread.scratch(shards, block)
    collect = Collect.scratch(shards, block)
    gather = Gather2.scratch(piece)
    swap = [DMA((2, 1))]
    share = [DMA((2, 6))]

    x, a1, w1_full, a1_turned = comm_call(
        partial(front_kernel, shards), "front", 0,
        (tokens, qkv_weight, proj_weight.T, vec),
        (S(own, BF16), S(full, BF16), S(blocks, BF16), S((D, tok), BF16)),
        [pltpu.VMEM(block, BF16)] + swap + share + spread, hbm_out=(2,), early=(0, 1, 3),
    )
    w1_full = w1_full.reshape(D, -1)
    vh, oh, o_low, lse, qa, ka, g, cot, fc1_full, proj_part = comm_call(
        partial(fwd_kernel, shards, heads, HD, COLS, rows, 256), "attn_fwd", 1,
        (a1.reshape(tok, D), w1_full, vec, rel_rows, rel_cols, cotangent, fc1_weight),
        (
            S((heads, tok, 128), BF16), S((heads, tok, 128), F32), S((tok, width), BF16), S((heads, 1, tok), F32),
            S((heads, tok, 256), BF16), S((heads, tok, 256), BF16),
            S(own, BF16), S(full, BF16), S(blocks, BF16), S((tok, D), BF16),
        ),
        [
            pltpu.VMEM((heads, tok, 128), BF16), pltpu.VMEM((128, tok), BF16), pltpu.VMEM((256, 128), BF16),
            pltpu.VMEM((256, 128), BF16), pltpu.VMEM((tok, 256), BF16),
        ]
        + swap + share + spread, hbm_in=(6,), hbm_out=(8,), late=(1, 0), early=(0, 1, 2, 4, 5, 7, 9),
    )
    fc1_full = fc1_full.reshape(D, ff)
    mid, a2, fc2_full, act, slope, cot_turned = comm_call(
        partial(mid_kernel, shards), "mid", 2,
        (proj_part.reshape(full), x, vec, fc2_t, fc1_full, cot),
        (
            S(own, F32), S(full, BF16), S(blocks, BF16), S((tok, ff), BF16), S((tok, ff), F32),
            S((D, tok), BF16),
        ),
        gather + share + spread, hbm_in=(3,), hbm_out=(2,), late=(0, 5, 1, 4), early=(0, 1, 3, 4, 5),
    )
    fc2_full = fc2_full.reshape(D, ff)
    d_mid, d_branch_turned, fc2_own, sums, fc1_grad, mlp_part, d_o = comm_call(
        partial(turn_kernel, shards), "turn", 3,
        (
            cot_turned, act, slope, cot.reshape(tok, D), fc2_full, fc1_full, a2.reshape(tok, D), mid, g, vec,
            w1_full,
        ),
        (
            S(own, F32), S((D, tok), BF16), S(block, F32), S((8, D), F32),
            S((D, ff), BF16), S((tok, D), BF16), S((tok, width), BF16),
        ),
        [pltpu.VMEM(full, BF16), pltpu.VMEM((D, ff), BF16), pltpu.VMEM(full, BF16), pltpu.VMEM((tok, ff), BF16)]
        + gather + share + collect,
        late=(0, 1, 2, 3, 4, 5, 6, 7, 8, 10), early=(0, 1, 4, 5, 6),
    )
    dqkv, rel_grad, fc1_own, qkv_sum, output = comm_call(
        partial(bwd_kernel, shards, heads, HD, COLS, rows, 256), "attn_bwd", 4,
        (qa, ka, vh, d_o, oh, lse, rel_rows, rel_cols, fc1_grad, mlp_part.reshape(full), mid, vec),
        (S((tok, qkv_cols), BF16), S((256, 128), F32), S(block, F32), S((8, qkv_cols), F32), S(own, BF16)),
        [
            pltpu.VMEM((heads, tok, 128), BF16), pltpu.VMEM((3 * heads, tok, 128), BF16),
            pltpu.VMEM((256, tok), BF16), pltpu.VMEM((tok, 128), F32), pltpu.VMEM((tok, 128), F32),
            pltpu.VMEM((8, tok), F32), pltpu.VMEM((256, 128), BF16), pltpu.VMEM((tok, 256), BF16),
            pltpu.VMEM(own, BF16),
        ] + gather + swap + collect,
        late=(8, 9, 3, 2, 4, 1, 0, 10), early=(0,),
    )
    tokens_grad, qkv_own, proj_own, total, late = comm_call(
        partial(end_kernel, shards), "end", 5,
        (x, d_mid, vec, a1_turned, dqkv, d_branch_turned, o_low, sums, w1_full, rel_grad, qkv_sum),
        (
            S(own, BF16), S((3, block[0], width), F32), S((block[0], width), F32), S((32, D), F32), S((8, width), F32),
        ),
        [pltpu.VMEM((D, ff), BF16), pltpu.VMEM(block, F32), pltpu.VMEM(full, BF16), pltpu.VMEM(own, BF16)]
        + gather + swap
        + [
            pltpu.VMEM((4, 32, D), F32), pltpu.VMEM((3, 32, D), F32),
            pltpu.VMEM((shards, 8, D), F32), DMA((2, 5 + shards)),
            pltpu.VMEM((4, 8, width), F32), pltpu.VMEM((2 * shards, 8, width), F32), DMA((2, 3 + 2 * shards)),
        ]
        + collect,
        late=(4, 8, 3, 5, 6, 0, 1),
    )
    big = (output, tokens_grad, qkv_own, proj_own, fc1_own, fc2_own)
    vector = S((D,), F32)
    (
        output, tokens_grad, qkv_own, proj_own, fc1_own, fc2_own,
        gain1, bias1, qv_grad, rows_grad, cols_grad, gain2, bias2, projb, fc2b, fc1b,
    ) = pl.pallas_call(
        settle_kernel,
        out_shape=tuple(S(b.shape, b.dtype) for b in big)
        + (vector, vector, S((2, D), F32), S(rel_rows.shape, F32), S(rel_cols.shape, F32))
        + (vector, vector, vector, vector, S((tp_count, ff), F32)),
        compiler_params=pltpu.CompilerParams(vmem_limit_bytes=VMEM_GRANT),
        name="settle",
    )(total, late, *big)
    return (
        output, tokens_grad, gain1, bias1, qkv_own, qv_grad, rows_grad, cols_grad, proj_own.T, projb,
        gain2, bias2, fc1_own, fc1b.reshape(FF), fc2_own.T, fc2b,
    )


def solution(mesh):
    in_specs = (
        P("shard", ("ctx", "tp"), None),
        P(),
        P(),
        P(None, ("shard", "ctx"), "tp"),
        P(),
        P(),
        P(),
        P("tp", ("shard", "ctx")),
        P(),
        P(),
        P(),
        P(("shard", "ctx"), "tp"),
        P(),
        P("tp", ("shard", "ctx")),
        P(),
        P("shard", ("ctx", "tp"), None),
    )
    out_specs = (
        P("shard", ("ctx", "tp"), None),
        P("shard", ("ctx", "tp"), None),
        P(),
        P(),
        P(None, ("shard", "ctx"), "tp"),
        P(),
        P(),
        P(),
        P("tp", ("shard", "ctx")),
        P(),
        P(),
        P(),
        P(("shard", "ctx"), "tp"),
        P(),
        P("tp", ("shard", "ctx")),
        P(),
    )
    def on_device(*arrays):
        rows = (arrays[5].shape[0] + 1) // 2
        fits = (mesh.shape["shard"], mesh.shape["ctx"], mesh.shape["tp"]) == (4, 2, 4)
        fits = fits and arrays[0].shape[0] == mesh.shape["ctx"] and HD + 2 * rows <= 128
        fits = fits and arrays[5].shape[0] <= 32 and arrays[6].shape[0] <= 128
        return (on_device_images if fits else on_device_rows)(*arrays)

    return jax.shard_map(
        on_device, mesh=mesh, in_specs=in_specs, out_specs=out_specs, check_vma=False
    )
```

```python
from functools import partial
import math

import jax
import jax.numpy as jnp
from jax import lax
from jax.experimental import pallas as pl
from jax.experimental.pallas import tpu as pltpu
from jax.sharding import PartitionSpec as P

D = 1280
H = 16
HD = 80
FF = 5120
COLS = 64
ROWS_DEV = 8


PRECISE = lax.Precision.HIGHEST
EPSILON = 1e-06
NEGATIVE = -1e30


def layer_norm(values_in, gain_vec, shift_vec):
    average = jnp.mean(values_in, -1, keepdims=True)
    centred = values_in - average
    variance = jnp.mean(centred * centred, -1, keepdims=True)
    return centred * lax.rsqrt(variance + EPSILON) * gain_vec + shift_vec


def block_size():
    return 512


def to_heads(flat_rows, heads_local):
    images, length, feat_width = flat_rows.shape
    return flat_rows.reshape(images, length, heads_local, feat_width // heads_local).transpose(
        0, 2, 1, 3
    )


def from_heads(per_head):
    images, heads_local, length, head_dim = per_head.shape
    return per_head.transpose(0, 2, 1, 3).reshape(images, length, heads_local * head_dim)


def block_scores(query_heads, key_flat, rows_bias, cols_bias, first_key, scale_factor):
    key_heads = to_heads(key_flat, query_heads.shape[1])
    key_len = key_flat.shape[1]
    key_rows = key_len // COLS
    scores = scale_factor * jnp.einsum(
        "ihqc,ihkc->ihqk", query_heads, key_heads, preferred_element_type=jnp.float32
    )
    images, heads_local, query_len, unused_len = scores.shape
    row_part = lax.dynamic_slice_in_dim(rows_bias, first_key // COLS, key_rows, 3)
    scores = scores.reshape(images, heads_local, query_len, key_rows, COLS)
    scores = scores + row_part[..., :, None] + cols_bias[..., None, :]
    return scores.reshape(images, heads_local, query_len, key_len)


def relative_terms(query_flat, rows_param, cols_param, first_row, heads_local):
    images, length, feat_width = query_flat.shape
    rows_dev = length // COLS
    grid_rows = (rows_param.shape[0] + 1) // 2
    own_rows = first_row + jnp.arange(rows_dev, dtype=jnp.int32)
    key_rows = jnp.arange(grid_rows, dtype=jnp.int32)
    row_slots = jnp.arange(rows_param.shape[0], dtype=jnp.int32)
    pick_rows = (
        row_slots[None, None, :]
        == own_rows[:, None, None] - key_rows[None, :, None] + grid_rows - 1
    ).astype(jnp.float32)
    table_rows = jnp.einsum("rkj,jc->rkc", pick_rows, rows_param, precision=PRECISE)
    col_ids = jnp.arange(COLS, dtype=jnp.int32)
    col_slots = jnp.arange(cols_param.shape[0], dtype=jnp.int32)
    pick_cols = (
        col_slots[None, None, :] == col_ids[:, None, None] - col_ids[None, :, None] + COLS - 1
    ).astype(jnp.float32)
    table_cols = jnp.einsum("wkj,jc->wkc", pick_cols, cols_param, precision=PRECISE)
    grid_form = query_flat.reshape(images, rows_dev, COLS, heads_local, feat_width // heads_local)
    along_rows = jnp.einsum("irwhc,rkc->ihrwk", grid_form, table_rows, precision=PRECISE).reshape(
        images, heads_local, length, grid_rows
    )
    along_cols = jnp.einsum("irwhc,wkc->ihrwk", grid_form, table_cols, precision=PRECISE).reshape(
        images, heads_local, length, COLS
    )
    return (along_rows, along_cols)


def on_device_rows(
    tokens,
    norm1_gain,
    norm1_bias,
    qkv_weight,
    qv_bias,
    rel_rows,
    rel_cols,
    proj_weight,
    proj_bias,
    norm2_gain,
    norm2_bias,
    fc1_weight,
    fc1_bias,
    fc2_weight,
    fc2_bias,
    cotangent,
):
    scale_factor = HD ** (-0.5)
    tp_count = lax.axis_size("tp")
    ctx_count = lax.axis_size("ctx")
    tp_rank = lax.axis_index("tp")
    ctx_rank = lax.axis_index("ctx")
    grid_rows = ROWS_DEV * ctx_count
    tok_image = grid_rows * COLS
    tok_ctx = ROWS_DEV * COLS
    heads_local = H // tp_count
    width_local = heads_local * HD
    ff_local = FF // tp_count
    images = tokens.shape[0]
    rows_table = rel_rows.astype(jnp.float32)
    cols_table = rel_cols.astype(jnp.float32)
    qkv_full, proj_full, fc1_full, fc2_full = (
        lax.all_gather(qkv_weight, ("shard", "ctx"), axis=1, tiled=True),
        lax.all_gather(proj_weight, ("shard", "ctx"), axis=1, tiled=True),
        lax.all_gather(fc1_weight, ("shard", "ctx"), axis=0, tiled=True),
        lax.all_gather(fc2_weight, ("shard", "ctx"), axis=1, tiled=True),
    )
    qv_local = lax.dynamic_slice_in_dim(qv_bias, tp_rank * width_local, width_local, 1)
    fc1_local = lax.dynamic_slice_in_dim(fc1_bias, tp_rank * ff_local, ff_local, 0)
    resid_in = tokens.astype(jnp.float32)
    normed1 = layer_norm(resid_in, norm1_gain, norm1_bias).astype(jnp.bfloat16)
    normed1_full = lax.all_gather(normed1, "tp", axis=1, tiled=True)
    projected = jnp.einsum(
        "itd,sde->itse", normed1_full, qkv_full, preferred_element_type=jnp.float32
    )
    queries = (projected[:, :, 0] + qv_local[0]).astype(jnp.bfloat16)
    keys_own = projected[:, :, 1].astype(jnp.bfloat16)
    values_own = (projected[:, :, 2] + qv_local[1]).astype(jnp.bfloat16)
    first_row = ctx_rank * ROWS_DEV
    rel_fn = partial(relative_terms, first_row=first_row, heads_local=heads_local)
    (along_rows, along_cols), rel_pull = jax.vjp(
        rel_fn, queries.astype(jnp.float32), rows_table, cols_table
    )
    query_heads = to_heads(queries, heads_local)
    start_state = (
        jnp.full((images, heads_local, tok_ctx), NEGATIVE, jnp.float32),
        jnp.zeros((images, heads_local, tok_ctx), jnp.float32),
        jnp.zeros((images, heads_local, tok_ctx, HD), jnp.float32),
        jnp.zeros((images, tok_image, width_local), jnp.bfloat16),
        jnp.zeros((images, tok_image, width_local), jnp.bfloat16),
    )
    shard_piece = (
        lax.all_gather(keys_own, "ctx", axis=1, tiled=True),
        lax.all_gather(values_own, "ctx", axis=1, tiled=True),
    )
    piece_len = shard_piece[0].shape[1]
    step_len = block_size()

    def one_step(inner, offset):
        run_max, run_sum, run_acc, keys_all, values_all = inner
        key_blk = lax.dynamic_slice_in_dim(shard_piece[0], offset, step_len, 1)
        value_blk = lax.dynamic_slice_in_dim(shard_piece[1], offset, step_len, 1)
        scores = block_scores(query_heads, key_blk, along_rows, along_cols, offset, scale_factor)
        new_max = jnp.maximum(run_max, jnp.max(scores, -1))
        factor = jnp.exp(run_max - new_max)
        weights_blk = jnp.exp(scores - new_max[..., None])
        run_sum = run_sum * factor + jnp.sum(weights_blk, -1)
        value_heads = to_heads(value_blk, heads_local)
        run_acc = run_acc * factor[..., None] + jnp.einsum(
            "ihqk,ihkc->ihqc",
            weights_blk.astype(jnp.bfloat16),
            value_heads,
            preferred_element_type=jnp.float32,
        )
        keys_all = lax.dynamic_update_slice_in_dim(keys_all, key_blk, offset, 1)
        values_all = lax.dynamic_update_slice_in_dim(values_all, value_blk, offset, 1)
        return ((new_max, run_sum, run_acc, keys_all, values_all), None)

    offsets = jnp.arange(piece_len // step_len, dtype=jnp.int32) * step_len
    result, unused = lax.scan(one_step, start_state, offsets)
    run_max, run_sum, run_acc, keys_all, values_all = result
    attn_heads = run_acc / run_sum[..., None]
    log_total = run_max + jnp.log(run_sum)
    attn_low = from_heads(attn_heads).astype(jnp.bfloat16)
    proj_part = jnp.einsum("itd,de->ite", attn_low, proj_full, preferred_element_type=jnp.float32)
    branch = lax.psum_scatter(
        proj_part.astype(jnp.bfloat16), "tp", scatter_dimension=1, tiled=True
    ).astype(jnp.float32)
    middle = resid_in + branch + proj_bias
    normed2 = layer_norm(middle, norm2_gain, norm2_bias).astype(jnp.bfloat16)
    normed2_full = lax.all_gather(normed2, "tp", axis=1, tiled=True)
    hidden_pre = (
        jnp.einsum("itd,df->itf", normed2_full, fc1_full, preferred_element_type=jnp.float32)
        + fc1_local
    )
    gelu_exact = partial(jax.nn.gelu, approximate=False)
    activated_f, gelu_pull = jax.vjp(gelu_exact, hidden_pre)
    activated = activated_f.astype(jnp.bfloat16)
    mlp_part = jnp.einsum("itf,fe->ite", activated, fc2_full, preferred_element_type=jnp.float32)
    mlp_out = lax.psum_scatter(
        mlp_part.astype(jnp.bfloat16), "tp", scatter_dimension=1, tiled=True
    ).astype(jnp.float32)
    output = (middle + mlp_out + fc2_bias).astype(jnp.bfloat16)
    cot_full = lax.all_gather(cotangent, "tp", axis=1, tiled=True)
    d_act = jnp.einsum("ite,fe->itf", cot_full, fc2_full, preferred_element_type=jnp.float32)
    d_hidden = gelu_pull(d_act)[0].astype(jnp.bfloat16)
    fc2_grad = jnp.einsum("itf,ite->fe", activated, cot_full, preferred_element_type=jnp.float32)
    fc1_grad = jnp.einsum("itd,itf->df", normed2_full, d_hidden, preferred_element_type=jnp.float32)
    fc1_bias_part = jnp.sum(d_hidden.astype(jnp.float32), (0, 1))
    fc2_bias_part = jnp.sum(cotangent.astype(jnp.float32), (0, 1))
    d_norm2_part = jnp.einsum("itf,df->itd", d_hidden, fc1_full, preferred_element_type=jnp.float32)
    d_norm2 = lax.psum_scatter(
        d_norm2_part.astype(jnp.bfloat16), "tp", scatter_dimension=1, tiled=True
    ).astype(jnp.float32)
    unused_out, norm2_pull = jax.vjp(layer_norm, middle, norm2_gain, norm2_bias)
    d_mid_part, gain2_part, bias2_part = norm2_pull(d_norm2)
    d_middle = cotangent.astype(jnp.float32) + d_mid_part
    d_branch = d_middle.astype(jnp.bfloat16)
    proj_bias_part = jnp.sum(d_branch.astype(jnp.float32), (0, 1))
    d_branch_full = lax.all_gather(d_branch, "tp", axis=1, tiled=True)
    proj_grad = jnp.einsum(
        "itd,ite->de", attn_low, d_branch_full, preferred_element_type=jnp.float32
    )
    d_attn = jnp.einsum(
        "ite,de->itd", d_branch_full, proj_full, preferred_element_type=jnp.float32
    ).astype(jnp.bfloat16)
    d_attn_heads = to_heads(d_attn, heads_local)
    delta_rows = jnp.sum(d_attn_heads.astype(jnp.float32) * attn_heads, -1)
    key_step = block_size()
    key_rows = key_step // COLS
    key_offsets = jnp.arange(tok_image // key_step, dtype=jnp.int32) * key_step

    def back_step(carried, offset):
        grad_query, grad_rows, grad_cols = carried
        key_blk = lax.dynamic_slice_in_dim(keys_all, offset, key_step, 1)
        value_blk = lax.dynamic_slice_in_dim(values_all, offset, key_step, 1)
        scores = block_scores(query_heads, key_blk, along_rows, along_cols, offset, scale_factor)
        soft_probs = jnp.exp(scores - log_total[..., None])
        value_heads = to_heads(value_blk, heads_local)
        key_heads = to_heads(key_blk, heads_local)
        d_probs = jnp.einsum(
            "ihqc,ihkc->ihqk", d_attn_heads, value_heads, preferred_element_type=jnp.float32
        )
        d_scores = (soft_probs * (d_probs - delta_rows[..., None])).astype(jnp.bfloat16)
        grad_query = grad_query + jnp.einsum(
            "ihqk,ihkc->ihqc", d_scores, key_heads, preferred_element_type=jnp.float32
        )
        grid_scores = d_scores.astype(jnp.float32).reshape(
            images, heads_local, tok_ctx, key_rows, COLS
        )
        row_sums = jnp.sum(grid_scores, 4)
        row_now = lax.dynamic_slice_in_dim(grad_rows, offset // COLS, key_rows, 3)
        grad_rows = lax.dynamic_update_slice_in_dim(
            grad_rows, row_now + row_sums, offset // COLS, 3
        )
        grad_cols = grad_cols + jnp.sum(grid_scores, 3)
        key_part = scale_factor * jnp.einsum(
            "ihqk,ihqc->ikhc", d_scores, query_heads, preferred_element_type=jnp.float32
        )
        value_part = jnp.einsum(
            "ihqk,ihqc->ikhc",
            soft_probs.astype(jnp.bfloat16),
            d_attn_heads,
            preferred_element_type=jnp.float32,
        )
        emitted = (
            key_part.reshape(images, key_step, width_local),
            value_part.reshape(images, key_step, width_local),
        )
        return ((grad_query, grad_rows, grad_cols), emitted)

    back_start = (
        jnp.zeros((images, heads_local, tok_ctx, HD), jnp.float32),
        jnp.zeros((images, heads_local, tok_ctx, grid_rows), jnp.float32),
        jnp.zeros((images, heads_local, tok_ctx, COLS), jnp.float32),
    )
    (grad_query, grad_rows, grad_cols), emitted = lax.scan(back_step, back_start, key_offsets)
    key_terms = emitted[0].transpose(1, 0, 2, 3).reshape(images, tok_image, width_local)
    value_terms = emitted[1].transpose(1, 0, 2, 3).reshape(images, tok_image, width_local)
    grad_keys, grad_values = (
        lax.psum_scatter(
            key_terms.astype(jnp.bfloat16), "ctx", scatter_dimension=1, tiled=True
        ).astype(jnp.float32),
        lax.psum_scatter(
            value_terms.astype(jnp.bfloat16), "ctx", scatter_dimension=1, tiled=True
        ).astype(jnp.float32),
    )
    d_query_rel, rows_grad_part, cols_grad_part = rel_pull((grad_rows, grad_cols))
    d_query = (scale_factor * from_heads(grad_query) + d_query_rel).astype(jnp.bfloat16)
    d_keys = grad_keys.astype(jnp.bfloat16)
    d_values = grad_values.astype(jnp.bfloat16)
    d_projected = jnp.stack((d_query, d_keys, d_values), axis=2)
    qkv_grad = jnp.einsum(
        "itd,itse->sde", normed1_full, d_projected, preferred_element_type=jnp.float32
    )
    qv_bias_part = jnp.stack(
        (
            jnp.sum(d_query.astype(jnp.float32), (0, 1)),
            jnp.sum(d_values.astype(jnp.float32), (0, 1)),
        )
    )
    d_norm1_part = jnp.einsum(
        "itse,sde->itd", d_projected, qkv_full, preferred_element_type=jnp.float32
    )
    d_norm1 = lax.psum_scatter(
        d_norm1_part.astype(jnp.bfloat16), "tp", scatter_dimension=1, tiled=True
    ).astype(jnp.float32)
    unused_in, norm1_pull = jax.vjp(layer_norm, resid_in, norm1_gain, norm1_bias)
    d_in_part, gain1_part, bias1_part = norm1_pull(d_norm1)
    tokens_grad = (d_middle + d_in_part).astype(jnp.bfloat16)
    qkv_out, proj_out, fc1_out, fc2_out = (
        lax.psum_scatter(
            qkv_grad.astype(jnp.bfloat16), ("shard", "ctx"), scatter_dimension=1, tiled=True
        ).astype(jnp.float32),
        lax.psum_scatter(
            proj_grad.astype(jnp.bfloat16), ("shard", "ctx"), scatter_dimension=1, tiled=True
        ).astype(jnp.float32),
        lax.psum_scatter(
            fc1_grad.astype(jnp.bfloat16), ("shard", "ctx"), scatter_dimension=0, tiled=True
        ).astype(jnp.float32),
        lax.psum_scatter(
            fc2_grad.astype(jnp.bfloat16), ("shard", "ctx"), scatter_dimension=1, tiled=True
        ).astype(jnp.float32),
    )
    qv_placed = lax.dynamic_update_slice_in_dim(
        jnp.zeros((2, D), jnp.float32), qv_bias_part, tp_rank * width_local, 1
    )
    fc1_placed = lax.dynamic_update_slice_in_dim(
        jnp.zeros((FF,), jnp.float32), fc1_bias_part, tp_rank * ff_local, 0
    )
    (
        gain1_sum,
        bias1_sum,
        qv_sum,
        rows_sum,
        cols_sum,
        projb_sum,
        gain2_sum,
        bias2_sum,
        fc1b_sum,
        fc2b_sum,
    ) = lax.psum(
        (
            gain1_part,
            bias1_part,
            qv_placed,
            rows_grad_part,
            cols_grad_part,
            proj_bias_part,
            gain2_part,
            bias2_part,
            fc1_placed,
            fc2_bias_part,
        ),
        ("shard", "ctx", "tp"),
    )
    return (
        output,
        tokens_grad,
        gain1_sum,
        bias1_sum,
        qkv_out,
        qv_sum,
        rows_sum,
        cols_sum,
        proj_out,
        projb_sum,
        gain2_sum,
        bias2_sum,
        fc1_out,
        fc1b_sum,
        fc2_out,
        fc2b_sum,
    )


F32 = jnp.float32
BF16 = jnp.bfloat16
NT = (((1,), (1,)), ((), ()))
NN = (((1,), (0,)), ((), ()))
TN = (((0,), (0,)), ((), ()))
VMEM_GRANT = 60 * 2**20
DMA = pltpu.SemaphoreType.DMA
ANY = pl.BlockSpec(memory_space=pl.ANY)
VM = pl.BlockSpec(memory_space=pltpu.VMEM)


def mm(left, right, dims=NN):
    return lax.dot_general(left, right, dims, preferred_element_type=F32)


def lane_ids(shape):
    return lax.broadcasted_iota(jnp.int32, shape, 1)


def place():
    return lax.axis_index("shard"), lax.axis_index("ctx"), lax.axis_index("tp")


def core_mate(t):
    return t + 1 - 2 * lax.rem(t, 2)


def far_mate(t):
    return lax.rem(t + 2, 4)


def aim(src, dst, sems, k, where):
    return pltpu.make_async_remote_copy(
        src_ref=src,
        dst_ref=dst,
        send_sem=sems.at[0, k],
        recv_sem=sems.at[1, k],
        device_id=where,
        device_id_type=pl.DeviceIdType.MESH,
    )


def send(src, dst, sems, k, where):
    copy = aim(src, dst, sems, k, where)
    copy.start()
    return copy


def swap_copy(src, dst, sems):
    _, c, _ = place()
    return pltpu.make_async_remote_copy(
        src_ref=src,
        dst_ref=dst,
        send_sem=sems.at[0, 0],
        recv_sem=sems.at[1, 0],
        device_id={"ctx": 1 - c},
        device_id_type=pl.DeviceIdType.MESH,
    )


def fill_tables(tab_ref, rr_ref, rc_ref):
    tab_ref[...] = jnp.zeros_like(tab_ref)
    tab_ref[0 : rr_ref.shape[0], 0 : rr_ref.shape[1]] = rr_ref[...]
    wide = jnp.concatenate([rc_ref[...], jnp.zeros((rc_ref.shape[0], 128 - rc_ref.shape[1]), BF16)], 1)
    square = jnp.concatenate([wide, jnp.zeros((128 - rc_ref.shape[0], 128), BF16)], 0)
    tab_ref[128:256, :] = square.T


def fill_hots(hot_ref, hd, cols, rows, second):
    shift = cols.bit_length() - 1
    down = lax.broadcasted_iota(jnp.int32, hot_ref.shape, 0)
    kr = lax.shift_right_logical(down, shift)
    kw = down & (cols - 1)
    l = lane_ids(hot_ref.shape)
    if second:
        hit = (l == hd + rows - 1 - kr) | (l == 128 + cols - 1 - kw)
    else:
        hit = (l == hd + kr) | (l == hd + rows + kr) | (l == 128 + kw) | (l == 192 + kw)
    hot_ref[...] = jnp.where(hit, 1.0, 0.0).astype(BF16)


def reverser(top):
    down = lax.broadcasted_iota(jnp.int32, (128, 128), 0)
    return jnp.where(down + lane_ids((128, 128)) == top, 1.0, 0.0).astype(BF16)


def greet(shards, line=False):
    s, c, t = place()
    size = 2 * shards
    at = s * (1 - c) + (size - 1 - s) * c
    peers = [{"ctx": 1 - c}, {"tp": core_mate(t)}, {"tp": far_mate(t)}]
    for step in (1, size - 1):
        to = lax.rem(at + step, size)
        back = to // shards
        peers.append({"shard": to * (1 - back) + (size - 1 - to) * back, "ctx": back})
    if line:
        peers.append({"tp": core_mate(far_mate(t))})
        for d in range(1, shards):
            peers.append({"shard": lax.rem(s + d, shards)})
            peers.append({"shard": lax.rem(s + d, shards), "ctx": 1 - c})
    barrier = pltpu.get_barrier_semaphore()
    for peer in peers:
        pl.semaphore_signal(barrier, inc=1, device_id=peer, device_id_type=pl.DeviceIdType.MESH)
    pl.semaphore_wait(barrier, len(peers))


class Ring:
    def __init__(self, shards, block, sems):
        s, c, _ = place()
        self.shards, self.size, self.sems = shards, 2 * shards, sems
        self.at = s * (1 - c) + (self.size - 1 - s) * c
        self.half = block // 2
        self.pieces = ring_pieces(block)
        self.rows = self.half // self.pieces
        self.first, self.end = self.pieces, self.pieces * (self.size - 1)
        self.now = self.first

    def coords(self, position):
        back = position // self.shards
        return position * (1 - back) + (self.size - 1 - position) * back, back

    def peer(self, way):
        to = lax.rem(self.at + (1 if way == 0 else self.size - 1), self.size)
        shard, ctx = self.coords(to)
        return {"shard": shard, "ctx": ctx}

    def owner(self, offset):
        shard, ctx = self.coords(lax.rem(self.at + 2 * self.size + offset, self.size))
        return 2 * shard + ctx

    def split(self, event):
        if isinstance(event, int):
            return event // self.pieces, event % self.pieces
        return lax.div(event, self.pieces), lax.rem(event, self.pieces)

    def rows_of(self, way, piece):
        start = way * self.half + piece * self.rows
        return pl.ds(start if isinstance(start, int) else pl.multiple_of(start, self.rows), self.rows)

    def make(self, src, dst, way, event):
        slot = way * self.end + event
        return pltpu.make_async_remote_copy(
            src_ref=src,
            dst_ref=dst,
            send_sem=self.sems.at[0, slot],
            recv_sem=self.sems.at[1, slot],
            device_id=self.peer(way),
            device_id_type=pl.DeviceIdType.MESH,
        )

    def run(self, low, high):
        low, high = max(low, self.first), min(high, self.end)
        if low < high:
            lax.fori_loop(low, high, lambda event, _: (self.step(event), 0)[1], 0)

    def tick(self, count):
        self.run(self.now, self.now + count)
        self.now += count

    def poll(self, event):
        pl.when((event >= self.first) & (event < self.end))(lambda: self.step(event))


def ring_pieces(block):
    return 5 if block % 160 == 0 else 1


def ring_sems(shards, block):
    return DMA((2, 2 * ring_pieces(block) * (2 * shards - 1)))


class Spread(Ring):
    def __init__(self, shards, src, dst, sems, local):
        super().__init__(shards, src.shape[0], sems)
        self.src, self.dst = src, dst
        self.local = pltpu.make_async_copy(src, dst.at[self.owner(0)], local)
        self.local.start()
        for event in range(self.first):
            for way in range(2):
                self.hop(way, event, True).start()

    def hop(self, way, event, own=False):
        j, piece = self.split(event)
        rows = self.rows_of(way, piece)
        there = self.dst.at[self.owner(-j if way == 0 else j), rows]
        return self.make(self.src.at[rows] if own else there, there, way, event)

    def step(self, event):
        for way in range(2):
            self.hop(way, event - self.pieces).wait_recv()
            self.hop(way, event).start()

    def finish(self):
        self.local.wait()
        for way in range(2):
            for event in range(self.end - self.pieces, self.end):
                self.hop(way, event).wait_recv()

        def sent(event, _):
            for way in range(2):
                self.hop(way, event).wait_send()
            return 0

        lax.fori_loop(0, self.end, sent, 0)

    @staticmethod
    def scratch(shards, block):
        return [ring_sems(shards, block[0]), DMA]


class Collect(Ring):
    def __init__(self, shards, src, held, sems):
        super().__init__(shards, src.shape[0] // (2 * shards), sems)
        self.src, self.held, self.block = src, held, src.shape[0] // (2 * shards)

    def begin(self):
        for event in range(self.first):
            for way in range(2):
                self.hop(way, event, True).start()

    def pair_rows(self, n, j):
        offset = (n + 1) * (2 * j - 1)
        last = (2 * n + j + 1) // self.size
        return pl.ds(pl.multiple_of(self.owner(offset * (1 - last)) * self.block, self.rows), self.block)

    def own(self, way, j, piece):
        ahead = self.size - 1 - j
        start = self.owner(ahead if way == 0 else -ahead) * self.block + way * self.half + piece * self.rows
        return pl.ds(pl.multiple_of(start, self.rows), self.rows)

    def hop(self, way, event, own=False):
        j, piece = self.split(event)
        rows = self.rows_of(0, piece)
        there = self.held.at[way, j, rows]
        here = self.src.at[self.own(way, j, piece)] if own else self.held.at[way, j - 1, rows]
        return self.make(here, there, way, event)

    def arrived(self, way, event):
        j, piece = self.split(event)
        there = self.held.at[way, j, self.rows_of(0, piece)]
        self.make(there, there, way, event).wait_recv()

    def step(self, event):
        j, piece = self.split(event)
        rows = self.rows_of(0, piece)
        for way in range(2):
            self.arrived(way, event - self.pieces)
            both = self.held[way, j - 1, rows].astype(F32) + self.src[self.own(way, j, piece)].astype(F32)
            self.held[way, j - 1, rows] = both.astype(BF16)
            self.hop(way, event).start()

    def finish(self, out):
        for piece in range(self.pieces):
            for way in range(2):
                self.arrived(way, self.end - self.pieces + piece)
                last = self.held[way, self.size - 2, self.rows_of(0, piece)].astype(F32)
                own = self.src[self.own(way, self.size - 1, piece)].astype(F32)
                out[self.rows_of(way, piece)] = last + own

        def sent(event, _):
            for way in range(2):
                j, piece = self.split(event)
                there = self.held.at[way, j, self.rows_of(0, piece)]
                self.make(there, there, way, event).wait_send()
            return 0

        lax.fori_loop(0, self.end, sent, 0)

    @staticmethod
    def scratch(shards, block):
        return [pltpu.VMEM((2, 2 * shards - 1, block[0] // 2, block[1]), BF16), ring_sems(shards, block[0])]


class Share:
    def __init__(self, full, sems):
        self.full, self.sems = full, sems

    def copies(self, k, p, src=None):
        _, _, t = place()
        block, passed = self.full.at[p, t], self.full.at[p, far_mate(t)]
        src = block if src is None else src
        return (
            partial(aim, src, block, self.sems, 3 * k, {"tp": far_mate(t)}),
            partial(aim, src, block, self.sems, 3 * k + 1, {"tp": core_mate(t)}),
            partial(aim, passed, passed, self.sems, 3 * k + 2, {"tp": core_mate(t)}),
        )

    def push(self, k, p, src=None):
        for copy in self.copies(k, p, src)[:2]:
            copy().start()

    def forward(self, k, p):
        far, _, third = self.copies(k, p)
        far().wait_recv()
        third().start()

    def finish(self, k, p):
        far, core, third = self.copies(k, p)
        far().wait_send()
        core().wait()
        third().wait()


class Gather2:
    def __init__(self, part, mate, far, out, sems):
        self.part, self.mate, self.far, self.out, self.sems = part, mate, far, out, sems

    def copies(self, p):
        _, _, t = place()
        m = core_mate(t)
        return (
            partial(aim, self.part.at[p, far_mate(m)], self.mate.at[p, 1], self.sems, 3 * p, {"tp": m}),
            partial(aim, self.part.at[p, m], self.mate.at[p, 0], self.sems, 3 * p + 1, {"tp": m}),
            partial(aim, self.out.at[p], self.far.at[p], self.sems, 3 * p + 2, {"tp": far_mate(t)}),
        )

    def push(self, p):
        for copy in self.copies(p)[:2]:
            copy().start()

    def forward(self, p):
        _, _, t = place()
        passing, _, onward = self.copies(p)
        passing().wait_recv()
        both = self.part[p, far_mate(t)].astype(F32) + self.mate[p, 1].astype(F32)
        self.out[p] = both.astype(BF16)
        onward().start()

    def result(self, p):
        _, _, t = place()
        _, own, onward = self.copies(p)
        own().wait_recv()
        onward().wait_recv()
        return self.part[p, t].astype(F32) + self.mate[p, 0].astype(F32) + self.far[p].astype(F32)

    def finish(self, p):
        for copy in self.copies(p):
            copy().wait_send()

    @staticmethod
    def scratch(block):
        return [
            pltpu.VMEM((2, 2) + block, BF16),
            pltpu.VMEM((2,) + block, BF16),
            pltpu.VMEM((2,) + block, BF16),
            DMA((2, 6)),
        ]


def ln_stats(values):
    average = jnp.mean(values, -1, keepdims=True)
    centred = values - average
    inverse = lax.rsqrt(jnp.mean(centred * centred, -1, keepdims=True) + EPSILON)
    return centred * inverse, inverse


def ln_back(unit, inverse, gain, grad):
    scaled = grad * gain
    first = jnp.mean(scaled, -1, keepdims=True)
    second = jnp.mean(scaled * unit, -1, keepdims=True)
    return inverse * (scaled - first - unit * second)


class Stream:
    def __init__(self, loads, stores, sems):
        self.loads, self.stores, self.sems, self.flying = loads, stores, sems, []

    def need(self, *operands):
        for i in operands:
            if i in self.loads:
                self.loads.pop(i).wait()

    def put(self, j, half=None):
        src, dst, q = self.stores[j]
        if half is not None:
            size = src.shape[0] // 2
            src, dst = src.at[half * size : (half + 1) * size], dst.at[half * size : (half + 1) * size]
        copy = pltpu.make_async_copy(src, dst, self.sems.at[2 * q + (half or 0)])
        copy.start()
        self.flying.append((j, copy))

    def close(self):
        self.need(*list(self.loads))
        done = [j for j, _ in self.flying]
        for j in self.stores:
            if j not in done:
                self.put(j)
        for _, copy in self.flying:
            copy.wait()


def comm_call(kernel, name, ident, args, outs, scratch, hbm_in=(), hbm_out=(), late=(), early=()):
    count, results, own = len(args), len(outs), len(scratch)

    def body(*refs):
        ins, out = list(refs[:count]), list(refs[count : count + results])
        inner = refs[count + results : count + results + own]
        extra = refs[count + results + own :]
        buffers, load_sems, store_sems = extra[:-2], extra[-2], extra[-1]
        loads, stores = {}, {}
        for q, i in enumerate(late):
            loads[i] = pltpu.make_async_copy(ins[i], buffers[q], load_sems.at[q])
            loads[i].start()
            ins[i] = buffers[q]
        for q, j in enumerate(early):
            held = buffers[len(late) + q]
            stores[j] = (held, out[j], q)
            out[j] = held
        stream = Stream(loads, stores, store_sems)
        kernel(stream, *ins, *out, *inner)
        stream.close()

    return pl.pallas_call(
        body,
        out_shape=tuple(outs),
        in_specs=[ANY if i in hbm_in or i in late else VM for i in range(count)],
        out_specs=tuple(ANY if j in hbm_out or j in early else VM for j in range(results)),
        scratch_shapes=list(scratch)
        + [pltpu.VMEM(args[i].shape, args[i].dtype) for i in late]
        + [pltpu.VMEM(outs[j].shape, outs[j].dtype) for j in early]
        + [DMA((max(len(late), 1),)), DMA((max(2 * len(early), 1),))],
        compiler_params=pltpu.CompilerParams(
            vmem_limit_bytes=VMEM_GRANT, collective_id=ident, has_side_effects=True
        ),
        name=name,
    )(*args)


def turned(out_ref, full_ref, p):
    count, length = full_ref.shape[1:3]

    def one(i, _):
        start = pl.multiple_of((p * count + i) * length, 128)
        out_ref[:, pl.ds(start, length)] = full_ref[p, i].T
        return 0

    lax.fori_loop(0, count, one, 0)


def front_kernel(
    shards, io, tok_ref, qkvw_ref, pw_ref, vec_ref, x_ref, a_ref, wf_ref, at_ref,
    w1_ref, swap_sems, share_sems, w_sems, w_local,
):
    s, c, t = place()
    wide = qkvw_ref.shape[2]
    for j in range(3):
        w1_ref[:, j * wide : (j + 1) * wide] = qkvw_ref[j]
    w1_ref[:, 3 * wide : 4 * wide] = pw_ref[...]
    greet(shards)
    swap = send(tok_ref.at[1 - c], x_ref.at[c], swap_sems, 0, {"ctx": 1 - c})
    spread = Spread(shards, w1_ref, wf_ref, w_sems, w_local)
    share = Share(a_ref, share_sems)

    def norm(block):
        unit, _ = ln_stats(block.astype(F32))
        return (unit * vec_ref[0:1, :] + vec_ref[1:2, :]).astype(BF16)

    own = tok_ref[c]
    x_ref[c] = own
    a_ref[c, t] = norm(own)
    share.push(0, c)
    swap.wait()
    a_ref[1 - c, t] = norm(x_ref[1 - c])
    share.push(1, 1 - c)
    share.forward(0, c)
    spread.tick(9)
    share.forward(1, 1 - c)
    spread.tick(6)
    share.finish(0, c)
    share.finish(1, 1 - c)
    io.put(0)
    io.put(1)
    turned(at_ref, a_ref, 0)
    spread.tick(2)
    spread.tick(4)
    turned(at_ref, a_ref, 1)
    io.put(3)
    spread.tick(2)
    spread.tick(spread.end)
    spread.finish()


def fwd_kernel(
    shards, heads, hd, cols, rows, qb, io,
    a1_ref, w1_ref, vec_ref, rr_ref, rc_ref, cot_ref, w_ref,
    vh_ref, oh_ref, ob_ref, lse_ref, qa_ref, ka_ref, g_ref, cf_ref, wf_ref, pp_ref,
    qh_ref, vt_ref, rt_ref, tab_ref, hot_ref, swap_sems, share_sems, w_sems, w_local,
):
    _, me, t = place()
    tok, width = ob_ref.shape
    wide = 3 * width
    blocks = tok // qb
    fill_tables(tab_ref, rr_ref, rc_ref)
    fill_hots(hot_ref, hd, cols, rows, False)
    rt_ref[0:128, :] = mm(reverser(2 * rows - 2), tab_ref[0:128, :]).astype(BF16)
    rt_ref[128:256, :] = mm(reverser(2 * cols - 2), tab_ref[128:256, :]).astype(BF16)
    greet(shards)
    swap = swap_copy(cot_ref.at[1 - me], g_ref.at[me], swap_sems)
    swap.start()
    spread = Spread(shards, w_ref, wf_ref, w_sems, w_local)
    share = Share(cf_ref, share_sems)
    own = cot_ref[me]
    g_ref[me] = own
    cf_ref[me, t] = own
    share.push(0, me, cot_ref.at[me])

    io.need(0, 1)

    def project(i, _):
        at = pl.ds(pl.multiple_of(i * qb, qb), qb)
        tile = (mm(a1_ref[at, :], w1_ref[:, 0:wide]) + vec_ref[7:8, 0:wide]).astype(BF16)
        pad = jnp.zeros((qb, 128 - hd), BF16)
        front = lane_ids((qb, 128)) < hd
        for h in range(heads):
            part = [tile[:, (j * heads + h) * hd : (j * heads + h + 1) * hd] for j in range(3)]
            part = [jnp.concatenate([x, pad], 1) for x in part]
            qh_ref[h, at, :] = part[0]
            ka_ref[h, at, 0:128] = jnp.where(front, part[1], hot_ref[at, 0:128])
            ka_ref[h, at, 128:256] = hot_ref[at, 128:256]
            vh_ref[h, at, :] = part[2]
        return 0

    lax.fori_loop(0, blocks, project, 0)
    io.put(0)
    io.put(5)
    swap.wait()
    cf_ref[1 - me, t] = g_ref[1 - me]
    share.push(1, 1 - me, g_ref.at[1 - me])
    c = hd**-0.5 * math.log2(math.e)
    up = hd**0.5

    def head(h, _):
        vt_ref[...] = vh_ref[h].T
        terms = mm(qh_ref[h], rt_ref[...], NT) * up
        ln = lane_ids((cols, 128))
        for r in range(rows):
            rs = slice(r * cols, (r + 1) * cols)
            tr = pltpu.roll(terms[rs, 0:128], (65 + r) % 128, 1)
            tc = pltpu.roll(terms[rs, 128:256], 65, 1, stride=1, stride_axis=0)
            rh = tr.astype(BF16).astype(F32)
            rl = pltpu.roll(tr - rh, rows, 1)
            ch = tc.astype(BF16).astype(F32)
            cl = pltpu.roll(tc - ch, 64, 1)
            low = jnp.where(ln < hd + 2 * rows, rl, jnp.zeros_like(tr))
            left = jnp.where(ln < hd, qh_ref[h, rs, :].astype(F32), jnp.where(ln < hd + rows, rh, low))
            qa_ref[h, rs, 0:128] = left.astype(BF16)
            qa_ref[h, rs, 128:256] = jnp.where(ln < 64, ch, cl).astype(BF16)

        def blk(i, _):
            at = pl.ds(pl.multiple_of(i * qb, qb), qb)
            s = mm(ka_ref[h], qa_ref[h, at, :], NT)
            m = jnp.max(s, 0, keepdims=True)
            p = jnp.exp2((s - m) * c)
            l = jnp.sum(p, 0, keepdims=True)
            lse_ref[h, :, at] = m * c + jnp.log2(l)
            oh_ref[h, at, :] = (mm(vt_ref[...], p.astype(BF16)) / l).T
            turn = h * blocks + i
            event = spread.first + turn + (turn + 1) // 2
            spread.poll(event)
            pl.when(turn % 2 == 0)(lambda: spread.poll(event + 1))
            return 0

        lax.fori_loop(0, blocks, blk, 0)
        pl.when(h == 0)(lambda: share.forward(0, me))
        pl.when(h == min(1, heads - 1))(lambda: share.forward(1, 1 - me))
        return 0

    lax.fori_loop(0, heads, head, 0)
    io.put(1)
    io.put(4)
    for h in range(heads):
        ob_ref[:, h * hd : (h + 1) * hd] = oh_ref[h, :, 0:hd].astype(BF16)

    io.put(2)
    done = spread.first + heads * blocks * 3 // 2

    def out_rows(i, _):
        at = pl.ds(pl.multiple_of(i * qb, qb), qb)
        pp_ref[at, :] = mm(ob_ref[at, :], w1_ref[:, wide:], NT).astype(BF16)
        for k in range(2):
            spread.poll(done + 2 * i + k)
        return 0

    lax.fori_loop(0, blocks, out_rows, 0)
    io.put(9)
    spread.run(done + 2 * blocks, spread.end)
    share.finish(0, me)
    share.finish(1, 1 - me)
    io.put(7)
    spread.finish()


def mid_kernel(
    shards, io, part_ref, x_ref, vec_ref, w_ref, f1_ref, cf_ref,
    mid_ref, a_ref, wf_ref, act_ref, slope_ref, ct_ref,
    mate, far, outb, sum_sems, share_sems, w_sems, w_local,
):
    _, _, t = place()
    greet(shards)
    gather = Gather2(part_ref, mate, far, outb, sum_sems)
    io.need(0)
    gather.push(0)
    gather.push(1)
    spread = Spread(shards, w_ref, wf_ref, w_sems, w_local)
    share = Share(a_ref, share_sems)
    gather.forward(0)
    gather.forward(1)
    io.need(5, 1)
    turned(ct_ref, cf_ref, 0)
    spread.tick(8)
    for p in range(2):
        mid = x_ref[p].astype(F32) + gather.result(p) + vec_ref[2:3, :]
        mid_ref[p] = mid
        unit, _ = ln_stats(mid)
        a_ref[p, t] = (unit * vec_ref[3:4, :] + vec_ref[4:5, :]).astype(BF16)
        share.push(p, p)
        if p == 1:
            turned(ct_ref, cf_ref, 1)
            io.put(0)
            io.put(5)
        spread.tick(7)
    share.forward(0, 0)
    half = a_ref.shape[1] * a_ref.shape[2]

    def hidden(p):
        def one(i, _):
            rows = a_ref[p, pl.ds(2 * i, 2)].reshape(-1, a_ref.shape[3])
            pre = mm(rows, f1_ref[...]) + vec_ref[6:7, :]
            cdf = 0.5 * (1.0 + lax.erf(pre * (2.0**-0.5)))
            bell = jnp.exp(-0.5 * pre * pre) * ((2.0 * math.pi) ** -0.5)
            at = pl.ds(pl.multiple_of(p * half + i * rows.shape[0], 128), rows.shape[0])
            act_ref[at, :] = (pre * cdf).astype(BF16)
            slope_ref[at, :] = cdf + pre * bell
            for k in range(2):
                spread.poll(base + 2 * i + k)
            return 0

        base = spread.now
        lax.fori_loop(0, a_ref.shape[1] // 2, one, 0)
        spread.now += a_ref.shape[1]

    share.finish(0, 0)
    io.need(4)
    hidden(0)
    io.put(3, 0)
    io.put(4, 0)
    spread.tick(spread.end)
    share.forward(1, 1)
    share.finish(1, 1)
    io.put(1)
    hidden(1)
    io.put(4, 1)
    io.put(3, 1)
    for p in range(2):
        gather.finish(p)
    spread.finish()


def turn_kernel(
    shards, io, ct_ref, act_ref, slope_ref, cot_ref, f2_ref, f1_ref, a2_ref, mid_ref, g_ref, vec_ref, w1_ref,
    dm_ref, dbt_ref, wg_ref, sums_ref, f1g_ref, mlp_ref, do_ref,
    db_ref, w2g_ref, part_ref, dp_ref, mate, far, outb, sum_sems, share_sems, w_held, w_sems,
):
    _, _, t = place()
    greet(shards)
    collect = Collect(shards, w2g_ref, w_held, w_sems)
    gather = Gather2(part_ref, mate, far, outb, sum_sems)
    share = Share(db_ref, share_sems)
    tile = 2 * db_ref.shape[2]
    halves = db_ref.shape[1] // 2
    sums_ref[...] = jnp.zeros_like(sums_ref)
    step = collect.pieces

    io.need(0, 1)

    def first(j, _):
        at = collect.pair_rows(0, j)
        w2g_ref[at, :] = mm(ct_ref[at, :], act_ref[...]).astype(BF16)
        return 0

    lax.fori_loop(0, 2, first, 0)
    collect.begin()
    io.need(2, 3, 4, 5)

    def back(n, _):
        def block(j, _):
            at = collect.pair_rows(n, j)
            w2g_ref[at, :] = mm(ct_ref[at, :], act_ref[...]).astype(BF16)
            return 0

        def blocks():
            lax.fori_loop(0, 2, block, 0)

        pl.when((n > 0) & (n < halves))(lambda: blocks())
        p, i = n // halves, n % halves
        at = pl.ds(pl.multiple_of(n * tile, tile), tile)
        d_pre = (mm(cot_ref[at, :], f2_ref[...]) * slope_ref[at, :]).astype(BF16)
        dp_ref[at, :] = d_pre
        sums_ref[4:5, :] += jnp.sum(d_pre.astype(F32), 0, keepdims=True)
        for k in range(2):
            collect.poll(step * n - 2 + k)
        pl.when(n == halves)(lambda: gather.forward(0))
        d_a2 = mm(d_pre, f1_ref[...], NT).astype(BF16)
        part_ref[p, pl.ds(2 * i, 2)] = d_a2.reshape(2, tile // 2, -1)
        pl.when(n == halves - 1)(lambda: gather.push(0))
        pl.when(n == 2 * halves - 1)(lambda: gather.push(1))
        pl.when(n >= halves)(lambda: blocks())
        for k in range(2, step):
            collect.poll(step * n - 2 + k)
        return 0

    lax.fori_loop(0, 2 * halves, back, 0)
    base = 2 * halves * step - 2

    def hidden_grad(i, _):
        at = pl.ds(pl.multiple_of(i * 256, 256), 256)
        f1g_ref[at, :] = mm(a2_ref[:, at], dp_ref[...], TN).astype(BF16)
        collect.poll(base + i)
        pl.when(i == 0)(lambda: gather.forward(1))

        @pl.when((i == 1) | (i == count - 1))
        def _():
            p = lax.div(i, count - 1)
            unit, inverse = ln_stats(mid_ref[p])
            g = g_ref[p].astype(F32)
            da = gather.result(p)
            dm = g + ln_back(unit, inverse, vec_ref[3:4, :], da)
            dm_ref[p] = dm
            low_dm = dm.astype(BF16)
            db_ref[p, t] = low_dm
            share.push(p, p)
            for k, term in enumerate((da * unit, da, low_dm.astype(F32), g)):
                sums_ref[k : k + 1, :] += jnp.sum(term, 0, keepdims=True)

        return 0

    count = f1g_ref.shape[0] // 256
    io.need(6, 7, 8)
    lax.fori_loop(0, count, hidden_grad, 0)
    io.put(0)
    io.put(4)
    base2 = base + count

    def mlp(n, _):
        at = pl.ds(pl.multiple_of(n * tile, tile), tile)
        mlp_ref[at, :] = mm(act_ref[at, :], f2_ref[...], NT).astype(BF16)
        for k in range(2):
            collect.poll(base2 + 2 * n + k)
        pl.when(n == 2 * halves - 1)(lambda: share.forward(0, 0))
        return 0

    lax.fori_loop(0, 2 * halves, mlp, 0)
    io.put(5)
    collect.run(base2 + 4 * halves, collect.end)
    share.forward(1, 1)
    wide = do_ref.shape[1]
    io.need(10)

    def d_o(n, _):
        p, i = n // halves, n % halves
        pl.when(i == 0)(lambda: share.finish(p, p))
        rows = db_ref[p, pl.ds(2 * i, 2)].reshape(tile, -1)
        at = pl.ds(pl.multiple_of(n * tile, tile), tile)
        do_ref[at, :] = mm(rows, w1_ref[:, 3 * wide :]).astype(BF16)
        dbt_ref[:, at] = rows.T
        return 0

    lax.fori_loop(0, 2 * halves, d_o, 0)
    io.put(1)
    io.put(6)
    for p in range(2):
        gather.finish(p)
    collect.finish(wg_ref)


def bwd_kernel(
    shards, heads, hd, cols, rows, qb, io,
    qa_ref, ka_ref, vh_ref, do_ref, oh_ref, lse_ref, rr_ref, rc_ref, w_ref, part_ref, mid_ref, vec_ref,
    dqkv_ref, rg_ref, wg_ref, qs_ref, out_ref,
    doh_ref, dh_ref, kt_ref, acc_k, acc_v, del_ref, tab_ref, hot_ref, res_ref,
    mate, far, outb, sum_sems, swap_sems, w_held, w_sems,
):
    fill_tables(tab_ref, rr_ref, rc_ref)
    fill_hots(hot_ref, hd, cols, rows, True)
    _, me, _ = place()
    greet(shards)
    gather = Gather2(part_ref, mate, far, outb, sum_sems)
    io.need(9)
    gather.push(0)
    gather.push(1)
    swap = swap_copy(res_ref.at[1 - me], out_ref.at[me], swap_sems)
    collect = Collect(shards, w_ref, w_held, w_sems)
    io.need(8)
    collect.begin()
    io.need(3)
    tok, wide = dqkv_ref.shape
    blocks = tok // qb
    for h in range(heads):
        pad = jnp.zeros((tok, 128 - hd), BF16)
        doh_ref[h] = jnp.concatenate([do_ref[:, h * hd : (h + 1) * hd], pad], 1)
    gather.forward(0)
    gather.forward(1)
    scale = hd**-0.5
    c = scale * math.log2(math.e)
    rg_ref[...] = jnp.zeros_like(rg_ref)

    io.need(0, 1, 2, 4, 10)

    def head(h, _):
        kt_ref[0:128, :] = jnp.where(lane_ids((tok, 128)) < hd, ka_ref[h, :, 0:128], hot_ref[:, 0:128]).T
        kt_ref[128:256, :] = hot_ref[:, 128:256].T
        del_ref[...] = lax.dot_general(
            jnp.ones((8, 128), F32), doh_ref[h].astype(F32) * oh_ref[h], NT,
            preferred_element_type=F32, precision=PRECISE,
        )
        acc_k[...] = jnp.zeros_like(acc_k)
        acc_v[...] = jnp.zeros_like(acc_v)

        def blk(i, _):
            at = pl.ds(pl.multiple_of(i * qb, qb), qb)
            qblk = qa_ref[h, at, :]
            dob = doh_ref[h, at, :]
            s = mm(ka_ref[h], qblk, NT)
            p = jnp.exp2(s * c - lse_ref[h, :, at])
            dp = mm(vh_ref[h], dob, NT)
            ds = (p * (dp - del_ref[0:1, at])).astype(BF16)
            acc_v[...] += mm(p.astype(BF16), dob)
            acc_k[...] += mm(ds, qblk[:, 0:128])
            dqa = mm(kt_ref[...], ds).T
            ln = lane_ids((cols, 128))
            parts = []
            for j in range(qb // cols):
                r = i * (qb // cols) + j
                js = slice(j * cols, (j + 1) * cols)
                dr = dqa[js, 0:128]
                dr = jnp.where((ln >= hd) & (ln < hd + rows), dr, 0.0)
                dr = pltpu.roll(dr, lax.rem(48 + r, 128), 1)
                dc = pltpu.roll(dqa[js, 128:256], 0, 1, stride=1, stride_axis=0)
                parts.append(jnp.concatenate([dr, dc], 1))
            d = jnp.concatenate(parts, 0).astype(BF16)
            rel = mm(d, tab_ref[...])
            rg_ref[...] += mm(d, qblk[:, 0:128], TN)
            dh_ref[h, at, :] = (scale * dqa[:, 0:128] + rel).astype(BF16)
            for k in range(2):
                collect.poll(collect.first + 2 * (h * blocks + i) + k)
            return 0

        lax.fori_loop(0, blocks, blk, 0)
        dh_ref[heads + h] = (scale * acc_k[...]).astype(BF16)
        dh_ref[2 * heads + h] = acc_v[...].astype(BF16)

        @pl.when(h == min(2, heads - 1))
        def _():
            for p in range(2):
                total = mid_ref[p] + gather.result(p) + vec_ref[5:6, :]
                res_ref[p] = total.astype(BF16)

        return 0

    lax.fori_loop(0, heads, head, 0)
    swap.start()
    out_ref[me] = res_ref[me]
    for j in range(3 * heads):
        dqkv_ref[:, j * hd : (j + 1) * hd] = dh_ref[j, :, 0:hd]
    io.put(0)
    collect.run(collect.first + 2 * heads * blocks, collect.end)
    qs_ref[...] = mm(jnp.ones((8, tok), BF16), dqkv_ref[...])
    for p in range(2):
        gather.finish(p)
    collect.finish(wg_ref)
    swap.wait()


def end_kernel(
    shards, io, x_ref, dm_ref, vec_ref, at_ref, dqkv_ref, dbt_ref, ob_ref, sums_ref, w1_ref, rg_ref, qs_ref,
    grad_ref, qg_ref, pg_ref, total_ref, late_ref,
    w1g_ref, wg_ref, part_ref, gres_ref, mate, far, outb, sum_sems, swap_sems,
    held, got, line, small_sems, near, wide_all, late_sems, w_held, w_sems,
):
    s, me, t = place()
    half = held.shape[2] // 2
    held[0] = jnp.zeros_like(held[0])
    held[0, :, 0:128] = rg_ref[0:32, :]
    for k in range(4):
        held[0, :, 128 * (k + 1) : 128 * (k + 2)] = rg_ref[128 + 32 * k : 160 + 32 * k, :]
    for k in range(4):
        for u in range(2):
            held[0, 2 * k + u : 2 * k + u + 1, half:] = sums_ref[k : k + 1, u * half : (u + 1) * half]
    for u in range(2):
        held[0, pl.ds(8 + 2 * t + u, 1), half:] = sums_ref[4:5, u * half : (u + 1) * half]
    span = dqkv_ref.shape[1] // 3
    pair = jnp.concatenate([qs_ref[0:1, 0:span], qs_ref[0:1, 2 * span :]], 1)
    held[0, pl.ds(16 + t, 1), half:] = pair
    mine = pl.ds(pl.multiple_of(8 * t, 8), 8)
    mates = ({"tp": core_mate(t)}, {"tp": far_mate(t)}, {"tp": core_mate(far_mate(t))})

    def whole(k):
        return aim(held.at[k], got.at[k], small_sems, k, mates[k])

    def cross():
        return aim(held.at[2, mine], got.at[2, mine], small_sems, 2, {"ctx": 1 - me})

    def along(d):
        return aim(held.at[3, mine], line.at[s], small_sems, 2 + d, {"shard": lax.rem(s + d, shards)})

    def spread_sum(k):
        return aim(total_ref.at[mine], total_ref.at[mine], small_sems, 2 + shards + k, mates[k])

    def close_by(k):
        return aim(near.at[t], near.at[t], late_sems, k, mates[k])

    def far_off(d, flip):
        there = {"shard": lax.rem(s + d, shards), "ctx": 1 - me if flip else me}
        own = wide_all.at[2 * s + me]
        return aim(own, own, late_sems, 3 + 2 * d + flip, there)

    others = [(d, flip) for d in range(shards) for flip in range(2) if d + flip > 0]
    greet(shards, True)
    whole(0).start()
    gather = Gather2(part_ref, mate, far, outb, sum_sems)
    collect = Collect(shards, w1g_ref, w_held, w_sems)
    wide = dqkv_ref.shape[1]
    tile = 2 * part_ref.shape[2]
    halves = part_ref.shape[1] // 2
    step = collect.pieces

    io.need(4, 8, 3, 5, 6)

    def back(n, _):
        def block(j, _):
            at = collect.pair_rows(n, j)
            w1g_ref[at, 0:wide] = mm(at_ref[at, :], dqkv_ref[...]).astype(BF16)
            w1g_ref[at, wide:] = mm(dbt_ref[at, :], ob_ref[...]).astype(BF16)
            return 0

        lax.fori_loop(0, 2, block, 0)
        pl.when(n == 0)(collect.begin)
        for k in range(2):
            collect.poll(step * n + k)
        pl.when(n == 2)(lambda: gather.forward(1))

        def rows_of(i, _):
            rows = pl.ds(pl.multiple_of((n * halves + i) * tile, tile), tile)
            d_a1 = mm(dqkv_ref[rows, :], w1_ref[:, 0:wide], NT).astype(BF16)
            part_ref[n, pl.ds(2 * i, 2)] = d_a1.reshape(2, tile // 2, -1)
            return 0

        @pl.when(n < 2)
        def _():
            lax.fori_loop(0, halves, rows_of, 0)
            gather.push(n)

        for k in range(2, step):
            collect.poll(step * n + k)
        pl.when(n == 1)(lambda: gather.forward(0))

        @pl.when(n == 0)
        def _():
            whole(0).wait_recv()
            held[1] = held[0] + got[0]
            whole(1).start()

        @pl.when(n == 1)
        def _():
            whole(1).wait_recv()
            held[2] = held[1] + got[1]
            cross().start()

        @pl.when(n == 2)
        def _():
            cross().wait_recv()
            held[3, mine] = held[2, mine] + got[2, mine]
            line[s] = held[3, mine]
            for d in range(1, shards):
                along(d).start()

        return 0

    lax.fori_loop(0, 2 * halves, back, 0)
    collect.now = step * 2 * halves
    io.need(0, 1)
    first = jnp.zeros((1, x_ref.shape[2]), F32)
    second = jnp.zeros((1, x_ref.shape[2]), F32)
    for p in range(2):
        unit, inverse = ln_stats(x_ref[p].astype(F32))
        collect.tick(1)
        da = gather.result(p)
        gres_ref[p] = (dm_ref[p] + ln_back(unit, inverse, vec_ref[0:1, :], da)).astype(BF16)
        first = first + jnp.sum(da * unit, 0, keepdims=True)
        second = second + jnp.sum(da, 0, keepdims=True)
        collect.tick(1)
    for k in range(4):
        near[t, k : k + 1, :] = first[:, k * span : (k + 1) * span]
        near[t, 4 + k : 5 + k, :] = second[:, k * span : (k + 1) * span]
    for k in range(3):
        close_by(k).start()
    grad_ref[me] = gres_ref[me]
    swap = swap_copy(gres_ref.at[1 - me], grad_ref.at[me], swap_sems)
    for d in range(1, shards):
        along(d).wait_recv()
    acc = line[0]
    for k in range(1, shards):
        acc = acc + line[k]
    total_ref[mine] = acc
    for k in range(3):
        spread_sum(k).start()
    collect.tick(2)
    for k in range(3):
        close_by(k).wait_recv()
    wide_all[2 * s + me] = near[0] + near[1] + near[2] + near[3]
    for d, flip in others:
        far_off(d, flip).start()
    swap.start()
    collect.tick(collect.end)
    collect.finish(wg_ref)
    part = wide // 3
    for j in range(3):
        qg_ref[j] = wg_ref[:, j * part : (j + 1) * part]
    pg_ref[...] = wg_ref[:, wide:]
    for d, flip in others:
        far_off(d, flip).wait()
    acc = wide_all[0]
    for k in range(1, 2 * shards):
        acc = acc + wide_all[k]
    late_ref[...] = acc
    for k in range(3):
        spread_sum(k).wait()
        close_by(k).wait_send()
    for k in range(2):
        whole(k).wait_send()
    cross().wait_send()
    for d in range(1, shards):
        along(d).wait_send()
    for p in range(2):
        gather.finish(p)
    swap.wait()


def settle_kernel(
    total_ref, late_ref, out_ref, grad_ref, qg_ref, pg_ref, f1_ref, f2_ref,
    out_to, grad_to, qg_to, pg_to, f1_to, f2_to,
    gain1_to, bias1_to, qv_to, rr_to, rc_to, gain2_to, bias2_to, projb_to, fc2b_to, fc1b_to,
):
    for here, there in (
        (out_ref, out_to), (grad_ref, grad_to), (qg_ref, qg_to), (pg_ref, pg_to), (f1_ref, f1_to), (f2_ref, f2_to)
    ):
        there[...] = here[...]
    half = total_ref.shape[1] // 2
    span = late_ref.shape[1]

    def side(parts):
        return jnp.concatenate(parts, 1)

    gain1_to[...] = side([late_ref[k : k + 1, :] for k in range(4)])[0, :]
    bias1_to[...] = side([late_ref[4 + k : 5 + k, :] for k in range(4)])[0, :]
    for u in range(2):
        at = slice(half + u * span, half + (u + 1) * span)
        qv_to[u : u + 1, :] = side([total_ref[16 + k : 17 + k, at] for k in range(4)])
    rr_to[...] = total_ref[0 : rr_to.shape[0], 0 : rr_to.shape[1]]
    square = jnp.concatenate([total_ref[:, 128 * (k + 1) : 128 * (k + 2)] for k in range(4)], 0).T
    rc_to[...] = square[0 : rc_to.shape[0], 0 : rc_to.shape[1]]
    for k, there in enumerate((gain2_to, bias2_to, projb_to, fc2b_to)):
        there[...] = side([total_ref[2 * k + u : 2 * k + u + 1, half:] for u in range(2)])[0, :]
    fc1b_to[...] = side([total_ref[8 + k : 9 + k, half:] for k in range(8)])[0, :]


def on_device_images(
    tokens, norm1_gain, norm1_bias, qkv_weight, qv_bias, rel_rows, rel_cols, proj_weight, proj_bias,
    norm2_gain, norm2_bias, fc1_weight, fc1_bias, fc2_weight, fc2_bias, cotangent,
):
    S = jax.ShapeDtypeStruct
    shards = lax.axis_size("shard")
    tp_count = lax.axis_size("tp")
    tp_rank = lax.axis_index("tp")
    heads = H // tp_count
    width = heads * HD
    ff = FF // tp_count
    rows = (rel_rows.shape[0] + 1) // 2
    tok = rows * COLS
    own = tokens.shape
    piece = own[1:]
    full = (2, tp_count) + piece
    block = fc1_weight.shape
    blocks = (2 * shards,) + block
    qkv_cols = 3 * width
    fc2_t = fc2_weight.T
    qv_local = lax.dynamic_slice_in_dim(qv_bias, tp_rank * width, width, 1)
    qkv_bias = jnp.concatenate([qv_local[0], jnp.zeros((width,), F32), qv_local[1]])
    fc1_local = lax.dynamic_slice_in_dim(fc1_bias, tp_rank * ff, ff, 0)
    vec = jnp.concatenate(
        [
            norm1_gain, norm1_bias, proj_bias, norm2_gain, norm2_bias, fc2_bias, fc1_local,
            qkv_bias, jnp.zeros((D - qkv_cols,), F32),
        ]
    ).reshape(8, D)
    spread = Spread.scratch(shards, block)
    collect = Collect.scratch(shards, block)
    gather = Gather2.scratch(piece)
    swap = [DMA((2, 1))]
    share = [DMA((2, 6))]

    x, a1, w1_full, a1_turned = comm_call(
        partial(front_kernel, shards), "front", 0,
        (tokens, qkv_weight, proj_weight.T, vec),
        (S(own, BF16), S(full, BF16), S(blocks, BF16), S((D, tok), BF16)),
        [pltpu.VMEM(block, BF16)] + swap + share + spread, hbm_out=(2,), early=(0, 1, 3),
    )
    w1_full = w1_full.reshape(D, -1)
    vh, oh, o_low, lse, qa, ka, g, cot, fc1_full, proj_part = comm_call(
        partial(fwd_kernel, shards, heads, HD, COLS, rows, 256), "attn_fwd", 1,
        (a1.reshape(tok, D), w1_full, vec, rel_rows, rel_cols.T, cotangent, fc1_weight),
        (
            S((heads, tok, 128), BF16), S((heads, tok, 128), F32), S((tok, width), BF16), S((heads, 1, tok), F32),
            S((heads, tok, 256), BF16), S((heads, tok, 256), BF16),
            S(own, BF16), S(full, BF16), S(blocks, BF16), S((tok, D), BF16),
        ),
        [
            pltpu.VMEM((heads, tok, 128), BF16), pltpu.VMEM((128, tok), BF16), pltpu.VMEM((256, 128), BF16),
            pltpu.VMEM((256, 128), BF16), pltpu.VMEM((tok, 256), BF16),
        ]
        + swap + share + spread, hbm_in=(6,), hbm_out=(8,), late=(1, 0), early=(0, 1, 2, 4, 5, 7, 9),
    )
    fc1_full = fc1_full.reshape(D, ff)
    mid, a2, fc2_full, act, slope, cot_turned = comm_call(
        partial(mid_kernel, shards), "mid", 2,
        (proj_part.reshape(full), x, vec, fc2_t, fc1_full, cot),
        (
            S(own, F32), S(full, BF16), S(blocks, BF16), S((tok, ff), BF16), S((tok, ff), F32),
            S((D, tok), BF16),
        ),
        gather + share + spread, hbm_in=(3,), hbm_out=(2,), late=(0, 5, 1, 4), early=(0, 1, 3, 4, 5),
    )
    fc2_full = fc2_full.reshape(D, ff)
    d_mid, d_branch_turned, fc2_own, sums, fc1_grad, mlp_part, d_o = comm_call(
        partial(turn_kernel, shards), "turn", 3,
        (
            cot_turned, act, slope, cot.reshape(tok, D), fc2_full, fc1_full, a2.reshape(tok, D), mid, g, vec,
            w1_full,
        ),
        (
            S(own, F32), S((D, tok), BF16), S(block, F32), S((8, D), F32),
            S((D, ff), BF16), S((tok, D), BF16), S((tok, width), BF16),
        ),
        [pltpu.VMEM(full, BF16), pltpu.VMEM((D, ff), BF16), pltpu.VMEM(full, BF16), pltpu.VMEM((tok, ff), BF16)]
        + gather + share + collect,
        late=(0, 1, 2, 3, 4, 5, 6, 7, 8, 10), early=(0, 1, 4, 5, 6),
    )
    dqkv, rel_grad, fc1_own, qkv_sum, output = comm_call(
        partial(bwd_kernel, shards, heads, HD, COLS, rows, 256), "attn_bwd", 4,
        (qa, ka, vh, d_o, oh, lse, rel_rows, rel_cols.T, fc1_grad, mlp_part.reshape(full), mid, vec),
        (S((tok, qkv_cols), BF16), S((256, 128), F32), S(block, F32), S((8, qkv_cols), F32), S(own, BF16)),
        [
            pltpu.VMEM((heads, tok, 128), BF16), pltpu.VMEM((3 * heads, tok, 128), BF16),
            pltpu.VMEM((256, tok), BF16), pltpu.VMEM((tok, 128), F32), pltpu.VMEM((tok, 128), F32),
            pltpu.VMEM((8, tok), F32), pltpu.VMEM((256, 128), BF16), pltpu.VMEM((tok, 256), BF16),
            pltpu.VMEM(own, BF16),
        ] + gather + swap + collect,
        late=(8, 9, 3, 2, 4, 1, 0, 10), early=(0,),
    )
    tokens_grad, qkv_own, proj_own, total, late = comm_call(
        partial(end_kernel, shards), "end", 5,
        (x, d_mid, vec, a1_turned, dqkv, d_branch_turned, o_low, sums, w1_full, rel_grad, qkv_sum),
        (
            S(own, BF16), S((3, block[0], width), F32), S((block[0], width), F32), S((32, D), F32), S((8, width), F32),
        ),
        [pltpu.VMEM((D, ff), BF16), pltpu.VMEM(block, F32), pltpu.VMEM(full, BF16), pltpu.VMEM(own, BF16)]
        + gather + swap
        + [
            pltpu.VMEM((4, 32, D), F32), pltpu.VMEM((3, 32, D), F32),
            pltpu.VMEM((shards, 8, D), F32), DMA((2, 5 + shards)),
            pltpu.VMEM((4, 8, width), F32), pltpu.VMEM((2 * shards, 8, width), F32), DMA((2, 3 + 2 * shards)),
        ]
        + collect,
        late=(4, 8, 3, 5, 6, 0, 1),
    )
    big = (output, tokens_grad, qkv_own, proj_own, fc1_own, fc2_own)
    vector = S((D,), F32)
    (
        output, tokens_grad, qkv_own, proj_own, fc1_own, fc2_own,
        gain1, bias1, qv_grad, rows_grad, cols_grad, gain2, bias2, projb, fc2b, fc1b,
    ) = pl.pallas_call(
        settle_kernel,
        out_shape=tuple(S(b.shape, b.dtype) for b in big)
        + (vector, vector, S((2, D), F32), S(rel_rows.shape, F32), S(rel_cols.shape[::-1], F32))
        + (vector, vector, vector, vector, S((FF,), F32)),
        compiler_params=pltpu.CompilerParams(vmem_limit_bytes=VMEM_GRANT),
        name="settle",
    )(total, late, *big)
    return (
        output, tokens_grad, gain1, bias1, qkv_own, qv_grad, rows_grad, cols_grad.T, proj_own.T, projb,
        gain2, bias2, fc1_own, fc1b, fc2_own.T, fc2b,
    )


def solution(mesh):
    in_specs = (
        P("shard", ("ctx", "tp"), None),
        P(),
        P(),
        P(None, ("shard", "ctx"), "tp"),
        P(),
        P(),
        P(),
        P("tp", ("shard", "ctx")),
        P(),
        P(),
        P(),
        P(("shard", "ctx"), "tp"),
        P(),
        P("tp", ("shard", "ctx")),
        P(),
        P("shard", ("ctx", "tp"), None),
    )
    out_specs = (
        P("shard", ("ctx", "tp"), None),
        P("shard", ("ctx", "tp"), None),
        P(),
        P(),
        P(None, ("shard", "ctx"), "tp"),
        P(),
        P(),
        P(),
        P("tp", ("shard", "ctx")),
        P(),
        P(),
        P(),
        P(("shard", "ctx"), "tp"),
        P(),
        P("tp", ("shard", "ctx")),
        P(),
    )
    def on_device(*arrays):
        rows = (arrays[5].shape[0] + 1) // 2
        fits = (mesh.shape["shard"], mesh.shape["ctx"], mesh.shape["tp"]) == (4, 2, 4)
        fits = fits and arrays[0].shape[0] == mesh.shape["ctx"] and HD + 2 * rows <= 128
        fits = fits and arrays[5].shape[0] <= 32 and arrays[6].shape[0] <= 128
        return (on_device_images if fits else on_device_rows)(*arrays)

    return jax.shard_map(
        on_device, mesh=mesh, in_specs=in_specs, out_specs=out_specs, check_vma=False
    )
```
